32 devices in a mesh: dp: 8 (over z, y), tensor: 4 (over x, core).
Axes of the slice: x: 2, y: 2, z: 4, core: 2. Of those that a mesh axis runs over, the one named last changes fastest.
Arguments:
- hidden_in: bfloat16 [16384, 768], P(('dp', 'tensor')), may hold values from -6 to 6
- lengths: int32 [16], P('dp'), may hold values from 1 to 1024, as said below
- ln1_gain: float32 [768], replicated, may hold values from 0.5 to 1.5
- ln1_shift: float32 [768], replicated, may hold values from -1.75 to 1.75
- qkv_weight: bfloat16 [3, 768, 768], P(None, None, 'tensor'), may hold values from -0.21875 to 0.21875
- qv_bias: float32 [2, 768], P(None, 'tensor'), may hold values from -3 to 3
- out_weight: bfloat16 [768, 768], P('tensor'), may hold values from -1.75 to 1.75
- out_bias: float32 [768], replicated, may hold values from -1.75 to 1.75
- ln2_gain: float32 [768], replicated, may hold values from 0.5 to 1.5
- ln2_shift: float32 [768], replicated, may hold values from -1.75 to 1.75
- up_weight: bfloat16 [768, 3072], P(None, 'tensor'), may hold values from -0.21875 to 0.21875
- up_bias: bfloat16 [3072], P('tensor'), may hold values from -3 to 3
- down_weight: bfloat16 [3072, 768], P('tensor'), may hold values from -0.109375 to 0.109375
- down_bias: float32 [768], replicated, may hold values from -1.75 to 1.75
- out_grad: bfloat16 [16384, 768], P(('dp', 'tensor')), may hold values from -6 to 6
Outputs:
- output: bfloat16 [16384, 768], P(('dp', 'tensor'))
- input_grad: bfloat16 [16384, 768], P(('dp', 'tensor'))
- ln1_gain_grad: float32 [768], replicated
- ln1_shift_grad: float32 [768], replicated
- qkv_weight_grad: float32 [3, 768, 768], P(None, None, 'tensor')
- qv_bias_grad: float32 [2, 768], P(None, 'tensor')
- out_weight_grad: float32 [768, 768], P('tensor')
- out_bias_grad: float32 [768], replicated
- ln2_gain_grad: float32 [768], replicated
- ln2_shift_grad: float32 [768], replicated
- up_weight_grad: float32 [768, 3072], P(None, 'tensor')
- up_bias_grad: float32 [3072], P('tensor')
- down_weight_grad: float32 [3072, 768], P('tensor')
- down_bias_grad: float32 [768], replicated
The draws below stay inside these ranges and needn't reach their ends.
Inputs may be any that keep to these rules, and one draw needn't show every extreme that they name: `lengths`: some slot's length is exactly 1024.
All inputs are finite; a program needn't handle non-finite values.
Results may differ from the reference program's by a relative error of at most 0.012.
The reference program's roundings to bfloat16 on the way count: a program that leaves them out, or rounds other values in their place, can miss the bound.
Values may be sent and summed in bfloat16 or wider, within the bound.
A program may use at most 192 MiB of HBM per device.

```python
import math
from functools import partial
import jax
import jax.numpy as jnp
from jax import lax

D = 768
HEADS = 12
HD = 64
FF = 3072
LEN = 1024
SEQS = 16
TOKENS = 16384
N_TENSOR = 4


def draw_lengths(key, part):
    first_key, second_key, third_key, fourth_key = jax.random.split(key, 4)
    level = jnp.minimum(jax.random.randint(first_key, (SEQS,), 0, 4), jax.random.randint(second_key, (SEQS,), 0, 4))
    base_len = jnp.maximum(LEN // jnp.left_shift(1, level), 1)
    trimmed = jax.random.randint(third_key, (SEQS,), 0, base_len // 4 + 1)
    length = base_len - trimmed
    longest = jax.random.randint(fourth_key, (), 0, SEQS)
    return jnp.where(jnp.arange(SEQS) == longest, LEN, length).astype(jnp.int32)


def block_levels(rng, shape, pieces, smallest, top_value):
    loudness = 1.0
    for position, blocks in pieces:
        heights = jax.random.uniform(jax.random.fold_in(jax.random.fold_in(rng, 6), position), (blocks,), jnp.float32, smallest / len(pieces), top_value / len(pieces))
        loudness = loudness * jnp.repeat(jnp.exp(heights), shape[position] // blocks).reshape((-1,) + (1,) * (len(shape) - 1 - position))
    return loudness


def scatter_about(stream_key, dims, scale, limit, cuts=(), kind=jnp.bfloat16):
    values = scale * jax.random.normal(stream_key, dims, jnp.float32)
    if cuts:
        values = values * block_levels(stream_key, dims, cuts, -0.22, 0.18)
    return jnp.clip(values, -limit, limit).astype(kind)


def setup_inputs(seed: int = 0) -> dict:
    streams_of = jax.random.split(jax.random.key(seed), 16)
    return {
        "hidden_in": scatter_about(streams_of[0], (TOKENS, D), 1.0, 6.0, ((0, 32),)),
        "lengths": draw_lengths(jax.random.fold_in(streams_of[15], 71), 0),
        "ln1_gain": jnp.clip(1.0 + 0.1 * jax.random.normal(streams_of[2], (D,), jnp.float32), 0.5, 1.5),
        "ln1_shift": scatter_about(streams_of[3], (D,), 0.3, 1.75, (), jnp.float32),
        "qkv_weight": scatter_about(streams_of[4], (3, D, D), D ** -0.5, 0.21875, ((2, 4),)),
        "qv_bias": scatter_about(streams_of[5], (2, D), 0.5, 3.0, ((1, 4),), jnp.float32),
        "out_weight": scatter_about(streams_of[6], (D, D), (D // 64) ** -0.5, 1.75, ((0, 4),)),
        "out_bias": scatter_about(streams_of[7], (D,), 0.3, 1.75, (), jnp.float32),
        "ln2_gain": jnp.clip(1.0 + 0.1 * jax.random.normal(streams_of[8], (D,), jnp.float32), 0.5, 1.5),
        "ln2_shift": scatter_about(streams_of[9], (D,), 0.3, 1.75, (), jnp.float32),
        "up_weight": scatter_about(streams_of[10], (D, FF), D ** -0.5, 0.21875, ((1, 4),)),
        "up_bias": scatter_about(streams_of[11], (FF,), 0.5, 3.0, ((0, 4),)),
        "down_weight": scatter_about(streams_of[12], (FF, D), FF ** -0.5, 0.109375, ((0, 4),)),
        "down_bias": scatter_about(streams_of[13], (D,), 0.3, 1.75, (), jnp.float32),
        "out_grad": scatter_about(streams_of[14], (TOKENS, D), 1.0, 6.0, ((0, 32),)),
    }


highest = lax.Precision.HIGHEST
epsilon = 1e-05
sel_factor = 4.0

@jax.custom_vjp
def low(v):
    return lax.optimization_barrier(v.astype(jnp.bfloat16)).astype(jnp.float32)

@jax.custom_vjp
def low_back(v):
    return v

def low_keep(v):
    return (low(v), None)

def low_pass(kept, grad):
    return (grad,)

def back_keep(v):
    return (v, None)

def back_low(kept, grad):
    return (low(grad),)
low.defvjp(low_keep, low_pass)
low_back.defvjp(back_keep, back_low)

def layer_norm(source, scales, offset):
    centre = source - lax.optimization_barrier(jnp.mean(source, -1, keepdims=True))
    spread = lax.optimization_barrier(jnp.mean(centre * centre, -1, keepdims=True))
    return centre * lax.rsqrt(spread + epsilon) * scales + offset

def attend(slot_args):
    queries, keys_in, valued, length = slot_args
    seq_len = queries.shape[0]
    scores = jnp.einsum('ihd,jhd->hij', queries, keys_in, precision=highest) * (1.0 / math.sqrt(HD))
    row_ids = jnp.arange(seq_len)[:, None]
    col_ids = jnp.arange(seq_len)[None, :]
    allowed = (col_ids <= row_ids) & (col_ids < length)
    picked = (col_ids >= 1) & (col_ids < row_ids)
    group_size = HEADS // N_TENSOR
    weights_all = []
    for part_index in range(N_TENSOR):
        selected = low_back(scores[0])
        gated = jnp.where(picked, jax.nn.relu(selected), 0.0) * (sel_factor / seq_len)
        selection = jnp.cumsum(gated, axis=0) - gated
        logits = low_back(scores[part_index * group_size:(part_index + 1) * group_size] - selection[None])
        logits = jnp.where(allowed[None], logits, -jnp.inf)
        weights_all.append(jax.nn.softmax(logits, axis=-1))
    attn_probs = jnp.concatenate(weights_all, 0)
    return jnp.einsum('hij,jhd->ihd', low(attn_probs), valued, precision=highest)

def forward(lengths, hidden_in, ln1_gain, ln1_shift, qkv_weight, qv_bias, out_weight, out_bias, ln2_gain, ln2_shift, up_weight, up_bias, down_weight, down_bias):
    tokens = hidden_in.shape[0]
    normed = low(layer_norm(hidden_in, ln1_gain, ln1_shift))
    bias_rows = jnp.stack([qv_bias[0], jnp.zeros_like(qv_bias[0]), qv_bias[1]])
    projected = jnp.einsum('td,kdc->tkc', normed, qkv_weight, precision=highest) + bias_rows[None]
    projected = low_back(low(projected))
    slot_shape = (SEQS, LEN, HEADS, HD)
    attended = lax.map(jax.checkpoint(attend), (projected[:, 0].reshape(slot_shape), projected[:, 1].reshape(slot_shape), projected[:, 2].reshape(slot_shape), lengths))
    attended = low_back(low(attended.reshape(tokens, D)))
    middle = hidden_in + low_back(jnp.dot(attended, out_weight, precision=highest) + out_bias)
    mlp_input = low(layer_norm(middle, ln2_gain, ln2_shift))
    pre_act = low_back(jnp.dot(mlp_input, up_weight, precision=highest) + up_bias)
    activated = low(jax.nn.gelu(pre_act, approximate=True))
    branch = low_back(jnp.dot(activated, down_weight, precision=highest) + down_bias)
    positions = jnp.arange(tokens)
    slot_length = jnp.repeat(lengths, LEN)
    live_mask = (positions % LEN < slot_length).astype(hidden_in.dtype)[:, None]
    return live_mask * (middle + branch)

def reference(hidden_in, lengths, ln1_gain, ln1_shift, qkv_weight, qv_bias, out_weight, out_bias, ln2_gain, ln2_shift, up_weight, up_bias, down_weight, down_bias, out_grad):
    as_floats = [arr.astype(jnp.float32) for arr in (hidden_in, ln1_gain, ln1_shift, qkv_weight, qv_bias, out_weight, out_bias, ln2_gain, ln2_shift, up_weight, up_bias, down_weight, down_bias)]
    result, pullback = jax.vjp(partial(forward, lengths), *as_floats)
    gradients = pullback(out_grad.astype(jnp.float32))
    return (result.astype(jnp.bfloat16), gradients[0].astype(jnp.bfloat16), gradients[1], gradients[2], gradients[3], gradients[4], gradients[5], gradients[6], gradients[7], gradients[8], gradients[9], gradients[10], gradients[11], gradients[12])
```

```python
import math

import jax
import jax.numpy as jnp
from jax import lax
from jax.experimental import pallas as pl
from jax.experimental.pallas import tpu as pltpu
from jax.sharding import PartitionSpec as P

HD = 64
BLK = 256
BIG = 1e30
sel_factor = 4.0
score_scale = 1.0 / math.sqrt(HD)
f32 = jnp.float32
bf16 = jnp.bfloat16


def mm(a, b):
    return lax.dot_general(a, b, (((1,), (0,)), ((), ())), preferred_element_type=f32)


def mm_nt(a, b):
    return lax.dot_general(a, b, (((1,), (1,)), ((), ())), preferred_element_type=f32)


def flip(a):
    return a.astype(f32).T.astype(bf16)


def split_mm(tri, x):
    hi = x.astype(bf16)
    lo = (x - hi.astype(f32)).astype(bf16)
    return mm(tri, hi) + mm(tri, lo)


def head_mask(h, width):
    return lax.broadcasted_iota(jnp.int32, (BLK, width), 1) // HD == h


def masked_rows(x, mask, scale):
    return jnp.where(mask, x.astype(f32) * scale, 0.0).astype(bf16)


def fwd_block(i, heads, first, q_ref, k_ref, v_ref, fence, o_ref, lse_ref):
    width = q_ref.shape[1]
    cols = (i + 1) * BLK
    keys = k_ref[:cols, :]
    vals = v_ref[:cols, :]
    fenced = fence[:, :cols]
    lane = lax.broadcasted_iota(jnp.int32, (BLK, 128), 1)
    lse_ref[...] = jnp.zeros_like(lse_ref)
    out_scr = first

    def head(h, _):
        mask = head_mask(h, width)
        s = mm_nt(masked_rows(q_ref[...], mask, score_scale), keys) - fenced
        top = jnp.max(s, -1, keepdims=True)
        e = jnp.exp(s - top)
        total = jnp.sum(e, -1, keepdims=True)
        p = (e * (1.0 / total)).astype(bf16)
        out = mm(p, vals)
        out_scr[...] = jnp.where(mask, out, out_scr[...])
        lse_ref[...] = jnp.where(lane == h, top + jnp.log(total), lse_ref[...])
        return 0

    lax.fori_loop(0, heads, head, 0)
    o_ref[...] = out_scr[...].astype(bf16)


def make_fence(i, seq_len, length, sq_ref, sk_ref, fence, carry):
    cols = (i + 1) * BLK
    s0 = mm_nt(sq_ref[...], sk_ref[:cols, :]) * score_scale
    row = i * BLK + lax.broadcasted_iota(jnp.int32, (BLK, cols), 0)
    col = lax.broadcasted_iota(jnp.int32, (BLK, cols), 1)
    picked = (col >= 1) & (col < row)
    sel = jnp.where(picked, jnp.maximum(s0, 0.0), 0.0) * (sel_factor / seq_len)
    r2 = lax.broadcasted_iota(jnp.int32, (BLK, BLK), 0)
    c2 = lax.broadcasted_iota(jnp.int32, (BLK, BLK), 1)
    tri = jnp.where(c2 < r2, 1.0, 0.0).astype(bf16)
    total = carry[0:1, :cols] + split_mm(tri, sel)
    carry[0:1, :cols] = total[BLK - 1 : BLK, :] + sel[BLK - 1 : BLK, :]
    fence[:, :cols] = jnp.where((col <= row) & (col < length), total, BIG)


def fwd_first_kernel(heads, len_ref, q_ref, k_ref, v_ref, sq_ref, sk_ref, o_ref, lse_ref, f_ref, out_scr, carry):
    r = pl.program_id(0)
    seq_len = k_ref.shape[0]

    @pl.when(r == 0)
    def _():
        carry[...] = jnp.zeros_like(carry)

    for i in range(seq_len // BLK):

        @pl.when(r == i)
        def _():
            make_fence(i, seq_len, len_ref[0], sq_ref, sk_ref, f_ref, carry)
            fwd_block(i, heads, out_scr, q_ref, k_ref, v_ref, f_ref, o_ref, lse_ref)


def fwd_next_kernel(heads, q_ref, k_ref, v_ref, f_ref, o_ref, lse_ref, out_scr):
    r = pl.program_id(0)
    for i in range(k_ref.shape[0] // BLK):

        @pl.when(r == i)
        def _():
            fwd_block(i, heads, out_scr, q_ref, k_ref, v_ref, f_ref, o_ref, lse_ref)


def row_spec(width, back=None):
    if back is None:
        return pl.BlockSpec((BLK, width), lambda r: (r, 0))
    return pl.BlockSpec((BLK, width), lambda r: (back - 1 - r, 0))


def full_spec(rows, width):
    return pl.BlockSpec((rows, width), lambda r: (0, 0))


def attend_first(q, k, v, sq, sk, length):
    n, width = q.shape
    heads = width // HD
    return pl.pallas_call(
        lambda *refs: fwd_first_kernel(heads, *refs),
        grid=(n // BLK,),
        in_specs=[
            pl.BlockSpec(memory_space=pltpu.SMEM),
            row_spec(width),
            full_spec(n, width),
            full_spec(n, width),
            row_spec(HD),
            full_spec(n, HD),
        ],
        out_specs=[row_spec(width), row_spec(128), row_spec(n)],
        out_shape=[
            jax.ShapeDtypeStruct((n, width), bf16),
            jax.ShapeDtypeStruct((n, 128), f32),
            jax.ShapeDtypeStruct((n, n), f32),
        ],
        scratch_shapes=[pltpu.VMEM((BLK, width), f32), pltpu.VMEM((8, n), f32)],
        name="attend_first",
        cost_estimate=pl.CostEstimate(flops=6 * n * n * 256, bytes_accessed=8 * n * n, transcendentals=0),
    )(length, q, k, v, sq, sk)


def attend_next(q, k, v, fence):
    n, width = q.shape
    heads = width // HD
    return pl.pallas_call(
        lambda *refs: fwd_next_kernel(heads, *refs),
        grid=(n // BLK,),
        in_specs=[row_spec(width), full_spec(n, width), full_spec(n, width), row_spec(n)],
        out_specs=[row_spec(width), row_spec(128)],
        out_shape=[
            jax.ShapeDtypeStruct((n, width), bf16),
            jax.ShapeDtypeStruct((n, 128), f32),
        ],
        scratch_shapes=[pltpu.VMEM((BLK, width), f32)],
        name="attend_next",
        cost_estimate=pl.CostEstimate(flops=6 * n * n * 256, bytes_accessed=8 * n * n, transcendentals=0),
    )(q, k, v, fence)


def bwd_block(i, heads, q_ref, k_ref, v_ref, do_ref, lse_ref, f_ref, sq_ref, sk_ref,
              dq_ref, dsq_ref, dq_scr, dkt, dvt, dskt, later, fsum, qt, dot_):
    width = q_ref.shape[1]
    seq_len = k_ref.shape[0]
    cols = (i + 1) * BLK
    keys = k_ref[:cols, :]
    vals = v_ref[:cols, :]
    lane = lax.broadcasted_iota(jnp.int32, (BLK, 128), 1)
    qt[...] = (q_ref[...].astype(f32) * score_scale).T.astype(bf16)
    dot_[...] = flip(do_ref[...])
    fsum[:, :cols] = jnp.zeros((BLK, cols), f32)

    def head(h, _):
        mask = head_mask(h, width)
        lse = jnp.sum(jnp.where(lane == h, lse_ref[...], 0.0), -1, keepdims=True)
        s = mm_nt(masked_rows(q_ref[...], mask, score_scale), keys)
        p = jnp.exp(s - f_ref[:, :cols] - lse)
        dp = mm_nt(masked_rows(do_ref[...], mask, 1.0), vals)
        delta = jnp.sum(p * dp, -1, keepdims=True)
        g = (p * (dp - delta)).astype(bf16)
        rows = pl.ds(pl.multiple_of(h * HD, HD), HD)
        dq_scr[...] = jnp.where(mask, mm(g, keys), dq_scr[...])
        dkt[rows, :cols] += mm(qt[rows, :], g)
        dvt[rows, :cols] += mm(dot_[rows, :], p.astype(bf16))
        fsum[:, :cols] += g.astype(f32)
        return 0

    lax.fori_loop(0, heads, head, 0)
    dq_ref[...] = (dq_scr[...] * score_scale).astype(bf16)
    grad = -fsum[:, :cols]
    r2 = lax.broadcasted_iota(jnp.int32, (BLK, BLK), 0)
    c2 = lax.broadcasted_iota(jnp.int32, (BLK, BLK), 1)
    tri = jnp.where(c2 > r2, 1.0, 0.0).astype(bf16)
    dsel = later[0:1, :cols] + split_mm(tri, grad)
    later[0:1, :cols] = dsel[0:1, :] + grad[0:1, :]
    s0 = mm_nt(sq_ref[...], sk_ref[:cols, :])
    row = i * BLK + lax.broadcasted_iota(jnp.int32, (BLK, cols), 0)
    col = lax.broadcasted_iota(jnp.int32, (BLK, cols), 1)
    keep = (col >= 1) & (col < row) & (s0 > 0)
    gsel = jnp.where(keep, dsel * (sel_factor / seq_len), 0.0).astype(bf16)
    dsq_ref[...] = mm(gsel, sk_ref[:cols, :]) * score_scale
    sqt = (sq_ref[...].astype(f32) * score_scale).T.astype(bf16)
    dskt[:, :cols] += mm(sqt, gsel)


def bwd_kernel(heads, q_ref, k_ref, v_ref, do_ref, lse_ref, f_ref, sq_ref, sk_ref,
               dq_ref, dk_ref, dv_ref, dsq_ref, dsk_ref,
               dq_scr, dkt, dvt, dskt, later, fsum, qt, dot_):
    g = pl.program_id(0)
    n = k_ref.shape[0] // BLK

    @pl.when(g == 0)
    def _():
        dkt[...] = jnp.zeros_like(dkt)
        dvt[...] = jnp.zeros_like(dvt)
        dskt[...] = jnp.zeros_like(dskt)
        later[...] = jnp.zeros_like(later)

    for i in range(n):

        @pl.when(g == n - 1 - i)
        def _():
            bwd_block(i, heads, q_ref, k_ref, v_ref, do_ref, lse_ref, f_ref, sq_ref, sk_ref,
                      dq_ref, dsq_ref, dq_scr, dkt, dvt, dskt, later, fsum, qt, dot_)

    @pl.when(g == n - 1)
    def _():
        dk_ref[...] = dkt[...].T.astype(bf16)
        dv_ref[...] = dvt[...].T.astype(bf16)
        dsk_ref[...] = dskt[...].T


def attend_back(q, k, v, do, lse, fence, sq, sk):
    n, width = q.shape
    heads = width // HD
    back = n // BLK
    return pl.pallas_call(
        lambda *refs: bwd_kernel(heads, *refs),
        grid=(back,),
        in_specs=[
            row_spec(width, back),
            full_spec(n, width),
            full_spec(n, width),
            row_spec(width, back),
            row_spec(128, back),
            row_spec(n, back),
            row_spec(HD, back),
            full_spec(n, HD),
        ],
        out_specs=[
            row_spec(width, back),
            full_spec(n, width),
            full_spec(n, width),
            row_spec(HD, back),
            full_spec(n, HD),
        ],
        out_shape=[
            jax.ShapeDtypeStruct((n, width), bf16),
            jax.ShapeDtypeStruct((n, width), bf16),
            jax.ShapeDtypeStruct((n, width), bf16),
            jax.ShapeDtypeStruct((n, HD), f32),
            jax.ShapeDtypeStruct((n, HD), f32),
        ],
        scratch_shapes=[
            pltpu.VMEM((BLK, width), f32),
            pltpu.VMEM((width, n), f32),
            pltpu.VMEM((width, n), f32),
            pltpu.VMEM((HD, n), f32),
            pltpu.VMEM((8, n), f32),
            pltpu.VMEM((BLK, n), f32),
            pltpu.VMEM((width, BLK), bf16),
            pltpu.VMEM((width, BLK), bf16),
        ],
        name="attend_back",
        cost_estimate=pl.CostEstimate(flops=18 * n * n * 256, bytes_accessed=8 * n * n, transcendentals=0),
    )(q, k, v, do, lse, fence, sq, sk)


epsilon = 1e-05


def layer_norm(source, scales, offset):
    centre = source - jnp.mean(source, -1, keepdims=True)
    spread = jnp.mean(centre * centre, -1, keepdims=True)
    return centre * lax.rsqrt(spread + epsilon) * scales + offset


def gelu_tanh(source):
    return jax.nn.gelu(source, approximate=True)


def mm_tn(a, b):
    return lax.dot_general(a, b, (((0,), (0,)), ((), ())), preferred_element_type=f32)


def swap_core(x):
    n = lax.axis_size("tensor")
    return lax.ppermute(x, "tensor", [(i, i ^ 1) for i in range(n)])


def swap_chip(x):
    n = lax.axis_size("tensor")
    return lax.ppermute(x, "tensor", [(i, i ^ 2) for i in range(n)])


def reduce_dp(x):
    n = lax.axis_size("dp")
    idx = lax.axis_index("dp")
    total = x
    step = 1
    while step < n:
        pairs = [(i, i ^ step) for i in range(n)]
        upper = (idx // step) % 2
        half = total.shape[0] // 2
        kept = lax.dynamic_slice_in_dim(total, upper * half, half, 0)
        given = lax.dynamic_slice_in_dim(total, (1 - upper) * half, half, 0)
        total = kept + lax.ppermute(given.astype(bf16), "dp", pairs).astype(f32)
        step *= 2
    full = total.astype(bf16)
    while step > 1:
        step //= 2
        pairs = [(i, i ^ step) for i in range(n)]
        upper = (idx // step) % 2
        got = lax.ppermute(full, "dp", pairs)
        full = jnp.concatenate(
            [jnp.where(upper == 0, full, got), jnp.where(upper == 0, got, full)], 0
        )
    return full.astype(f32)


def shards(
    hidden_in,
    lengths,
    ln1_gain,
    ln1_shift,
    qkv_weight,
    qv_bias,
    out_weight,
    out_bias,
    ln2_gain,
    ln2_shift,
    up_weight,
    up_bias,
    down_weight,
    down_bias,
    out_grad,
):
    rows = hidden_in.shape[0]
    ranks = lax.axis_size("tensor")
    me = lax.axis_index("tensor")
    odd = me % 2
    length = jnp.where(me < 2, lengths[0], lengths[1])
    live = (odd * rows + jnp.arange(rows) < length).astype(f32)[:, None]

    def join(mine, other):
        first = jnp.where(odd == 0, mine, other)
        second = jnp.where(odd == 0, other, mine)
        return jnp.concatenate([first, second], 0)

    def my_half(x):
        return lax.dynamic_slice_in_dim(x, odd * rows, rows, 0)

    def other_half(x):
        return lax.dynamic_slice_in_dim(x, (1 - odd) * rows, rows, 0)

    sel_w = jnp.concatenate([qkv_weight[0][:, :HD], qkv_weight[1][:, :HD]], 1)
    sel_b = qv_bias[:1, :HD]
    sel_w = jnp.where(me == 0, sel_w, lax.ppermute(sel_w, "tensor", [(0, 2)]))
    sel_b = jnp.where(me == 0, sel_b, lax.ppermute(sel_b, "tensor", [(0, 2)]))
    sel_w = jnp.where(odd == 0, sel_w, lax.ppermute(sel_w, "tensor", [(0, 1), (2, 3)]))
    sel_b = jnp.where(odd == 0, sel_b, lax.ppermute(sel_b, "tensor", [(0, 1), (2, 3)]))

    residual = hidden_in.astype(f32)
    normed_mine, ln1_back = jax.vjp(layer_norm, residual, ln1_gain, ln1_shift)
    normed_mine = normed_mine.astype(bf16)
    normed = join(normed_mine, swap_core(normed_mine))

    qkv_far = swap_chip(qkv_weight)
    bias_far = swap_chip(qv_bias)
    out_far = swap_chip(out_weight)

    grad_out = out_grad.astype(f32) * live
    grad_branch = grad_out.astype(bf16)
    grad_near = join(grad_branch, swap_core(grad_branch))
    grad_far = swap_chip(grad_branch)
    grad_far = join(grad_far, swap_core(grad_far))

    def project(weights, bias):
        q = (mm(normed, weights[0]) + bias[0]).astype(bf16)
        k = mm(normed, weights[1]).astype(bf16)
        v = (mm(normed, weights[2]) + bias[1]).astype(bf16)
        return q, k, v

    sq = (mm(normed, sel_w[:, :HD]) + sel_b).astype(bf16)
    sk = mm(normed, sel_w[:, HD:]).astype(bf16)
    q1, k1, v1 = project(qkv_weight, qv_bias)
    o1, lse1, fence = attend_first(q1, k1, v1, sq, sk, length[None])
    q2, k2, v2 = project(qkv_far, bias_far)
    o2, lse2 = attend_next(q2, k2, v2, fence)

    def attn_out(part):
        return mm(part(o1), out_weight) + mm(part(o2), out_far)

    attn_given = swap_core(attn_out(other_half).astype(bf16))
    middle = residual + (attn_out(my_half) + attn_given.astype(f32)) + out_bias
    inner, ln2_back = jax.vjp(layer_norm, middle, ln2_gain, ln2_shift)
    inner = inner.astype(bf16)
    inner_near = join(inner, swap_core(inner))
    inner_far = swap_chip(inner)
    inner_far = join(inner_far, swap_core(inner_far))

    def feed(inner_rows, grad_rows):
        pre = mm(inner_rows, up_weight) + up_bias.astype(f32)
        act, gelu_back = jax.vjp(gelu_tanh, pre)
        grad_act = mm_nt(grad_rows, down_weight)
        grad_pre = gelu_back(grad_act)[0].astype(bf16)
        return act.astype(bf16), grad_pre

    act_near, pre_near = feed(inner_near, grad_near)
    act_far, pre_far = feed(inner_far, grad_far)

    def gather_sum(near, far, weight, product):
        far_given = swap_core(product(other_half(far), weight).astype(bf16))
        far_sum = product(my_half(far), weight) + far_given.astype(f32)
        from_chip = swap_chip(far_sum.astype(bf16))
        near_given = swap_core(product(other_half(near), weight).astype(bf16))
        return product(my_half(near), weight) + near_given.astype(f32) + from_chip.astype(f32)

    grad_inner = gather_sum(pre_near, pre_far, up_weight, mm_nt)
    branch = gather_sum(act_near, act_far, down_weight, mm)
    output = (live * (middle + branch + down_bias)).astype(bf16)

    down_grad = mm_tn(act_near, grad_near) + mm_tn(act_far, grad_far)
    up_grad = mm_tn(inner_near, pre_near) + mm_tn(inner_far, pre_far)
    up_bias_grad = jnp.sum(pre_near, 0, dtype=f32) + jnp.sum(pre_far, 0, dtype=f32)

    grad_norm2, ln2_gain_grad, ln2_shift_grad = ln2_back(grad_inner)
    grad_middle = grad_out + grad_norm2
    grad_attn = grad_middle.astype(bf16)
    out_bias_grad = jnp.sum(grad_attn, 0, dtype=f32)
    down_bias_grad = jnp.sum(grad_out, 0)
    attn_rows = join(grad_attn, swap_core(grad_attn))

    go2 = mm_nt(attn_rows, out_far).astype(bf16)
    go1 = mm_nt(attn_rows, out_weight).astype(bf16)
    dq2, dk2, dv2, dsq2, dsk2 = attend_back(q2, k2, v2, go2, lse2, fence, sq, sk)
    dq1, dk1, dv1, dsq1, dsk1 = attend_back(q1, k1, v1, go1, lse1, fence, sq, sk)

    out_grad_far = swap_chip(mm_tn(o2, attn_rows).astype(bf16))
    out_weight_grad = mm_tn(o1, attn_rows) + out_grad_far.astype(f32)

    def weight_grads(dq, dk, dv):
        return jnp.concatenate([mm_tn(normed, dq), mm_tn(normed, dk), mm_tn(normed, dv)], 0)

    qkv_grad_far = swap_chip(weight_grads(dq2, dk2, dv2).astype(bf16))
    dsel = jnp.concatenate([dsq1 + dsq2, dsk1 + dsk2], 1).astype(bf16)
    sel_grad = mm_tn(normed, dsel)
    sel_given = lax.ppermute(sel_grad.astype(bf16), "tensor", [(1, 0), (3, 2)])
    sel_grad = sel_grad + sel_given.astype(f32)
    sel_far = lax.ppermute(sel_grad.astype(bf16), "tensor", [(2, 0)])
    sel_grad = jnp.where(me == 0, sel_grad + sel_far.astype(f32), 0.0)
    width = q1.shape[1]
    depth = normed.shape[1]
    pad = ((0, 0), (0, width - HD))
    sel_full = jnp.concatenate(
        [jnp.pad(sel_grad[:, :HD], pad), jnp.pad(sel_grad[:, HD:], pad), jnp.zeros((depth, width), f32)], 0
    )
    qkv_grad = weight_grads(dq1, dk1, dv1) + qkv_grad_far.astype(f32) + sel_full

    def normed_grad(part):
        total = mm_nt(part(dsel), sel_w)
        for d, w in zip((dq1, dk1, dv1), (0, 1, 2)):
            total = total + mm_nt(part(d), qkv_weight[w])
        for d, w in zip((dq2, dk2, dv2), (0, 1, 2)):
            total = total + mm_nt(part(d), qkv_far[w])
        return total

    normed_given = swap_core(normed_grad(other_half).astype(bf16))
    grad_normed = normed_grad(my_half) + normed_given.astype(f32)
    grad_norm1, ln1_gain_grad, ln1_shift_grad = ln1_back(grad_normed)
    input_grad = (grad_middle + grad_norm1).astype(bf16)

    ffn_grad = reduce_dp(jnp.concatenate([up_grad, down_grad], 0))
    out_weight_grad = reduce_dp(out_weight_grad)
    qkv_grad = reduce_dp(qkv_grad)

    def bias_of(dq, dv):
        return jnp.stack([jnp.sum(dq, 0, dtype=f32), jnp.sum(dv, 0, dtype=f32)])

    slot = jnp.arange(ranks)[:, None, None]
    sel_bias = jnp.pad(jnp.sum(dsel[:, :HD], 0, dtype=f32)[None], ((0, 1), (0, width - HD)))
    qv_parts = (
        jnp.where(slot == me, bias_of(dq1, dv1)[None], 0.0)
        + jnp.where(slot == me ^ 2, bias_of(dq2, dv2)[None], 0.0)
        + jnp.where(slot == 0, sel_bias[None], 0.0)
    )
    up_parts = jnp.where(slot[:, 0] == me, up_bias_grad[None], 0.0)
    small = jnp.concatenate(
        [
            ln1_gain_grad,
            ln1_shift_grad,
            out_bias_grad,
            ln2_gain_grad,
            ln2_shift_grad,
            down_bias_grad,
            up_parts.reshape(-1),
            qv_parts.reshape(-1),
        ]
    )
    small = lax.psum(small, ("dp", "tensor"))
    vectors = small[: 6 * depth].reshape(6, depth)
    hidden = up_bias.shape[0]
    up_all = small[6 * depth : 6 * depth + ranks * hidden].reshape(ranks, hidden)
    qv_all = small[6 * depth + ranks * hidden :].reshape(ranks, 2, width)
    up_bias_grad = lax.dynamic_index_in_dim(up_all, me, 0, keepdims=False)
    qv_bias_grad = lax.dynamic_index_in_dim(qv_all, me, 0, keepdims=False)
    return (
        output,
        input_grad,
        vectors[0],
        vectors[1],
        qkv_grad.reshape(3, depth, width),
        qv_bias_grad,
        out_weight_grad,
        vectors[2],
        vectors[3],
        vectors[4],
        ffn_grad[:depth],
        up_bias_grad,
        ffn_grad[depth:],
        vectors[5],
    )


def solution(mesh):
    return jax.shard_map(
        shards,
        mesh=mesh,
        in_specs=(
            P(("dp", "tensor"), None),
            P("dp"),
            P(),
            P(),
            P(None, None, "tensor"),
            P(None, "tensor"),
            P("tensor", None),
            P(),
            P(),
            P(),
            P(None, "tensor"),
            P("tensor"),
            P("tensor", None),
            P(),
            P(("dp", "tensor"), None),
        ),
        out_specs=(
            P(("dp", "tensor"), None),
            P(("dp", "tensor"), None),
            P(),
            P(),
            P(None, None, "tensor"),
            P(None, "tensor"),
            P("tensor", None),
            P(),
            P(),
            P(),
            P(None, "tensor"),
            P("tensor"),
            P("tensor", None),
            P(),
        ),
        check_vma=False,
    )
```

```python
import math

import jax
import jax.numpy as jnp
from jax import lax
from jax.experimental import pallas as pl
from jax.experimental.pallas import tpu as pltpu
from jax.sharding import PartitionSpec as P

HD = 64
BLK = 256
BIG = 1e30
sel_factor = 4.0
score_scale = 1.0 / math.sqrt(HD)
f32 = jnp.float32
bf16 = jnp.bfloat16


def mm(a, b):
    return lax.dot_general(a, b, (((1,), (0,)), ((), ())), preferred_element_type=f32)


def mm_nt(a, b):
    return lax.dot_general(a, b, (((1,), (1,)), ((), ())), preferred_element_type=f32)


def flip(a):
    return a.astype(f32).T.astype(bf16)


def split_mm(tri, x):
    hi = x.astype(bf16)
    lo = (x - hi.astype(f32)).astype(bf16)
    return mm(tri, hi) + mm(tri, lo)


def head_mask(h, width):
    return lax.broadcasted_iota(jnp.int32, (BLK, width), 1) // HD == h


def masked_rows(x, mask, scale):
    return jnp.where(mask, x.astype(f32) * scale, 0.0).astype(bf16)


def fwd_block(i, heads, first, q_ref, k_ref, v_ref, fence, o_ref, lse_ref):
    width = q_ref.shape[1]
    cols = (i + 1) * BLK
    keys = k_ref[:cols, :]
    vals = v_ref[:cols, :]
    fenced = fence[:, :cols]
    lane = lax.broadcasted_iota(jnp.int32, (BLK, 128), 1)
    lse_ref[...] = jnp.zeros_like(lse_ref)
    out_scr = first

    def head(h, _):
        mask = head_mask(h, width)
        s = mm_nt(masked_rows(q_ref[...], mask, score_scale), keys) - fenced
        top = jnp.max(s, -1, keepdims=True)
        e = jnp.exp(s - top)
        total = jnp.sum(e, -1, keepdims=True)
        p = (e * (1.0 / total)).astype(bf16)
        out = mm(p, vals)
        out_scr[...] = jnp.where(mask, out, out_scr[...])
        lse_ref[...] = jnp.where(lane == h, top + jnp.log(total), lse_ref[...])
        return 0

    lax.fori_loop(0, heads, head, 0)
    o_ref[...] = out_scr[...].astype(bf16)


def make_fence(i, seq_len, length, sq_ref, sk_ref, fence, carry):
    cols = (i + 1) * BLK
    s0 = mm_nt(sq_ref[...], sk_ref[:cols, :]) * score_scale
    row = i * BLK + lax.broadcasted_iota(jnp.int32, (BLK, cols), 0)
    col = lax.broadcasted_iota(jnp.int32, (BLK, cols), 1)
    picked = (col >= 1) & (col < row)
    sel = jnp.where(picked, jnp.maximum(s0, 0.0), 0.0) * (sel_factor / seq_len)
    r2 = lax.broadcasted_iota(jnp.int32, (BLK, BLK), 0)
    c2 = lax.broadcasted_iota(jnp.int32, (BLK, BLK), 1)
    tri = jnp.where(c2 < r2, 1.0, 0.0).astype(bf16)
    total = carry[0:1, :cols] + split_mm(tri, sel)
    carry[0:1, :cols] = total[BLK - 1 : BLK, :] + sel[BLK - 1 : BLK, :]
    fence[:, :cols] = jnp.where((col <= row) & (col < length), total, BIG)


def fwd_first_kernel(heads, len_ref, q_ref, k_ref, v_ref, sq_ref, sk_ref, o_ref, lse_ref, f_ref, out_scr, carry):
    r = pl.program_id(0)
    seq_len = k_ref.shape[0]

    @pl.when(r == 0)
    def _():
        carry[...] = jnp.zeros_like(carry)

    for i in range(seq_len // BLK):

        @pl.when(r == i)
        def _():
            make_fence(i, seq_len, len_ref[0], sq_ref, sk_ref, f_ref, carry)
            fwd_block(i, heads, out_scr, q_ref, k_ref, v_ref, f_ref, o_ref, lse_ref)


def fwd_next_kernel(heads, q_ref, k_ref, v_ref, f_ref, o_ref, lse_ref, out_scr):
    r = pl.program_id(0)
    for i in range(k_ref.shape[0] // BLK):

        @pl.when(r == i)
        def _():
            fwd_block(i, heads, out_scr, q_ref, k_ref, v_ref, f_ref, o_ref, lse_ref)


def row_spec(width, back=None):
    if back is None:
        return pl.BlockSpec((BLK, width), lambda r: (r, 0))
    return pl.BlockSpec((BLK, width), lambda r: (back - 1 - r, 0))


def full_spec(rows, width):
    return pl.BlockSpec((rows, width), lambda r: (0, 0))


def attend_first(q, k, v, sq, sk, length):
    n, width = q.shape
    heads = width // HD
    return pl.pallas_call(
        lambda *refs: fwd_first_kernel(heads, *refs),
        grid=(n // BLK,),
        in_specs=[
            pl.BlockSpec(memory_space=pltpu.SMEM),
            row_spec(width),
            full_spec(n, width),
            full_spec(n, width),
            row_spec(HD),
            full_spec(n, HD),
        ],
        out_specs=[row_spec(width), row_spec(128), row_spec(n)],
        out_shape=[
            jax.ShapeDtypeStruct((n, width), bf16),
            jax.ShapeDtypeStruct((n, 128), f32),
            jax.ShapeDtypeStruct((n, n), f32),
        ],
        scratch_shapes=[pltpu.VMEM((BLK, width), f32), pltpu.VMEM((8, n), f32)],
        name="attend_first",
        cost_estimate=pl.CostEstimate(flops=6 * n * n * 256, bytes_accessed=8 * n * n, transcendentals=0),
    )(length, q, k, v, sq, sk)


def attend_next(q, k, v, fence):
    n, width = q.shape
    heads = width // HD
    return pl.pallas_call(
        lambda *refs: fwd_next_kernel(heads, *refs),
        grid=(n // BLK,),
        in_specs=[row_spec(width), full_spec(n, width), full_spec(n, width), row_spec(n)],
        out_specs=[row_spec(width), row_spec(128)],
        out_shape=[
            jax.ShapeDtypeStruct((n, width), bf16),
            jax.ShapeDtypeStruct((n, 128), f32),
        ],
        scratch_shapes=[pltpu.VMEM((BLK, width), f32)],
        name="attend_next",
        cost_estimate=pl.CostEstimate(flops=6 * n * n * 256, bytes_accessed=8 * n * n, transcendentals=0),
    )(q, k, v, fence)


def bwd_block(i, heads, q_ref, k_ref, v_ref, do_ref, lse_ref, f_ref, sq_ref, sk_ref,
              dq_ref, dsq_ref, dq_scr, dkt, dvt, dskt, later, fsum, qt, dot_):
    width = q_ref.shape[1]
    seq_len = k_ref.shape[0]
    cols = (i + 1) * BLK
    keys = k_ref[:cols, :]
    vals = v_ref[:cols, :]
    lane = lax.broadcasted_iota(jnp.int32, (BLK, 128), 1)
    qt[...] = (q_ref[...].astype(f32) * score_scale).T.astype(bf16)
    dot_[...] = flip(do_ref[...])
    fsum[:, :cols] = jnp.zeros((BLK, cols), f32)

    def head(h, _):
        mask = head_mask(h, width)
        lse = jnp.sum(jnp.where(lane == h, lse_ref[...], 0.0), -1, keepdims=True)
        s = mm_nt(masked_rows(q_ref[...], mask, score_scale), keys)
        p = jnp.exp(s - f_ref[:, :cols] - lse)
        dp = mm_nt(masked_rows(do_ref[...], mask, 1.0), vals)
        delta = jnp.sum(p * dp, -1, keepdims=True)
        g = (p * (dp - delta)).astype(bf16)
        rows = pl.ds(pl.multiple_of(h * HD, HD), HD)
        dq_scr[...] = jnp.where(mask, mm(g, keys), dq_scr[...])
        dkt[rows, :cols] += mm(qt[rows, :], g)
        dvt[rows, :cols] += mm(dot_[rows, :], p.astype(bf16))
        fsum[:, :cols] += g.astype(f32)
        return 0

    lax.fori_loop(0, heads, head, 0)
    dq_ref[...] = (dq_scr[...] * score_scale).astype(bf16)
    grad = -fsum[:, :cols]
    r2 = lax.broadcasted_iota(jnp.int32, (BLK, BLK), 0)
    c2 = lax.broadcasted_iota(jnp.int32, (BLK, BLK), 1)
    tri = jnp.where(c2 > r2, 1.0, 0.0).astype(bf16)
    dsel = later[0:1, :cols] + split_mm(tri, grad)
    later[0:1, :cols] = dsel[0:1, :] + grad[0:1, :]
    s0 = mm_nt(sq_ref[...], sk_ref[:cols, :])
    row = i * BLK + lax.broadcasted_iota(jnp.int32, (BLK, cols), 0)
    col = lax.broadcasted_iota(jnp.int32, (BLK, cols), 1)
    keep = (col >= 1) & (col < row) & (s0 > 0)
    gsel = jnp.where(keep, dsel * (sel_factor / seq_len), 0.0).astype(bf16)
    dsq_ref[...] = mm(gsel, sk_ref[:cols, :]) * score_scale
    sqt = (sq_ref[...].astype(f32) * score_scale).T.astype(bf16)
    dskt[:, :cols] += mm(sqt, gsel)


def bwd_kernel(heads, q_ref, k_ref, v_ref, do_ref, lse_ref, f_ref, sq_ref, sk_ref,
               dq_ref, dk_ref, dv_ref, dsq_ref, dsk_ref,
               dq_scr, dkt, dvt, dskt, later, fsum, qt, dot_):
    g = pl.program_id(0)
    n = k_ref.shape[0] // BLK

    @pl.when(g == 0)
    def _():
        dkt[...] = jnp.zeros_like(dkt)
        dvt[...] = jnp.zeros_like(dvt)
        dskt[...] = jnp.zeros_like(dskt)
        later[...] = jnp.zeros_like(later)

    for i in range(n):

        @pl.when(g == n - 1 - i)
        def _():
            bwd_block(i, heads, q_ref, k_ref, v_ref, do_ref, lse_ref, f_ref, sq_ref, sk_ref,
                      dq_ref, dsq_ref, dq_scr, dkt, dvt, dskt, later, fsum, qt, dot_)

    @pl.when(g == n - 1)
    def _():
        dk_ref[...] = dkt[...].T.astype(bf16)
        dv_ref[...] = dvt[...].T.astype(bf16)
        dsk_ref[...] = dskt[...].T


def attend_back(q, k, v, do, lse, fence, sq, sk):
    n, width = q.shape
    heads = width // HD
    back = n // BLK
    return pl.pallas_call(
        lambda *refs: bwd_kernel(heads, *refs),
        grid=(back,),
        in_specs=[
            row_spec(width, back),
            full_spec(n, width),
            full_spec(n, width),
            row_spec(width, back),
            row_spec(128, back),
            row_spec(n, back),
            row_spec(HD, back),
            full_spec(n, HD),
        ],
        out_specs=[
            row_spec(width, back),
            full_spec(n, width),
            full_spec(n, width),
            row_spec(HD, back),
            full_spec(n, HD),
        ],
        out_shape=[
            jax.ShapeDtypeStruct((n, width), bf16),
            jax.ShapeDtypeStruct((n, width), bf16),
            jax.ShapeDtypeStruct((n, width), bf16),
            jax.ShapeDtypeStruct((n, HD), f32),
            jax.ShapeDtypeStruct((n, HD), f32),
        ],
        scratch_shapes=[
            pltpu.VMEM((BLK, width), f32),
            pltpu.VMEM((width, n), f32),
            pltpu.VMEM((width, n), f32),
            pltpu.VMEM((HD, n), f32),
            pltpu.VMEM((8, n), f32),
            pltpu.VMEM((BLK, n), f32),
            pltpu.VMEM((width, BLK), bf16),
            pltpu.VMEM((width, BLK), bf16),
        ],
        name="attend_back",
        cost_estimate=pl.CostEstimate(flops=18 * n * n * 256, bytes_accessed=8 * n * n, transcendentals=0),
    )(q, k, v, do, lse, fence, sq, sk)


epsilon = 1e-05


def layer_norm(source, scales, offset):
    centre = source - jnp.mean(source, -1, keepdims=True)
    spread = jnp.mean(centre * centre, -1, keepdims=True)
    return centre * lax.rsqrt(spread + epsilon) * scales + offset


def gelu_tanh(source):
    return jax.nn.gelu(source, approximate=True)


def mm_tn(a, b):
    return lax.dot_general(a, b, (((0,), (0,)), ((), ())), preferred_element_type=f32)


def swap_core(x):
    n = lax.axis_size("tensor")
    return lax.ppermute(x, "tensor", [(i, i ^ 1) for i in range(n)])


def swap_chip(x):
    n = lax.axis_size("tensor")
    return lax.ppermute(x, "tensor", [(i, i ^ 2) for i in range(n)])

def send(src, dst, send_sem, recv_sem, **where):
    copy = pltpu.make_async_remote_copy(
        src_ref=src,
        dst_ref=dst,
        send_sem=send_sem,
        recv_sem=recv_sem,
        device_id=where,
        device_id_type=pl.DeviceIdType.MESH,
    )
    copy.start()
    return copy


def meet(devices):
    barrier = pltpu.get_barrier_semaphore()
    for where in devices:
        pl.semaphore_signal(barrier, inc=1, device_id=where, device_id_type=pl.DeviceIdType.MESH)
    pl.semaphore_wait(barrier, len(devices))


def finish_kernel(
    n, chunk, piece,
    gb, ga, small_in, dq1, dk1, dv1, dq2, dk2, dv2, dsel, w1, w2, sel_w, hidden, gain, gmid,
    fb, fa, small_out, input_grad,
    ng_send, ng_recv, yb, ya, sb, sa, zb, za, own_b, tb,
    small, ys, ss, zs, ts, out_s,
    core_s, core_r, y_s, y_r, z_s, z_r, t_s, t_r, az_s, az_r, ay_s, ay_r,
):
    idx = lax.axis_index("dp")
    me = lax.axis_index("tensor")
    odd = lax.rem(me, 2)
    par = lax.rem(idx, 2)
    z = lax.div(idx, 2)
    m = n // 2
    half = m * chunk
    shalf = m * piece
    rows = hidden.shape[0]
    ranks = 4
    core = me + 1 - 2 * odd
    ydev = idx + 1 - 2 * par
    peers = [lax.rem(me + d, ranks) for d in range(1, ranks)]
    zdev = [lax.rem(z + d, m) for d in range(1, m)]
    meet(
        [{"tensor": p} for p in peers]
        + [{"dp": ydev}]
        + [{"dp": 2 * p + par} for p in zdev]
    )
    give = pl.multiple_of((1 - par) * half, half)
    keep = pl.multiple_of(par * half, half)
    cyb = send(gb.at[pl.ds(give, half)], yb, y_s.at[0], y_r.at[0], dp=ydev)
    cya = send(ga.at[pl.ds(give, half)], ya, y_s.at[1], y_r.at[1], dp=ydev)

    def normed_grad(start):
        part = pl.ds(pl.multiple_of(start, rows), rows)
        total = mm_nt(dsel[part, :], sel_w[...])
        for grads, weights in (((dq1, dk1, dv1), w1), ((dq2, dk2, dv2), w2)):
            for j in range(3):
                total = total + mm_nt(grads[j][part, :], weights[j])
        return total

    ng_send[...] = normed_grad((1 - odd) * rows).astype(bf16)
    ccore = send(ng_send, ng_recv, core_s, core_r, tensor=core)
    grad = normed_grad(odd * rows)
    x = hidden[...].astype(f32)
    centre = x - jnp.mean(x, -1, keepdims=True)
    r = lax.rsqrt(jnp.mean(centre * centre, -1, keepdims=True) + epsilon)
    xhat = centre * r
    ccore.wait_recv()
    grad = grad + ng_recv[...].astype(f32)
    e = grad * gain[...]
    back = r * (e - jnp.mean(e, -1, keepdims=True) - xhat * jnp.mean(e * xhat, -1, keepdims=True))
    input_grad[...] = (gmid[...] + back).astype(bf16)
    small[...] = small_in[...]
    dgain = jnp.sum(grad * xhat, 0, keepdims=True)
    dshift = jnp.sum(grad, 0, keepdims=True)
    lines = dgain.shape[1] // 128
    for j in range(lines):
        small[j : j + 1, :] = dgain[:, j * 128 : (j + 1) * 128]
        small[lines + j : lines + j + 1, :] = dshift[:, j * 128 : (j + 1) * 128]
    sgive = pl.multiple_of((1 - par) * shalf, shalf)
    skeep = pl.multiple_of(par * shalf, shalf)
    cys = send(small.at[pl.ds(sgive, shalf)], ys, y_s.at[2], y_r.at[2], dp=ydev)

    def z_stage(total, recv, size, k):
        return [
            send(
                total.at[pl.ds(pl.multiple_of(zdev[d] * size, size), size)],
                recv.at[d],
                z_s.at[k, d],
                z_r.at[k, d],
                dp=2 * zdev[d] + par,
            )
            for d in range(m - 1)
        ]

    cyb.wait_recv()
    sb[...] = (gb[pl.ds(keep, half), :].astype(f32) + yb[...].astype(f32)).astype(bf16)
    czb = z_stage(sb, zb, chunk, 0)
    cys.wait_recv()
    ss[...] = small[pl.ds(skeep, shalf), :] + ys[...]
    czs = z_stage(ss, zs, piece, 2)
    cya.wait_recv()
    sa[...] = (ga[pl.ds(keep, half), :].astype(f32) + ya[...].astype(f32)).astype(bf16)
    cza = z_stage(sa, za, chunk, 1)

    def z_sum(total, recv, size, copies):
        acc = total[pl.ds(pl.multiple_of(z * size, size), size), :].astype(f32)
        for d in range(m - 1):
            copies[d].wait_recv()
            acc = acc + recv[d].astype(f32)
        return acc

    acc_b = z_sum(sb, zb, chunk, czb)
    own_b[...] = acc_b[:, :384]
    tb[me] = acc_b[:, 384:].astype(bf16)
    ts[me] = z_sum(ss, zs, piece, czs)
    ct = []
    for d in range(ranks - 1):
        ct.append(send(tb.at[me], tb.at[me], t_s.at[0, d], t_r.at[0, d], tensor=peers[d]))
        ct.append(send(ts.at[me], ts.at[me], t_s.at[1, d], t_r.at[1, d], tensor=peers[d]))
    at = par * m + z
    mine = pl.ds(pl.multiple_of(at * chunk, chunk), chunk)
    smine = pl.ds(pl.multiple_of(at * piece, piece), piece)

    def spread(full, where, k):
        out = [
            send(full.at[where], full.at[where], az_s.at[k, d], az_r.at[k, d], dp=2 * zdev[d] + par)
            for d in range(m - 1)
        ]
        return out, [send(full.at[where], full.at[where], ay_s.at[k, 0], ay_r.at[k, 0], dp=ydev)]

    def forward(full, size, k, copies, ahead):
        for d in range(m - 1):
            copies[d].wait_recv()
            came = par * m + lax.rem(z - (d + 1) + m, m)
            where = pl.ds(pl.multiple_of(came * size, size), size)
            ahead.append(
                send(full.at[where], full.at[where], ay_s.at[k, d + 1], ay_r.at[k, d + 1], dp=ydev)
            )

    fa[mine, :] = z_sum(sa, za, chunk, cza).astype(bf16)
    aza, aya = spread(fa, mine, 1)
    for c in ct:
        c.wait_recv()
    sel = tb[0].astype(f32)
    vec = ts[0]
    for d in range(1, ranks):
        sel = sel + tb[d].astype(f32)
        vec = vec + ts[d]
    first = jnp.where(me == 0, 1.0, 0.0)
    lane = lax.broadcasted_iota(jnp.int32, sel.shape, 1)
    lower = jnp.where(lane < HD, sel, 0.0) * first
    upper = jnp.where(lane < HD, 0.0, sel) * first
    fb[mine, :128] = (own_b[:, :128] + lower).astype(bf16)
    fb[mine, 128:256] = (own_b[:, 128:256] + upper).astype(bf16)
    fb[mine, 256:] = own_b[:, 256:].astype(bf16)
    azb, ayb = spread(fb, mine, 0)
    out_s[smine, :] = vec
    azs, ays = spread(out_s, smine, 2)
    forward(fa, chunk, 1, aza, aya)
    forward(fb, chunk, 0, azb, ayb)
    forward(out_s, piece, 2, azs, ays)
    for c in aya + ayb + ays:
        c.wait_recv()
    small_out[...] = out_s[...]
    for c in [cyb, cya, cys, ccore] + czb + cza + czs + ct + aza + azb + azs + aya + ayb + ays:
        c.wait_send()


def finish(n, gb, ga, small, grads1, grads2, dsel, w1, w2, sel_w, hidden, gain, gmid):
    m = n // 2
    chunk = gb.shape[0] // n
    piece = small.shape[0] // n
    rows, depth = hidden.shape
    half, shalf = m * chunk, m * piece
    wb, wa = gb.shape[1], ga.shape[1]
    ranks = 4
    vmem = pl.BlockSpec(memory_space=pltpu.VMEM)
    dma = pltpu.SemaphoreType.DMA
    return pl.pallas_call(
        lambda *refs: finish_kernel(n, chunk, piece, *refs),
        in_specs=[vmem] * 16,
        out_specs=[vmem] * 4,
        out_shape=[
            jax.ShapeDtypeStruct((n * chunk, wb - 128), bf16),
            jax.ShapeDtypeStruct((n * chunk, wa), bf16),
            jax.ShapeDtypeStruct(small.shape, f32),
            jax.ShapeDtypeStruct((rows, depth), bf16),
        ],
        scratch_shapes=[
            pltpu.VMEM((rows, depth), bf16),
            pltpu.VMEM((rows, depth), bf16),
            pltpu.VMEM((half, wb), bf16),
            pltpu.VMEM((half, wa), bf16),
            pltpu.VMEM((half, wb), bf16),
            pltpu.VMEM((half, wa), bf16),
            pltpu.VMEM((m - 1, chunk, wb), bf16),
            pltpu.VMEM((m - 1, chunk, wa), bf16),
            pltpu.VMEM((chunk, wb - 128), f32),
            pltpu.VMEM((ranks, chunk, 128), bf16),
            pltpu.VMEM(small.shape, f32),
            pltpu.VMEM((shalf, 128), f32),
            pltpu.VMEM((shalf, 128), f32),
            pltpu.VMEM((m - 1, piece, 128), f32),
            pltpu.VMEM((ranks, piece, 128), f32),
            pltpu.VMEM(small.shape, f32),
            dma, dma,
            dma((3,)), dma((3,)),
            dma((3, m - 1)), dma((3, m - 1)),
            dma((2, 3)), dma((2, 3)),
            dma((3, m - 1)), dma((3, m - 1)),
            dma((3, m)), dma((3, m)),
        ],
        compiler_params=pltpu.CompilerParams(
            collective_id=0, has_side_effects=True, vmem_limit_bytes=60 * 1024 * 1024
        ),
        name="finish",
    )(gb, ga, small, *grads1, *grads2, dsel, w1, w2, sel_w, hidden, gain, gmid)


def shards(
    hidden_in,
    lengths,
    ln1_gain,
    ln1_shift,
    qkv_weight,
    qv_bias,
    out_weight,
    out_bias,
    ln2_gain,
    ln2_shift,
    up_weight,
    up_bias,
    down_weight,
    down_bias,
    out_grad,
):
    rows = hidden_in.shape[0]
    ranks = lax.axis_size("tensor")
    me = lax.axis_index("tensor")
    odd = me % 2
    length = jnp.where(me < 2, lengths[0], lengths[1])
    live = (odd * rows + jnp.arange(rows) < length).astype(f32)[:, None]

    def join(mine, other):
        first = jnp.where(odd == 0, mine, other)
        second = jnp.where(odd == 0, other, mine)
        return jnp.concatenate([first, second], 0)

    def my_half(x):
        return lax.dynamic_slice_in_dim(x, odd * rows, rows, 0)

    def other_half(x):
        return lax.dynamic_slice_in_dim(x, (1 - odd) * rows, rows, 0)

    sel_w = jnp.concatenate([qkv_weight[0][:, :HD], qkv_weight[1][:, :HD]], 1)
    sel_b = qv_bias[:1, :HD]
    sel_w = jnp.where(me == 0, sel_w, lax.ppermute(sel_w, "tensor", [(0, 2)]))
    sel_b = jnp.where(me == 0, sel_b, lax.ppermute(sel_b, "tensor", [(0, 2)]))
    sel_w = jnp.where(odd == 0, sel_w, lax.ppermute(sel_w, "tensor", [(0, 1), (2, 3)]))
    sel_b = jnp.where(odd == 0, sel_b, lax.ppermute(sel_b, "tensor", [(0, 1), (2, 3)]))

    residual = hidden_in.astype(f32)
    normed_mine = layer_norm(residual, ln1_gain, ln1_shift).astype(bf16)
    normed = join(normed_mine, swap_core(normed_mine))

    qkv_far = swap_chip(qkv_weight)
    bias_far = swap_chip(qv_bias)
    out_far = swap_chip(out_weight)

    grad_out = out_grad.astype(f32) * live
    grad_branch = grad_out.astype(bf16)
    grad_near = join(grad_branch, swap_core(grad_branch))
    grad_far = swap_chip(grad_branch)
    grad_far = join(grad_far, swap_core(grad_far))

    def project(weights, bias):
        q = (mm(normed, weights[0]) + bias[0]).astype(bf16)
        k = mm(normed, weights[1]).astype(bf16)
        v = (mm(normed, weights[2]) + bias[1]).astype(bf16)
        return q, k, v

    sq = (mm(normed, sel_w[:, :HD]) + sel_b).astype(bf16)
    sk = mm(normed, sel_w[:, HD:]).astype(bf16)
    q1, k1, v1 = project(qkv_weight, qv_bias)
    o1, lse1, fence = attend_first(q1, k1, v1, sq, sk, length[None])
    q2, k2, v2 = project(qkv_far, bias_far)
    o2, lse2 = attend_next(q2, k2, v2, fence)

    def attn_out(part):
        return mm(part(o1), out_weight) + mm(part(o2), out_far)

    attn_given = swap_core(attn_out(other_half).astype(bf16))
    middle = residual + (attn_out(my_half) + attn_given.astype(f32)) + out_bias
    inner, ln2_back = jax.vjp(layer_norm, middle, ln2_gain, ln2_shift)
    inner = inner.astype(bf16)
    inner_near = join(inner, swap_core(inner))
    inner_far = swap_chip(inner)
    inner_far = join(inner_far, swap_core(inner_far))

    def feed(inner_rows, grad_rows):
        pre = mm(inner_rows, up_weight) + up_bias.astype(f32)
        act, gelu_back = jax.vjp(gelu_tanh, pre)
        grad_act = mm_nt(grad_rows, down_weight)
        grad_pre = gelu_back(grad_act)[0].astype(bf16)
        return act.astype(bf16), grad_pre

    act_near, pre_near = feed(inner_near, grad_near)
    act_far, pre_far = feed(inner_far, grad_far)

    def gather_sum(near, far, weight, product):
        far_given = swap_core(product(other_half(far), weight).astype(bf16))
        far_sum = product(my_half(far), weight) + far_given.astype(f32)
        from_chip = swap_chip(far_sum.astype(bf16))
        near_given = swap_core(product(other_half(near), weight).astype(bf16))
        return product(my_half(near), weight) + near_given.astype(f32) + from_chip.astype(f32)

    grad_inner = gather_sum(pre_near, pre_far, up_weight, mm_nt)
    branch = gather_sum(act_near, act_far, down_weight, mm)
    output = (live * (middle + branch + down_bias)).astype(bf16)

    down_grad = mm_tn(act_near, grad_near) + mm_tn(act_far, grad_far)
    up_grad = mm_tn(inner_near, pre_near) + mm_tn(inner_far, pre_far)
    up_bias_grad = jnp.sum(pre_near, 0, dtype=f32) + jnp.sum(pre_far, 0, dtype=f32)

    grad_norm2, ln2_gain_grad, ln2_shift_grad = ln2_back(grad_inner)
    grad_middle = grad_out + grad_norm2
    grad_attn = grad_middle.astype(bf16)
    out_bias_grad = jnp.sum(grad_attn, 0, dtype=f32)
    down_bias_grad = jnp.sum(grad_out, 0)
    attn_rows = join(grad_attn, swap_core(grad_attn))

    go2 = mm_nt(attn_rows, out_far).astype(bf16)
    go1 = mm_nt(attn_rows, out_weight).astype(bf16)
    dq2, dk2, dv2, dsq2, dsk2 = attend_back(q2, k2, v2, go2, lse2, fence, sq, sk)
    dq1, dk1, dv1, dsq1, dsk1 = attend_back(q1, k1, v1, go1, lse1, fence, sq, sk)

    def grad_block(dq, dk, dv, o):
        return jnp.concatenate(
            [mm_tn(normed, dq), mm_tn(normed, dk), mm_tn(normed, dv), mm_tn(attn_rows, o)], 1
        )

    n = lax.axis_size("dp")
    width = q1.shape[1]
    depth = normed.shape[1]
    chunk = -(-depth // (16 * n)) * 16
    far_block = swap_chip(grad_block(dq2, dk2, dv2, o2).astype(bf16))
    block = grad_block(dq1, dk1, dv1, o1) + far_block.astype(f32)
    dsel = jnp.concatenate([dsq1 + dsq2, dsk1 + dsk2], 1).astype(bf16)
    sel_grad = mm_tn(normed, dsel)
    fill = ((0, n * chunk - depth), (0, 0))
    block_b = jnp.pad(jnp.concatenate([block[:, : 2 * width], sel_grad], 1), fill).astype(bf16)
    block_a = jnp.pad(block[:, 2 * width :], fill).astype(bf16)

    ffn_grad = lax.psum(jnp.concatenate([up_grad, down_grad], 0).astype(bf16), "dp").astype(f32)

    def bias_of(dq, dv):
        return jnp.stack([jnp.sum(dq, 0, dtype=f32), jnp.sum(dv, 0, dtype=f32)])

    slot = jnp.arange(ranks)[:, None, None]
    sel_bias = jnp.pad(jnp.sum(dsel[:, :HD], 0, dtype=f32)[None], ((0, 1), (0, width - HD)))
    qv_parts = (
        jnp.where(slot == me, bias_of(dq1, dv1)[None], 0.0)
        + jnp.where(slot == me ^ 2, bias_of(dq2, dv2)[None], 0.0)
        + jnp.where(slot == 0, sel_bias[None], 0.0)
    )
    up_parts = jnp.where(slot[:, 0] == me, up_bias_grad[None], 0.0)
    none = jnp.zeros_like(out_bias_grad)
    small = jnp.concatenate(
        [
            none,
            none,
            out_bias_grad,
            ln2_gain_grad,
            ln2_shift_grad,
            down_bias_grad,
            up_parts.reshape(-1),
            qv_parts.reshape(-1),
        ]
    )
    lines = small.shape[0] // 128
    piece = -(-lines // (8 * n)) * 8
    small = jnp.pad(small.reshape(lines, 128), ((0, n * piece - lines), (0, 0)))
    full_b, full_a, small, input_grad = finish(
        n, block_b, block_a, small, (dq1, dk1, dv1), (dq2, dk2, dv2), dsel,
        qkv_weight, qkv_far, sel_w, hidden_in, ln1_gain[None], grad_middle,
    )
    small = small[:lines].reshape(-1)
    vectors = small[: 6 * depth].reshape(6, depth)
    hidden = up_bias.shape[0]
    up_all = small[6 * depth : 6 * depth + ranks * hidden].reshape(ranks, hidden)
    qv_all = small[6 * depth + ranks * hidden :].reshape(ranks, 2, width)
    up_bias_grad = lax.dynamic_index_in_dim(up_all, me, 0, keepdims=False)
    qv_bias_grad = lax.dynamic_index_in_dim(qv_all, me, 0, keepdims=False)
    qkv_grad = jnp.stack(
        [full_b[:depth, :width], full_b[:depth, width:], full_a[:depth, :width]]
    ).astype(f32)
    out_weight_grad = full_a[:depth, width:].T.astype(f32)
    return (
        output,
        input_grad,
        vectors[0],
        vectors[1],
        qkv_grad,
        qv_bias_grad,
        out_weight_grad,
        vectors[2],
        vectors[3],
        vectors[4],
        ffn_grad[:depth],
        up_bias_grad,
        ffn_grad[depth:],
        vectors[5],
    )


def solution(mesh):
    return jax.shard_map(
        shards,
        mesh=mesh,
        in_specs=(
            P(("dp", "tensor"), None),
            P("dp"),
            P(),
            P(),
            P(None, None, "tensor"),
            P(None, "tensor"),
            P("tensor", None),
            P(),
            P(),
            P(),
            P(None, "tensor"),
            P("tensor"),
            P("tensor", None),
            P(),
            P(("dp", "tensor"), None),
        ),
        out_specs=(
            P(("dp", "tensor"), None),
            P(("dp", "tensor"), None),
            P(),
            P(),
            P(None, None, "tensor"),
            P(None, "tensor"),
            P("tensor", None),
            P(),
            P(),
            P(),
            P(None, "tensor"),
            P("tensor"),
            P("tensor", None),
            P(),
        ),
        check_vma=False,
    )
```

```python
import math

import jax
import jax.numpy as jnp
from jax import lax
from jax.experimental import pallas as pl
from jax.experimental.pallas import tpu as pltpu
from jax.sharding import PartitionSpec as P

HD = 64
BLK = 256
BIG = 1e30
sel_factor = 4.0
score_scale = 1.0 / math.sqrt(HD)
f32 = jnp.float32
bf16 = jnp.bfloat16


def mm(a, b):
    return lax.dot_general(a, b, (((1,), (0,)), ((), ())), preferred_element_type=f32)


def mm_nt(a, b):
    return lax.dot_general(a, b, (((1,), (1,)), ((), ())), preferred_element_type=f32)


def flip(a):
    return a.astype(f32).T.astype(bf16)


def split_mm(tri, x):
    hi = x.astype(bf16)
    lo = (x - hi.astype(f32)).astype(bf16)
    return mm(tri, hi) + mm(tri, lo)


def head_mask(h, width):
    return lax.broadcasted_iota(jnp.int32, (BLK, width), 1) // HD == h


def masked_rows(x, mask, scale):
    return jnp.where(mask, x.astype(f32) * scale, 0.0).astype(bf16)


def fwd_block(i, heads, first, q_ref, k_ref, v_ref, fence, o_ref, lse_ref):
    width = q_ref.shape[1]
    cols = (i + 1) * BLK
    keys = k_ref[:cols, :]
    vals = v_ref[:cols, :]
    fenced = fence[:, :cols]
    lane = lax.broadcasted_iota(jnp.int32, (BLK, 128), 1)
    lse_ref[...] = jnp.zeros_like(lse_ref)
    out_scr = first

    def head(h, _):
        mask = head_mask(h, width)
        s = mm_nt(masked_rows(q_ref[...], mask, score_scale), keys) - fenced
        top = jnp.max(s, -1, keepdims=True)
        e = jnp.exp(s - top)
        total = jnp.sum(e, -1, keepdims=True)
        p = (e * (1.0 / total)).astype(bf16)
        out = mm(p, vals)
        out_scr[...] = jnp.where(mask, out, out_scr[...])
        lse_ref[...] = jnp.where(lane == h, top + jnp.log(total), lse_ref[...])
        return 0

    lax.fori_loop(0, heads, head, 0)
    o_ref[...] = out_scr[...].astype(bf16)


def make_fence(i, seq_len, length, sq_ref, sk_ref, fence, carry):
    cols = (i + 1) * BLK
    s0 = mm_nt(sq_ref[...], sk_ref[:cols, :]) * score_scale
    row = i * BLK + lax.broadcasted_iota(jnp.int32, (BLK, cols), 0)
    col = lax.broadcasted_iota(jnp.int32, (BLK, cols), 1)
    picked = (col >= 1) & (col < row)
    sel = jnp.where(picked, jnp.maximum(s0, 0.0), 0.0) * (sel_factor / seq_len)
    r2 = lax.broadcasted_iota(jnp.int32, (BLK, BLK), 0)
    c2 = lax.broadcasted_iota(jnp.int32, (BLK, BLK), 1)
    tri = jnp.where(c2 < r2, 1.0, 0.0).astype(bf16)
    total = carry[0:1, :cols] + split_mm(tri, sel)
    carry[0:1, :cols] = total[BLK - 1 : BLK, :] + sel[BLK - 1 : BLK, :]
    fence[:, :cols] = jnp.where((col <= row) & (col < length), total, BIG)


def fwd_first_kernel(heads, len_ref, q_ref, k_ref, v_ref, sq_ref, sk_ref, o_ref, lse_ref, f_ref, out_scr, carry):
    r = pl.program_id(0)
    seq_len = k_ref.shape[0]

    @pl.when(r == 0)
    def _():
        carry[...] = jnp.zeros_like(carry)

    for i in range(seq_len // BLK):

        @pl.when(r == i)
        def _():
            make_fence(i, seq_len, len_ref[0], sq_ref, sk_ref, f_ref, carry)
            fwd_block(i, heads, out_scr, q_ref, k_ref, v_ref, f_ref, o_ref, lse_ref)


def fwd_next_kernel(heads, q_ref, k_ref, v_ref, f_ref, o_ref, lse_ref, out_scr):
    r = pl.program_id(0)
    for i in range(k_ref.shape[0] // BLK):

        @pl.when(r == i)
        def _():
            fwd_block(i, heads, out_scr, q_ref, k_ref, v_ref, f_ref, o_ref, lse_ref)


def row_spec(width, back=None):
    if back is None:
        return pl.BlockSpec((BLK, width), lambda r: (r, 0))
    return pl.BlockSpec((BLK, width), lambda r: (back - 1 - r, 0))


def full_spec(rows, width):
    return pl.BlockSpec((rows, width), lambda r: (0, 0))


def attend_first(q, k, v, sq, sk, length):
    n, width = q.shape
    heads = width // HD
    return pl.pallas_call(
        lambda *refs: fwd_first_kernel(heads, *refs),
        grid=(n // BLK,),
        in_specs=[
            pl.BlockSpec(memory_space=pltpu.SMEM),
            row_spec(width),
            full_spec(n, width),
            full_spec(n, width),
            row_spec(HD),
            full_spec(n, HD),
        ],
        out_specs=[row_spec(width), row_spec(128), row_spec(n)],
        out_shape=[
            jax.ShapeDtypeStruct((n, width), bf16),
            jax.ShapeDtypeStruct((n, 128), f32),
            jax.ShapeDtypeStruct((n, n), f32),
        ],
        scratch_shapes=[pltpu.VMEM((BLK, width), f32), pltpu.VMEM((8, n), f32)],
        name="attend_first",
        cost_estimate=pl.CostEstimate(flops=6 * n * n * 256, bytes_accessed=8 * n * n, transcendentals=0),
    )(length, q, k, v, sq, sk)


def attend_next(q, k, v, fence):
    n, width = q.shape
    heads = width // HD
    return pl.pallas_call(
        lambda *refs: fwd_next_kernel(heads, *refs),
        grid=(n // BLK,),
        in_specs=[row_spec(width), full_spec(n, width), full_spec(n, width), row_spec(n)],
        out_specs=[row_spec(width), row_spec(128)],
        out_shape=[
            jax.ShapeDtypeStruct((n, width), bf16),
            jax.ShapeDtypeStruct((n, 128), f32),
        ],
        scratch_shapes=[pltpu.VMEM((BLK, width), f32)],
        name="attend_next",
        cost_estimate=pl.CostEstimate(flops=6 * n * n * 256, bytes_accessed=8 * n * n, transcendentals=0),
    )(q, k, v, fence)


def bwd_block(i, heads, q_ref, k_ref, v_ref, do_ref, lse_ref, f_ref, sq_ref, sk_ref,
              dq_ref, dsq_ref, dq_scr, dkt, dvt, dskt, later, fsum, qt, dot_):
    width = q_ref.shape[1]
    seq_len = k_ref.shape[0]
    cols = (i + 1) * BLK
    keys = k_ref[:cols, :]
    vals = v_ref[:cols, :]
    lane = lax.broadcasted_iota(jnp.int32, (BLK, 128), 1)
    qt[...] = (q_ref[...].astype(f32) * score_scale).T.astype(bf16)
    dot_[...] = flip(do_ref[...])
    fsum[:, :cols] = jnp.zeros((BLK, cols), f32)

    def head(h, _):
        mask = head_mask(h, width)
        lse = jnp.sum(jnp.where(lane == h, lse_ref[...], 0.0), -1, keepdims=True)
        s = mm_nt(masked_rows(q_ref[...], mask, score_scale), keys)
        p = jnp.exp(s - f_ref[:, :cols] - lse)
        dp = mm_nt(masked_rows(do_ref[...], mask, 1.0), vals)
        delta = jnp.sum(p * dp, -1, keepdims=True)
        g = (p * (dp - delta)).astype(bf16)
        rows = pl.ds(pl.multiple_of(h * HD, HD), HD)
        dq_scr[...] = jnp.where(mask, mm(g, keys), dq_scr[...])
        dkt[rows, :cols] += mm(qt[rows, :], g)
        dvt[rows, :cols] += mm(dot_[rows, :], p.astype(bf16))
        fsum[:, :cols] += g.astype(f32)
        return 0

    lax.fori_loop(0, heads, head, 0)
    dq_ref[...] = (dq_scr[...] * score_scale).astype(bf16)
    grad = -fsum[:, :cols]
    r2 = lax.broadcasted_iota(jnp.int32, (BLK, BLK), 0)
    c2 = lax.broadcasted_iota(jnp.int32, (BLK, BLK), 1)
    tri = jnp.where(c2 > r2, 1.0, 0.0).astype(bf16)
    dsel = later[0:1, :cols] + split_mm(tri, grad)
    later[0:1, :cols] = dsel[0:1, :] + grad[0:1, :]
    s0 = mm_nt(sq_ref[...], sk_ref[:cols, :])
    row = i * BLK + lax.broadcasted_iota(jnp.int32, (BLK, cols), 0)
    col = lax.broadcasted_iota(jnp.int32, (BLK, cols), 1)
    keep = (col >= 1) & (col < row) & (s0 > 0)
    gsel = jnp.where(keep, dsel * (sel_factor / seq_len), 0.0).astype(bf16)
    dsq_ref[...] = mm(gsel, sk_ref[:cols, :]) * score_scale
    sqt = (sq_ref[...].astype(f32) * score_scale).T.astype(bf16)
    dskt[:, :cols] += mm(sqt, gsel)


def bwd_kernel(heads, q_ref, k_ref, v_ref, do_ref, lse_ref, f_ref, sq_ref, sk_ref,
               dq_ref, dk_ref, dv_ref, dsq_ref, dsk_ref,
               dq_scr, dkt, dvt, dskt, later, fsum, qt, dot_):
    g = pl.program_id(0)
    n = k_ref.shape[0] // BLK

    @pl.when(g == 0)
    def _():
        dkt[...] = jnp.zeros_like(dkt)
        dvt[...] = jnp.zeros_like(dvt)
        dskt[...] = jnp.zeros_like(dskt)
        later[...] = jnp.zeros_like(later)

    for i in range(n):

        @pl.when(g == n - 1 - i)
        def _():
            bwd_block(i, heads, q_ref, k_ref, v_ref, do_ref, lse_ref, f_ref, sq_ref, sk_ref,
                      dq_ref, dsq_ref, dq_scr, dkt, dvt, dskt, later, fsum, qt, dot_)

    @pl.when(g == n - 1)
    def _():
        dk_ref[...] = dkt[...].T.astype(bf16)
        dv_ref[...] = dvt[...].T.astype(bf16)
        dsk_ref[...] = dskt[...].T


def attend_back(q, k, v, do, lse, fence, sq, sk):
    n, width = q.shape
    heads = width // HD
    back = n // BLK
    return pl.pallas_call(
        lambda *refs: bwd_kernel(heads, *refs),
        grid=(back,),
        in_specs=[
            row_spec(width, back),
            full_spec(n, width),
            full_spec(n, width),
            row_spec(width, back),
            row_spec(128, back),
            row_spec(n, back),
            row_spec(HD, back),
            full_spec(n, HD),
        ],
        out_specs=[
            row_spec(width, back),
            full_spec(n, width),
            full_spec(n, width),
            row_spec(HD, back),
            full_spec(n, HD),
        ],
        out_shape=[
            jax.ShapeDtypeStruct((n, width), bf16),
            jax.ShapeDtypeStruct((n, width), bf16),
            jax.ShapeDtypeStruct((n, width), bf16),
            jax.ShapeDtypeStruct((n, HD), f32),
            jax.ShapeDtypeStruct((n, HD), f32),
        ],
        scratch_shapes=[
            pltpu.VMEM((BLK, width), f32),
            pltpu.VMEM((width, n), f32),
            pltpu.VMEM((width, n), f32),
            pltpu.VMEM((HD, n), f32),
            pltpu.VMEM((8, n), f32),
            pltpu.VMEM((BLK, n), f32),
            pltpu.VMEM((width, BLK), bf16),
            pltpu.VMEM((width, BLK), bf16),
        ],
        name="attend_back",
        cost_estimate=pl.CostEstimate(flops=18 * n * n * 256, bytes_accessed=8 * n * n, transcendentals=0),
    )(q, k, v, do, lse, fence, sq, sk)


epsilon = 1e-05


def layer_norm(source, scales, offset):
    centre = source - jnp.mean(source, -1, keepdims=True)
    spread = jnp.mean(centre * centre, -1, keepdims=True)
    return centre * lax.rsqrt(spread + epsilon) * scales + offset


def mm_tn(a, b):
    return lax.dot_general(a, b, (((0,), (0,)), ((), ())), preferred_element_type=f32)


def swap_core(x):
    n = lax.axis_size("tensor")
    return lax.ppermute(x, "tensor", [(i, i ^ 1) for i in range(n)])


def swap_chip(x):
    n = lax.axis_size("tensor")
    return lax.ppermute(x, "tensor", [(i, i ^ 2) for i in range(n)])

def send(src, dst, send_sem, recv_sem, **where):
    copy = pltpu.make_async_remote_copy(
        src_ref=src,
        dst_ref=dst,
        send_sem=send_sem,
        recv_sem=recv_sem,
        device_id=where,
        device_id_type=pl.DeviceIdType.MESH,
    )
    copy.start()
    return copy


def meet(devices):
    barrier = pltpu.get_barrier_semaphore()
    for where in devices:
        pl.semaphore_signal(barrier, inc=1, device_id=where, device_id_type=pl.DeviceIdType.MESH)
    pl.semaphore_wait(barrier, len(devices))


def finish_kernel(
    n, chunk, piece,
    gb, ga, small_in, dq1, dk1, dv1, dq2, dk2, dv2, dsel, w1, w2, sel_w, hidden, gain, gmid,
    fb, fa, small_out, input_grad,
    ng_send, ng_recv, yb, ya, sb, sa, zb, za, own_b, tb,
    small, ys, ss, zs, ts, out_s,
    core_s, core_r, y_s, y_r, z_s, z_r, t_s, t_r, az_s, az_r, ay_s, ay_r,
):
    idx = lax.axis_index("dp")
    me = lax.axis_index("tensor")
    odd = lax.rem(me, 2)
    par = lax.rem(idx, 2)
    z = lax.div(idx, 2)
    m = n // 2
    half = m * chunk
    shalf = m * piece
    rows = hidden.shape[0]
    ranks = 4
    core = me + 1 - 2 * odd
    ydev = idx + 1 - 2 * par
    peers = [lax.rem(me + d, ranks) for d in range(1, ranks)]
    zdev = [lax.rem(z + d, m) for d in range(1, m)]
    meet(
        [{"tensor": p} for p in peers]
        + [{"dp": ydev}]
        + [{"dp": 2 * p + par} for p in zdev]
    )
    give = pl.multiple_of((1 - par) * half, half)
    keep = pl.multiple_of(par * half, half)
    cyb = send(gb.at[pl.ds(give, half)], yb, y_s.at[0], y_r.at[0], dp=ydev)
    cya = send(ga.at[pl.ds(give, half)], ya, y_s.at[1], y_r.at[1], dp=ydev)

    def normed_grad(start):
        part = pl.ds(pl.multiple_of(start, rows), rows)
        total = mm_nt(dsel[part, :], sel_w[...])
        for grads, weights in (((dq1, dk1, dv1), w1), ((dq2, dk2, dv2), w2)):
            for j in range(3):
                total = total + mm_nt(grads[j][part, :], weights[j])
        return total

    ng_send[...] = normed_grad((1 - odd) * rows).astype(bf16)
    ccore = send(ng_send, ng_recv, core_s, core_r, tensor=core)
    grad = normed_grad(odd * rows)
    x = hidden[...].astype(f32)
    centre = x - jnp.mean(x, -1, keepdims=True)
    r = lax.rsqrt(jnp.mean(centre * centre, -1, keepdims=True) + epsilon)
    xhat = centre * r
    ccore.wait_recv()
    grad = grad + ng_recv[...].astype(f32)
    e = grad * gain[...]
    back = r * (e - jnp.mean(e, -1, keepdims=True) - xhat * jnp.mean(e * xhat, -1, keepdims=True))
    input_grad[...] = (gmid[...] + back).astype(bf16)
    small[...] = small_in[...]
    dgain = jnp.sum(grad * xhat, 0, keepdims=True)
    dshift = jnp.sum(grad, 0, keepdims=True)
    lines = dgain.shape[1] // 128
    for j in range(lines):
        small[j : j + 1, :] = dgain[:, j * 128 : (j + 1) * 128]
        small[lines + j : lines + j + 1, :] = dshift[:, j * 128 : (j + 1) * 128]
    sgive = pl.multiple_of((1 - par) * shalf, shalf)
    skeep = pl.multiple_of(par * shalf, shalf)
    cys = send(small.at[pl.ds(sgive, shalf)], ys, y_s.at[2], y_r.at[2], dp=ydev)

    def z_stage(total, recv, size, k):
        return [
            send(
                total.at[pl.ds(pl.multiple_of(zdev[d] * size, size), size)],
                recv.at[d],
                z_s.at[k, d],
                z_r.at[k, d],
                dp=2 * zdev[d] + par,
            )
            for d in range(m - 1)
        ]

    cyb.wait_recv()
    sb[...] = (gb[pl.ds(keep, half), :].astype(f32) + yb[...].astype(f32)).astype(bf16)
    czb = z_stage(sb, zb, chunk, 0)
    cys.wait_recv()
    ss[...] = small[pl.ds(skeep, shalf), :] + ys[...]
    czs = z_stage(ss, zs, piece, 2)
    cya.wait_recv()
    sa[...] = (ga[pl.ds(keep, half), :].astype(f32) + ya[...].astype(f32)).astype(bf16)
    cza = z_stage(sa, za, chunk, 1)

    def z_sum(total, recv, size, copies):
        acc = total[pl.ds(pl.multiple_of(z * size, size), size), :].astype(f32)
        for d in range(m - 1):
            copies[d].wait_recv()
            acc = acc + recv[d].astype(f32)
        return acc

    acc_b = z_sum(sb, zb, chunk, czb)
    own_b[...] = acc_b[:, :384]
    tb[me] = acc_b[:, 384:].astype(bf16)
    ts[me] = z_sum(ss, zs, piece, czs)
    ct = []
    for d in range(ranks - 1):
        ct.append(send(tb.at[me], tb.at[me], t_s.at[0, d], t_r.at[0, d], tensor=peers[d]))
        ct.append(send(ts.at[me], ts.at[me], t_s.at[1, d], t_r.at[1, d], tensor=peers[d]))
    at = par * m + z
    mine = pl.ds(pl.multiple_of(at * chunk, chunk), chunk)
    smine = pl.ds(pl.multiple_of(at * piece, piece), piece)

    def spread(full, where, k):
        out = [
            send(full.at[where], full.at[where], az_s.at[k, d], az_r.at[k, d], dp=2 * zdev[d] + par)
            for d in range(m - 1)
        ]
        return out, [send(full.at[where], full.at[where], ay_s.at[k, 0], ay_r.at[k, 0], dp=ydev)]

    def forward(full, size, k, copies, ahead):
        for d in range(m - 1):
            copies[d].wait_recv()
            came = par * m + lax.rem(z - (d + 1) + m, m)
            where = pl.ds(pl.multiple_of(came * size, size), size)
            ahead.append(
                send(full.at[where], full.at[where], ay_s.at[k, d + 1], ay_r.at[k, d + 1], dp=ydev)
            )

    fa[mine, :] = z_sum(sa, za, chunk, cza).astype(bf16)
    aza, aya = spread(fa, mine, 1)
    for c in ct:
        c.wait_recv()
    sel = tb[0].astype(f32)
    vec = ts[0]
    for d in range(1, ranks):
        sel = sel + tb[d].astype(f32)
        vec = vec + ts[d]
    first = jnp.where(me == 0, 1.0, 0.0)
    lane = lax.broadcasted_iota(jnp.int32, sel.shape, 1)
    lower = jnp.where(lane < HD, sel, 0.0) * first
    upper = jnp.where(lane < HD, 0.0, sel) * first
    fb[mine, :128] = (own_b[:, :128] + lower).astype(bf16)
    fb[mine, 128:256] = (own_b[:, 128:256] + upper).astype(bf16)
    fb[mine, 256:] = own_b[:, 256:].astype(bf16)
    azb, ayb = spread(fb, mine, 0)
    out_s[smine, :] = vec
    azs, ays = spread(out_s, smine, 2)
    forward(fa, chunk, 1, aza, aya)
    forward(fb, chunk, 0, azb, ayb)
    forward(out_s, piece, 2, azs, ays)
    for c in aya + ayb + ays:
        c.wait_recv()
    small_out[...] = out_s[...]
    for c in [cyb, cya, cys, ccore] + czb + cza + czs + ct + aza + azb + azs + aya + ayb + ays:
        c.wait_send()


def finish(n, gb, ga, small, grads1, grads2, dsel, w1, w2, sel_w, hidden, gain, gmid):
    m = n // 2
    chunk = gb.shape[0] // n
    piece = small.shape[0] // n
    rows, depth = hidden.shape
    half, shalf = m * chunk, m * piece
    wb, wa = gb.shape[1], ga.shape[1]
    ranks = 4
    vmem = pl.BlockSpec(memory_space=pltpu.VMEM)
    dma = pltpu.SemaphoreType.DMA
    return pl.pallas_call(
        lambda *refs: finish_kernel(n, chunk, piece, *refs),
        in_specs=[vmem] * 16,
        out_specs=[vmem] * 4,
        out_shape=[
            jax.ShapeDtypeStruct((n * chunk, wb - 128), bf16),
            jax.ShapeDtypeStruct((n * chunk, wa), bf16),
            jax.ShapeDtypeStruct(small.shape, f32),
            jax.ShapeDtypeStruct((rows, depth), bf16),
        ],
        scratch_shapes=[
            pltpu.VMEM((rows, depth), bf16),
            pltpu.VMEM((rows, depth), bf16),
            pltpu.VMEM((half, wb), bf16),
            pltpu.VMEM((half, wa), bf16),
            pltpu.VMEM((half, wb), bf16),
            pltpu.VMEM((half, wa), bf16),
            pltpu.VMEM((m - 1, chunk, wb), bf16),
            pltpu.VMEM((m - 1, chunk, wa), bf16),
            pltpu.VMEM((chunk, wb - 128), f32),
            pltpu.VMEM((ranks, chunk, 128), bf16),
            pltpu.VMEM(small.shape, f32),
            pltpu.VMEM((shalf, 128), f32),
            pltpu.VMEM((shalf, 128), f32),
            pltpu.VMEM((m - 1, piece, 128), f32),
            pltpu.VMEM((ranks, piece, 128), f32),
            pltpu.VMEM(small.shape, f32),
            dma, dma,
            dma((3,)), dma((3,)),
            dma((3, m - 1)), dma((3, m - 1)),
            dma((2, 3)), dma((2, 3)),
            dma((3, m - 1)), dma((3, m - 1)),
            dma((3, m)), dma((3, m)),
        ],
        compiler_params=pltpu.CompilerParams(
            collective_id=0, has_side_effects=True, vmem_limit_bytes=60 * 1024 * 1024
        ),
        name="finish",
    )(gb, ga, small, *grads1, *grads2, dsel, w1, w2, sel_w, hidden, gain, gmid)

def norm_parts(x):
    centre = x - jnp.mean(x, -1, keepdims=True)
    r = lax.rsqrt(jnp.mean(centre * centre, -1, keepdims=True) + epsilon)
    return centre * r, r


def norm_back(e, xhat, r):
    return r * (e - jnp.mean(e, -1, keepdims=True) - xhat * jnp.mean(e * xhat, -1, keepdims=True))


def gelu_pair(u):
    k = math.sqrt(2.0 / math.pi)
    square = u * u
    t = jnp.tanh(k * u * (1.0 + 0.044715 * square))
    act = 0.5 * u * (1.0 + t)
    slope = 0.5 * (1.0 + t) + 0.5 * u * (1.0 - t * t) * (k * (1.0 + 3.0 * 0.044715 * square))
    return act, slope


def feed_kernel(
    o1, o2, wo1, wo2, hidden, g0, g1, g2, g3, vecs, up, down,
    rows_out, gmid, partial, branch_x, grads, sums,
    inner, gs, act, gpre, mid, attn_send, attn_recv,
    near_send, near_recv, far_send, far_recv, x_send, x_recv,
    bn_send, bn_recv, bf_send, bf_recv, gin,
    g_sem, a_s, a_r, i_s, i_r, x_s, x_r, f_s, f_r, n_s, n_r, c_s, c_r, r_s, r_r, b_s, b_r, o_s, o_r,
):
    me = lax.axis_index("tensor")
    odd = lax.rem(me, 2)
    core = me + 1 - 2 * odd
    far = lax.rem(me + 2, 4)
    rows = hidden.shape[0]
    pieces = rows // BLK
    loads = [pltpu.make_async_copy(g, gs.at[i], g_sem.at[i]) for i, g in enumerate((g0, g1, g2, g3))]
    for c in loads:
        c.start()
    meet([{"tensor": core}, {"tensor": far}])
    out_bias, gain, shift, down_bias, up_bias = (vecs[j : j + 1, :] for j in range(5))

    def attn(start):
        part = pl.ds(pl.multiple_of(start, BLK), BLK)
        return mm(o1[part, :], wo1[...]) + mm(o2[part, :], wo2[...])

    sends = []
    attn_copies = []
    for c in range(pieces):
        here = pl.ds(c * BLK, BLK)
        attn_send[here, :] = attn((1 - odd) * rows + c * BLK).astype(bf16)
        attn_copies.append(send(attn_send.at[here], attn_recv.at[here], a_s.at[c], a_r.at[c], tensor=core))
    inner_copies, far_copies = [], []
    for c in range(pieces):
        here = pl.ds(c * BLK, BLK)
        mine = attn(odd * rows + c * BLK)
        attn_copies[c].wait_recv()
        m = hidden[here, :].astype(f32) + (mine + attn_recv[here, :].astype(f32)) + out_bias
        mid[here, :] = m
        xhat, r = norm_parts(m)
        inner[0, here, :] = (xhat * gain + shift).astype(bf16)
        far_copies.append(send(inner.at[0, here], inner.at[2, here], x_s.at[c], x_r.at[c], tensor=far))
        inner_copies.append(send(inner.at[0, here], inner.at[1, here], i_s.at[c], i_r.at[c], tensor=core))
    sends += attn_copies + inner_copies + far_copies
    for c in loads:
        c.wait()
    sums[...] = jnp.zeros_like(sums)

    def feed(slot, start):
        part = pl.ds(pl.multiple_of(start, BLK), BLK)
        pre = mm(inner[slot, part, :], up[...]) + up_bias
        a, slope = gelu_pair(pre)
        act[slot, part, :] = a.astype(bf16)
        gp = (mm_nt(gs[slot, part, :], down[...]) * slope).astype(bf16)
        gpre[slot, part, :] = gp
        sums[4:5, :] += jnp.sum(gp.astype(f32), 0, keepdims=True)

    def near(c, _):
        feed(0, c * BLK)
        return 0

    lax.fori_loop(0, pieces, near, 0)
    for c in range(pieces):
        inner_copies[c].wait_recv()

    def near_other(c, _):
        part = pl.ds(pl.multiple_of(c * BLK, BLK), BLK)
        feed(1, c * BLK)
        near_send[part, :] = mm_nt(gpre[1, part, :], up[...]).astype(bf16)
        bn_send[part, :] = mm(act[1, part, :], down[...]).astype(bf16)
        return 0

    lax.fori_loop(0, pieces, near_other, 0)
    near_copy = send(near_send, near_recv, n_s.at[0], n_r.at[0], tensor=core)
    branch_copy = send(bn_send, bn_recv, n_s.at[1], n_r.at[1], tensor=core)

    def near_own(c, _):
        part = pl.ds(pl.multiple_of(c * BLK, BLK), BLK)
        gin[part, :] = mm_nt(gpre[0, part, :], up[...])
        partial[part, :] = mid[part, :] + mm(act[0, part, :], down[...]) + down_bias
        return 0

    lax.fori_loop(0, pieces, near_own, 0)

    passed, crossed, back = [], [], []
    for c in range(pieces):
        here = pl.ds(c * BLK, BLK)
        far_copies[c].wait_recv()
        passed.append(send(inner.at[2, here], inner.at[3, here], f_s.at[c], f_r.at[c], tensor=core))
        feed(2, c * BLK)
        passed[c].wait_recv()
        feed(3, c * BLK)
        far_send[here, :] = mm_nt(gpre[3, here, :], up[...]).astype(bf16)
        crossed.append(send(far_send.at[here], far_recv.at[here], c_s.at[c], c_r.at[c], tensor=core))
        g = mm_nt(gpre[2, here, :], up[...])
        crossed[c].wait_recv()
        x_send[here, :] = (g + far_recv[here, :].astype(f32)).astype(bf16)
        back.append(send(x_send.at[here], x_recv.at[here], r_s.at[c], r_r.at[c], tensor=far))
    for c in range(pieces):
        here = pl.ds(c * BLK, BLK)
        bf_send[here, :] = mm(act[3, here, :], down[...]).astype(bf16)
    far_branch = send(bf_send, bf_recv, b_s, b_r, tensor=core)
    depth = up.shape[0]

    def weights(j, _):
        part = pl.ds(pl.multiple_of(j * BLK, BLK), BLK)
        total = mm_tn(inner[0, :, part], gpre[0])
        other = mm_tn(act[0, :, part], gs[0])
        for s in range(1, 4):
            total = total + mm_tn(inner[s, :, part], gpre[s])
            other = other + mm_tn(act[s, :, part], gs[s])
        grads[part, :] = total.astype(bf16)
        grads[pl.ds(pl.multiple_of(depth + j * BLK, BLK), BLK), :] = other.astype(bf16)
        return 0

    for j in range(depth // BLK):
        weights(j, 0)
    far_branch.wait_recv()
    for c in range(pieces):
        here = pl.ds(c * BLK, BLK)
        b = mm(act[2, here, :], down[...])
        branch_x[here, :] = (b + bf_recv[here, :].astype(f32)).astype(bf16)
    near_copy.wait_recv()
    branch_copy.wait_recv()
    partial[...] += bn_recv[...].astype(f32)
    rows_copies = []
    for c in range(pieces):
        here = pl.ds(c * BLK, BLK)
        xhat, r = norm_parts(mid[here, :])
        back[c].wait_recv()
        g = gin[here, :] + near_recv[here, :].astype(f32) + x_recv[here, :].astype(f32)
        g_out = gs[0, here, :].astype(f32)
        gm = g_out + norm_back(g * gain, xhat, r)
        gmid[here, :] = gm
        there = pl.ds(pl.multiple_of(odd * rows + c * BLK, BLK), BLK)
        ga = gm.astype(bf16)
        rows_out[there, :] = ga
        rows_copies.append(
            send(rows_out.at[there], rows_out.at[there], o_s.at[c], o_r.at[c], tensor=core)
        )
        sums[0:1, :] += jnp.sum(g * xhat, 0, keepdims=True)
        sums[1:2, :] += jnp.sum(g, 0, keepdims=True)
        sums[2:3, :] += jnp.sum(ga.astype(f32), 0, keepdims=True)
        sums[3:4, :] += jnp.sum(g_out, 0, keepdims=True)
    for c in rows_copies:
        c.wait_recv()
    for c in sends + passed + crossed + back + rows_copies + [near_copy, branch_copy, far_branch]:
        c.wait_send()


def feed_forward(o1, o2, wo1, wo2, hidden, gs, vecs, up, down):
    rows, depth = hidden.shape
    width = up.shape[1]
    pieces = rows // BLK
    vmem = pl.BlockSpec(memory_space=pltpu.VMEM)
    anyw = pl.BlockSpec(memory_space=pl.ANY)
    dma = pltpu.SemaphoreType.DMA
    wide = pltpu.VMEM((rows, depth), bf16)
    each = [dma((pieces,))] * 2
    return pl.pallas_call(
        feed_kernel,
        in_specs=[vmem] * 5 + [anyw] * 4 + [vmem] * 3,
        out_specs=[vmem] * 6,
        out_shape=[
            jax.ShapeDtypeStruct((2 * rows, depth), bf16),
            jax.ShapeDtypeStruct((rows, depth), f32),
            jax.ShapeDtypeStruct((rows, depth), f32),
            jax.ShapeDtypeStruct((rows, depth), bf16),
            jax.ShapeDtypeStruct((depth + width, depth), bf16),
            jax.ShapeDtypeStruct((8, depth), f32),
        ],
        scratch_shapes=[
            pltpu.VMEM((4, rows, depth), bf16),
            pltpu.VMEM((4, rows, depth), bf16),
            pltpu.VMEM((4, rows, width), bf16),
            pltpu.VMEM((4, rows, width), bf16),
            pltpu.VMEM((rows, depth), f32),
            wide, wide, wide, wide, wide, wide, wide, wide, wide, wide, wide, wide,
            pltpu.VMEM((rows, depth), f32),
            dma((4,)),
            *each, *each, *each, *each,
            dma((2,)), dma((2,)),
            *each, *each,
            dma, dma,
            *each,
        ],
        compiler_params=pltpu.CompilerParams(
            collective_id=1, has_side_effects=True, vmem_limit_bytes=62 * 1024 * 1024
        ),
        name="feed_forward",
    )(o1, o2, wo1, wo2, hidden, *gs, vecs, up, down)


def shards(
    hidden_in,
    lengths,
    ln1_gain,
    ln1_shift,
    qkv_weight,
    qv_bias,
    out_weight,
    out_bias,
    ln2_gain,
    ln2_shift,
    up_weight,
    up_bias,
    down_weight,
    down_bias,
    out_grad,
):
    rows = hidden_in.shape[0]
    ranks = lax.axis_size("tensor")
    me = lax.axis_index("tensor")
    odd = me % 2
    length = jnp.where(me < 2, lengths[0], lengths[1])
    live = (odd * rows + jnp.arange(rows) < length).astype(f32)[:, None]

    def join(mine, other):
        first = jnp.where(odd == 0, mine, other)
        second = jnp.where(odd == 0, other, mine)
        return jnp.concatenate([first, second], 0)

    sel_w = jnp.concatenate([qkv_weight[0][:, :HD], qkv_weight[1][:, :HD]], 1)
    sel_b = qv_bias[:1, :HD]
    sel_w = jnp.where(me == 0, sel_w, lax.ppermute(sel_w, "tensor", [(0, 2)]))
    sel_b = jnp.where(me == 0, sel_b, lax.ppermute(sel_b, "tensor", [(0, 2)]))
    sel_w = jnp.where(odd == 0, sel_w, lax.ppermute(sel_w, "tensor", [(0, 1), (2, 3)]))
    sel_b = jnp.where(odd == 0, sel_b, lax.ppermute(sel_b, "tensor", [(0, 1), (2, 3)]))

    residual = hidden_in.astype(f32)
    normed_mine = layer_norm(residual, ln1_gain, ln1_shift).astype(bf16)
    normed = join(normed_mine, swap_core(normed_mine))

    qkv_far = swap_chip(qkv_weight)
    bias_far = swap_chip(qv_bias)
    out_far = swap_chip(out_weight)

    grad_out = out_grad.astype(f32) * live
    grad_branch = grad_out.astype(bf16)
    grad_core = swap_core(grad_branch)
    grad_far = swap_chip(grad_branch)
    grad_cross = lax.ppermute(grad_branch, "tensor", [(i, i ^ 3) for i in range(ranks)])

    def project(weights, bias):
        q = (mm(normed, weights[0]) + bias[0]).astype(bf16)
        k = mm(normed, weights[1]).astype(bf16)
        v = (mm(normed, weights[2]) + bias[1]).astype(bf16)
        return q, k, v

    sq = (mm(normed, sel_w[:, :HD]) + sel_b).astype(bf16)
    sk = mm(normed, sel_w[:, HD:]).astype(bf16)
    q1, k1, v1 = project(qkv_weight, qv_bias)
    o1, lse1, fence = attend_first(q1, k1, v1, sq, sk, length[None])
    q2, k2, v2 = project(qkv_far, bias_far)
    o2, lse2 = attend_next(q2, k2, v2, fence)

    vecs = jnp.stack([out_bias, ln2_gain, ln2_shift, down_bias, up_bias.astype(f32)])
    attn_rows, grad_middle, partial, branch_x, ffn_part, sums = feed_forward(
        o1, o2, out_weight, out_far, hidden_in,
        (grad_branch, grad_core, grad_far, grad_cross), vecs, up_weight, down_weight,
    )
    output = (live * (partial + swap_chip(branch_x).astype(f32))).astype(bf16)

    go2 = mm_nt(attn_rows, out_far).astype(bf16)
    go1 = mm_nt(attn_rows, out_weight).astype(bf16)
    dq2, dk2, dv2, dsq2, dsk2 = attend_back(q2, k2, v2, go2, lse2, fence, sq, sk)
    dq1, dk1, dv1, dsq1, dsk1 = attend_back(q1, k1, v1, go1, lse1, fence, sq, sk)

    def grad_block(dq, dk, dv, o):
        return jnp.concatenate(
            [mm_tn(normed, dq), mm_tn(normed, dk), mm_tn(normed, dv), mm_tn(attn_rows, o)], 1
        )

    n = lax.axis_size("dp")
    width = q1.shape[1]
    depth = normed.shape[1]
    chunk = -(-depth // (16 * n)) * 16
    far_block = swap_chip(grad_block(dq2, dk2, dv2, o2).astype(bf16))
    block = grad_block(dq1, dk1, dv1, o1) + far_block.astype(f32)
    dsel = jnp.concatenate([dsq1 + dsq2, dsk1 + dsk2], 1).astype(bf16)
    sel_grad = mm_tn(normed, dsel)
    fill = ((0, n * chunk - depth), (0, 0))
    block_b = jnp.pad(jnp.concatenate([block[:, : 2 * width], sel_grad], 1), fill).astype(bf16)
    block_a = jnp.pad(block[:, 2 * width :], fill).astype(bf16)

    ffn_grad = lax.psum(ffn_part, "dp").astype(f32)

    def bias_of(dq, dv):
        return jnp.stack([jnp.sum(dq, 0, dtype=f32), jnp.sum(dv, 0, dtype=f32)])

    slot = jnp.arange(ranks)[:, None, None]
    sel_bias = jnp.pad(jnp.sum(dsel[:, :HD], 0, dtype=f32)[None], ((0, 1), (0, width - HD)))
    qv_parts = (
        jnp.where(slot == me, bias_of(dq1, dv1)[None], 0.0)
        + jnp.where(slot == me ^ 2, bias_of(dq2, dv2)[None], 0.0)
        + jnp.where(slot == 0, sel_bias[None], 0.0)
    )
    up_parts = jnp.where(slot[:, 0] == me, sums[4:5], 0.0)
    none = jnp.zeros((depth,), f32)
    small = jnp.concatenate(
        [
            none,
            none,
            sums[2],
            sums[0],
            sums[1],
            sums[3],
            up_parts.reshape(-1),
            qv_parts.reshape(-1),
        ]
    )
    lines = small.shape[0] // 128
    piece = -(-lines // (8 * n)) * 8
    small = jnp.pad(small.reshape(lines, 128), ((0, n * piece - lines), (0, 0)))
    full_b, full_a, small, input_grad = finish(
        n, block_b, block_a, small, (dq1, dk1, dv1), (dq2, dk2, dv2), dsel,
        qkv_weight, qkv_far, sel_w, hidden_in, ln1_gain[None], grad_middle,
    )
    small = small[:lines].reshape(-1)
    vectors = small[: 6 * depth].reshape(6, depth)
    hidden = up_bias.shape[0]
    up_all = small[6 * depth : 6 * depth + ranks * hidden].reshape(ranks, hidden)
    qv_all = small[6 * depth + ranks * hidden :].reshape(ranks, 2, width)
    up_bias_grad = lax.dynamic_index_in_dim(up_all, me, 0, keepdims=False)
    qv_bias_grad = lax.dynamic_index_in_dim(qv_all, me, 0, keepdims=False)
    qkv_grad = jnp.stack(
        [full_b[:depth, :width], full_b[:depth, width:], full_a[:depth, :width]]
    ).astype(f32)
    out_weight_grad = full_a[:depth, width:].T.astype(f32)
    return (
        output,
        input_grad,
        vectors[0],
        vectors[1],
        qkv_grad,
        qv_bias_grad,
        out_weight_grad,
        vectors[2],
        vectors[3],
        vectors[4],
        ffn_grad[:depth],
        up_bias_grad,
        ffn_grad[depth:],
        vectors[5],
    )


def solution(mesh):
    return jax.shard_map(
        shards,
        mesh=mesh,
        in_specs=(
            P(("dp", "tensor"), None),
            P("dp"),
            P(),
            P(),
            P(None, None, "tensor"),
            P(None, "tensor"),
            P("tensor", None),
            P(),
            P(),
            P(),
            P(None, "tensor"),
            P("tensor"),
            P("tensor", None),
            P(),
            P(("dp", "tensor"), None),
        ),
        out_specs=(
            P(("dp", "tensor"), None),
            P(("dp", "tensor"), None),
            P(),
            P(),
            P(None, None, "tensor"),
            P(None, "tensor"),
            P("tensor", None),
            P(),
            P(),
            P(),
            P(None, "tensor"),
            P("tensor"),
            P("tensor", None),
            P(),
        ),
        check_vma=False,
    )
```

```python
import math

import jax
import jax.numpy as jnp
from jax import lax
from jax.experimental import pallas as pl
from jax.experimental.pallas import tpu as pltpu
from jax.sharding import PartitionSpec as P

HD = 64
BLK = 256
BIG = 1e30
sel_factor = 4.0
score_scale = 1.0 / math.sqrt(HD)
f32 = jnp.float32
bf16 = jnp.bfloat16


def mm(a, b):
    return lax.dot_general(a, b, (((1,), (0,)), ((), ())), preferred_element_type=f32)


def mm_nt(a, b):
    return lax.dot_general(a, b, (((1,), (1,)), ((), ())), preferred_element_type=f32)


def flip(a):
    return a.astype(f32).T.astype(bf16)


def split_mm(tri, x):
    hi = x.astype(bf16)
    lo = (x - hi.astype(f32)).astype(bf16)
    return mm(tri, hi) + mm(tri, lo)


def head_mask(h, width):
    return lax.broadcasted_iota(jnp.int32, (BLK, width), 1) // HD == h


def masked_rows(x, mask, scale):
    return jnp.where(mask, x.astype(f32) * scale, 0.0).astype(bf16)


def fwd_block(i, heads, first, q_ref, k_ref, v_ref, fence, o_ref, lse_ref):
    width = q_ref.shape[1]
    cols = (i + 1) * BLK
    keys = k_ref[:cols, :]
    vals = v_ref[:cols, :]
    fenced = fence[:, :cols]
    lane = lax.broadcasted_iota(jnp.int32, (BLK, 128), 1)
    lse_ref[...] = jnp.zeros_like(lse_ref)
    out_scr = first

    def head(h, _):
        mask = head_mask(h, width)
        s = mm_nt(masked_rows(q_ref[...], mask, score_scale), keys) - fenced
        top = jnp.max(s, -1, keepdims=True)
        e = jnp.exp(s - top)
        total = jnp.sum(e, -1, keepdims=True)
        p = (e * (1.0 / total)).astype(bf16)
        out = mm(p, vals)
        out_scr[...] = jnp.where(mask, out, out_scr[...])
        lse_ref[...] = jnp.where(lane == h, top + jnp.log(total), lse_ref[...])
        return 0

    lax.fori_loop(0, heads, head, 0)
    o_ref[...] = out_scr[...].astype(bf16)


def make_fence(i, seq_len, length, sq_ref, sk_ref, fence, carry):
    cols = (i + 1) * BLK
    s0 = mm_nt(sq_ref[...], sk_ref[:cols, :]) * score_scale
    row = i * BLK + lax.broadcasted_iota(jnp.int32, (BLK, cols), 0)
    col = lax.broadcasted_iota(jnp.int32, (BLK, cols), 1)
    picked = (col >= 1) & (col < row)
    sel = jnp.where(picked, jnp.maximum(s0, 0.0), 0.0) * (sel_factor / seq_len)
    r2 = lax.broadcasted_iota(jnp.int32, (BLK, BLK), 0)
    c2 = lax.broadcasted_iota(jnp.int32, (BLK, BLK), 1)
    tri = jnp.where(c2 < r2, 1.0, 0.0).astype(bf16)
    total = carry[0:1, :cols] + split_mm(tri, sel)
    carry[0:1, :cols] = total[BLK - 1 : BLK, :] + sel[BLK - 1 : BLK, :]
    fence[:, :cols] = jnp.where((col <= row) & (col < length), total, BIG)


def fwd_first_kernel(heads, len_ref, q_ref, k_ref, v_ref, sq_ref, sk_ref, o_ref, lse_ref, f_ref, out_scr, carry):
    r = pl.program_id(0)
    seq_len = k_ref.shape[0]

    @pl.when(r == 0)
    def _():
        carry[...] = jnp.zeros_like(carry)

    for i in range(seq_len // BLK):

        @pl.when(r == i)
        def _():
            make_fence(i, seq_len, len_ref[0], sq_ref, sk_ref, f_ref, carry)
            fwd_block(i, heads, out_scr, q_ref, k_ref, v_ref, f_ref, o_ref, lse_ref)


def fwd_next_kernel(heads, q_ref, k_ref, v_ref, f_ref, o_ref, lse_ref, out_scr):
    r = pl.program_id(0)
    for i in range(k_ref.shape[0] // BLK):

        @pl.when(r == i)
        def _():
            fwd_block(i, heads, out_scr, q_ref, k_ref, v_ref, f_ref, o_ref, lse_ref)


def row_spec(width, back=None):
    if back is None:
        return pl.BlockSpec((BLK, width), lambda r: (r, 0))
    return pl.BlockSpec((BLK, width), lambda r: (back - 1 - r, 0))


def full_spec(rows, width):
    return pl.BlockSpec((rows, width), lambda r: (0, 0))


def attend_first(q, k, v, sq, sk, length):
    n, width = q.shape
    heads = width // HD
    return pl.pallas_call(
        lambda *refs: fwd_first_kernel(heads, *refs),
        grid=(n // BLK,),
        in_specs=[
            pl.BlockSpec(memory_space=pltpu.SMEM),
            row_spec(width),
            full_spec(n, width),
            full_spec(n, width),
            row_spec(HD),
            full_spec(n, HD),
        ],
        out_specs=[row_spec(width), row_spec(128), row_spec(n)],
        out_shape=[
            jax.ShapeDtypeStruct((n, width), bf16),
            jax.ShapeDtypeStruct((n, 128), f32),
            jax.ShapeDtypeStruct((n, n), f32),
        ],
        scratch_shapes=[pltpu.VMEM((BLK, width), f32), pltpu.VMEM((8, n), f32)],
        name="attend_first",
        cost_estimate=pl.CostEstimate(flops=6 * n * n * 256, bytes_accessed=8 * n * n, transcendentals=0),
    )(length, q, k, v, sq, sk)


def attend_next(q, k, v, fence):
    n, width = q.shape
    heads = width // HD
    return pl.pallas_call(
        lambda *refs: fwd_next_kernel(heads, *refs),
        grid=(n // BLK,),
        in_specs=[row_spec(width), full_spec(n, width), full_spec(n, width), row_spec(n)],
        out_specs=[row_spec(width), row_spec(128)],
        out_shape=[
            jax.ShapeDtypeStruct((n, width), bf16),
            jax.ShapeDtypeStruct((n, 128), f32),
        ],
        scratch_shapes=[pltpu.VMEM((BLK, width), f32)],
        name="attend_next",
        cost_estimate=pl.CostEstimate(flops=6 * n * n * 256, bytes_accessed=8 * n * n, transcendentals=0),
    )(q, k, v, fence)


def bwd_block(i, heads, q_ref, k_ref, v_ref, do_ref, lse_ref, f_ref, sq_ref, sk_ref,
              dq_ref, dsq_ref, dq_scr, dkt, dvt, dskt, later, fsum, qt, dot_):
    width = q_ref.shape[1]
    seq_len = k_ref.shape[0]
    cols = (i + 1) * BLK
    keys = k_ref[:cols, :]
    vals = v_ref[:cols, :]
    lane = lax.broadcasted_iota(jnp.int32, (BLK, 128), 1)
    qt[...] = (q_ref[...].astype(f32) * score_scale).T.astype(bf16)
    dot_[...] = flip(do_ref[...])
    fsum[:, :cols] = jnp.zeros((BLK, cols), f32)

    def head(h, _):
        mask = head_mask(h, width)
        lse = jnp.sum(jnp.where(lane == h, lse_ref[...], 0.0), -1, keepdims=True)
        s = mm_nt(masked_rows(q_ref[...], mask, score_scale), keys)
        p = jnp.exp(s - f_ref[:, :cols] - lse)
        dp = mm_nt(masked_rows(do_ref[...], mask, 1.0), vals)
        delta = jnp.sum(p * dp, -1, keepdims=True)
        g = (p * (dp - delta)).astype(bf16)
        rows = pl.ds(pl.multiple_of(h * HD, HD), HD)
        dq_scr[...] = jnp.where(mask, mm(g, keys), dq_scr[...])
        dkt[rows, :cols] += mm(qt[rows, :], g)
        dvt[rows, :cols] += mm(dot_[rows, :], p.astype(bf16))
        fsum[:, :cols] += g.astype(f32)
        return 0

    lax.fori_loop(0, heads, head, 0)
    dq_ref[...] = (dq_scr[...] * score_scale).astype(bf16)
    grad = -fsum[:, :cols]
    r2 = lax.broadcasted_iota(jnp.int32, (BLK, BLK), 0)
    c2 = lax.broadcasted_iota(jnp.int32, (BLK, BLK), 1)
    tri = jnp.where(c2 > r2, 1.0, 0.0).astype(bf16)
    dsel = later[0:1, :cols] + split_mm(tri, grad)
    later[0:1, :cols] = dsel[0:1, :] + grad[0:1, :]
    s0 = mm_nt(sq_ref[...], sk_ref[:cols, :])
    row = i * BLK + lax.broadcasted_iota(jnp.int32, (BLK, cols), 0)
    col = lax.broadcasted_iota(jnp.int32, (BLK, cols), 1)
    keep = (col >= 1) & (col < row) & (s0 > 0)
    gsel = jnp.where(keep, dsel * (sel_factor / seq_len), 0.0).astype(bf16)
    dsq_ref[...] = mm(gsel, sk_ref[:cols, :]) * score_scale
    sqt = (sq_ref[...].astype(f32) * score_scale).T.astype(bf16)
    dskt[:, :cols] += mm(sqt, gsel)


epsilon = 1e-05


def layer_norm(source, scales, offset):
    centre = source - jnp.mean(source, -1, keepdims=True)
    spread = jnp.mean(centre * centre, -1, keepdims=True)
    return centre * lax.rsqrt(spread + epsilon) * scales + offset


def mm_tn(a, b):
    return lax.dot_general(a, b, (((0,), (0,)), ((), ())), preferred_element_type=f32)


def swap_core(x):
    n = lax.axis_size("tensor")
    return lax.ppermute(x, "tensor", [(i, i ^ 1) for i in range(n)])


def swap_chip(x):
    n = lax.axis_size("tensor")
    return lax.ppermute(x, "tensor", [(i, i ^ 2) for i in range(n)])

def send(src, dst, send_sem, recv_sem, **where):
    copy = pltpu.make_async_remote_copy(
        src_ref=src,
        dst_ref=dst,
        send_sem=send_sem,
        recv_sem=recv_sem,
        device_id=where,
        device_id_type=pl.DeviceIdType.MESH,
    )
    copy.start()
    return copy


def meet(devices):
    barrier = pltpu.get_barrier_semaphore()
    for where in devices:
        pl.semaphore_signal(barrier, inc=1, device_id=where, device_id_type=pl.DeviceIdType.MESH)
    pl.semaphore_wait(barrier, len(devices))


def norm_parts(x):
    centre = x - jnp.mean(x, -1, keepdims=True)
    r = lax.rsqrt(jnp.mean(centre * centre, -1, keepdims=True) + epsilon)
    return centre * r, r


def norm_back(e, xhat, r):
    return r * (e - jnp.mean(e, -1, keepdims=True) - xhat * jnp.mean(e * xhat, -1, keepdims=True))


def gelu_pair(u):
    k = math.sqrt(2.0 / math.pi)
    square = u * u
    t = jnp.tanh(k * u * (1.0 + 0.044715 * square))
    act = 0.5 * u * (1.0 + t)
    slope = 0.5 * (1.0 + t) + 0.5 * u * (1.0 - t * t) * (k * (1.0 + 3.0 * 0.044715 * square))
    return act, slope


def feed_kernel(
    o1, o2, wo1, wo2, hidden, g0, g1, g2, g3, vecs, up, down,
    rows_out, gmid, partial, branch_x, grads, sums,
    inner, gs, act, gpre, mid, attn_send, attn_recv,
    near_send, near_recv, far_send, far_recv, x_send, x_recv,
    bn_send, bn_recv, bf_send, bf_recv, gin,
    g_sem, a_s, a_r, i_s, i_r, x_s, x_r, f_s, f_r, n_s, n_r, c_s, c_r, r_s, r_r, b_s, b_r, o_s, o_r,
):
    me = lax.axis_index("tensor")
    odd = lax.rem(me, 2)
    core = me + 1 - 2 * odd
    far = lax.rem(me + 2, 4)
    rows = hidden.shape[0]
    pieces = rows // BLK
    loads = [pltpu.make_async_copy(g, gs.at[i], g_sem.at[i]) for i, g in enumerate((g0, g1, g2, g3))]
    for c in loads:
        c.start()
    meet([{"tensor": core}, {"tensor": far}])
    out_bias, gain, shift, down_bias, up_bias = (vecs[j : j + 1, :] for j in range(5))

    def attn(start):
        part = pl.ds(pl.multiple_of(start, BLK), BLK)
        return mm(o1[part, :], wo1[...]) + mm(o2[part, :], wo2[...])

    sends = []
    attn_copies = []
    for c in range(pieces):
        here = pl.ds(c * BLK, BLK)
        attn_send[here, :] = attn((1 - odd) * rows + c * BLK).astype(bf16)
        attn_copies.append(send(attn_send.at[here], attn_recv.at[here], a_s.at[c], a_r.at[c], tensor=core))
    inner_copies, far_copies = [], []
    for c in range(pieces):
        here = pl.ds(c * BLK, BLK)
        mine = attn(odd * rows + c * BLK)
        attn_copies[c].wait_recv()
        m = hidden[here, :].astype(f32) + (mine + attn_recv[here, :].astype(f32)) + out_bias
        mid[here, :] = m
        xhat, r = norm_parts(m)
        inner[0, here, :] = (xhat * gain + shift).astype(bf16)
        far_copies.append(send(inner.at[0, here], inner.at[2, here], x_s.at[c], x_r.at[c], tensor=far))
        inner_copies.append(send(inner.at[0, here], inner.at[1, here], i_s.at[c], i_r.at[c], tensor=core))
    sends += attn_copies + inner_copies + far_copies
    for c in loads:
        c.wait()
    sums[...] = jnp.zeros_like(sums)

    def feed(slot, start):
        part = pl.ds(pl.multiple_of(start, BLK), BLK)
        pre = mm(inner[slot, part, :], up[...]) + up_bias
        a, slope = gelu_pair(pre)
        act[slot, part, :] = a.astype(bf16)
        gp = (mm_nt(gs[slot, part, :], down[...]) * slope).astype(bf16)
        gpre[slot, part, :] = gp
        sums[4:5, :] += jnp.sum(gp.astype(f32), 0, keepdims=True)

    def near(c, _):
        feed(0, c * BLK)
        return 0

    lax.fori_loop(0, pieces, near, 0)
    for c in range(pieces):
        inner_copies[c].wait_recv()

    def near_other(c, _):
        part = pl.ds(pl.multiple_of(c * BLK, BLK), BLK)
        feed(1, c * BLK)
        near_send[part, :] = mm_nt(gpre[1, part, :], up[...]).astype(bf16)
        bn_send[part, :] = mm(act[1, part, :], down[...]).astype(bf16)
        return 0

    lax.fori_loop(0, pieces, near_other, 0)
    near_copy = send(near_send, near_recv, n_s.at[0], n_r.at[0], tensor=core)
    branch_copy = send(bn_send, bn_recv, n_s.at[1], n_r.at[1], tensor=core)

    def near_own(c, _):
        part = pl.ds(pl.multiple_of(c * BLK, BLK), BLK)
        gin[part, :] = mm_nt(gpre[0, part, :], up[...])
        partial[part, :] = mid[part, :] + mm(act[0, part, :], down[...]) + down_bias
        return 0

    lax.fori_loop(0, pieces, near_own, 0)

    passed, crossed, back = [], [], []
    for c in range(pieces):
        here = pl.ds(c * BLK, BLK)
        far_copies[c].wait_recv()
        passed.append(send(inner.at[2, here], inner.at[3, here], f_s.at[c], f_r.at[c], tensor=core))
        feed(2, c * BLK)
        passed[c].wait_recv()
        feed(3, c * BLK)
        far_send[here, :] = mm_nt(gpre[3, here, :], up[...]).astype(bf16)
        crossed.append(send(far_send.at[here], far_recv.at[here], c_s.at[c], c_r.at[c], tensor=core))
        g = mm_nt(gpre[2, here, :], up[...])
        crossed[c].wait_recv()
        x_send[here, :] = (g + far_recv[here, :].astype(f32)).astype(bf16)
        back.append(send(x_send.at[here], x_recv.at[here], r_s.at[c], r_r.at[c], tensor=far))
    for c in range(pieces):
        here = pl.ds(c * BLK, BLK)
        bf_send[here, :] = mm(act[3, here, :], down[...]).astype(bf16)
    far_branch = send(bf_send, bf_recv, b_s, b_r, tensor=core)
    depth = up.shape[0]

    def weights(j, _):
        part = pl.ds(pl.multiple_of(j * BLK, BLK), BLK)
        total = mm_tn(inner[0, :, part], gpre[0])
        other = mm_tn(act[0, :, part], gs[0])
        for s in range(1, 4):
            total = total + mm_tn(inner[s, :, part], gpre[s])
            other = other + mm_tn(act[s, :, part], gs[s])
        grads[part, :] = total.astype(bf16)
        grads[pl.ds(pl.multiple_of(depth + j * BLK, BLK), BLK), :] = other.astype(bf16)
        return 0

    for j in range(depth // BLK):
        weights(j, 0)
    far_branch.wait_recv()
    for c in range(pieces):
        here = pl.ds(c * BLK, BLK)
        b = mm(act[2, here, :], down[...])
        branch_x[here, :] = (b + bf_recv[here, :].astype(f32)).astype(bf16)
    near_copy.wait_recv()
    branch_copy.wait_recv()
    partial[...] += bn_recv[...].astype(f32)
    rows_copies = []
    for c in range(pieces):
        here = pl.ds(c * BLK, BLK)
        xhat, r = norm_parts(mid[here, :])
        back[c].wait_recv()
        g = gin[here, :] + near_recv[here, :].astype(f32) + x_recv[here, :].astype(f32)
        g_out = gs[0, here, :].astype(f32)
        gm = g_out + norm_back(g * gain, xhat, r)
        gmid[here, :] = gm
        there = pl.ds(pl.multiple_of(odd * rows + c * BLK, BLK), BLK)
        ga = gm.astype(bf16)
        rows_out[there, :] = ga
        rows_copies.append(
            send(rows_out.at[there], rows_out.at[there], o_s.at[c], o_r.at[c], tensor=core)
        )
        sums[0:1, :] += jnp.sum(g * xhat, 0, keepdims=True)
        sums[1:2, :] += jnp.sum(g, 0, keepdims=True)
        sums[2:3, :] += jnp.sum(ga.astype(f32), 0, keepdims=True)
        sums[3:4, :] += jnp.sum(g_out, 0, keepdims=True)
    for c in rows_copies:
        c.wait_recv()
    for c in sends + passed + crossed + back + rows_copies + [near_copy, branch_copy, far_branch]:
        c.wait_send()


def feed_forward(o1, o2, wo1, wo2, hidden, gs, vecs, up, down):
    rows, depth = hidden.shape
    width = up.shape[1]
    pieces = rows // BLK
    vmem = pl.BlockSpec(memory_space=pltpu.VMEM)
    anyw = pl.BlockSpec(memory_space=pl.ANY)
    dma = pltpu.SemaphoreType.DMA
    wide = pltpu.VMEM((rows, depth), bf16)
    each = [dma((pieces,))] * 2
    return pl.pallas_call(
        feed_kernel,
        in_specs=[vmem] * 5 + [anyw] * 4 + [vmem] * 3,
        out_specs=[vmem] * 6,
        out_shape=[
            jax.ShapeDtypeStruct((2 * rows, depth), bf16),
            jax.ShapeDtypeStruct((rows, depth), f32),
            jax.ShapeDtypeStruct((rows, depth), f32),
            jax.ShapeDtypeStruct((rows, depth), bf16),
            jax.ShapeDtypeStruct((depth + width, depth), bf16),
            jax.ShapeDtypeStruct((8, depth), f32),
        ],
        scratch_shapes=[
            pltpu.VMEM((4, rows, depth), bf16),
            pltpu.VMEM((4, rows, depth), bf16),
            pltpu.VMEM((4, rows, width), bf16),
            pltpu.VMEM((4, rows, width), bf16),
            pltpu.VMEM((rows, depth), f32),
            wide, wide, wide, wide, wide, wide, wide, wide, wide, wide, wide, wide,
            pltpu.VMEM((rows, depth), f32),
            dma((4,)),
            *each, *each, *each, *each,
            dma((2,)), dma((2,)),
            *each, *each,
            dma, dma,
            *each,
        ],
        compiler_params=pltpu.CompilerParams(
            collective_id=1, has_side_effects=True, vmem_limit_bytes=62 * 1024 * 1024
        ),
        name="feed_forward",
    )(o1, o2, wo1, wo2, hidden, *gs, vecs, up, down)

def back_kernel(
    n, chunk, piece, depth,
    q1, k1, v1, lse1, q2, k2, v2, lse2, fence, sq, sk, rows_in, o1, o2, wo1, wo2,
    normed, w1, w2, sel_w, hidden, gain, gmid, small_in, up_g, down_g,
    fu, fd, fb, fa, small_out, input_grad,
    go, dq1, dk1, dv1, dq2, dk2, dv2, dsq1, dsk1, dsq2, dsk2,
    dq_scr, dkt, dvt, dskt, later, fsum, qt, dot_,
    dsel, ng_send, ng_recv, far_s, far_r, faro_s, faro_r, gb, ga,
    yu, yd, yb, ya, ys, su, sd, sb, sa, ss, zu, zd, zb, za, zs,
    own_b, tb, ts, small, out_s,
    core_s, core_r, f_s, f_r, y_s, y_r, z_s, z_r, t_s, t_r, az_s, az_r, ay_s, ay_r,
):
    idx = lax.axis_index("dp")
    me = lax.axis_index("tensor")
    odd = lax.rem(me, 2)
    par = lax.rem(idx, 2)
    z = lax.div(idx, 2)
    m = n // 2
    rows = hidden.shape[0]
    seq_len = k1.shape[0]
    width = q1.shape[1]
    heads = width // HD
    ranks = 4
    core = me + 1 - 2 * odd
    far = lax.rem(me + 2, ranks)
    ydev = idx + 1 - 2 * par
    peers = [lax.rem(me + d, ranks) for d in range(1, ranks)]
    zdev = [lax.rem(z + d, m) for d in range(1, m)]
    meet(
        [{"tensor": p} for p in peers]
        + [{"dp": ydev}]
        + [{"dp": 2 * p + par} for p in zdev]
    )
    at = par * m + z
    source = (gb, ga, small, up_g, down_g)
    yrecv = (yb, ya, ys, yu, yd)
    ysum = (sb, sa, ss, su, sd)
    zrecv = (zb, za, zs, zu, zd)
    full = (fb, fa, out_s, fu, fd)
    size = (chunk, chunk, piece, chunk, chunk)
    done = []

    def block(start, k):
        return pl.ds(pl.multiple_of(start * size[k], size[k]), size[k])

    def y_start(k):
        half = m * size[k]
        give = pl.ds(pl.multiple_of((1 - par) * half, half), half)
        copy = send(source[k].at[give], yrecv[k], y_s.at[k], y_r.at[k], dp=ydev)
        done.append(copy)
        return copy

    def y_finish(k, copy):
        half = m * size[k]
        keep = pl.ds(pl.multiple_of(par * half, half), half)
        copy.wait_recv()
        total = source[k][keep, :].astype(f32) + yrecv[k][...].astype(f32)
        ysum[k][...] = total.astype(ysum[k].dtype)
        copies = [
            send(
                ysum[k].at[block(zdev[d], k)], zrecv[k].at[d], z_s.at[k, d], z_r.at[k, d],
                dp=2 * zdev[d] + par,
            )
            for d in range(m - 1)
        ]
        done.extend(copies)
        return copies

    def z_finish(k, copies):
        acc = ysum[k][block(z, k), :].astype(f32)
        for d in range(m - 1):
            copies[d].wait_recv()
            acc = acc + zrecv[k][d].astype(f32)
        return acc

    def spread(k):
        mine = full[k].at[block(at, k)]
        out = [
            send(mine, mine, az_s.at[k, d], az_r.at[k, d], dp=2 * zdev[d] + par)
            for d in range(m - 1)
        ]
        own = send(mine, mine, ay_s.at[k, 0], ay_r.at[k, 0], dp=ydev)
        done.extend(out + [own])
        return out, [own]

    def forward(k, out, ahead):
        for d in range(m - 1):
            out[d].wait_recv()
            came = full[k].at[block(par * m + lax.rem(z - (d + 1) + m, m), k)]
            copy = send(came, came, ay_s.at[k, d + 1], ay_r.at[k, d + 1], dp=ydev)
            ahead.append(copy)
            done.append(copy)

    cu = y_start(3)
    faro_s[...] = mm_tn(o2[...], rows_in[...]).astype(bf16)
    cfo = send(faro_s, faro_r, f_s.at[0], f_r.at[0], tensor=far)

    def attention(q, k, v, lse, wo, dq, dk, dv, dsq, dsk, hooks):
        for j in range(seq_len // BLK):
            here = pl.ds(j * BLK, BLK)
            go[here, :] = mm_nt(rows_in[here, :], wo[...]).astype(bf16)
        for r in (dkt, dvt, dskt, later):
            r[...] = jnp.zeros_like(r)
        for i in reversed(range(seq_len // BLK)):
            here = pl.ds(i * BLK, BLK)
            bwd_block(
                i, heads, q.at[here], k, v, go.at[here], lse.at[here], fence.at[here],
                sq.at[here], sk, dq.at[here], dsq.at[here],
                dq_scr, dkt, dvt, dskt, later, fsum, qt, dot_,
            )
            if i in hooks:
                hooks[i]()
        dk[...] = dkt[...].T.astype(bf16)
        dv[...] = dvt[...].T.astype(bf16)
        dsk[...] = dskt[...].T

    last = seq_len // BLK - 1
    keep = {}

    def start_down():
        keep["yd"] = y_start(4)

    attention(q2, k2, v2, lse2, wo2, dq2, dk2, dv2, dsq2, dsk2, {last: start_down})
    for j, d in enumerate((dq2, dk2, dv2)):
        far_s[:, j * width : (j + 1) * width] = mm_tn(normed[...], d[...]).astype(bf16)
    cfar = send(far_s, far_r, f_s.at[1], f_r.at[1], tensor=far)
    keep["zu"] = y_finish(3, cu)

    def down_z():
        keep["zd"] = y_finish(4, keep["yd"])

    def up_spread():
        fu[block(at, 3), :] = z_finish(3, keep["zu"]).astype(bf16)
        keep["au"] = spread(3)

    attention(q1, k1, v1, lse1, wo1, dq1, dk1, dv1, dsq1, dsk1, {last: down_z, last - 1: up_spread})
    dsel[:, :HD] = (dsq1[...] + dsq2[...]).astype(bf16)
    dsel[:, HD:] = (dsk1[...] + dsk2[...]).astype(bf16)

    def normed_grad(start):
        part = pl.ds(pl.multiple_of(start, rows), rows)
        total = mm_nt(dsel[part, :], sel_w[...])
        for grads, weights in (((dq1, dk1, dv1), w1), ((dq2, dk2, dv2), w2)):
            for j in range(3):
                total = total + mm_nt(grads[j][part, :], weights[j])
        return total

    ng_send[...] = normed_grad((1 - odd) * rows).astype(bf16)
    ccore = send(ng_send, ng_recv, core_s, core_r, tensor=core)
    gq = mm_tn(normed[...], dq1[...])
    gk = mm_tn(normed[...], dk1[...])
    gs = mm_tn(normed[...], dsel[...])
    cfar.wait_recv()
    if n * chunk > depth:
        gb[...] = jnp.zeros_like(gb)
        ga[...] = jnp.zeros_like(ga)
    real = pl.ds(0, depth)
    gb[real, :width] = (gq + far_r[:, :width].astype(f32)).astype(bf16)
    gb[real, width : 2 * width] = (gk + far_r[:, width : 2 * width].astype(f32)).astype(bf16)
    gb[real, 2 * width :] = gs.astype(bf16)
    cb = y_start(0)
    gv = mm_tn(normed[...], dv1[...])
    ga[real, :width] = (gv + far_r[:, 2 * width :].astype(f32)).astype(bf16)
    cfo.wait_recv()
    wide = mm_tn(o1[...], rows_in[...]) + faro_r[...].astype(f32)
    ga[real, width:] = wide.T.astype(bf16)
    ca = y_start(1)
    fd[block(at, 4), :] = z_finish(4, keep["zd"]).astype(bf16)
    ad = spread(4)
    forward(3, *keep["au"])

    grad = normed_grad(odd * rows)
    xhat, r = norm_parts(hidden[...].astype(f32))
    ccore.wait_recv()
    grad = grad + ng_recv[...].astype(f32)
    input_grad[...] = (gmid[...] + norm_back(grad * gain[...], xhat, r)).astype(bf16)
    small[...] = small_in[...]
    dgain = jnp.sum(grad * xhat, 0, keepdims=True)
    dshift = jnp.sum(grad, 0, keepdims=True)
    lines = depth // 128
    for j in range(lines):
        small[j : j + 1, :] = dgain[:, j * 128 : (j + 1) * 128]
        small[lines + j : lines + j + 1, :] = dshift[:, j * 128 : (j + 1) * 128]
    base = small_lines(depth, up_g.shape[1]) - 4 * ranks
    for owner, q, v in ((me, dq1, dv1), (far, dq2, dv2)):
        for j, d in enumerate((q, v)):
            total = jnp.sum(d[...].astype(f32), 0, keepdims=True)
            line = base + 4 * owner + 2 * j
            small[pl.ds(line, 1), :] = total[:, :128]
            small[pl.ds(line + 1, 1), : width - 128] = total[:, 128:]
    total = jnp.sum(dsel[...].astype(f32), 0, keepdims=True)
    lane = lax.broadcasted_iota(jnp.int32, total.shape, 1)
    small[base : base + 1, :] += jnp.where(lane < HD, total, 0.0)
    cs = y_start(2)

    czb = y_finish(0, cb)
    czs = y_finish(2, cs)
    cza = y_finish(1, ca)
    acc_b = z_finish(0, czb)
    own_b[...] = acc_b[:, : 2 * width]
    tb[me] = acc_b[:, 2 * width :].astype(bf16)
    ts[me] = z_finish(2, czs)
    ct = []
    for d in range(ranks - 1):
        ct.append(send(tb.at[me], tb.at[me], t_s.at[0, d], t_r.at[0, d], tensor=peers[d]))
        ct.append(send(ts.at[me], ts.at[me], t_s.at[1, d], t_r.at[1, d], tensor=peers[d]))
    done.extend(ct)
    fa[block(at, 1), :] = z_finish(1, cza).astype(bf16)
    aa = spread(1)
    for c in ct:
        c.wait_recv()
    sel = tb[0].astype(f32)
    vec = ts[0]
    for d in range(1, ranks):
        sel = sel + tb[d].astype(f32)
        vec = vec + ts[d]
    first = jnp.where(me == 0, 1.0, 0.0)
    lane = lax.broadcasted_iota(jnp.int32, sel.shape, 1)
    mine = block(at, 0)
    fb[mine, :128] = (own_b[:, :128] + jnp.where(lane < HD, sel, 0.0) * first).astype(bf16)
    fb[mine, 128:256] = (own_b[:, 128:256] + jnp.where(lane < HD, 0.0, sel) * first).astype(bf16)
    fb[mine, 256:] = own_b[:, 256:].astype(bf16)
    ab = spread(0)
    out_s[block(at, 2), :] = vec
    asm = spread(2)
    forward(4, *ad)
    forward(1, *aa)
    forward(0, *ab)
    forward(2, *asm)
    for _, ahead in (keep["au"], ad, aa, ab, asm):
        for c in ahead:
            c.wait_recv()
    small_out[...] = out_s[...]
    for c in done + [cfo, cfar, ccore]:
        c.wait_send()


def small_lines(depth, hidden):
    return (6 * depth + 4 * hidden) // 128 + 16


def go_back(n, set1, set2, fence, sq, sk, rows_in, o1, o2, wo1, wo2, normed, w1, w2, sel_w,
            hidden, gain, gmid, small, up_g, down_g):
    m = n // 2
    chunk = up_g.shape[0] // n
    piece = small.shape[0] // n
    rows, depth = hidden.shape
    seq_len, width = set1[0].shape
    half, shalf = m * chunk, m * piece
    ranks = 4
    wb, wa, wf = 2 * width + 128, 2 * width, up_g.shape[1]
    vmem = pl.BlockSpec(memory_space=pltpu.VMEM)
    dma = pltpu.SemaphoreType.DMA
    args = (*set1, *set2, fence, sq, sk, rows_in, o1, o2, wo1, wo2, normed, w1, w2, sel_w,
            hidden, gain, gmid, small, up_g, down_g)
    heads = pltpu.VMEM((seq_len, width), bf16)
    part = pltpu.VMEM((seq_len, HD), f32)
    return pl.pallas_call(
        lambda *refs: back_kernel(n, chunk, piece, depth, *refs),
        in_specs=[vmem] * len(args),
        out_specs=[vmem] * 6,
        out_shape=[
            jax.ShapeDtypeStruct((n * chunk, wf), bf16),
            jax.ShapeDtypeStruct((n * chunk, wf), bf16),
            jax.ShapeDtypeStruct((n * chunk, 2 * width), bf16),
            jax.ShapeDtypeStruct((n * chunk, wa), bf16),
            jax.ShapeDtypeStruct(small.shape, f32),
            jax.ShapeDtypeStruct((rows, depth), bf16),
        ],
        scratch_shapes=[
            heads, heads, heads, heads, heads, heads, heads, part, part, part, part,
            pltpu.VMEM((BLK, width), f32),
            pltpu.VMEM((width, seq_len), f32),
            pltpu.VMEM((width, seq_len), f32),
            pltpu.VMEM((HD, seq_len), f32),
            pltpu.VMEM((8, seq_len), f32),
            pltpu.VMEM((BLK, seq_len), f32),
            pltpu.VMEM((width, BLK), bf16),
            pltpu.VMEM((width, BLK), bf16),
            pltpu.VMEM((seq_len, 128), bf16),
            pltpu.VMEM((rows, depth), bf16),
            pltpu.VMEM((rows, depth), bf16),
            pltpu.VMEM((depth, 3 * width), bf16),
            pltpu.VMEM((depth, 3 * width), bf16),
            pltpu.VMEM((width, depth), bf16),
            pltpu.VMEM((width, depth), bf16),
            pltpu.VMEM((n * chunk, wb), bf16),
            pltpu.VMEM((n * chunk, wa), bf16),
            *[pltpu.VMEM((half, w), bf16) for w in (wf, wf, wb, wa)],
            pltpu.VMEM((shalf, 128), f32),
            *[pltpu.VMEM((half, w), bf16) for w in (wf, wf, wb, wa)],
            pltpu.VMEM((shalf, 128), f32),
            *[pltpu.VMEM((m - 1, chunk, w), bf16) for w in (wf, wf, wb, wa)],
            pltpu.VMEM((m - 1, piece, 128), f32),
            pltpu.VMEM((chunk, 2 * width), f32),
            pltpu.VMEM((ranks, chunk, 128), bf16),
            pltpu.VMEM((ranks, piece, 128), f32),
            pltpu.VMEM(small.shape, f32),
            pltpu.VMEM(small.shape, f32),
            dma, dma,
            dma((2,)), dma((2,)),
            dma((5,)), dma((5,)),
            dma((5, m - 1)), dma((5, m - 1)),
            dma((2, 3)), dma((2, 3)),
            dma((5, m - 1)), dma((5, m - 1)),
            dma((5, m)), dma((5, m)),
        ],
        compiler_params=pltpu.CompilerParams(
            collective_id=0, has_side_effects=True, vmem_limit_bytes=63 * 1024 * 1024
        ),
        name="go_back",
    )(*args)


def shards(
    hidden_in,
    lengths,
    ln1_gain,
    ln1_shift,
    qkv_weight,
    qv_bias,
    out_weight,
    out_bias,
    ln2_gain,
    ln2_shift,
    up_weight,
    up_bias,
    down_weight,
    down_bias,
    out_grad,
):
    rows = hidden_in.shape[0]
    ranks = lax.axis_size("tensor")
    me = lax.axis_index("tensor")
    odd = me % 2
    length = jnp.where(me < 2, lengths[0], lengths[1])
    live = (odd * rows + jnp.arange(rows) < length).astype(f32)[:, None]

    def join(mine, other):
        first = jnp.where(odd == 0, mine, other)
        second = jnp.where(odd == 0, other, mine)
        return jnp.concatenate([first, second], 0)

    sel_w = jnp.concatenate([qkv_weight[0][:, :HD], qkv_weight[1][:, :HD]], 1)
    sel_b = qv_bias[:1, :HD]
    sel_w = jnp.where(me == 0, sel_w, lax.ppermute(sel_w, "tensor", [(0, 2)]))
    sel_b = jnp.where(me == 0, sel_b, lax.ppermute(sel_b, "tensor", [(0, 2)]))
    sel_w = jnp.where(odd == 0, sel_w, lax.ppermute(sel_w, "tensor", [(0, 1), (2, 3)]))
    sel_b = jnp.where(odd == 0, sel_b, lax.ppermute(sel_b, "tensor", [(0, 1), (2, 3)]))

    residual = hidden_in.astype(f32)
    normed_mine = layer_norm(residual, ln1_gain, ln1_shift).astype(bf16)
    normed = join(normed_mine, swap_core(normed_mine))

    qkv_far = swap_chip(qkv_weight)
    bias_far = swap_chip(qv_bias)
    out_far = swap_chip(out_weight)

    grad_out = out_grad.astype(f32) * live
    grad_branch = grad_out.astype(bf16)
    grad_core = swap_core(grad_branch)
    grad_far = swap_chip(grad_branch)
    grad_cross = lax.ppermute(grad_branch, "tensor", [(i, i ^ 3) for i in range(ranks)])

    def project(weights, bias):
        q = (mm(normed, weights[0]) + bias[0]).astype(bf16)
        k = mm(normed, weights[1]).astype(bf16)
        v = (mm(normed, weights[2]) + bias[1]).astype(bf16)
        return q, k, v

    sq = (mm(normed, sel_w[:, :HD]) + sel_b).astype(bf16)
    sk = mm(normed, sel_w[:, HD:]).astype(bf16)
    q1, k1, v1 = project(qkv_weight, qv_bias)
    o1, lse1, fence = attend_first(q1, k1, v1, sq, sk, length[None])
    q2, k2, v2 = project(qkv_far, bias_far)
    o2, lse2 = attend_next(q2, k2, v2, fence)

    vecs = jnp.stack([out_bias, ln2_gain, ln2_shift, down_bias, up_bias.astype(f32)])
    attn_rows, grad_middle, partial, branch_x, ffn_part, sums = feed_forward(
        o1, o2, out_weight, out_far, hidden_in,
        (grad_branch, grad_core, grad_far, grad_cross), vecs, up_weight, down_weight,
    )
    output = (live * (partial + swap_chip(branch_x).astype(f32))).astype(bf16)

    n = lax.axis_size("dp")
    width = q1.shape[1]
    depth = normed.shape[1]
    hidden = up_bias.shape[0]
    chunk = -(-depth // (16 * n)) * 16
    fill = ((0, n * chunk - depth), (0, 0))
    up_part = jnp.pad(ffn_part[:depth], fill)
    down_part = jnp.pad(ffn_part[depth:], fill)
    slot = jnp.arange(ranks)[:, None]
    up_rows = jnp.where(slot == me, sums[4:5], 0.0)
    none = jnp.zeros((depth,), f32)
    small = jnp.concatenate([none, none, sums[2], sums[0], sums[1], sums[3], up_rows.reshape(-1)])
    small = small.reshape(-1, 128)
    piece = -(-small_lines(depth, hidden) // (8 * n)) * 8
    small = jnp.pad(small, ((0, n * piece - small.shape[0]), (0, 0)))
    full_u, full_d, full_b, full_a, small, input_grad = go_back(
        n, (q1, k1, v1, lse1), (q2, k2, v2, lse2), fence, sq, sk, attn_rows, o1, o2,
        out_weight, out_far, normed, qkv_weight, qkv_far, sel_w, hidden_in, ln1_gain[None],
        grad_middle, small, up_part, down_part,
    )
    vectors = small[: 6 * depth // 128].reshape(6, depth)
    lines = (6 * depth + ranks * hidden) // 128
    up_all = small[6 * depth // 128 : lines].reshape(ranks, hidden)
    qv_all = small[lines : lines + 4 * ranks].reshape(ranks, 2, 256)
    up_bias_grad = lax.dynamic_index_in_dim(up_all, me, 0, keepdims=False)
    qv_bias_grad = lax.dynamic_index_in_dim(qv_all, me, 0, keepdims=False)[:, :width]
    qkv_grad = jnp.stack(
        [full_b[:depth, :width], full_b[:depth, width:], full_a[:depth, :width]]
    ).astype(f32)
    out_weight_grad = full_a[:depth, width:].T.astype(f32)
    return (
        output,
        input_grad,
        vectors[0],
        vectors[1],
        qkv_grad,
        qv_bias_grad,
        out_weight_grad,
        vectors[2],
        vectors[3],
        vectors[4],
        full_u[:depth].astype(f32),
        up_bias_grad,
        full_d[:depth].astype(f32),
        vectors[5],
    )


def solution(mesh):
    return jax.shard_map(
        shards,
        mesh=mesh,
        in_specs=(
            P(("dp", "tensor"), None),
            P("dp"),
            P(),
            P(),
            P(None, None, "tensor"),
            P(None, "tensor"),
            P("tensor", None),
            P(),
            P(),
            P(),
            P(None, "tensor"),
            P("tensor"),
            P("tensor", None),
            P(),
            P(("dp", "tensor"), None),
        ),
        out_specs=(
            P(("dp", "tensor"), None),
            P(("dp", "tensor"), None),
            P(),
            P(),
            P(None, None, "tensor"),
            P(None, "tensor"),
            P("tensor", None),
            P(),
            P(),
            P(),
            P(None, "tensor"),
            P("tensor"),
            P("tensor", None),
            P(),
        ),
        check_vma=False,
    )
```

```python
import math

import jax
import jax.numpy as jnp
from jax import lax
from jax.experimental import pallas as pl
from jax.experimental.pallas import tpu as pltpu
from jax.sharding import PartitionSpec as P

HD = 64
BLK = 256
BIG = 1e30
sel_factor = 4.0
score_scale = 1.0 / math.sqrt(HD)
f32 = jnp.float32
bf16 = jnp.bfloat16


def mm(a, b):
    return lax.dot_general(a, b, (((1,), (0,)), ((), ())), preferred_element_type=f32)


def mm_nt(a, b):
    return lax.dot_general(a, b, (((1,), (1,)), ((), ())), preferred_element_type=f32)


def flip(a):
    return a.astype(f32).T.astype(bf16)


def split_mm(tri, x):
    hi = x.astype(bf16)
    lo = (x - hi.astype(f32)).astype(bf16)
    return mm(tri, hi) + mm(tri, lo)


def head_mask(h, width):
    return lax.broadcasted_iota(jnp.int32, (BLK, width), 1) // HD == h


def masked_rows(x, mask, scale):
    return jnp.where(mask, x.astype(f32) * scale, 0.0).astype(bf16)


def fwd_block(i, heads, first, q_ref, k_ref, v_ref, fence, o_ref, lse_ref):
    width = q_ref.shape[1]
    cols = (i + 1) * BLK
    keys = k_ref[:cols, :]
    vals = v_ref[:cols, :]
    fenced = fence[:, :cols]
    lane = lax.broadcasted_iota(jnp.int32, (BLK, 128), 1)
    lse_ref[...] = jnp.zeros_like(lse_ref)
    out_scr = first

    def head(h, _):
        mask = head_mask(h, width)
        s = mm_nt(masked_rows(q_ref[...], mask, score_scale), keys) - fenced
        top = jnp.max(s, -1, keepdims=True)
        e = jnp.exp(s - top)
        total = jnp.sum(e, -1, keepdims=True)
        p = (e * (1.0 / total)).astype(bf16)
        out = mm(p, vals)
        out_scr[...] = jnp.where(mask, out, out_scr[...])
        lse_ref[...] = jnp.where(lane == h, top + jnp.log(total), lse_ref[...])
        return 0

    lax.fori_loop(0, heads, head, 0, unroll=True)
    o_ref[...] = out_scr[...].astype(bf16)


def make_fence(i, seq_len, length, sq_ref, sk_ref, fence, carry):
    cols = (i + 1) * BLK
    s0 = mm_nt(sq_ref[...], sk_ref[:cols, :]) * score_scale
    row = i * BLK + lax.broadcasted_iota(jnp.int32, (BLK, cols), 0)
    col = lax.broadcasted_iota(jnp.int32, (BLK, cols), 1)
    picked = (col >= 1) & (col < row)
    sel = jnp.where(picked, jnp.maximum(s0, 0.0), 0.0) * (sel_factor / seq_len)
    r2 = lax.broadcasted_iota(jnp.int32, (BLK, BLK), 0)
    c2 = lax.broadcasted_iota(jnp.int32, (BLK, BLK), 1)
    tri = jnp.where(c2 < r2, 1.0, 0.0).astype(bf16)
    total = carry[0:1, :cols] + split_mm(tri, sel)
    carry[0:1, :cols] = total[BLK - 1 : BLK, :] + sel[BLK - 1 : BLK, :]
    fence[:, :cols] = jnp.where((col <= row) & (col < length), total, BIG)


def bwd_block(i, heads, q_ref, k_ref, v_ref, do_ref, lse_ref, f_ref, sq_ref, sk_ref,
              dq_ref, dsq_ref, dq_scr, dkt, dvt, dskt, later, fsum, qt, dot_):
    width = q_ref.shape[1]
    seq_len = k_ref.shape[0]
    cols = (i + 1) * BLK
    keys = k_ref[:cols, :]
    vals = v_ref[:cols, :]
    lane = lax.broadcasted_iota(jnp.int32, (BLK, 128), 1)
    qt[...] = (q_ref[...].astype(f32) * score_scale).T.astype(bf16)
    dot_[...] = flip(do_ref[...])
    fsum[:, :cols] = jnp.zeros((BLK, cols), f32)

    def head(h, _):
        mask = head_mask(h, width)
        lse = jnp.sum(jnp.where(lane == h, lse_ref[...], 0.0), -1, keepdims=True)
        s = mm_nt(masked_rows(q_ref[...], mask, score_scale), keys)
        p = jnp.exp(s - f_ref[:, :cols] - lse)
        dp = mm_nt(masked_rows(do_ref[...], mask, 1.0), vals)
        delta = jnp.sum(p * dp, -1, keepdims=True)
        g = (p * (dp - delta)).astype(bf16)
        rows = pl.ds(pl.multiple_of(h * HD, HD), HD)
        dq_scr[...] = jnp.where(mask, mm(g, keys), dq_scr[...])
        dkt[rows, :cols] += mm(qt[rows, :], g)
        dvt[rows, :cols] += mm(dot_[rows, :], p.astype(bf16))
        fsum[:, :cols] += g.astype(f32)
        return 0

    lax.fori_loop(0, heads, head, 0, unroll=True)
    dq_ref[...] = (dq_scr[...] * score_scale).astype(bf16)
    grad = -fsum[:, :cols]
    r2 = lax.broadcasted_iota(jnp.int32, (BLK, BLK), 0)
    c2 = lax.broadcasted_iota(jnp.int32, (BLK, BLK), 1)
    tri = jnp.where(c2 > r2, 1.0, 0.0).astype(bf16)
    dsel = later[0:1, :cols] + split_mm(tri, grad)
    later[0:1, :cols] = dsel[0:1, :] + grad[0:1, :]
    s0 = mm_nt(sq_ref[...], sk_ref[:cols, :])
    row = i * BLK + lax.broadcasted_iota(jnp.int32, (BLK, cols), 0)
    col = lax.broadcasted_iota(jnp.int32, (BLK, cols), 1)
    keep = (col >= 1) & (col < row) & (s0 > 0)
    gsel = jnp.where(keep, dsel * (sel_factor / seq_len), 0.0).astype(bf16)
    dsq_ref[...] = mm(gsel, sk_ref[:cols, :]) * score_scale
    sqt = (sq_ref[...].astype(f32) * score_scale).T.astype(bf16)
    dskt[:, :cols] += mm(sqt, gsel)


epsilon = 1e-05


def mm_tn(a, b):
    return lax.dot_general(a, b, (((0,), (0,)), ((), ())), preferred_element_type=f32)


def send(src, dst, send_sem, recv_sem, **where):
    copy = pltpu.make_async_remote_copy(
        src_ref=src,
        dst_ref=dst,
        send_sem=send_sem,
        recv_sem=recv_sem,
        device_id=where,
        device_id_type=pl.DeviceIdType.MESH,
    )
    copy.start()
    return copy


def meet(devices):
    barrier = pltpu.get_barrier_semaphore()
    for where in devices:
        pl.semaphore_signal(barrier, inc=1, device_id=where, device_id_type=pl.DeviceIdType.MESH)
    pl.semaphore_wait(barrier, len(devices))


def norm_parts(x):
    centre = x - jnp.mean(x, -1, keepdims=True)
    r = lax.rsqrt(jnp.mean(centre * centre, -1, keepdims=True) + epsilon)
    return centre * r, r


def norm_back(e, xhat, r):
    return r * (e - jnp.mean(e, -1, keepdims=True) - xhat * jnp.mean(e * xhat, -1, keepdims=True))


def gelu_pair(u):
    k = math.sqrt(2.0 / math.pi)
    square = u * u
    t = jnp.tanh(k * u * (1.0 + 0.044715 * square))
    act = 0.5 * u * (1.0 + t)
    slope = 0.5 * (1.0 + t) + 0.5 * u * (1.0 - t * t) * (k * (1.0 + 3.0 * 0.044715 * square))
    return act, slope


def feed_kernel(
    o1, o2, wo1, wo2, hidden, g0, g1, g2, g3, vecs, up, down,
    rows_out, gmid, partial, branch_x, up_g, down_g, sums,
    inner, gs, act, gpre, mid, attn_send, attn_recv,
    near_send, near_recv, far_send, far_recv, x_send, x_recv,
    bn_send, bn_recv, bf_send, bf_recv, gin,
    g_sem, a_s, a_r, i_s, i_r, x_s, x_r, f_s, f_r, n_s, n_r, c_s, c_r, r_s, r_r, b_s, b_r, o_s, o_r, l_s, l_r,
):
    me = lax.axis_index("tensor")
    odd = lax.rem(me, 2)
    core = me + 1 - 2 * odd
    far = lax.rem(me + 2, 4)
    rows = hidden.shape[0]
    pieces = rows // BLK
    early, late = pl.ds(0, BLK), pl.ds(BLK, rows - BLK)
    places = (gs.at[0], gs.at[1], gs.at[2, early], gs.at[3, early])
    loads = [
        pltpu.make_async_copy(g, p, g_sem.at[i])
        for i, (g, p) in enumerate(zip((g0, g1, g2, g3), places))
    ]
    for c in loads:
        c.start()
    meet([{"tensor": core}, {"tensor": far}])
    late_copy = send(g0.at[late], gs.at[2, late], l_s.at[0], l_r.at[0], tensor=far)
    out_bias, gain, shift, down_bias, up_bias = (vecs[j : j + 1, :] for j in range(5))

    def attn(start):
        part = pl.ds(pl.multiple_of(start, BLK), BLK)
        return mm(o1[part, :], wo1[...]) + mm(o2[part, :], wo2[...])

    sends = []
    attn_copies = []
    for c in range(pieces):
        here = pl.ds(c * BLK, BLK)
        attn_send[here, :] = attn((1 - odd) * rows + c * BLK).astype(bf16)
        attn_copies.append(send(attn_send.at[here], attn_recv.at[here], a_s.at[c], a_r.at[c], tensor=core))
    inner_copies, far_copies = [], []
    for c in range(pieces):
        here = pl.ds(c * BLK, BLK)
        mine = attn(odd * rows + c * BLK)
        attn_copies[c].wait_recv()
        m = hidden[here, :].astype(f32) + (mine + attn_recv[here, :].astype(f32)) + out_bias
        mid[here, :] = m
        xhat, r = norm_parts(m)
        inner[0, here, :] = (xhat * gain + shift).astype(bf16)
        far_copies.append(send(inner.at[0, here], inner.at[2, here], x_s.at[c], x_r.at[c], tensor=far))
        inner_copies.append(send(inner.at[0, here], inner.at[1, here], i_s.at[c], i_r.at[c], tensor=core))
    sends += attn_copies + inner_copies + far_copies
    for c in loads:
        c.wait()
    sums[...] = jnp.zeros_like(sums)

    def feed(slot, start):
        part = pl.ds(pl.multiple_of(start, BLK), BLK)
        pre = mm(inner[slot, part, :], up[...]) + up_bias
        a, slope = gelu_pair(pre)
        act[slot, part, :] = a.astype(bf16)
        gp = (mm_nt(gs[slot, part, :], down[...]) * slope).astype(bf16)
        gpre[slot, part, :] = gp
        sums[4:5, :] += jnp.sum(gp.astype(f32), 0, keepdims=True)

    def near(c, _):
        feed(0, c * BLK)
        return 0

    lax.fori_loop(0, pieces, near, 0)
    for c in range(pieces):
        inner_copies[c].wait_recv()

    def near_other(c, _):
        part = pl.ds(pl.multiple_of(c * BLK, BLK), BLK)
        feed(1, c * BLK)
        near_send[part, :] = mm_nt(gpre[1, part, :], up[...]).astype(bf16)
        bn_send[part, :] = mm(act[1, part, :], down[...]).astype(bf16)
        return 0

    lax.fori_loop(0, pieces, near_other, 0)
    near_copy = send(near_send, near_recv, n_s.at[0], n_r.at[0], tensor=core)
    branch_copy = send(bn_send, bn_recv, n_s.at[1], n_r.at[1], tensor=core)

    def near_own(c, _):
        part = pl.ds(pl.multiple_of(c * BLK, BLK), BLK)
        gin[part, :] = mm_nt(gpre[0, part, :], up[...])
        partial[part, :] = mid[part, :] + mm(act[0, part, :], down[...]) + down_bias
        return 0

    lax.fori_loop(0, pieces, near_own, 0)

    late_copy.wait_recv()
    late_pass = send(gs.at[2, late], gs.at[3, late], l_s.at[1], l_r.at[1], tensor=core)
    passed, crossed, back = [], [], []
    for c in range(pieces):
        here = pl.ds(c * BLK, BLK)
        far_copies[c].wait_recv()
        passed.append(send(inner.at[2, here], inner.at[3, here], f_s.at[c], f_r.at[c], tensor=core))
        feed(2, c * BLK)
        passed[c].wait_recv()
        if c == 1:
            late_pass.wait_recv()
        feed(3, c * BLK)
        far_send[here, :] = mm_nt(gpre[3, here, :], up[...]).astype(bf16)
        crossed.append(send(far_send.at[here], far_recv.at[here], c_s.at[c], c_r.at[c], tensor=core))
        g = mm_nt(gpre[2, here, :], up[...])
        crossed[c].wait_recv()
        x_send[here, :] = (g + far_recv[here, :].astype(f32)).astype(bf16)
        back.append(send(x_send.at[here], x_recv.at[here], r_s.at[c], r_r.at[c], tensor=far))
    for c in range(pieces):
        here = pl.ds(c * BLK, BLK)
        bf_send[here, :] = mm(act[3, here, :], down[...]).astype(bf16)
    far_branch = send(bf_send, bf_recv, b_s, b_r, tensor=core)
    depth = up.shape[0]
    if up_g.shape[0] > depth:
        up_g[depth:, :] = jnp.zeros((up_g.shape[0] - depth, up_g.shape[1]), bf16)
        down_g[depth:, :] = jnp.zeros((up_g.shape[0] - depth, up_g.shape[1]), bf16)

    def weights(j, _):
        part = pl.ds(pl.multiple_of(j * BLK, BLK), BLK)
        total = mm_tn(inner[0, :, part], gpre[0])
        other = mm_tn(act[0, :, part], gs[0])
        for s in range(1, 4):
            total = total + mm_tn(inner[s, :, part], gpre[s])
            other = other + mm_tn(act[s, :, part], gs[s])
        up_g[part, :] = total.astype(bf16)
        down_g[part, :] = other.astype(bf16)
        return 0

    for j in range(depth // BLK):
        weights(j, 0)
    far_branch.wait_recv()
    for c in range(pieces):
        here = pl.ds(c * BLK, BLK)
        b = mm(act[2, here, :], down[...])
        branch_x[here, :] = (b + bf_recv[here, :].astype(f32)).astype(bf16)
    near_copy.wait_recv()
    branch_copy.wait_recv()
    partial[...] += bn_recv[...].astype(f32)
    rows_copies = []
    for c in range(pieces):
        here = pl.ds(c * BLK, BLK)
        xhat, r = norm_parts(mid[here, :])
        back[c].wait_recv()
        g = gin[here, :] + near_recv[here, :].astype(f32) + x_recv[here, :].astype(f32)
        g_out = gs[0, here, :].astype(f32)
        gm = g_out + norm_back(g * gain, xhat, r)
        gmid[here, :] = gm
        there = pl.ds(pl.multiple_of(odd * rows + c * BLK, BLK), BLK)
        ga = gm.astype(bf16)
        rows_out[there, :] = ga
        rows_copies.append(
            send(rows_out.at[there], rows_out.at[there], o_s.at[c], o_r.at[c], tensor=core)
        )
        sums[0:1, :] += jnp.sum(g * xhat, 0, keepdims=True)
        sums[1:2, :] += jnp.sum(g, 0, keepdims=True)
        sums[2:3, :] += jnp.sum(ga.astype(f32), 0, keepdims=True)
        sums[3:4, :] += jnp.sum(g_out, 0, keepdims=True)
    for c in rows_copies:
        c.wait_recv()
    for c in sends + passed + crossed + back + rows_copies + [near_copy, branch_copy, far_branch, late_copy, late_pass]:
        c.wait_send()


def feed_forward(padded, o1, o2, wo1, wo2, hidden, gs, vecs, up, down):
    rows, depth = hidden.shape
    width = up.shape[1]
    pieces = rows // BLK
    vmem = pl.BlockSpec(memory_space=pltpu.VMEM)
    anyw = pl.BlockSpec(memory_space=pl.ANY)
    dma = pltpu.SemaphoreType.DMA
    wide = pltpu.VMEM((rows, depth), bf16)
    each = [dma((pieces,))] * 2
    return pl.pallas_call(
        feed_kernel,
        in_specs=[vmem] * 5 + [anyw] * 4 + [vmem] * 3,
        out_specs=[vmem] * 7,
        out_shape=[
            jax.ShapeDtypeStruct((2 * rows, depth), bf16),
            jax.ShapeDtypeStruct((rows, depth), f32),
            jax.ShapeDtypeStruct((rows, depth), f32),
            jax.ShapeDtypeStruct((rows, depth), bf16),
            jax.ShapeDtypeStruct((padded, width), bf16),
            jax.ShapeDtypeStruct((padded, width), bf16),
            jax.ShapeDtypeStruct((8, depth), f32),
        ],
        scratch_shapes=[
            pltpu.VMEM((4, rows, depth), bf16),
            pltpu.VMEM((4, rows, depth), bf16),
            pltpu.VMEM((4, rows, width), bf16),
            pltpu.VMEM((4, rows, width), bf16),
            pltpu.VMEM((rows, depth), f32),
            wide, wide, wide, wide, wide, wide, wide, wide, wide, wide, wide, wide,
            pltpu.VMEM((rows, depth), f32),
            dma((4,)),
            *each, *each, *each, *each,
            dma((2,)), dma((2,)),
            *each, *each,
            dma, dma,
            *each,
            dma((2,)), dma((2,)),
        ],
        compiler_params=pltpu.CompilerParams(
            collective_id=1, has_side_effects=True, vmem_limit_bytes=62 * 1024 * 1024
        ),
        name="feed_forward",
    )(o1, o2, wo1, wo2, hidden, *gs, vecs, up, down)

def back_kernel(
    n, chunk, piece, depth,
    q1, k1, v1, lse1, q2, k2, v2, lse2, fence, sq, sk, rows_in, o1, o2, wo1, wo2,
    normed, w1, w2, sel_w, hidden, gain, gmid, sums, partial, branch_x, length, up_g, down_g,
    fu, fd, fb, fa, small_out, input_grad, output,
    go, dq1, dk1, dv1, dq2, dk2, dv2, dsq1, dsk1, dsq2, dsk2,
    dq_scr, dkt, dvt, dskt, later, fsum, qt, dot_,
    dsel, ng_send, ng_recv, far_s, far_r, faro_s, faro_r, gb, ga,
    yu, yd, yb, ya, ys, su, sd, sb, sa, ss, zu, zd, zb, za, zs,
    own_b, tb, ts, small, out_s, bx_recv,
    core_s, core_r, f_s, f_r, y_s, y_r, z_s, z_r, t_s, t_r, az_s, az_r, ay_s, ay_r,
):
    idx = lax.axis_index("dp")
    me = lax.axis_index("tensor")
    odd = lax.rem(me, 2)
    par = lax.rem(idx, 2)
    z = lax.div(idx, 2)
    m = n // 2
    rows = hidden.shape[0]
    seq_len = k1.shape[0]
    width = q1.shape[1]
    heads = width // HD
    ranks = 4
    core = me + 1 - 2 * odd
    far = lax.rem(me + 2, ranks)
    ydev = idx + 1 - 2 * par
    peers = [lax.rem(me + d, ranks) for d in range(1, ranks)]
    zdev = [lax.rem(z + d, m) for d in range(1, m)]
    meet(
        [{"tensor": p} for p in peers]
        + [{"dp": ydev}]
        + [{"dp": 2 * p + par} for p in zdev]
    )
    at = par * m + z
    source = (gb, ga, small, up_g, down_g)
    yrecv = (yb, ya, ys, yu, yd)
    ysum = (sb, sa, ss, su, sd)
    zrecv = (zb, za, zs, zu, zd)
    full = (fb, fa, out_s, fu, fd)
    size = (chunk, chunk, piece, chunk, chunk)
    done = []

    def block(start, k):
        return pl.ds(pl.multiple_of(start * size[k], size[k]), size[k])

    def y_start(k):
        half = m * size[k]
        give = pl.ds(pl.multiple_of((1 - par) * half, half), half)
        copy = send(source[k].at[give], yrecv[k], y_s.at[k], y_r.at[k], dp=ydev)
        done.append(copy)
        return copy

    def y_finish(k, copy):
        half = m * size[k]
        keep = pl.ds(pl.multiple_of(par * half, half), half)
        copy.wait_recv()
        total = source[k][keep, :].astype(f32) + yrecv[k][...].astype(f32)
        ysum[k][...] = total.astype(ysum[k].dtype)
        copies = [
            send(
                ysum[k].at[block(zdev[d], k)], zrecv[k].at[d], z_s.at[k, d], z_r.at[k, d],
                dp=2 * zdev[d] + par,
            )
            for d in range(m - 1)
        ]
        done.extend(copies)
        return copies

    def z_finish(k, copies):
        acc = ysum[k][block(z, k), :].astype(f32)
        for d in range(m - 1):
            copies[d].wait_recv()
            acc = acc + zrecv[k][d].astype(f32)
        return acc

    def spread(k):
        mine = full[k].at[block(at, k)]
        out = [
            send(mine, mine, az_s.at[k, d], az_r.at[k, d], dp=2 * zdev[d] + par)
            for d in range(m - 1)
        ]
        own = send(mine, mine, ay_s.at[k, 0], ay_r.at[k, 0], dp=ydev)
        done.extend(out + [own])
        return out, [own]

    def forward(k, out, ahead):
        for d in range(m - 1):
            out[d].wait_recv()
            came = full[k].at[block(par * m + lax.rem(z - (d + 1) + m, m), k)]
            copy = send(came, came, ay_s.at[k, d + 1], ay_r.at[k, d + 1], dp=ydev)
            ahead.append(copy)
            done.append(copy)

    cu = y_start(3)
    faro_s[...] = mm_tn(o2[...], rows_in[...]).astype(bf16)
    cfo = send(faro_s, faro_r, f_s.at[0], f_r.at[0], tensor=far)
    cbx = send(branch_x, bx_recv, f_s.at[2], f_r.at[2], tensor=far)

    def attention(q, k, v, lse, wo, dq, dk, dv, dsq, dsk, hooks):
        for j in range(seq_len // BLK):
            here = pl.ds(j * BLK, BLK)
            go[here, :] = mm_nt(rows_in[here, :], wo[...]).astype(bf16)
        for r in (dkt, dvt, dskt, later):
            r[...] = jnp.zeros_like(r)
        for i in reversed(range(seq_len // BLK)):
            here = pl.ds(i * BLK, BLK)
            bwd_block(
                i, heads, q.at[here], k, v, go.at[here], lse.at[here], fence.at[here],
                sq.at[here], sk, dq.at[here], dsq.at[here],
                dq_scr, dkt, dvt, dskt, later, fsum, qt, dot_,
            )
            if i in hooks:
                hooks[i]()
        dk[...] = dkt[...].T.astype(bf16)
        dv[...] = dvt[...].T.astype(bf16)
        dsk[...] = dskt[...].T

    last = seq_len // BLK - 1
    keep = {}

    def start_down():
        keep["yd"] = y_start(4)

    attention(q2, k2, v2, lse2, wo2, dq2, dk2, dv2, dsq2, dsk2, {last: start_down})
    for j, d in enumerate((dq2, dk2, dv2)):
        far_s[:, j * width : (j + 1) * width] = mm_tn(normed[...], d[...]).astype(bf16)
    cfar = send(far_s, far_r, f_s.at[1], f_r.at[1], tensor=far)
    keep["zu"] = y_finish(3, cu)

    def down_z():
        keep["zd"] = y_finish(4, keep["yd"])

    def up_spread():
        fu[block(at, 3), :] = z_finish(3, keep["zu"]).astype(bf16)
        keep["au"] = spread(3)

    attention(q1, k1, v1, lse1, wo1, dq1, dk1, dv1, dsq1, dsk1, {last: down_z, last - 1: up_spread})
    dsel[:, :HD] = (dsq1[...] + dsq2[...]).astype(bf16)
    dsel[:, HD:] = (dsk1[...] + dsk2[...]).astype(bf16)

    def normed_grad(start):
        part = pl.ds(pl.multiple_of(start, rows), rows)
        total = mm_nt(dsel[part, :], sel_w[...])
        for grads, weights in (((dq1, dk1, dv1), w1), ((dq2, dk2, dv2), w2)):
            for j in range(3):
                total = total + mm_nt(grads[j][part, :], weights[j])
        return total

    ng_send[...] = normed_grad((1 - odd) * rows).astype(bf16)
    ccore = send(ng_send, ng_recv, core_s, core_r, tensor=core)
    gq = mm_tn(normed[...], dq1[...])
    gk = mm_tn(normed[...], dk1[...])
    gs = mm_tn(normed[...], dsel[...])
    cfar.wait_recv()
    if n * chunk > depth:
        gb[...] = jnp.zeros_like(gb)
        ga[...] = jnp.zeros_like(ga)
    real = pl.ds(0, depth)
    gb[real, :width] = (gq + far_r[:, :width].astype(f32)).astype(bf16)
    gb[real, width : 2 * width] = (gk + far_r[:, width : 2 * width].astype(f32)).astype(bf16)
    gb[real, 2 * width :] = gs.astype(bf16)
    cb = y_start(0)
    gv = mm_tn(normed[...], dv1[...])
    ga[real, :width] = (gv + far_r[:, 2 * width :].astype(f32)).astype(bf16)
    cfo.wait_recv()
    wide = mm_tn(o1[...], rows_in[...]) + faro_r[...].astype(f32)
    ga[real, width:] = wide.T.astype(bf16)
    ca = y_start(1)
    fd[block(at, 4), :] = z_finish(4, keep["zd"]).astype(bf16)
    ad = spread(4)
    forward(3, *keep["au"])

    grad = normed_grad(odd * rows)
    xhat, r = norm_parts(hidden[...].astype(f32))
    ccore.wait_recv()
    grad = grad + ng_recv[...].astype(f32)
    input_grad[...] = (gmid[...] + norm_back(grad * gain[...], xhat, r)).astype(bf16)
    small[...] = jnp.zeros_like(small)
    token = odd * rows + lax.broadcasted_iota(jnp.int32, (rows, 1), 0)
    live = jnp.where(token < length[0], 1.0, 0.0)
    cbx.wait_recv()
    output[...] = (live * (partial[...] + bx_recv[...].astype(f32))).astype(bf16)
    dgain = jnp.sum(grad * xhat, 0, keepdims=True)
    dshift = jnp.sum(grad, 0, keepdims=True)
    lines = depth // 128
    for j in range(lines):
        small[j : j + 1, :] = dgain[:, j * 128 : (j + 1) * 128]
        small[lines + j : lines + j + 1, :] = dshift[:, j * 128 : (j + 1) * 128]
    for slot, which in ((2, 2), (3, 0), (4, 1), (5, 3)):
        for j in range(lines):
            small[slot * lines + j : slot * lines + j + 1, :] = sums[
                which : which + 1, j * 128 : (j + 1) * 128
            ]
    wide_lines = up_g.shape[1] // 128
    for j in range(wide_lines):
        small[pl.ds(6 * lines + me * wide_lines + j, 1), :] = sums[4:5, j * 128 : (j + 1) * 128]
    base = small_lines(depth, up_g.shape[1]) - 4 * ranks
    for owner, q, v in ((me, dq1, dv1), (far, dq2, dv2)):
        for j, d in enumerate((q, v)):
            total = jnp.sum(d[...].astype(f32), 0, keepdims=True)
            line = base + 4 * owner + 2 * j
            small[pl.ds(line, 1), :] = total[:, :128]
            small[pl.ds(line + 1, 1), : width - 128] = total[:, 128:]
    total = jnp.sum(dsel[...].astype(f32), 0, keepdims=True)
    lane = lax.broadcasted_iota(jnp.int32, total.shape, 1)
    small[base : base + 1, :] += jnp.where(lane < HD, total, 0.0)
    cs = y_start(2)

    czb = y_finish(0, cb)
    czs = y_finish(2, cs)
    cza = y_finish(1, ca)
    acc_b = z_finish(0, czb)
    own_b[...] = acc_b[:, : 2 * width]
    tb[me] = acc_b[:, 2 * width :].astype(bf16)
    ts[me] = z_finish(2, czs)
    ct = []
    for d in range(ranks - 1):
        ct.append(send(tb.at[me], tb.at[me], t_s.at[0, d], t_r.at[0, d], tensor=peers[d]))
        ct.append(send(ts.at[me], ts.at[me], t_s.at[1, d], t_r.at[1, d], tensor=peers[d]))
    done.extend(ct)
    fa[block(at, 1), :] = z_finish(1, cza).astype(bf16)
    aa = spread(1)
    for c in ct:
        c.wait_recv()
    sel = tb[0].astype(f32)
    vec = ts[0]
    for d in range(1, ranks):
        sel = sel + tb[d].astype(f32)
        vec = vec + ts[d]
    first = jnp.where(me == 0, 1.0, 0.0)
    lane = lax.broadcasted_iota(jnp.int32, sel.shape, 1)
    mine = block(at, 0)
    fb[mine, :128] = (own_b[:, :128] + jnp.where(lane < HD, sel, 0.0) * first).astype(bf16)
    fb[mine, 128:256] = (own_b[:, 128:256] + jnp.where(lane < HD, 0.0, sel) * first).astype(bf16)
    fb[mine, 256:] = own_b[:, 256:].astype(bf16)
    ab = spread(0)
    out_s[block(at, 2), :] = vec
    asm = spread(2)
    forward(4, *ad)
    forward(1, *aa)
    forward(0, *ab)
    forward(2, *asm)
    for _, ahead in (keep["au"], ad, aa, ab, asm):
        for c in ahead:
            c.wait_recv()
    small_out[...] = out_s[...]
    for c in done + [cfo, cbx, cfar, ccore]:
        c.wait_send()

def front_kernel(
    length, hidden, out_grad, ln, qkv, qv_bias, wo,
    normed, q1, k1, v1, lse1, o1, q2, k2, v2, lse2, o2, fence, sq, sk, w2, wo2, selw,
    g0, gcore, gfar, gcross,
    out_scr, carry, sel_b, bias2,
    nm_s, nm_r, gc_s, gc_r, sl_s, sl_r, w_s, w_r, e_s, e_r, g_s, g_r,
):
    me = lax.axis_index("tensor")
    odd = lax.rem(me, 2)
    core = me + 1 - 2 * odd
    far = lax.rem(me + 2, 4)
    rows = hidden.shape[0]
    seq_len = 2 * rows
    width = qkv.shape[2]
    heads = width // HD

    def sel_copies(k, where):
        return [
            pltpu.make_async_remote_copy(
                src_ref=a, dst_ref=a, send_sem=sl_s.at[k, j], recv_sem=sl_r.at[j],
                device_id={"tensor": where}, device_id_type=pl.DeviceIdType.MESH,
            )
            for j, a in enumerate((selw, sel_b))
        ]

    @pl.when(me == 0)
    def _():
        selw[:, :HD] = qkv[0, :, :HD]
        selw[:, HD:] = qkv[1, :, :HD]
        sel_b[...] = qv_bias[...]

    meet([{"tensor": core}, {"tensor": far}])

    @pl.when(me == 0)
    def _():
        for c in sel_copies(0, far) + sel_copies(1, core):
            c.start()

    weight_copies = [
        send(qkv.at[j], w2.at[j], w_s.at[j], w_r.at[j], tensor=far) for j in range(3)
    ]
    extra = [
        send(qv_bias, bias2, e_s.at[0], e_r.at[0], tensor=far),
        send(wo, wo2, e_s.at[1], e_r.at[1], tensor=far),
    ]
    spot = pl.multiple_of(odd * rows, rows)
    norm_copies = []
    for c in range(rows // BLK):
        here = pl.ds(c * BLK, BLK)
        there = pl.ds(pl.multiple_of(spot + c * BLK, BLK), BLK)
        xhat, _ = norm_parts(hidden[here, :].astype(f32))
        normed[there, :] = (xhat * ln[0:1, :] + ln[1:2, :]).astype(bf16)
        norm_copies.append(
            send(normed.at[there], normed.at[there], nm_s.at[c], nm_r.at[c], tensor=core)
        )
    row = odd * rows + lax.broadcasted_iota(jnp.int32, (rows, 1), 0)
    live = jnp.where(row < length[0], 1.0, 0.0)
    g0[...] = (out_grad[...].astype(f32) * live).astype(bf16)
    gc = send(g0, gcore, gc_s, gc_r, tensor=core)
    early = pl.ds(0, BLK)
    gf = send(g0.at[early], gfar, g_s.at[0], g_r.at[0], tensor=far)

    def project(which, weight, bias, out):
        for j in range(seq_len // BLK):
            here = pl.ds(j * BLK, BLK)
            y = mm(normed[here, :], weight)
            if bias is not None:
                y = y + bias
            out[here, :] = y.astype(bf16)

    @pl.when(me == 2)
    def _():
        for c in sel_copies(0, far):
            c.wait_recv()
        for c in sel_copies(1, core):
            c.start()

    @pl.when(odd == 1)
    def _():
        for c in sel_copies(1, core):
            c.wait_recv()

    for c in norm_copies:
        c.wait_recv()
    project(0, qkv[0], qv_bias[0:1, :], q1)
    project(1, qkv[1], None, k1)
    project(2, qkv[2], qv_bias[1:2, :], v1)
    for j in range(seq_len // BLK):
        here = pl.ds(j * BLK, BLK)
        y = mm(normed[here, :], selw[...])
        sq[here, :] = (y[:, :HD] + sel_b[0:1, :HD]).astype(bf16)
        sk[here, :] = y[:, HD:].astype(bf16)
    carry[...] = jnp.zeros_like(carry)
    for i in range(seq_len // BLK):
        here = pl.ds(i * BLK, BLK)
        make_fence(i, seq_len, length[0], sq.at[here], sk, fence.at[here], carry)
        fwd_block(
            i, heads, out_scr, q1.at[here], k1, v1, fence.at[here], o1.at[here], lse1.at[here]
        )
    extra[0].wait_recv()
    for j, (out, bias) in enumerate(((q2, bias2[0:1, :]), (k2, None), (v2, bias2[1:2, :]))):
        weight_copies[j].wait_recv()
        project(j, w2[j], bias, out)
    for i in range(seq_len // BLK):
        here = pl.ds(i * BLK, BLK)
        fwd_block(
            i, heads, out_scr, q2.at[here], k2, v2, fence.at[here], o2.at[here], lse2.at[here]
        )
    gf.wait_recv()
    gx = send(gfar, gcross, g_s.at[1], g_r.at[1], tensor=core)
    gc.wait_recv()
    extra[1].wait_recv()
    gx.wait_recv()

    @pl.when(me == 0)
    def _():
        for c in sel_copies(0, far):
            c.wait_send()

    @pl.when(odd == 0)
    def _():
        for c in sel_copies(1, core):
            c.wait_send()

    for c in weight_copies + extra + norm_copies + [gc, gf, gx]:
        c.wait_send()


def front(length, hidden, out_grad, ln, qkv, qv_bias, wo):
    rows, depth = hidden.shape
    seq_len, width = 2 * rows, qkv.shape[2]
    pieces = rows // BLK
    vmem = pl.BlockSpec(memory_space=pltpu.VMEM)
    dma = pltpu.SemaphoreType.DMA
    heads = jax.ShapeDtypeStruct((seq_len, width), bf16)
    lse = jax.ShapeDtypeStruct((seq_len, 128), f32)
    sel = jax.ShapeDtypeStruct((seq_len, HD), bf16)
    wide = jax.ShapeDtypeStruct((rows, depth), bf16)
    early = jax.ShapeDtypeStruct((BLK, depth), bf16)
    return pl.pallas_call(
        front_kernel,
        in_specs=[pl.BlockSpec(memory_space=pltpu.SMEM)] + [vmem] * 6,
        out_specs=[vmem] * 21,
        out_shape=[
            jax.ShapeDtypeStruct((seq_len, depth), bf16),
            heads, heads, heads, lse, heads,
            heads, heads, heads, lse, heads,
            jax.ShapeDtypeStruct((seq_len, seq_len), f32),
            sel, sel,
            jax.ShapeDtypeStruct(qkv.shape, bf16),
            jax.ShapeDtypeStruct(wo.shape, bf16),
            jax.ShapeDtypeStruct((depth, 2 * HD), bf16),
            wide, wide, early, early,
        ],
        scratch_shapes=[
            pltpu.VMEM((BLK, width), f32),
            pltpu.VMEM((8, seq_len), f32),
            pltpu.VMEM((2, width), f32),
            pltpu.VMEM((2, width), f32),
            dma((pieces,)), dma((pieces,)),
            dma, dma,
            dma((2, 2)), dma((2,)),
            dma((3,)), dma((3,)),
            dma((2,)), dma((2,)),
            dma((2,)), dma((2,)),
        ],
        compiler_params=pltpu.CompilerParams(
            collective_id=2, has_side_effects=True, vmem_limit_bytes=60 * 1024 * 1024
        ),
        name="front",
    )(length, hidden, out_grad, ln, qkv, qv_bias, wo)


def small_lines(depth, hidden):
    return (6 * depth + 4 * hidden) // 128 + 16


def go_back(n, set1, set2, fence, sq, sk, rows_in, o1, o2, wo1, wo2, normed, w1, w2, sel_w,
            hidden, gain, gmid, sums, partial, branch_x, length, up_g, down_g):
    m = n // 2
    chunk = up_g.shape[0] // n
    rows, depth = hidden.shape
    piece = -(-small_lines(depth, up_g.shape[1]) // (8 * n)) * 8
    seq_len, width = set1[0].shape
    half, shalf = m * chunk, m * piece
    ranks = 4
    wb, wa, wf = 2 * width + 128, 2 * width, up_g.shape[1]
    vmem = pl.BlockSpec(memory_space=pltpu.VMEM)
    dma = pltpu.SemaphoreType.DMA
    args = (*set1, *set2, fence, sq, sk, rows_in, o1, o2, wo1, wo2, normed, w1, w2, sel_w,
            hidden, gain, gmid, sums, partial, branch_x, length, up_g, down_g)
    heads = pltpu.VMEM((seq_len, width), bf16)
    part = pltpu.VMEM((seq_len, HD), f32)
    return pl.pallas_call(
        lambda *refs: back_kernel(n, chunk, piece, depth, *refs),
        in_specs=[vmem] * (len(args) - 3)
        + [pl.BlockSpec(memory_space=pltpu.SMEM)]
        + [vmem] * 2,
        out_specs=[vmem] * 7,
        out_shape=[
            jax.ShapeDtypeStruct((n * chunk, wf), bf16),
            jax.ShapeDtypeStruct((n * chunk, wf), bf16),
            jax.ShapeDtypeStruct((n * chunk, 2 * width), bf16),
            jax.ShapeDtypeStruct((n * chunk, wa), bf16),
            jax.ShapeDtypeStruct((n * piece, 128), f32),
            jax.ShapeDtypeStruct((rows, depth), bf16),
            jax.ShapeDtypeStruct((rows, depth), bf16),
        ],
        scratch_shapes=[
            heads, heads, heads, heads, heads, heads, heads, part, part, part, part,
            pltpu.VMEM((BLK, width), f32),
            pltpu.VMEM((width, seq_len), f32),
            pltpu.VMEM((width, seq_len), f32),
            pltpu.VMEM((HD, seq_len), f32),
            pltpu.VMEM((8, seq_len), f32),
            pltpu.VMEM((BLK, seq_len), f32),
            pltpu.VMEM((width, BLK), bf16),
            pltpu.VMEM((width, BLK), bf16),
            pltpu.VMEM((seq_len, 128), bf16),
            pltpu.VMEM((rows, depth), bf16),
            pltpu.VMEM((rows, depth), bf16),
            pltpu.VMEM((depth, 3 * width), bf16),
            pltpu.VMEM((depth, 3 * width), bf16),
            pltpu.VMEM((width, depth), bf16),
            pltpu.VMEM((width, depth), bf16),
            pltpu.VMEM((n * chunk, wb), bf16),
            pltpu.VMEM((n * chunk, wa), bf16),
            *[pltpu.VMEM((half, w), bf16) for w in (wf, wf, wb, wa)],
            pltpu.VMEM((shalf, 128), f32),
            *[pltpu.VMEM((half, w), bf16) for w in (wf, wf, wb, wa)],
            pltpu.VMEM((shalf, 128), f32),
            *[pltpu.VMEM((m - 1, chunk, w), bf16) for w in (wf, wf, wb, wa)],
            pltpu.VMEM((m - 1, piece, 128), f32),
            pltpu.VMEM((chunk, 2 * width), f32),
            pltpu.VMEM((ranks, chunk, 128), bf16),
            pltpu.VMEM((ranks, piece, 128), f32),
            pltpu.VMEM((n * piece, 128), f32),
            pltpu.VMEM((n * piece, 128), f32),
            pltpu.VMEM((rows, depth), bf16),
            dma, dma,
            dma((3,)), dma((3,)),
            dma((5,)), dma((5,)),
            dma((5, m - 1)), dma((5, m - 1)),
            dma((2, 3)), dma((2, 3)),
            dma((5, m - 1)), dma((5, m - 1)),
            dma((5, m)), dma((5, m)),
        ],
        compiler_params=pltpu.CompilerParams(
            collective_id=0, has_side_effects=True, vmem_limit_bytes=63 * 1024 * 1024
        ),
        name="go_back",
    )(*args)


def shards(
    hidden_in,
    lengths,
    ln1_gain,
    ln1_shift,
    qkv_weight,
    qv_bias,
    out_weight,
    out_bias,
    ln2_gain,
    ln2_shift,
    up_weight,
    up_bias,
    down_weight,
    down_bias,
    out_grad,
):
    n = lax.axis_size("dp")
    ranks = lax.axis_size("tensor")
    me = lax.axis_index("tensor")
    depth = hidden_in.shape[1]
    width = qkv_weight.shape[2]
    hidden = up_bias.shape[0]
    padded = -(-depth // (16 * n)) * 16 * n
    length = jnp.where(me < 2, lengths[:1], lengths[1:])
    ln1 = jnp.stack([ln1_gain, ln1_shift])
    vecs = jnp.stack([out_bias, ln2_gain, ln2_shift, down_bias, up_bias.astype(f32)])
    (normed, q1, k1, v1, lse1, o1, q2, k2, v2, lse2, o2, fence, sq, sk, qkv_far, out_far, sel_w,
     *grad_rows) = front(length, hidden_in, out_grad, ln1, qkv_weight, qv_bias, out_weight)
    attn_rows, grad_middle, partial, branch_x, up_part, down_part, sums = feed_forward(
        padded, o1, o2, out_weight, out_far, hidden_in, grad_rows, vecs, up_weight, down_weight
    )
    full_u, full_d, full_b, full_a, small, input_grad, output = go_back(
        n, (q1, k1, v1, lse1), (q2, k2, v2, lse2), fence, sq, sk, attn_rows, o1, o2,
        out_weight, out_far, normed, qkv_weight, qkv_far, sel_w, hidden_in, ln1_gain[None],
        grad_middle, sums, partial, branch_x, length, up_part, down_part,
    )
    vectors = small[: 6 * depth // 128].reshape(6, depth)
    lines = (6 * depth + ranks * hidden) // 128
    up_all = small[6 * depth // 128 : lines].reshape(ranks, hidden)
    qv_all = small[lines : lines + 4 * ranks].reshape(ranks, 2, 256)
    up_bias_grad = lax.dynamic_index_in_dim(up_all, me, 0, keepdims=False)
    qv_bias_grad = lax.dynamic_index_in_dim(qv_all, me, 0, keepdims=False)[:, :width]
    qkv_grad = jnp.stack(
        [full_b[:depth, :width], full_b[:depth, width:], full_a[:depth, :width]]
    ).astype(f32)
    out_weight_grad = full_a[:depth, width:].T.astype(f32)
    return (
        output,
        input_grad,
        vectors[0],
        vectors[1],
        qkv_grad,
        qv_bias_grad,
        out_weight_grad,
        vectors[2],
        vectors[3],
        vectors[4],
        full_u[:depth].astype(f32),
        up_bias_grad,
        full_d[:depth].astype(f32),
        vectors[5],
    )


def solution(mesh):
    return jax.shard_map(
        shards,
        mesh=mesh,
        in_specs=(
            P(("dp", "tensor"), None),
            P("dp"),
            P(),
            P(),
            P(None, None, "tensor"),
            P(None, "tensor"),
            P("tensor", None),
            P(),
            P(),
            P(),
            P(None, "tensor"),
            P("tensor"),
            P("tensor", None),
            P(),
            P(("dp", "tensor"), None),
        ),
        out_specs=(
            P(("dp", "tensor"), None),
            P(("dp", "tensor"), None),
            P(),
            P(),
            P(None, None, "tensor"),
            P(None, "tensor"),
            P("tensor", None),
            P(),
            P(),
            P(),
            P(None, "tensor"),
            P("tensor"),
            P("tensor", None),
            P(),
        ),
        check_vma=False,
    )
```

```python
import math

import jax
import jax.numpy as jnp
from jax import lax
from jax.experimental import pallas as pl
from jax.experimental.pallas import tpu as pltpu
from jax.sharding import PartitionSpec as P

HD = 64
BLK = 256
BIG = 1e30
sel_factor = 4.0
score_scale = 1.0 / math.sqrt(HD)
f32 = jnp.float32
bf16 = jnp.bfloat16


def mm(a, b):
    return lax.dot_general(a, b, (((1,), (0,)), ((), ())), preferred_element_type=f32)


def mm_nt(a, b):
    return lax.dot_general(a, b, (((1,), (1,)), ((), ())), preferred_element_type=f32)


def flip(a):
    return a.astype(f32).T.astype(bf16)


def split_mm(tri, x):
    hi = x.astype(bf16)
    lo = (x - hi.astype(f32)).astype(bf16)
    return mm(tri, hi) + mm(tri, lo)


def head_mask(h, width):
    return lax.broadcasted_iota(jnp.int32, (BLK, width), 1) // HD == h


def masked_rows(x, mask, scale):
    return jnp.where(mask, x.astype(f32) * scale, 0.0).astype(bf16)


def fwd_block(i, heads, first, q_ref, k_ref, v_ref, fence, o_ref, lse_ref):
    width = q_ref.shape[1]
    cols = (i + 1) * BLK
    keys = k_ref[:cols, :]
    vals = v_ref[:cols, :]
    fenced = fence[:, :cols]
    lane = lax.broadcasted_iota(jnp.int32, (BLK, 128), 1)
    lse_ref[...] = jnp.zeros_like(lse_ref)
    out_scr = first

    def head(h, _):
        mask = head_mask(h, width)
        s = mm_nt(masked_rows(q_ref[...], mask, score_scale), keys) - fenced
        top = jnp.max(s, -1, keepdims=True)
        e = jnp.exp(s - top)
        total = jnp.sum(e, -1, keepdims=True)
        p = (e * (1.0 / total)).astype(bf16)
        out = mm(p, vals)
        out_scr[...] = jnp.where(mask, out, out_scr[...])
        lse_ref[...] = jnp.where(lane == h, top + jnp.log(total), lse_ref[...])
        return 0

    lax.fori_loop(0, heads, head, 0, unroll=True)
    o_ref[...] = out_scr[...].astype(bf16)


def make_fence(i, seq_len, length, sq_ref, sk_ref, fence, carry):
    cols = (i + 1) * BLK
    s0 = mm_nt(sq_ref[...], sk_ref[:cols, :]) * score_scale
    row = i * BLK + lax.broadcasted_iota(jnp.int32, (BLK, cols), 0)
    col = lax.broadcasted_iota(jnp.int32, (BLK, cols), 1)
    picked = (col >= 1) & (col < row)
    sel = jnp.where(picked, jnp.maximum(s0, 0.0), 0.0) * (sel_factor / seq_len)
    r2 = lax.broadcasted_iota(jnp.int32, (BLK, BLK), 0)
    c2 = lax.broadcasted_iota(jnp.int32, (BLK, BLK), 1)
    tri = jnp.where(c2 < r2, 1.0, 0.0).astype(bf16)
    total = carry[0:1, :cols] + split_mm(tri, sel)
    carry[0:1, :cols] = total[BLK - 1 : BLK, :] + sel[BLK - 1 : BLK, :]
    fence[:, :cols] = jnp.where((col <= row) & (col < length), total, BIG)


def bwd_block(i, heads, q_ref, k_ref, v_ref, do_ref, lse_ref, f_ref, sq_ref, sk_ref,
              dq_ref, dsq_ref, dq_scr, dkt, dvt, dskt, later, fsum, qt, dot_):
    width = q_ref.shape[1]
    seq_len = k_ref.shape[0]
    cols = (i + 1) * BLK
    keys = k_ref[:cols, :]
    vals = v_ref[:cols, :]
    lane = lax.broadcasted_iota(jnp.int32, (BLK, 128), 1)
    qt[...] = (q_ref[...].astype(f32) * score_scale).T.astype(bf16)
    dot_[...] = flip(do_ref[...])
    fsum[:, :cols] = jnp.zeros((BLK, cols), f32)

    def head(h, _):
        mask = head_mask(h, width)
        lse = jnp.sum(jnp.where(lane == h, lse_ref[...], 0.0), -1, keepdims=True)
        s = mm_nt(masked_rows(q_ref[...], mask, score_scale), keys)
        p = jnp.exp(s - f_ref[:, :cols] - lse)
        dp = mm_nt(masked_rows(do_ref[...], mask, 1.0), vals)
        delta = jnp.sum(p * dp, -1, keepdims=True)
        g = (p * (dp - delta)).astype(bf16)
        rows = pl.ds(pl.multiple_of(h * HD, HD), HD)
        dq_scr[...] = jnp.where(mask, mm(g, keys), dq_scr[...])
        dkt[rows, :cols] += mm(qt[rows, :], g)
        dvt[rows, :cols] += mm(dot_[rows, :], p.astype(bf16))
        fsum[:, :cols] += g.astype(f32)
        return 0

    lax.fori_loop(0, heads, head, 0, unroll=True)
    dq_ref[...] = (dq_scr[...] * score_scale).astype(bf16)
    grad = -fsum[:, :cols]
    r2 = lax.broadcasted_iota(jnp.int32, (BLK, BLK), 0)
    c2 = lax.broadcasted_iota(jnp.int32, (BLK, BLK), 1)
    tri = jnp.where(c2 > r2, 1.0, 0.0).astype(bf16)
    dsel = later[0:1, :cols] + split_mm(tri, grad)
    later[0:1, :cols] = dsel[0:1, :] + grad[0:1, :]
    s0 = mm_nt(sq_ref[...], sk_ref[:cols, :])
    row = i * BLK + lax.broadcasted_iota(jnp.int32, (BLK, cols), 0)
    col = lax.broadcasted_iota(jnp.int32, (BLK, cols), 1)
    keep = (col >= 1) & (col < row) & (s0 > 0)
    gsel = jnp.where(keep, dsel * (sel_factor / seq_len), 0.0).astype(bf16)
    dsq_ref[...] = mm(gsel, sk_ref[:cols, :]) * score_scale
    sqt = (sq_ref[...].astype(f32) * score_scale).T.astype(bf16)
    dskt[:, :cols] += mm(sqt, gsel)


epsilon = 1e-05


def mm_tn(a, b):
    return lax.dot_general(a, b, (((0,), (0,)), ((), ())), preferred_element_type=f32)


def send(src, dst, send_sem, recv_sem, **where):
    copy = pltpu.make_async_remote_copy(
        src_ref=src,
        dst_ref=dst,
        send_sem=send_sem,
        recv_sem=recv_sem,
        device_id=where,
        device_id_type=pl.DeviceIdType.MESH,
    )
    copy.start()
    return copy


def meet(devices):
    barrier = pltpu.get_barrier_semaphore()
    for where in devices:
        pl.semaphore_signal(barrier, inc=1, device_id=where, device_id_type=pl.DeviceIdType.MESH)
    pl.semaphore_wait(barrier, len(devices))


def norm_parts(x):
    centre = x - jnp.mean(x, -1, keepdims=True)
    r = lax.rsqrt(jnp.mean(centre * centre, -1, keepdims=True) + epsilon)
    return centre * r, r


def norm_back(e, xhat, r):
    return r * (e - jnp.mean(e, -1, keepdims=True) - xhat * jnp.mean(e * xhat, -1, keepdims=True))


def gelu_pair(u):
    k = math.sqrt(2.0 / math.pi)
    square = u * u
    t = jnp.tanh(k * u * (1.0 + 0.044715 * square))
    act = 0.5 * u * (1.0 + t)
    slope = 0.5 * (1.0 + t) + 0.5 * u * (1.0 - t * t) * (k * (1.0 + 3.0 * 0.044715 * square))
    return act, slope


def feed_kernel(
    o1, o2, wo1, wo2, hidden, g0, g1, g2, g3, vecs, up, down,
    rows_out, gmid, partial, branch_x, up_g, down_g, sums,
    inner, gs, act, gpre, mid, attn_send, attn_recv,
    near_send, near_recv, far_send, far_recv, x_send, x_recv,
    bn_send, bn_recv, bf_send, bf_recv, gin,
    g_sem, a_s, a_r, i_s, i_r, x_s, x_r, f_s, f_r, n_s, n_r, c_s, c_r, r_s, r_r, b_s, b_r, o_s, o_r,
):
    me = lax.axis_index("tensor")
    odd = lax.rem(me, 2)
    core = me + 1 - 2 * odd
    far = lax.rem(me + 2, 4)
    rows = hidden.shape[0]
    pieces = rows // BLK
    loads = [pltpu.make_async_copy(g, gs.at[i], g_sem.at[i]) for i, g in enumerate((g0, g1, g2, g3))]
    for c in loads:
        c.start()
    meet([{"tensor": core}, {"tensor": far}])
    out_bias, gain, shift, down_bias, up_bias = (vecs[j : j + 1, :] for j in range(5))

    def attn(start):
        part = pl.ds(pl.multiple_of(start, BLK), BLK)
        return mm(o1[part, :], wo1[...]) + mm(o2[part, :], wo2[...])

    sends = []
    attn_copies = []
    for c in range(pieces):
        here = pl.ds(c * BLK, BLK)
        attn_send[here, :] = attn((1 - odd) * rows + c * BLK).astype(bf16)
        attn_copies.append(send(attn_send.at[here], attn_recv.at[here], a_s.at[c], a_r.at[c], tensor=core))
    inner_copies, far_copies = [], []
    for c in range(pieces):
        here = pl.ds(c * BLK, BLK)
        mine = attn(odd * rows + c * BLK)
        attn_copies[c].wait_recv()
        m = hidden[here, :].astype(f32) + (mine + attn_recv[here, :].astype(f32)) + out_bias
        mid[here, :] = m
        xhat, r = norm_parts(m)
        inner[0, here, :] = (xhat * gain + shift).astype(bf16)
        far_copies.append(send(inner.at[0, here], inner.at[2, here], x_s.at[c], x_r.at[c], tensor=far))
        inner_copies.append(send(inner.at[0, here], inner.at[1, here], i_s.at[c], i_r.at[c], tensor=core))
    sends += attn_copies + inner_copies + far_copies
    for c in loads:
        c.wait()
    sums[...] = jnp.zeros_like(sums)

    def feed(slot, start):
        part = pl.ds(pl.multiple_of(start, BLK), BLK)
        pre = mm(inner[slot, part, :], up[...]) + up_bias
        a, slope = gelu_pair(pre)
        act[slot, part, :] = a.astype(bf16)
        gp = (mm_nt(gs[slot, part, :], down[...]) * slope).astype(bf16)
        gpre[slot, part, :] = gp
        sums[4:5, :] += jnp.sum(gp.astype(f32), 0, keepdims=True)

    def near(c, _):
        feed(0, c * BLK)
        return 0

    lax.fori_loop(0, pieces, near, 0)
    for c in range(pieces):
        inner_copies[c].wait_recv()

    def near_other(c, _):
        part = pl.ds(pl.multiple_of(c * BLK, BLK), BLK)
        feed(1, c * BLK)
        near_send[part, :] = mm_nt(gpre[1, part, :], up[...]).astype(bf16)
        bn_send[part, :] = mm(act[1, part, :], down[...]).astype(bf16)
        return 0

    lax.fori_loop(0, pieces, near_other, 0)
    near_copy = send(near_send, near_recv, n_s.at[0], n_r.at[0], tensor=core)
    branch_copy = send(bn_send, bn_recv, n_s.at[1], n_r.at[1], tensor=core)

    def near_own(c, _):
        part = pl.ds(pl.multiple_of(c * BLK, BLK), BLK)
        gin[part, :] = mm_nt(gpre[0, part, :], up[...])
        partial[part, :] = mid[part, :] + mm(act[0, part, :], down[...]) + down_bias
        return 0

    lax.fori_loop(0, pieces, near_own, 0)

    passed, crossed, back = [], [], []
    for c in range(pieces):
        here = pl.ds(c * BLK, BLK)
        far_copies[c].wait_recv()
        passed.append(send(inner.at[2, here], inner.at[3, here], f_s.at[c], f_r.at[c], tensor=core))
        feed(2, c * BLK)
        passed[c].wait_recv()
        feed(3, c * BLK)
        far_send[here, :] = mm_nt(gpre[3, here, :], up[...]).astype(bf16)
        crossed.append(send(far_send.at[here], far_recv.at[here], c_s.at[c], c_r.at[c], tensor=core))
        g = mm_nt(gpre[2, here, :], up[...])
        crossed[c].wait_recv()
        x_send[here, :] = (g + far_recv[here, :].astype(f32)).astype(bf16)
        back.append(send(x_send.at[here], x_recv.at[here], r_s.at[c], r_r.at[c], tensor=far))
    for c in range(pieces):
        here = pl.ds(c * BLK, BLK)
        bf_send[here, :] = mm(act[3, here, :], down[...]).astype(bf16)
    far_branch = send(bf_send, bf_recv, b_s, b_r, tensor=core)
    depth = up.shape[0]
    if up_g.shape[0] > depth:
        up_g[depth:, :] = jnp.zeros((up_g.shape[0] - depth, up_g.shape[1]), bf16)
        down_g[depth:, :] = jnp.zeros((up_g.shape[0] - depth, up_g.shape[1]), bf16)

    def weights(j, _):
        part = pl.ds(pl.multiple_of(j * BLK, BLK), BLK)
        total = mm_tn(inner[0, :, part], gpre[0])
        other = mm_tn(act[0, :, part], gs[0])
        for s in range(1, 4):
            total = total + mm_tn(inner[s, :, part], gpre[s])
            other = other + mm_tn(act[s, :, part], gs[s])
        up_g[part, :] = total.astype(bf16)
        down_g[part, :] = other.astype(bf16)
        return 0

    for j in range(depth // BLK):
        weights(j, 0)
    far_branch.wait_recv()
    for c in range(pieces):
        here = pl.ds(c * BLK, BLK)
        b = mm(act[2, here, :], down[...])
        branch_x[here, :] = (b + bf_recv[here, :].astype(f32)).astype(bf16)
    near_copy.wait_recv()
    branch_copy.wait_recv()
    partial[...] += bn_recv[...].astype(f32)
    rows_copies = []
    for c in range(pieces):
        here = pl.ds(c * BLK, BLK)
        xhat, r = norm_parts(mid[here, :])
        back[c].wait_recv()
        g = gin[here, :] + near_recv[here, :].astype(f32) + x_recv[here, :].astype(f32)
        g_out = gs[0, here, :].astype(f32)
        gm = g_out + norm_back(g * gain, xhat, r)
        gmid[here, :] = gm
        there = pl.ds(pl.multiple_of(odd * rows + c * BLK, BLK), BLK)
        ga = gm.astype(bf16)
        rows_out[there, :] = ga
        rows_copies.append(
            send(rows_out.at[there], rows_out.at[there], o_s.at[c], o_r.at[c], tensor=core)
        )
        sums[0:1, :] += jnp.sum(g * xhat, 0, keepdims=True)
        sums[1:2, :] += jnp.sum(g, 0, keepdims=True)
        sums[2:3, :] += jnp.sum(ga.astype(f32), 0, keepdims=True)
        sums[3:4, :] += jnp.sum(g_out, 0, keepdims=True)
    for c in rows_copies:
        c.wait_recv()
    for c in sends + passed + crossed + back + rows_copies + [near_copy, branch_copy, far_branch]:
        c.wait_send()


def feed_forward(padded, o1, o2, wo1, wo2, hidden, gs, vecs, up, down):
    rows, depth = hidden.shape
    width = up.shape[1]
    pieces = rows // BLK
    vmem = pl.BlockSpec(memory_space=pltpu.VMEM)
    anyw = pl.BlockSpec(memory_space=pl.ANY)
    dma = pltpu.SemaphoreType.DMA
    wide = pltpu.VMEM((rows, depth), bf16)
    each = [dma((pieces,))] * 2
    return pl.pallas_call(
        feed_kernel,
        in_specs=[vmem] * 5 + [anyw] * 4 + [vmem] * 3,
        out_specs=[vmem] * 7,
        out_shape=[
            jax.ShapeDtypeStruct((2 * rows, depth), bf16),
            jax.ShapeDtypeStruct((rows, depth), f32),
            jax.ShapeDtypeStruct((rows, depth), f32),
            jax.ShapeDtypeStruct((rows, depth), bf16),
            jax.ShapeDtypeStruct((padded, width), bf16),
            jax.ShapeDtypeStruct((padded, width), bf16),
            jax.ShapeDtypeStruct((8, depth), f32),
        ],
        scratch_shapes=[
            pltpu.VMEM((4, rows, depth), bf16),
            pltpu.VMEM((4, rows, depth), bf16),
            pltpu.VMEM((4, rows, width), bf16),
            pltpu.VMEM((4, rows, width), bf16),
            pltpu.VMEM((rows, depth), f32),
            wide, wide, wide, wide, wide, wide, wide, wide, wide, wide, wide, wide,
            pltpu.VMEM((rows, depth), f32),
            dma((4,)),
            *each, *each, *each, *each,
            dma((2,)), dma((2,)),
            *each, *each,
            dma, dma,
            *each,
        ],
        compiler_params=pltpu.CompilerParams(
            collective_id=1, has_side_effects=True, vmem_limit_bytes=62 * 1024 * 1024
        ),
        name="feed_forward",
    )(o1, o2, wo1, wo2, hidden, *gs, vecs, up, down)

def back_kernel(
    n, chunk, piece, depth,
    q1, k1, v1, lse1, q2, k2, v2, lse2, fence, sq, sk, rows_in, o1, o2, wo1, wo2,
    normed, w1, w2, sel_w, hidden, vecs, gmid, sums, partial, branch_x, lengths, up_g, down_g,
    fu, fd, fb, fa, small_out, input_grad, output,
    go, dq1, dk1, dv1, dq2, dk2, dv2, dsq1, dsk1, dsq2, dsk2,
    dq_scr, dkt, dvt, dskt, later, fsum, qt, dot_,
    dsel, ng_send, ng_recv, far_s, far_r, faro_s, faro_r, gb, ga,
    yu, yd, yb, ya, ys, su, sd, sb, sa, ss, zu, zd, zb, za, zs,
    ts, small, out_s, bx_recv, sel_mine, sel_core, sel_far,
    core_s, core_r, f_s, f_r, sl_s, sl_r, y_s, y_r, z_s, z_r, t_s, t_r, az_s, az_r, ay_s, ay_r,
):
    idx = lax.axis_index("dp")
    me = lax.axis_index("tensor")
    odd = lax.rem(me, 2)
    par = lax.rem(idx, 2)
    z = lax.div(idx, 2)
    m = n // 2
    rows = hidden.shape[0]
    seq_len = k1.shape[0]
    width = q1.shape[1]
    heads = width // HD
    ranks = 4
    core = me + 1 - 2 * odd
    far = lax.rem(me + 2, ranks)
    ydev = idx + 1 - 2 * par
    peers = [lax.rem(me + d, ranks) for d in range(1, ranks)]
    zdev = [lax.rem(z + d, m) for d in range(1, m)]
    meet(
        [{"tensor": p} for p in peers]
        + [{"dp": ydev}]
        + [{"dp": 2 * p + par} for p in zdev]
    )
    at = par * m + z
    length = jnp.where(me < 2, lengths[0], lengths[1])
    source = (gb, ga, small, up_g, down_g)
    yrecv = (yb, ya, ys, yu, yd)
    ysum = (sb, sa, ss, su, sd)
    zrecv = (zb, za, zs, zu, zd)
    full = (fb, fa, out_s, fu, fd)
    size = (gb.shape[0] // n, ga.shape[0] // n, piece, chunk, chunk)
    done = []

    def block(start, k):
        return pl.ds(pl.multiple_of(start * size[k], size[k]), size[k])

    def y_start(k):
        half = m * size[k]
        give = pl.ds(pl.multiple_of((1 - par) * half, half), half)
        copy = send(source[k].at[give], yrecv[k], y_s.at[k], y_r.at[k], dp=ydev)
        done.append(copy)
        return copy

    def y_finish(k, copy):
        half = m * size[k]
        keep = pl.ds(pl.multiple_of(par * half, half), half)
        copy.wait_recv()
        total = source[k][keep, :].astype(f32) + yrecv[k][...].astype(f32)
        ysum[k][...] = total.astype(ysum[k].dtype)
        copies = [
            send(
                ysum[k].at[block(zdev[d], k)], zrecv[k].at[d], z_s.at[k, d], z_r.at[k, d],
                dp=2 * zdev[d] + par,
            )
            for d in range(m - 1)
        ]
        done.extend(copies)
        return copies

    def z_finish(k, copies):
        acc = ysum[k][block(z, k), :].astype(f32)
        for d in range(m - 1):
            copies[d].wait_recv()
            acc = acc + zrecv[k][d].astype(f32)
        return acc

    def spread(k):
        mine = full[k].at[block(at, k)]
        out = [
            send(mine, mine, az_s.at[k, d], az_r.at[k, d], dp=2 * zdev[d] + par)
            for d in range(m - 1)
        ]
        own = send(mine, mine, ay_s.at[k, 0], ay_r.at[k, 0], dp=ydev)
        done.extend(out + [own])
        return out, [own]

    def forward(k, out, ahead):
        for d in range(m - 1):
            out[d].wait_recv()
            came = full[k].at[block(par * m + lax.rem(z - (d + 1) + m, m), k)]
            copy = send(came, came, ay_s.at[k, d + 1], ay_r.at[k, d + 1], dp=ydev)
            ahead.append(copy)
            done.append(copy)

    cu = y_start(3)
    faro_s[...] = mm_tn(o2[...], rows_in[...]).astype(bf16)
    cfo = send(faro_s, faro_r, f_s.at[0], f_r.at[0], tensor=far)
    cbx = send(branch_x, bx_recv, f_s.at[2], f_r.at[2], tensor=far)

    def attention(q, k, v, lse, wo, dq, dk, dv, dsq, dsk, hooks):
        for j in range(seq_len // BLK):
            here = pl.ds(j * BLK, BLK)
            go[here, :] = mm_nt(rows_in[here, :], wo[...]).astype(bf16)
        for r in (dkt, dvt, dskt, later):
            r[...] = jnp.zeros_like(r)
        for i in reversed(range(seq_len // BLK)):
            here = pl.ds(i * BLK, BLK)
            bwd_block(
                i, heads, q.at[here], k, v, go.at[here], lse.at[here], fence.at[here],
                sq.at[here], sk, dq.at[here], dsq.at[here],
                dq_scr, dkt, dvt, dskt, later, fsum, qt, dot_,
            )
            if i in hooks:
                hooks[i]()
        dk[...] = dkt[...].T.astype(bf16)
        dv[...] = dvt[...].T.astype(bf16)
        dsk[...] = dskt[...].T

    last = seq_len // BLK - 1
    keep = {}

    def start_down():
        keep["yd"] = y_start(4)

    attention(q2, k2, v2, lse2, wo2, dq2, dk2, dv2, dsq2, dsk2, {last: start_down})
    for j, d in enumerate((dq2, dk2, dv2)):
        far_s[j * width : (j + 1) * width, :] = mm_tn(d[...], normed[...]).astype(bf16)
    cfar = send(far_s, far_r, f_s.at[1], f_r.at[1], tensor=far)
    keep["zu"] = y_finish(3, cu)

    def down_z():
        keep["zd"] = y_finish(4, keep["yd"])

    def up_spread():
        fu[block(at, 3), :] = z_finish(3, keep["zu"]).astype(bf16)
        keep["au"] = spread(3)

    attention(q1, k1, v1, lse1, wo1, dq1, dk1, dv1, dsq1, dsk1, {last: down_z, last - 1: up_spread})
    dsel[:, :HD] = (dsq1[...] + dsq2[...]).astype(bf16)
    dsel[:, HD:] = (dsk1[...] + dsk2[...]).astype(bf16)

    sel_mine[...] = mm_tn(dsel[...], normed[...]).astype(bf16)
    to_core = pltpu.make_async_remote_copy(
        src_ref=sel_mine, dst_ref=sel_core, send_sem=sl_s.at[0], recv_sem=sl_r.at[0],
        device_id={"tensor": core}, device_id_type=pl.DeviceIdType.MESH,
    )
    to_first = pltpu.make_async_remote_copy(
        src_ref=sel_mine, dst_ref=sel_far, send_sem=sl_s.at[1], recv_sem=sl_r.at[1],
        device_id={"tensor": far}, device_id_type=pl.DeviceIdType.MESH,
    )

    @pl.when(odd == 1)
    def _():
        to_core.start()

    def normed_grad(start):
        part = pl.ds(pl.multiple_of(start, rows), rows)
        total = mm(dsel[part, :], sel_w[...])
        for grads, weights in (((dq1, dk1, dv1), w1), ((dq2, dk2, dv2), w2)):
            for j in range(3):
                total = total + mm(grads[j][part, :], weights[j * width : (j + 1) * width, :])
        return total

    ng_send[...] = normed_grad((1 - odd) * rows).astype(bf16)
    ccore = send(ng_send, ng_recv, core_s, core_r, tensor=core)

    @pl.when(odd == 0)
    def _():
        to_core.wait_recv()
        sel_mine[...] = (sel_mine[...].astype(f32) + sel_core[...].astype(f32)).astype(bf16)

    @pl.when(me == 2)
    def _():
        to_first.start()

    gv = mm_tn(dv1[...], normed[...])
    go_own = mm_tn(o1[...], rows_in[...])
    if gb.shape[0] > 2 * width:
        gb[2 * width :, :] = jnp.zeros((gb.shape[0] - 2 * width, depth), bf16)
        ga[2 * width :, :] = jnp.zeros((ga.shape[0] - 2 * width, depth), bf16)
    cfo.wait_recv()
    ga[width : 2 * width, :] = (go_own + faro_r[...].astype(f32)).astype(bf16)
    cfar.wait_recv()
    ga[:width, :] = (gv + far_r[2 * width :, :].astype(f32)).astype(bf16)
    ca = y_start(1)
    gb[:width, :] = (mm_tn(dq1[...], normed[...]) + far_r[:width, :].astype(f32)).astype(bf16)
    gb[width : 2 * width, :] = (
        mm_tn(dk1[...], normed[...]) + far_r[width : 2 * width, :].astype(f32)
    ).astype(bf16)

    @pl.when(me == 0)
    def _():
        to_first.wait_recv()
        both = sel_mine[...].astype(f32) + sel_far[...].astype(f32)
        gb[:HD, :] = (gb[:HD, :].astype(f32) + both[:HD, :]).astype(bf16)
        gb[width : width + HD, :] = (
            gb[width : width + HD, :].astype(f32) + both[HD:, :]
        ).astype(bf16)

    cb = y_start(0)
    fd[block(at, 4), :] = z_finish(4, keep["zd"]).astype(bf16)
    ad = spread(4)
    forward(3, *keep["au"])

    grad = normed_grad(odd * rows)
    xhat, r = norm_parts(hidden[...].astype(f32))
    ccore.wait_recv()
    grad = grad + ng_recv[...].astype(f32)
    input_grad[...] = (gmid[...] + norm_back(grad * vecs[5:6, :], xhat, r)).astype(bf16)
    small[...] = jnp.zeros_like(small)
    token = odd * rows + lax.broadcasted_iota(jnp.int32, (rows, 1), 0)
    live = jnp.where(token < length, 1.0, 0.0)
    cbx.wait_recv()
    output[...] = (live * (partial[...] + bx_recv[...].astype(f32))).astype(bf16)
    dgain = jnp.sum(grad * xhat, 0, keepdims=True)
    dshift = jnp.sum(grad, 0, keepdims=True)
    lines = depth // 128
    for j in range(lines):
        small[j : j + 1, :] = dgain[:, j * 128 : (j + 1) * 128]
        small[lines + j : lines + j + 1, :] = dshift[:, j * 128 : (j + 1) * 128]
    for slot, which in ((2, 2), (3, 0), (4, 1), (5, 3)):
        for j in range(lines):
            small[slot * lines + j : slot * lines + j + 1, :] = sums[
                which : which + 1, j * 128 : (j + 1) * 128
            ]
    wide_lines = up_g.shape[1] // 128
    for j in range(wide_lines):
        small[pl.ds(6 * lines + me * wide_lines + j, 1), :] = sums[4:5, j * 128 : (j + 1) * 128]
    base = small_lines(depth, up_g.shape[1]) - 4 * ranks
    for owner, q, v in ((me, dq1, dv1), (far, dq2, dv2)):
        for j, d in enumerate((q, v)):
            total = jnp.sum(d[...].astype(f32), 0, keepdims=True)
            line = base + 4 * owner + 2 * j
            small[pl.ds(line, 1), :] = total[:, :128]
            small[pl.ds(line + 1, 1), : width - 128] = total[:, 128:]
    total = jnp.sum(dsel[...].astype(f32), 0, keepdims=True)
    lane = lax.broadcasted_iota(jnp.int32, total.shape, 1)
    small[base : base + 1, :] += jnp.where(lane < HD, total, 0.0)
    cs = y_start(2)

    cza = y_finish(1, ca)
    czb = y_finish(0, cb)
    czs = y_finish(2, cs)
    forward(4, *ad)
    fa[block(at, 1), :] = z_finish(1, cza).astype(bf16)
    aa = spread(1)
    fb[block(at, 0), :] = z_finish(0, czb).astype(bf16)
    ab = spread(0)
    ts[me] = z_finish(2, czs)
    ct = [
        send(ts.at[me], ts.at[me], t_s.at[d], t_r.at[d], tensor=peers[d]) for d in range(ranks - 1)
    ]
    done.extend(ct)
    for c in ct:
        c.wait_recv()
    vec = ts[0]
    for d in range(1, ranks):
        vec = vec + ts[d]
    out_s[block(at, 2), :] = vec
    asm = spread(2)
    forward(1, *aa)
    forward(0, *ab)
    forward(2, *asm)
    for _, ahead in (keep["au"], ad, aa, ab, asm):
        for c in ahead:
            c.wait_recv()

    @pl.when(odd == 1)
    def _():
        to_core.wait_send()

    @pl.when(me == 2)
    def _():
        to_first.wait_send()

    small_out[...] = out_s[...]
    for c in done + [cfo, cbx, cfar, ccore]:
        c.wait_send()

def front_kernel(
    lengths, hidden, out_grad, vecs, qkv, qv_bias, wo,
    normed, q1, k1, v1, lse1, o1, q2, k2, v2, lse2, o2, fence, sq, sk, w2, wo2, selw,
    g0, gcore, gfar, gcross,
    out_scr, carry, sel_b, bias2,
    nm_s, nm_r, gc_s, gc_r, sl_s, sl_r, w_s, w_r, p_s, p_r, e_s, e_r, g_s, g_r, h_s, h_r,
):
    me = lax.axis_index("tensor")
    idx = lax.axis_index("dp")
    odd = lax.rem(me, 2)
    core = me + 1 - 2 * odd
    far = lax.rem(me + 2, 4)
    par = lax.rem(idx, 2)
    ydev = idx + 1 - 2 * par
    rows = hidden.shape[0]
    seq_len = 2 * rows
    width = wo.shape[0]
    heads = width // HD
    length = jnp.where(me < 2, lengths[0], lengths[1])

    def sel_copies(k, where):
        return [
            pltpu.make_async_remote_copy(
                src_ref=a, dst_ref=a, send_sem=sl_s.at[k, j], recv_sem=sl_r.at[j],
                device_id={"tensor": where}, device_id_type=pl.DeviceIdType.MESH,
            )
            for j, a in enumerate((selw, sel_b))
        ]

    @pl.when(me == 0)
    def _():
        selw[:HD, :] = qkv[:HD, :]
        selw[HD:, :] = qkv[width : width + HD, :]
        sel_b[...] = qv_bias[...]

    meet([{"tensor": core}, {"tensor": far}, {"dp": ydev}])

    @pl.when(me == 0)
    def _():
        for c in sel_copies(0, far) + sel_copies(1, core):
            c.start()

    share = width // 2
    halves = [
        (src, dst, pl.ds(pl.multiple_of(base + par * share, share), share))
        for src, dst, base in (
            (qkv, w2, 0), (qkv, w2, width), (qkv, w2, 2 * width), (wo, wo2, 0)
        )
    ]
    extra = send(qv_bias, bias2, e_s, e_r, tensor=far)
    cross = [
        send(src.at[part], dst.at[part], w_s.at[j], w_r.at[j], tensor=far)
        for j, (src, dst, part) in enumerate(halves)
    ]
    passed = []

    def pass_on(j):
        cross[j].wait_recv()
        _, dst, part = halves[j]
        passed.append(send(dst.at[part], dst.at[part], p_s.at[j], p_r.at[j], dp=ydev))

    spot = pl.multiple_of(odd * rows, rows)
    norm_copies = []
    for c in range(rows // BLK):
        here = pl.ds(c * BLK, BLK)
        there = pl.ds(pl.multiple_of(spot + c * BLK, BLK), BLK)
        xhat, _ = norm_parts(hidden[here, :].astype(f32))
        normed[there, :] = (xhat * vecs[5:6, :] + vecs[6:7, :]).astype(bf16)
        norm_copies.append(
            send(normed.at[there], normed.at[there], nm_s.at[c], nm_r.at[c], tensor=core)
        )
    row = odd * rows + lax.broadcasted_iota(jnp.int32, (rows, 1), 0)
    live = jnp.where(row < length, 1.0, 0.0)
    g0[...] = (out_grad[...].astype(f32) * live).astype(bf16)
    gc = send(g0, gcore, gc_s, gc_r, tensor=core)
    g_parts = [pl.ds(c * BLK, BLK) for c in range(rows // BLK)]
    gf = [
        send(g0.at[p], gfar.at[p], g_s.at[c], g_r.at[c], tensor=far) for c, p in enumerate(g_parts)
    ]

    def project(weight, bias, out):
        for j in range(seq_len // BLK):
            here = pl.ds(j * BLK, BLK)
            y = mm_nt(normed[here, :], weight)
            if bias is not None:
                y = y + bias
            out[here, :] = y.astype(bf16)

    @pl.when(me == 2)
    def _():
        for c in sel_copies(0, far):
            c.wait_recv()
        for c in sel_copies(1, core):
            c.start()

    for c in norm_copies:
        c.wait_recv()
    project(qkv[:width, :], qv_bias[0:1, :], q1)
    project(qkv[width : 2 * width, :], None, k1)
    project(qkv[2 * width :, :], qv_bias[1:2, :], v1)

    @pl.when(odd == 1)
    def _():
        for c in sel_copies(1, core):
            c.wait_recv()

    for j in range(seq_len // BLK):
        here = pl.ds(j * BLK, BLK)
        y = mm_nt(normed[here, :], selw[...])
        sq[here, :] = (y[:, :HD] + sel_b[0:1, :HD]).astype(bf16)
        sk[here, :] = y[:, HD:].astype(bf16)
    carry[...] = jnp.zeros_like(carry)
    pass_on(0)
    for i in range(seq_len // BLK):
        here = pl.ds(i * BLK, BLK)
        make_fence(i, seq_len, length, sq.at[here], sk, fence.at[here], carry)
        fwd_block(
            i, heads, out_scr, q1.at[here], k1, v1, fence.at[here], o1.at[here], lse1.at[here]
        )
        if i < 3:
            pass_on(i + 1)
    extra.wait_recv()
    for j, (out, bias) in enumerate(((q2, bias2[0:1, :]), (k2, None), (v2, bias2[1:2, :]))):
        passed[j].wait_recv()
        project(w2[j * width : (j + 1) * width, :], bias, out)
    gx = []

    def pass_g(c):
        gf[c].wait_recv()
        p = g_parts[c]
        gx.append(send(gfar.at[p], gcross.at[p], h_s.at[c], h_r.at[c], tensor=core))

    for i in range(seq_len // BLK):
        here = pl.ds(i * BLK, BLK)
        fwd_block(
            i, heads, out_scr, q2.at[here], k2, v2, fence.at[here], o2.at[here], lse2.at[here]
        )
    for c in range(rows // BLK):
        pass_g(c)
    gc.wait_recv()
    passed[3].wait_recv()
    for c in gx:
        c.wait_recv()

    @pl.when(me == 0)
    def _():
        for c in sel_copies(0, far):
            c.wait_send()

    @pl.when(odd == 0)
    def _():
        for c in sel_copies(1, core):
            c.wait_send()

    for c in cross + passed + norm_copies + gf + gx + [gc, extra]:
        c.wait_send()


def front(lengths, hidden, out_grad, vecs, qkv, qv_bias, wo):
    rows, depth = hidden.shape
    seq_len, width = 2 * rows, wo.shape[0]
    pieces = rows // BLK
    vmem = pl.BlockSpec(memory_space=pltpu.VMEM)
    dma = pltpu.SemaphoreType.DMA
    heads = jax.ShapeDtypeStruct((seq_len, width), bf16)
    lse = jax.ShapeDtypeStruct((seq_len, 128), f32)
    sel = jax.ShapeDtypeStruct((seq_len, HD), bf16)
    wide = jax.ShapeDtypeStruct((rows, depth), bf16)
    return pl.pallas_call(
        front_kernel,
        in_specs=[pl.BlockSpec(memory_space=pltpu.SMEM)] + [vmem] * 6,
        out_specs=[vmem] * 21,
        out_shape=[
            jax.ShapeDtypeStruct((seq_len, depth), bf16),
            heads, heads, heads, lse, heads,
            heads, heads, heads, lse, heads,
            jax.ShapeDtypeStruct((seq_len, seq_len), f32),
            sel, sel,
            jax.ShapeDtypeStruct(qkv.shape, bf16),
            jax.ShapeDtypeStruct(wo.shape, bf16),
            jax.ShapeDtypeStruct((2 * HD, depth), bf16),
            wide, wide, wide, wide,
        ],
        scratch_shapes=[
            pltpu.VMEM((BLK, width), f32),
            pltpu.VMEM((8, seq_len), f32),
            pltpu.VMEM((2, width), f32),
            pltpu.VMEM((2, width), f32),
            dma((pieces,)), dma((pieces,)),
            dma, dma,
            dma((2, 2)), dma((2,)),
            dma((4,)), dma((4,)),
            dma((4,)), dma((4,)),
            dma, dma,
            dma((pieces,)), dma((pieces,)),
            dma((pieces,)), dma((pieces,)),
        ],
        compiler_params=pltpu.CompilerParams(
            collective_id=2, has_side_effects=True, vmem_limit_bytes=60 * 1024 * 1024
        ),
        name="front",
    )(lengths, hidden, out_grad, vecs, qkv, qv_bias, wo)


def small_lines(depth, hidden):
    return (6 * depth + 4 * hidden) // 128 + 16


def go_back(n, set1, set2, fence, sq, sk, rows_in, o1, o2, wo1, wo2, normed, w1, w2, sel_w,
            hidden, vecs, gmid, sums, partial, branch_x, lengths, up_g, down_g):
    m = n // 2
    chunk = up_g.shape[0] // n
    rows, depth = hidden.shape
    piece = -(-small_lines(depth, up_g.shape[1]) // (8 * n)) * 8
    seq_len, width = set1[0].shape
    half, shalf = m * chunk, m * piece
    ranks = 4
    wf = up_g.shape[1]
    small_chunk = -(-2 * width // (16 * n)) * 16
    part_half = m * small_chunk
    vmem = pl.BlockSpec(memory_space=pltpu.VMEM)
    dma = pltpu.SemaphoreType.DMA
    args = (*set1, *set2, fence, sq, sk, rows_in, o1, o2, wo1, wo2, normed, w1, w2, sel_w,
            hidden, vecs, gmid, sums, partial, branch_x, lengths, up_g, down_g)
    heads = pltpu.VMEM((seq_len, width), bf16)
    part = pltpu.VMEM((seq_len, HD), f32)
    return pl.pallas_call(
        lambda *refs: back_kernel(n, chunk, piece, depth, *refs),
        in_specs=[vmem] * (len(args) - 3)
        + [pl.BlockSpec(memory_space=pltpu.SMEM)]
        + [vmem] * 2,
        out_specs=[vmem] * 7,
        out_shape=[
            jax.ShapeDtypeStruct((n * chunk, wf), bf16),
            jax.ShapeDtypeStruct((n * chunk, wf), bf16),
            jax.ShapeDtypeStruct((n * small_chunk, depth), bf16),
            jax.ShapeDtypeStruct((n * small_chunk, depth), bf16),
            jax.ShapeDtypeStruct((n * piece, 128), f32),
            jax.ShapeDtypeStruct((rows, depth), bf16),
            jax.ShapeDtypeStruct((rows, depth), bf16),
        ],
        scratch_shapes=[
            heads, heads, heads, heads, heads, heads, heads, part, part, part, part,
            pltpu.VMEM((BLK, width), f32),
            pltpu.VMEM((width, seq_len), f32),
            pltpu.VMEM((width, seq_len), f32),
            pltpu.VMEM((HD, seq_len), f32),
            pltpu.VMEM((8, seq_len), f32),
            pltpu.VMEM((BLK, seq_len), f32),
            pltpu.VMEM((width, BLK), bf16),
            pltpu.VMEM((width, BLK), bf16),
            pltpu.VMEM((seq_len, 128), bf16),
            pltpu.VMEM((rows, depth), bf16),
            pltpu.VMEM((rows, depth), bf16),
            pltpu.VMEM((3 * width, depth), bf16),
            pltpu.VMEM((3 * width, depth), bf16),
            pltpu.VMEM((width, depth), bf16),
            pltpu.VMEM((width, depth), bf16),
            pltpu.VMEM((n * small_chunk, depth), bf16),
            pltpu.VMEM((n * small_chunk, depth), bf16),
            *[pltpu.VMEM((h, depth), bf16) for h in (half, half, part_half, part_half)],
            pltpu.VMEM((shalf, 128), f32),
            *[pltpu.VMEM((h, depth), bf16) for h in (half, half, part_half, part_half)],
            pltpu.VMEM((shalf, 128), f32),
            *[
                pltpu.VMEM((m - 1, c, depth), bf16)
                for c in (chunk, chunk, small_chunk, small_chunk)
            ],
            pltpu.VMEM((m - 1, piece, 128), f32),
            pltpu.VMEM((ranks, piece, 128), f32),
            pltpu.VMEM((n * piece, 128), f32),
            pltpu.VMEM((n * piece, 128), f32),
            pltpu.VMEM((rows, depth), bf16),
            *[pltpu.VMEM((2 * HD, depth), bf16)] * 3,
            dma, dma,
            dma((3,)), dma((3,)),
            dma((2,)), dma((2,)),
            dma((5,)), dma((5,)),
            dma((5, m - 1)), dma((5, m - 1)),
            dma((3,)), dma((3,)),
            dma((5, m - 1)), dma((5, m - 1)),
            dma((5, m)), dma((5, m)),
        ],
        compiler_params=pltpu.CompilerParams(
            collective_id=0, has_side_effects=True, vmem_limit_bytes=63 * 1024 * 1024
        ),
        name="go_back",
    )(*args)


def shards(
    hidden_in,
    lengths,
    ln1_gain,
    ln1_shift,
    qkv_weight,
    qv_bias,
    out_weight,
    out_bias,
    ln2_gain,
    ln2_shift,
    up_weight,
    up_bias,
    down_weight,
    down_bias,
    out_grad,
):
    n = lax.axis_size("dp")
    ranks = lax.axis_size("tensor")
    me = lax.axis_index("tensor")
    depth = hidden_in.shape[1]
    width = qkv_weight.shape[2]
    hidden = up_bias.shape[0]
    padded = -(-depth // (16 * n)) * 16 * n
    spot = jnp.arange(8)[:, None]
    vecs = jnp.zeros((8, depth), f32)
    for j, vec in enumerate(
        (out_bias, ln2_gain, ln2_shift, down_bias, up_bias.astype(f32), ln1_gain, ln1_shift)
    ):
        vecs = jnp.where(spot == j, vec[None], vecs)
    qkv_rows = jnp.swapaxes(qkv_weight, 1, 2).reshape(3 * width, depth)
    (normed, q1, k1, v1, lse1, o1, q2, k2, v2, lse2, o2, fence, sq, sk, qkv_far, out_far, sel_w,
     *grad_rows) = front(lengths, hidden_in, out_grad, vecs, qkv_rows, qv_bias, out_weight)
    attn_rows, grad_middle, partial, branch_x, up_part, down_part, sums = feed_forward(
        padded, o1, o2, out_weight, out_far, hidden_in, grad_rows, vecs, up_weight, down_weight
    )
    full_u, full_d, full_b, full_a, small, input_grad, output = go_back(
        n, (q1, k1, v1, lse1), (q2, k2, v2, lse2), fence, sq, sk, attn_rows, o1, o2,
        out_weight, out_far, normed, qkv_rows, qkv_far, sel_w, hidden_in, vecs,
        grad_middle, sums, partial, branch_x, lengths, up_part, down_part,
    )
    vectors = small[: 6 * depth // 128].reshape(6, depth)
    lines = (6 * depth + ranks * hidden) // 128
    up_all = small[6 * depth // 128 : lines].reshape(ranks, hidden)
    qv_all = small[lines : lines + 4 * ranks].reshape(ranks, 2, 256)
    up_bias_grad = lax.dynamic_index_in_dim(up_all, me, 0, keepdims=False)
    qv_bias_grad = lax.dynamic_index_in_dim(qv_all, me, 0, keepdims=False)[:, :width]
    qkv_grad = jnp.concatenate([full_b[: 2 * width], full_a[:width]], 0).astype(f32)
    qkv_grad = jnp.swapaxes(qkv_grad.reshape(3, width, depth), 1, 2)
    out_weight_grad = full_a[width : 2 * width].astype(f32)
    return (
        output,
        input_grad,
        vectors[0],
        vectors[1],
        qkv_grad,
        qv_bias_grad,
        out_weight_grad,
        vectors[2],
        vectors[3],
        vectors[4],
        full_u[:depth].astype(f32),
        up_bias_grad,
        full_d[:depth].astype(f32),
        vectors[5],
    )


def solution(mesh):
    return jax.shard_map(
        shards,
        mesh=mesh,
        in_specs=(
            P(("dp", "tensor"), None),
            P("dp"),
            P(),
            P(),
            P(None, None, "tensor"),
            P(None, "tensor"),
            P("tensor", None),
            P(),
            P(),
            P(),
            P(None, "tensor"),
            P("tensor"),
            P("tensor", None),
            P(),
            P(("dp", "tensor"), None),
        ),
        out_specs=(
            P(("dp", "tensor"), None),
            P(("dp", "tensor"), None),
            P(),
            P(),
            P(None, None, "tensor"),
            P(None, "tensor"),
            P("tensor", None),
            P(),
            P(),
            P(),
            P(None, "tensor"),
            P("tensor"),
            P("tensor", None),
            P(),
        ),
        check_vma=False,
    )
```

```python
import math

import jax
import jax.numpy as jnp
from jax import lax
from jax.experimental import pallas as pl
from jax.experimental.pallas import tpu as pltpu
from jax.sharding import PartitionSpec as P

HD = 64
BLK = 256
BIG = 1e30
sel_factor = 4.0
score_scale = 1.0 / math.sqrt(HD)
f32 = jnp.float32
bf16 = jnp.bfloat16


def mm(a, b):
    return lax.dot_general(a, b, (((1,), (0,)), ((), ())), preferred_element_type=f32)


def mm_nt(a, b):
    return lax.dot_general(a, b, (((1,), (1,)), ((), ())), preferred_element_type=f32)


def flip(a):
    return a.astype(f32).T.astype(bf16)


def split_mm(tri, x):
    hi = x.astype(bf16)
    lo = (x - hi.astype(f32)).astype(bf16)
    return mm(tri, hi) + mm(tri, lo)


def head_mask(h, width):
    return lax.broadcasted_iota(jnp.int32, (BLK, width), 1) // HD == h


def masked_rows(x, mask, scale):
    return jnp.where(mask, x.astype(f32) * scale, 0.0).astype(bf16)


def fwd_block(i, heads, first, q_ref, k_ref, v_ref, fence, o_ref, lse_ref):
    width = q_ref.shape[1]
    cols = (i + 1) * BLK
    keys = k_ref[:cols, :]
    vals = v_ref[:cols, :]
    fenced = fence[:, :cols]
    lane = lax.broadcasted_iota(jnp.int32, (BLK, 128), 1)
    lse_ref[...] = jnp.zeros_like(lse_ref)
    out_scr = first

    def head(h, _):
        mask = head_mask(h, width)
        s = mm_nt(masked_rows(q_ref[...], mask, score_scale), keys) - fenced
        top = jnp.max(s, -1, keepdims=True)
        e = jnp.exp(s - top)
        total = jnp.sum(e, -1, keepdims=True)
        p = (e * (1.0 / total)).astype(bf16)
        out = mm(p, vals)
        out_scr[...] = jnp.where(mask, out, out_scr[...])
        lse_ref[...] = jnp.where(lane == h, top + jnp.log(total), lse_ref[...])
        return 0

    lax.fori_loop(0, heads, head, 0, unroll=True)
    o_ref[...] = out_scr[...].astype(bf16)


def make_fence(i, seq_len, length, sq_ref, sk_ref, fence, carry):
    cols = (i + 1) * BLK
    s0 = mm_nt(sq_ref[...], sk_ref[:cols, :]) * score_scale
    row = i * BLK + lax.broadcasted_iota(jnp.int32, (BLK, cols), 0)
    col = lax.broadcasted_iota(jnp.int32, (BLK, cols), 1)
    picked = (col >= 1) & (col < row)
    sel = jnp.where(picked, jnp.maximum(s0, 0.0), 0.0) * (sel_factor / seq_len)
    r2 = lax.broadcasted_iota(jnp.int32, (BLK, BLK), 0)
    c2 = lax.broadcasted_iota(jnp.int32, (BLK, BLK), 1)
    tri = jnp.where(c2 < r2, 1.0, 0.0).astype(bf16)
    total = carry[0:1, :cols] + split_mm(tri, sel)
    carry[0:1, :cols] = total[BLK - 1 : BLK, :] + sel[BLK - 1 : BLK, :]
    fence[:, :cols] = jnp.where((col <= row) & (col < length), total, BIG)


def bwd_block(i, heads, q_ref, k_ref, v_ref, do_ref, lse_ref, f_ref, sq_ref, sk_ref,
              dq_ref, dsq_ref, dq_scr, dkt, dvt, dskt, later, fsum, qt, dot_):
    width = q_ref.shape[1]
    seq_len = k_ref.shape[0]
    cols = (i + 1) * BLK
    keys = k_ref[:cols, :]
    vals = v_ref[:cols, :]
    lane = lax.broadcasted_iota(jnp.int32, (BLK, 128), 1)
    qt[...] = (q_ref[...].astype(f32) * score_scale).T.astype(bf16)
    dot_[...] = flip(do_ref[...])
    fsum[:, :cols] = jnp.zeros((BLK, cols), f32)

    def head(h, _):
        mask = head_mask(h, width)
        lse = jnp.sum(jnp.where(lane == h, lse_ref[...], 0.0), -1, keepdims=True)
        s = mm_nt(masked_rows(q_ref[...], mask, score_scale), keys)
        p = jnp.exp(s - f_ref[:, :cols] - lse)
        dp = mm_nt(masked_rows(do_ref[...], mask, 1.0), vals)
        delta = jnp.sum(p * dp, -1, keepdims=True)
        g = (p * (dp - delta)).astype(bf16)
        rows = pl.ds(pl.multiple_of(h * HD, HD), HD)
        dq_scr[...] = jnp.where(mask, mm(g, keys), dq_scr[...])
        dkt[rows, :cols] += mm(qt[rows, :], g)
        dvt[rows, :cols] += mm(dot_[rows, :], p.astype(bf16))
        fsum[:, :cols] += g.astype(f32)
        return 0

    lax.fori_loop(0, heads, head, 0)
    dq_ref[...] = (dq_scr[...] * score_scale).astype(bf16)
    grad = -fsum[:, :cols]
    r2 = lax.broadcasted_iota(jnp.int32, (BLK, BLK), 0)
    c2 = lax.broadcasted_iota(jnp.int32, (BLK, BLK), 1)
    tri = jnp.where(c2 > r2, 1.0, 0.0).astype(bf16)
    dsel = later[0:1, :cols] + split_mm(tri, grad)
    later[0:1, :cols] = dsel[0:1, :] + grad[0:1, :]
    s0 = mm_nt(sq_ref[...], sk_ref[:cols, :])
    row = i * BLK + lax.broadcasted_iota(jnp.int32, (BLK, cols), 0)
    col = lax.broadcasted_iota(jnp.int32, (BLK, cols), 1)
    keep = (col >= 1) & (col < row) & (s0 > 0)
    gsel = jnp.where(keep, dsel * (sel_factor / seq_len), 0.0).astype(bf16)
    dsq_ref[...] = mm(gsel, sk_ref[:cols, :]) * score_scale
    sqt = (sq_ref[...].astype(f32) * score_scale).T.astype(bf16)
    dskt[:, :cols] += mm(sqt, gsel)


epsilon = 1e-05


def mm_tn(a, b):
    return lax.dot_general(a, b, (((0,), (0,)), ((), ())), preferred_element_type=f32)


def send(src, dst, send_sem, recv_sem, **where):
    copy = pltpu.make_async_remote_copy(
        src_ref=src,
        dst_ref=dst,
        send_sem=send_sem,
        recv_sem=recv_sem,
        device_id=where,
        device_id_type=pl.DeviceIdType.MESH,
    )
    copy.start()
    return copy


def meet(devices):
    barrier = pltpu.get_barrier_semaphore()
    for where in devices:
        pl.semaphore_signal(barrier, inc=1, device_id=where, device_id_type=pl.DeviceIdType.MESH)
    pl.semaphore_wait(barrier, len(devices))


def norm_parts(x):
    centre = x - jnp.mean(x, -1, keepdims=True)
    r = lax.rsqrt(jnp.mean(centre * centre, -1, keepdims=True) + epsilon)
    return centre * r, r


def norm_back(e, xhat, r):
    return r * (e - jnp.mean(e, -1, keepdims=True) - xhat * jnp.mean(e * xhat, -1, keepdims=True))


def gelu_pair(u):
    k = math.sqrt(2.0 / math.pi)
    square = u * u
    t = jnp.tanh(k * u * (1.0 + 0.044715 * square))
    act = 0.5 * u * (1.0 + t)
    slope = 0.5 * (1.0 + t) + 0.5 * u * (1.0 - t * t) * (k * (1.0 + 3.0 * 0.044715 * square))
    return act, slope


def feed_kernel(
    o1, o2, wo1, wo2, hidden, g0, g1, g2, g3, vecs, up, down,
    rows_out, gmid, partial, branch_x, up_g, down_g, sums, up_recv,
    inner, gs, act, gpre, mid, attn_send, attn_recv,
    near_send, near_recv, far_send, far_recv, x_send, x_recv,
    bn_send, bn_recv, bf_send, bf_recv, gin,
    g_sem, a_s, a_r, i_s, i_r, x_s, x_r, f_s, f_r, n_s, n_r, c_s, c_r, r_s, r_r, b_s, b_r, o_s, o_r, u_s, u_r,
):
    me = lax.axis_index("tensor")
    odd = lax.rem(me, 2)
    core = me + 1 - 2 * odd
    far = lax.rem(me + 2, 4)
    rows = hidden.shape[0]
    pieces = rows // BLK
    idx = lax.axis_index("dp")
    par = lax.rem(idx, 2)
    ydev = idx + 1 - 2 * par
    loads = [pltpu.make_async_copy(g, gs.at[i], g_sem.at[i]) for i, g in enumerate((g0, g1, g2, g3))]
    for c in loads:
        c.start()
    meet([{"tensor": core}, {"tensor": far}, {"dp": ydev}])
    out_bias, gain, shift, down_bias, up_bias = (vecs[j : j + 1, :] for j in range(5))

    def attn(start):
        part = pl.ds(pl.multiple_of(start, BLK), BLK)
        return mm(o1[part, :], wo1[...]) + mm(o2[part, :], wo2[...])

    sends = []
    attn_copies = []
    for c in range(pieces):
        here = pl.ds(c * BLK, BLK)
        attn_send[here, :] = attn((1 - odd) * rows + c * BLK).astype(bf16)
        attn_copies.append(send(attn_send.at[here], attn_recv.at[here], a_s.at[c], a_r.at[c], tensor=core))
    inner_copies, far_copies = [], []
    for c in range(pieces):
        here = pl.ds(c * BLK, BLK)
        mine = attn(odd * rows + c * BLK)
        attn_copies[c].wait_recv()
        m = hidden[here, :].astype(f32) + (mine + attn_recv[here, :].astype(f32)) + out_bias
        mid[here, :] = m
        xhat, r = norm_parts(m)
        inner[0, here, :] = (xhat * gain + shift).astype(bf16)
        far_copies.append(send(inner.at[0, here], inner.at[2, here], x_s.at[c], x_r.at[c], tensor=far))
        inner_copies.append(send(inner.at[0, here], inner.at[1, here], i_s.at[c], i_r.at[c], tensor=core))
    sends += attn_copies + inner_copies + far_copies
    for c in loads:
        c.wait()
    sums[...] = jnp.zeros_like(sums)

    def feed(slot, start):
        part = pl.ds(pl.multiple_of(start, BLK), BLK)
        pre = mm(inner[slot, part, :], up[...]) + up_bias
        a, slope = gelu_pair(pre)
        act[slot, part, :] = a.astype(bf16)
        gp = (mm_nt(gs[slot, part, :], down[...]) * slope).astype(bf16)
        gpre[slot, part, :] = gp
        sums[4:5, :] += jnp.sum(gp.astype(f32), 0, keepdims=True)

    def near(i, _):
        @pl.when(i == pieces)
        def _():
            for c in inner_copies:
                c.wait_recv()

        feed(i // pieces, lax.rem(i, pieces) * BLK)
        return 0

    lax.fori_loop(0, 2 * pieces, near, 0)

    def near_other(c, _):
        part = pl.ds(pl.multiple_of(c * BLK, BLK), BLK)
        near_send[part, :] = mm_nt(gpre[1, part, :], up[...]).astype(bf16)
        bn_send[part, :] = mm(act[1, part, :], down[...]).astype(bf16)
        return 0

    lax.fori_loop(0, pieces, near_other, 0)
    near_copy = send(near_send, near_recv, n_s.at[0], n_r.at[0], tensor=core)
    branch_copy = send(bn_send, bn_recv, n_s.at[1], n_r.at[1], tensor=core)

    def near_own(c, _):
        part = pl.ds(pl.multiple_of(c * BLK, BLK), BLK)
        gin[part, :] = mm_nt(gpre[0, part, :], up[...])
        partial[part, :] = mid[part, :] + mm(act[0, part, :], down[...]) + down_bias
        return 0

    lax.fori_loop(0, pieces, near_own, 0)

    def plan(src, dst, c, send_sem, recv_sem, where):
        here = pl.ds(pl.multiple_of(c * BLK, BLK), BLK)
        return pltpu.make_async_remote_copy(
            src_ref=src.at[here], dst_ref=dst.at[here], send_sem=send_sem.at[c],
            recv_sem=recv_sem.at[c], device_id={"tensor": where},
            device_id_type=pl.DeviceIdType.MESH,
        )

    def arrive(c):
        return plan(inner.at[0], inner.at[2], c, x_s, x_r, far)

    def hand_on(c):
        return plan(inner.at[2], inner.at[3], c, f_s, f_r, core)

    def crossed(c):
        return plan(far_send, far_recv, c, c_s, c_r, core)

    def back(c):
        return plan(x_send, x_recv, c, r_s, r_r, far)

    def far_step(i, _):
        c = i // 2
        which = lax.rem(i, 2)
        here = pl.ds(pl.multiple_of(c * BLK, BLK), BLK)

        @pl.when(which == 0)
        def _():
            arrive(c).wait_recv()
            hand_on(c).start()

        @pl.when(which == 1)
        def _():
            hand_on(c).wait_recv()

        feed(2 + which, c * BLK)

        @pl.when(which == 1)
        def _():
            far_send[here, :] = mm_nt(gpre[3, here, :], up[...]).astype(bf16)
            crossed(c).start()
            g = mm_nt(gpre[2, here, :], up[...])
            crossed(c).wait_recv()
            x_send[here, :] = (g + far_recv[here, :].astype(f32)).astype(bf16)
            back(c).start()

        return 0

    lax.fori_loop(0, 2 * pieces, far_step, 0)

    def far_out(c, _):
        here = pl.ds(pl.multiple_of(c * BLK, BLK), BLK)
        bf_send[here, :] = mm(act[3, here, :], down[...]).astype(bf16)
        return 0

    depth = up.shape[0]
    if up_g.shape[0] > depth:
        up_g[depth:, :] = jnp.zeros((up_g.shape[0] - depth, up_g.shape[1]), bf16)
        down_g[depth:, :] = jnp.zeros((up_g.shape[0] - depth, up_g.shape[1]), bf16)

    def weights(left, right, out):
        def tile(j, _):
            part = pl.ds(pl.multiple_of(j * BLK, BLK), BLK)
            total = mm_tn(left[0, :, part], right[0])
            for k in range(1, 4):
                total = total + mm_tn(left[k, :, part], right[k])
            out[part, :] = total.astype(bf16)
            return 0

        lax.fori_loop(0, depth // BLK, tile, 0)

    weights(inner, gpre, up_g)
    half = up_g.shape[0] // 2
    give = pl.ds(pl.multiple_of((1 - par) * half, half), half)
    up_copy = send(up_g.at[give], up_recv, u_s, u_r, dp=ydev)
    lax.fori_loop(0, pieces, far_out, 0)
    far_branch = send(bf_send, bf_recv, b_s, b_r, tensor=core)
    weights(act, gs, down_g)
    far_branch.wait_recv()
    for c in range(pieces):
        here = pl.ds(c * BLK, BLK)
        b = mm(act[2, here, :], down[...])
        branch_x[here, :] = (b + bf_recv[here, :].astype(f32)).astype(bf16)
    near_copy.wait_recv()
    branch_copy.wait_recv()
    partial[...] += bn_recv[...].astype(f32)
    rows_copies = []
    for c in range(pieces):
        here = pl.ds(c * BLK, BLK)
        xhat, r = norm_parts(mid[here, :])
        back(c).wait_recv()
        g = gin[here, :] + near_recv[here, :].astype(f32) + x_recv[here, :].astype(f32)
        g_out = gs[0, here, :].astype(f32)
        gm = g_out + norm_back(g * gain, xhat, r)
        gmid[here, :] = gm
        there = pl.ds(pl.multiple_of(odd * rows + c * BLK, BLK), BLK)
        ga = gm.astype(bf16)
        rows_out[there, :] = ga
        rows_copies.append(
            send(rows_out.at[there], rows_out.at[there], o_s.at[c], o_r.at[c], tensor=core)
        )
        sums[0:1, :] += jnp.sum(g * xhat, 0, keepdims=True)
        sums[1:2, :] += jnp.sum(g, 0, keepdims=True)
        sums[2:3, :] += jnp.sum(ga.astype(f32), 0, keepdims=True)
        sums[3:4, :] += jnp.sum(g_out, 0, keepdims=True)
    for c in rows_copies:
        c.wait_recv()
    up_copy.wait_recv()
    for c in range(pieces):
        sends += [hand_on(c), crossed(c), back(c)]
    for c in sends + rows_copies + [near_copy, branch_copy, far_branch, up_copy]:
        c.wait_send()


def feed_forward(padded, o1, o2, wo1, wo2, hidden, gs, vecs, up, down):
    rows, depth = hidden.shape
    width = up.shape[1]
    pieces = rows // BLK
    vmem = pl.BlockSpec(memory_space=pltpu.VMEM)
    anyw = pl.BlockSpec(memory_space=pl.ANY)
    dma = pltpu.SemaphoreType.DMA
    wide = pltpu.VMEM((rows, depth), bf16)
    each = [dma((pieces,))] * 2
    return pl.pallas_call(
        feed_kernel,
        in_specs=[vmem] * 5 + [anyw] * 4 + [vmem] * 3,
        out_specs=[vmem] * 8,
        out_shape=[
            jax.ShapeDtypeStruct((2 * rows, depth), bf16),
            jax.ShapeDtypeStruct((rows, depth), f32),
            jax.ShapeDtypeStruct((rows, depth), f32),
            jax.ShapeDtypeStruct((rows, depth), bf16),
            jax.ShapeDtypeStruct((padded, width), bf16),
            jax.ShapeDtypeStruct((padded, width), bf16),
            jax.ShapeDtypeStruct((8, depth), f32),
            jax.ShapeDtypeStruct((padded // 2, width), bf16),
        ],
        scratch_shapes=[
            pltpu.VMEM((4, rows, depth), bf16),
            pltpu.VMEM((4, rows, depth), bf16),
            pltpu.VMEM((4, rows, width), bf16),
            pltpu.VMEM((4, rows, width), bf16),
            pltpu.VMEM((rows, depth), f32),
            wide, wide, wide, wide, wide, wide, wide, wide, wide, wide, wide, wide,
            pltpu.VMEM((rows, depth), f32),
            dma((4,)),
            *each, *each, *each, *each,
            dma((2,)), dma((2,)),
            *each, *each,
            dma, dma,
            *each,
            dma, dma,
        ],
        compiler_params=pltpu.CompilerParams(
            collective_id=1, has_side_effects=True, vmem_limit_bytes=62 * 1024 * 1024
        ),
        name="feed_forward",
    )(o1, o2, wo1, wo2, hidden, *gs, vecs, up, down)

def back_kernel(
    n, chunk, piece, depth,
    lengths, down_h, branch_x, *rest,
):
    held, outs, kept = rest[:LOADS], rest[LOADS : LOADS + 7], rest[LOADS + 7 : 2 * LOADS + 7]
    back_body(n, chunk, piece, depth, lengths, down_h, branch_x, held, kept, outs, *rest[2 * LOADS + 7 :])


LOADS = 28


def back_body(
    n, chunk, piece, depth, lengths, down_h, branch_x, held, kept, outs, ld_s,
    go, dq1, dk1, dv1, dq2, dk2, dv2, dsq1, dsk1, dsq2, dsk2,
    dq_scr, dkt, dvt, dskt, later, fsum, qt, dot_,
    dsel, ng_send, ng_recv, far_s, far_r, faro_s, faro_r, gb, ga,
    yd, yb, ya, ys, su, sd, sb, sa, ss, zu, zd, zb, za, zs,
    ts, small, out_s, bx_recv, sel_mine, sel_core, sel_far,
    core_s, core_r, f_s, f_r, sl_s, sl_r, y_s, y_r, z_s, z_r, t_s, t_r, az_s, az_r, ay_s, ay_r,
):
    (up_g, up_recv, rows_in, o2, wo2, q2, k2, v2, lse2, fence, sq, sk, normed, down_g, wo1, q1, k1, v1,
     lse1, w2, w1, sel_w, o1, hidden, gmid, vecs, sums, partial) = kept
    fu, fd, fb, fa, small_out, input_grad, output = outs
    loads = [pltpu.make_async_copy(h, v, ld_s.at[j]) for j, (h, v) in enumerate(zip(held, kept))]
    for c in loads:
        c.start()
    ready = set()

    def need(*which):
        for j in which:
            if j not in ready:
                ready.add(j)
                loads[j].wait()

    idx = lax.axis_index("dp")
    me = lax.axis_index("tensor")
    odd = lax.rem(me, 2)
    par = lax.rem(idx, 2)
    z = lax.div(idx, 2)
    m = n // 2
    rows = hidden.shape[0]
    seq_len = k1.shape[0]
    width = q1.shape[1]
    heads = width // HD
    ranks = 4
    core = me + 1 - 2 * odd
    far = lax.rem(me + 2, ranks)
    ydev = idx + 1 - 2 * par
    peers = [lax.rem(me + d, ranks) for d in range(1, ranks)]
    zdev = [lax.rem(z + d, m) for d in range(1, m)]
    meet(
        [{"tensor": p} for p in peers]
        + [{"dp": ydev}]
        + [{"dp": 2 * p + par} for p in zdev]
    )
    at = par * m + z
    length = jnp.where(me < 2, lengths[0], lengths[1])
    source = (gb, ga, small, up_g, down_g)
    yrecv = (yb, ya, ys, up_recv, yd)
    ysum = (sb, sa, ss, su, sd)
    zrecv = (zb, za, zs, zu, zd)
    full = (fb, fa, out_s, fu, fd)
    size = (gb.shape[0] // n, ga.shape[0] // n, piece, chunk, chunk)
    done = []

    def block(start, k):
        return pl.ds(pl.multiple_of(start * size[k], size[k]), size[k])

    def y_start(k):
        half = m * size[k]
        give = pl.ds(pl.multiple_of((1 - par) * half, half), half)
        src = down_h if k == 4 else source[k]
        copy = send(src.at[give], yrecv[k], y_s.at[k], y_r.at[k], dp=ydev)
        done.append(copy)
        return copy

    def y_finish(k, copy):
        half = m * size[k]
        keep = pl.ds(pl.multiple_of(par * half, half), half)
        if copy is not None:
            copy.wait_recv()
        total = source[k][keep, :].astype(f32) + yrecv[k][...].astype(f32)
        ysum[k][...] = total.astype(ysum[k].dtype)
        copies = [
            send(
                ysum[k].at[block(zdev[d], k)], zrecv[k].at[d], z_s.at[k, d], z_r.at[k, d],
                dp=2 * zdev[d] + par,
            )
            for d in range(m - 1)
        ]
        done.extend(copies)
        return copies

    def z_finish(k, copies):
        acc = ysum[k][block(z, k), :].astype(f32)
        for d in range(m - 1):
            copies[d].wait_recv()
            acc = acc + zrecv[k][d].astype(f32)
        return acc

    def spread(k):
        mine = full[k].at[block(at, k)]
        out = [
            send(mine, mine, az_s.at[k, d], az_r.at[k, d], dp=2 * zdev[d] + par)
            for d in range(m - 1)
        ]
        own = send(mine, mine, ay_s.at[k, 0], ay_r.at[k, 0], dp=ydev)
        done.extend(out + [own])
        return out, [own]

    def forward(k, out, ahead):
        for d in range(m - 1):
            out[d].wait_recv()
            came = full[k].at[block(par * m + lax.rem(z - (d + 1) + m, m), k)]
            copy = send(came, came, ay_s.at[k, d + 1], ay_r.at[k, d + 1], dp=ydev)
            ahead.append(copy)
            done.append(copy)

    keep = {"yd": y_start(4)}
    need(0, 1)
    keep["zu"] = y_finish(3, None)
    need(2, 3)
    faro_s[...] = mm_tn(o2[...], rows_in[...]).astype(bf16)
    cfo = send(faro_s, faro_r, f_s.at[0], f_r.at[0], tensor=far)

    def attention(q, k, v, lse, wo, dq, dk, dv, dsq, dsk, hooks):
        for j in range(seq_len // BLK):
            here = pl.ds(j * BLK, BLK)
            go[here, :] = mm_nt(rows_in[here, :], wo[...]).astype(bf16)
        for r in (dkt, dvt, dskt, later):
            r[...] = jnp.zeros_like(r)
        for i in reversed(range(seq_len // BLK)):
            here = pl.ds(i * BLK, BLK)
            bwd_block(
                i, heads, q.at[here], k, v, go.at[here], lse.at[here], fence.at[here],
                sq.at[here], sk, dq.at[here], dsq.at[here],
                dq_scr, dkt, dvt, dskt, later, fsum, qt, dot_,
            )
            if i in hooks:
                hooks[i]()
        dk[...] = dkt[...].T.astype(bf16)
        dv[...] = dvt[...].T.astype(bf16)
        dsk[...] = dskt[...].T

    need(*range(4, 12))
    attention(q2, k2, v2, lse2, wo2, dq2, dk2, dv2, dsq2, dsk2, {})
    need(12)
    for j, d in enumerate((dq2, dk2, dv2)):
        far_s[j * width : (j + 1) * width, :] = mm_tn(d[...], normed[...]).astype(bf16)
    cfar = send(far_s, far_r, f_s.at[1], f_r.at[1], tensor=far)
    cbx = send(branch_x, bx_recv, f_s.at[2], f_r.at[2], tensor=far)
    fu[block(at, 3), :] = z_finish(3, keep["zu"]).astype(bf16)
    keep["au"] = spread(3)
    need(13)
    keep["zd"] = y_finish(4, keep["yd"])
    need(*range(14, LOADS))
    attention(q1, k1, v1, lse1, wo1, dq1, dk1, dv1, dsq1, dsk1, {})
    forward(3, *keep["au"])
    dsel[:, :HD] = (dsq1[...] + dsq2[...]).astype(bf16)
    dsel[:, HD:] = (dsk1[...] + dsk2[...]).astype(bf16)

    sel_mine[...] = mm_tn(dsel[...], normed[...]).astype(bf16)
    to_core = pltpu.make_async_remote_copy(
        src_ref=sel_mine, dst_ref=sel_core, send_sem=sl_s.at[0], recv_sem=sl_r.at[0],
        device_id={"tensor": core}, device_id_type=pl.DeviceIdType.MESH,
    )
    to_first = pltpu.make_async_remote_copy(
        src_ref=sel_mine, dst_ref=sel_far, send_sem=sl_s.at[1], recv_sem=sl_r.at[1],
        device_id={"tensor": far}, device_id_type=pl.DeviceIdType.MESH,
    )

    @pl.when(odd == 1)
    def _():
        to_core.start()

    def normed_grad(start):
        part = pl.ds(pl.multiple_of(start, rows), rows)
        total = mm(dsel[part, :], sel_w[...])
        for grads, weights in (((dq1, dk1, dv1), w1), ((dq2, dk2, dv2), w2)):
            for j in range(3):
                total = total + mm(grads[j][part, :], weights[j * width : (j + 1) * width, :])
        return total

    ng_send[...] = normed_grad((1 - odd) * rows).astype(bf16)
    ccore = send(ng_send, ng_recv, core_s, core_r, tensor=core)

    @pl.when(odd == 0)
    def _():
        to_core.wait_recv()
        sel_mine[...] = (sel_mine[...].astype(f32) + sel_core[...].astype(f32)).astype(bf16)

    @pl.when(me == 2)
    def _():
        to_first.start()

    gv = mm_tn(dv1[...], normed[...])
    go_own = mm_tn(o1[...], rows_in[...])
    if gb.shape[0] > 2 * width:
        gb[2 * width :, :] = jnp.zeros((gb.shape[0] - 2 * width, depth), bf16)
        ga[2 * width :, :] = jnp.zeros((ga.shape[0] - 2 * width, depth), bf16)
    cfo.wait_recv()
    ga[width : 2 * width, :] = (go_own + faro_r[...].astype(f32)).astype(bf16)
    cfar.wait_recv()
    ga[:width, :] = (gv + far_r[2 * width :, :].astype(f32)).astype(bf16)
    ca = y_start(1)
    gb[:width, :] = (mm_tn(dq1[...], normed[...]) + far_r[:width, :].astype(f32)).astype(bf16)
    gb[width : 2 * width, :] = (
        mm_tn(dk1[...], normed[...]) + far_r[width : 2 * width, :].astype(f32)
    ).astype(bf16)

    @pl.when(me == 0)
    def _():
        to_first.wait_recv()
        both = sel_mine[...].astype(f32) + sel_far[...].astype(f32)
        gb[:HD, :] = (gb[:HD, :].astype(f32) + both[:HD, :]).astype(bf16)
        gb[width : width + HD, :] = (
            gb[width : width + HD, :].astype(f32) + both[HD:, :]
        ).astype(bf16)

    cb = y_start(0)
    fd[block(at, 4), :] = z_finish(4, keep["zd"]).astype(bf16)
    ad = spread(4)

    grad = normed_grad(odd * rows)
    xhat, r = norm_parts(hidden[...].astype(f32))
    ccore.wait_recv()
    grad = grad + ng_recv[...].astype(f32)
    input_grad[...] = (gmid[...] + norm_back(grad * vecs[5:6, :], xhat, r)).astype(bf16)
    small[...] = jnp.zeros_like(small)
    token = odd * rows + lax.broadcasted_iota(jnp.int32, (rows, 1), 0)
    live = jnp.where(token < length, 1.0, 0.0)
    dgain = jnp.sum(grad * xhat, 0, keepdims=True)
    dshift = jnp.sum(grad, 0, keepdims=True)
    lines = depth // 128
    for j in range(lines):
        small[j : j + 1, :] = dgain[:, j * 128 : (j + 1) * 128]
        small[lines + j : lines + j + 1, :] = dshift[:, j * 128 : (j + 1) * 128]
    for slot, which in ((2, 2), (3, 0), (4, 1), (5, 3)):
        for j in range(lines):
            small[slot * lines + j : slot * lines + j + 1, :] = sums[
                which : which + 1, j * 128 : (j + 1) * 128
            ]
    wide_lines = up_g.shape[1] // 128
    for j in range(wide_lines):
        small[pl.ds(6 * lines + me * wide_lines + j, 1), :] = sums[4:5, j * 128 : (j + 1) * 128]
    base = small_lines(depth, up_g.shape[1]) - 4 * ranks
    for owner, q, v in ((me, dq1, dv1), (far, dq2, dv2)):
        for j, d in enumerate((q, v)):
            total = jnp.sum(d[...].astype(f32), 0, keepdims=True)
            line = base + 4 * owner + 2 * j
            small[pl.ds(line, 1), :] = total[:, :128]
            small[pl.ds(line + 1, 1), : width - 128] = total[:, 128:]
    total = jnp.sum(dsel[...].astype(f32), 0, keepdims=True)
    lane = lax.broadcasted_iota(jnp.int32, total.shape, 1)
    small[base : base + 1, :] += jnp.where(lane < HD, total, 0.0)
    cs = y_start(2)

    cza = y_finish(1, ca)
    cbx.wait_recv()
    output[...] = (live * (partial[...] + bx_recv[...].astype(f32))).astype(bf16)
    czb = y_finish(0, cb)
    czs = y_finish(2, cs)
    forward(4, *ad)
    fa[block(at, 1), :] = z_finish(1, cza).astype(bf16)
    aa = spread(1)
    fb[block(at, 0), :] = z_finish(0, czb).astype(bf16)
    ab = spread(0)
    ts[me] = z_finish(2, czs)
    ct = [
        send(ts.at[me], ts.at[me], t_s.at[d], t_r.at[d], tensor=peers[d]) for d in range(ranks - 1)
    ]
    done.extend(ct)
    for c in ct:
        c.wait_recv()
    vec = ts[0]
    for d in range(1, ranks):
        vec = vec + ts[d]
    out_s[block(at, 2), :] = vec
    asm = spread(2)
    forward(1, *aa)
    forward(0, *ab)
    forward(2, *asm)
    for _, ahead in (keep["au"], ad, aa, ab, asm):
        for c in ahead:
            c.wait_recv()

    @pl.when(odd == 1)
    def _():
        to_core.wait_send()

    @pl.when(me == 2)
    def _():
        to_first.wait_send()

    small_out[...] = out_s[...]
    for c in done + [cfo, cbx, cfar, ccore]:
        c.wait_send()

def front_kernel(
    lengths, hidden, out_grad, vecs, qkv, qv_bias, wo,
    *rest,
):
    outs, gcore, gfar, gcross = rest[:18], rest[18], rest[19], rest[20]
    kept = rest[21:39]
    front_body(
        lengths, hidden, out_grad, vecs, qkv, qv_bias, wo, outs, kept, gcore, gfar, gcross, *rest[39:]
    )


def front_body(
    lengths, hidden, out_grad, vecs, qkv, qv_bias, wo, outs, kept, gcore, gfar, gcross,
    out_scr, carry, sel_b, bias2,
    st_s, nm_s, nm_r, gc_s, gc_r, sl_s, sl_r, w_s, w_r, p_s, p_r, e_s, e_r, g_s, g_r, h_s, h_r,
):
    me = lax.axis_index("tensor")
    idx = lax.axis_index("dp")
    odd = lax.rem(me, 2)
    core = me + 1 - 2 * odd
    far = lax.rem(me + 2, 4)
    par = lax.rem(idx, 2)
    ydev = idx + 1 - 2 * par
    rows = hidden.shape[0]
    seq_len = 2 * rows
    width = wo.shape[0]
    heads = width // HD
    (normed, q1, k1, v1, lse1, o1, q2, k2, v2, lse2, o2, fence, sq, sk, w2, wo2, selw, g0) = kept
    stores = []

    def store(*which):
        for j in which:
            copy = pltpu.make_async_copy(kept[j], outs[j], st_s.at[j])
            copy.start()
            stores.append(copy)

    length = jnp.where(me < 2, lengths[0], lengths[1])

    def sel_copies(k, where):
        return [
            pltpu.make_async_remote_copy(
                src_ref=a, dst_ref=a, send_sem=sl_s.at[k, j], recv_sem=sl_r.at[j],
                device_id={"tensor": where}, device_id_type=pl.DeviceIdType.MESH,
            )
            for j, a in enumerate((selw, sel_b))
        ]

    @pl.when(me == 0)
    def _():
        selw[:HD, :] = qkv[:HD, :]
        selw[HD:, :] = qkv[width : width + HD, :]
        sel_b[...] = qv_bias[...]

    meet([{"tensor": core}, {"tensor": far}, {"dp": ydev}])

    @pl.when(me == 0)
    def _():
        for c in sel_copies(0, far) + sel_copies(1, core):
            c.start()

    share = width // 2
    halves = [
        (src, dst, pl.ds(pl.multiple_of(base + par * share, share), share))
        for src, dst, base in (
            (qkv, w2, 0), (qkv, w2, width), (qkv, w2, 2 * width), (wo, wo2, 0)
        )
    ]
    extra = send(qv_bias, bias2, e_s, e_r, tensor=far)
    cross = [
        send(src.at[part], dst.at[part], w_s.at[j], w_r.at[j], tensor=far)
        for j, (src, dst, part) in enumerate(halves)
    ]
    passed = []

    def pass_on(j):
        cross[j].wait_recv()
        _, dst, part = halves[j]
        passed.append(send(dst.at[part], dst.at[part], p_s.at[j], p_r.at[j], dp=ydev))

    spot = pl.multiple_of(odd * rows, rows)
    norm_copies = []
    for c in range(rows // BLK):
        here = pl.ds(c * BLK, BLK)
        there = pl.ds(pl.multiple_of(spot + c * BLK, BLK), BLK)
        xhat, _ = norm_parts(hidden[here, :].astype(f32))
        normed[there, :] = (xhat * vecs[5:6, :] + vecs[6:7, :]).astype(bf16)
        norm_copies.append(
            send(normed.at[there], normed.at[there], nm_s.at[c], nm_r.at[c], tensor=core)
        )
    row = odd * rows + lax.broadcasted_iota(jnp.int32, (rows, 1), 0)
    live = jnp.where(row < length, 1.0, 0.0)
    g0[...] = (out_grad[...].astype(f32) * live).astype(bf16)
    store(17)
    gc = send(g0, gcore, gc_s, gc_r, tensor=core)
    g_parts = [pl.ds(c * BLK, BLK) for c in range(rows // BLK)]
    gf = [
        send(g0.at[p], gfar.at[p], g_s.at[c], g_r.at[c], tensor=far) for c, p in enumerate(g_parts)
    ]

    def project(weight, bias, out):
        def tile(j, _):
            here = pl.ds(pl.multiple_of(j * BLK, BLK), BLK)
            y = mm_nt(normed[here, :], weight)
            if bias is not None:
                y = y + bias
            out[here, :] = y.astype(bf16)
            return 0

        lax.fori_loop(0, seq_len // BLK, tile, 0)

    @pl.when(me == 2)
    def _():
        for c in sel_copies(0, far):
            c.wait_recv()
        for c in sel_copies(1, core):
            c.start()

    for c in norm_copies:
        c.wait_recv()
    store(0)
    project(qkv[:width, :], qv_bias[0:1, :], q1)
    project(qkv[width : 2 * width, :], None, k1)
    project(qkv[2 * width :, :], qv_bias[1:2, :], v1)

    @pl.when(odd == 1)
    def _():
        for c in sel_copies(1, core):
            c.wait_recv()

    store(1, 2, 3)
    for j in range(seq_len // BLK):
        here = pl.ds(j * BLK, BLK)
        y = mm_nt(normed[here, :], selw[...])
        sq[here, :] = (y[:, :HD] + sel_b[0:1, :HD]).astype(bf16)
        sk[here, :] = y[:, HD:].astype(bf16)
    store(12, 13, 16)
    carry[...] = jnp.zeros_like(carry)
    pass_on(0)
    for i in range(seq_len // BLK):
        here = pl.ds(i * BLK, BLK)
        make_fence(i, seq_len, length, sq.at[here], sk, fence.at[here], carry)
        fwd_block(
            i, heads, out_scr, q1.at[here], k1, v1, fence.at[here], o1.at[here], lse1.at[here]
        )
        if i < 3:
            pass_on(i + 1)
    store(4, 5, 11)
    extra.wait_recv()
    for j, (out, bias) in enumerate(((q2, bias2[0:1, :]), (k2, None), (v2, bias2[1:2, :]))):
        passed[j].wait_recv()
        project(w2[j * width : (j + 1) * width, :], bias, out)
        store(6 + j)
    store(14)
    gx = []

    def pass_g(c):
        gf[c].wait_recv()
        p = g_parts[c]
        gx.append(send(gfar.at[p], gcross.at[p], h_s.at[c], h_r.at[c], tensor=core))

    for i in range(seq_len // BLK):
        here = pl.ds(i * BLK, BLK)
        fwd_block(
            i, heads, out_scr, q2.at[here], k2, v2, fence.at[here], o2.at[here], lse2.at[here]
        )
    store(9, 10)
    for c in range(rows // BLK):
        pass_g(c)
    gc.wait_recv()
    passed[3].wait_recv()
    store(15)
    for c in gx:
        c.wait_recv()

    @pl.when(me == 0)
    def _():
        for c in sel_copies(0, far):
            c.wait_send()

    @pl.when(odd == 0)
    def _():
        for c in sel_copies(1, core):
            c.wait_send()

    for c in cross + passed + norm_copies + gf + gx + [gc, extra]:
        c.wait_send()
    for c in stores:
        c.wait()


def front(lengths, hidden, out_grad, vecs, qkv, qv_bias, wo):
    rows, depth = hidden.shape
    seq_len, width = 2 * rows, wo.shape[0]
    pieces = rows // BLK
    vmem = pl.BlockSpec(memory_space=pltpu.VMEM)
    dma = pltpu.SemaphoreType.DMA
    heads = jax.ShapeDtypeStruct((seq_len, width), bf16)
    lse = jax.ShapeDtypeStruct((seq_len, 128), f32)
    sel = jax.ShapeDtypeStruct((seq_len, HD), bf16)
    wide = jax.ShapeDtypeStruct((rows, depth), bf16)
    kept = [
        jax.ShapeDtypeStruct((seq_len, depth), bf16),
        heads, heads, heads, lse, heads,
        heads, heads, heads, lse, heads,
        jax.ShapeDtypeStruct((seq_len, seq_len), f32),
        sel, sel,
        jax.ShapeDtypeStruct(qkv.shape, bf16),
        jax.ShapeDtypeStruct(wo.shape, bf16),
        jax.ShapeDtypeStruct((2 * HD, depth), bf16),
        wide,
    ]
    return pl.pallas_call(
        front_kernel,
        in_specs=[pl.BlockSpec(memory_space=pltpu.SMEM)] + [vmem] * 6,
        out_specs=[pl.BlockSpec(memory_space=pl.ANY)] * 21,
        out_shape=kept + [wide, wide, wide],
        scratch_shapes=[pltpu.VMEM(a.shape, a.dtype) for a in kept]
        + [
            pltpu.VMEM((BLK, width), f32),
            pltpu.VMEM((8, seq_len), f32),
            pltpu.VMEM((2, width), f32),
            pltpu.VMEM((2, width), f32),
            dma((18,)),
            dma((pieces,)), dma((pieces,)),
            dma, dma,
            dma((2, 2)), dma((2,)),
            dma((4,)), dma((4,)),
            dma((4,)), dma((4,)),
            dma, dma,
            dma((pieces,)), dma((pieces,)),
            dma((pieces,)), dma((pieces,)),
        ],
        compiler_params=pltpu.CompilerParams(
            collective_id=2, has_side_effects=True, vmem_limit_bytes=60 * 1024 * 1024
        ),
        name="front",
    )(lengths, hidden, out_grad, vecs, qkv, qv_bias, wo)


def small_lines(depth, hidden):
    return (6 * depth + 4 * hidden) // 128 + 16


def go_back(n, set1, set2, fence, sq, sk, rows_in, o1, o2, wo1, wo2, normed, w1, w2, sel_w,
            hidden, vecs, gmid, sums, partial, branch_x, lengths, up_g, up_recv, down_g):
    m = n // 2
    chunk = up_g.shape[0] // n
    rows, depth = hidden.shape
    piece = -(-small_lines(depth, up_g.shape[1]) // (8 * n)) * 8
    seq_len, width = set1[0].shape
    half, shalf = m * chunk, m * piece
    ranks = 4
    wf = up_g.shape[1]
    small_chunk = -(-2 * width // (16 * n)) * 16
    part_half = m * small_chunk
    vmem = pl.BlockSpec(memory_space=pltpu.VMEM)
    dma = pltpu.SemaphoreType.DMA
    q1, k1, v1, lse1 = set1
    q2, k2, v2, lse2 = set2
    held = (up_g, up_recv, rows_in, o2, wo2, q2, k2, v2, lse2, fence, sq, sk, normed, down_g, wo1,
            q1, k1, v1, lse1, w2, w1, sel_w, o1, hidden, gmid, vecs, sums, partial)
    anyw = pl.BlockSpec(memory_space=pl.ANY)
    heads = pltpu.VMEM((seq_len, width), bf16)
    part = pltpu.VMEM((seq_len, HD), f32)
    return pl.pallas_call(
        lambda *refs: back_kernel(n, chunk, piece, depth, *refs),
        in_specs=[pl.BlockSpec(memory_space=pltpu.SMEM)] + [anyw] * (LOADS + 2),
        out_specs=[vmem] * 7,
        out_shape=[
            jax.ShapeDtypeStruct((n * chunk, wf), bf16),
            jax.ShapeDtypeStruct((n * chunk, wf), bf16),
            jax.ShapeDtypeStruct((n * small_chunk, depth), bf16),
            jax.ShapeDtypeStruct((n * small_chunk, depth), bf16),
            jax.ShapeDtypeStruct((n * piece, 128), f32),
            jax.ShapeDtypeStruct((rows, depth), bf16),
            jax.ShapeDtypeStruct((rows, depth), bf16),
        ],
        scratch_shapes=[pltpu.VMEM(a.shape, a.dtype) for a in held]
        + [
            dma((LOADS,)),
            heads, heads, heads, heads, heads, heads, heads, part, part, part, part,
            pltpu.VMEM((BLK, width), f32),
            pltpu.VMEM((width, seq_len), f32),
            pltpu.VMEM((width, seq_len), f32),
            pltpu.VMEM((HD, seq_len), f32),
            pltpu.VMEM((8, seq_len), f32),
            pltpu.VMEM((BLK, seq_len), f32),
            pltpu.VMEM((width, BLK), bf16),
            pltpu.VMEM((width, BLK), bf16),
            pltpu.VMEM((seq_len, 128), bf16),
            pltpu.VMEM((rows, depth), bf16),
            pltpu.VMEM((rows, depth), bf16),
            pltpu.VMEM((3 * width, depth), bf16),
            pltpu.VMEM((3 * width, depth), bf16),
            pltpu.VMEM((width, depth), bf16),
            pltpu.VMEM((width, depth), bf16),
            pltpu.VMEM((n * small_chunk, depth), bf16),
            pltpu.VMEM((n * small_chunk, depth), bf16),
            *[pltpu.VMEM((h, depth), bf16) for h in (half, part_half, part_half)],
            pltpu.VMEM((shalf, 128), f32),
            *[pltpu.VMEM((h, depth), bf16) for h in (half, half, part_half, part_half)],
            pltpu.VMEM((shalf, 128), f32),
            *[
                pltpu.VMEM((m - 1, c, depth), bf16)
                for c in (chunk, chunk, small_chunk, small_chunk)
            ],
            pltpu.VMEM((m - 1, piece, 128), f32),
            pltpu.VMEM((ranks, piece, 128), f32),
            pltpu.VMEM((n * piece, 128), f32),
            pltpu.VMEM((n * piece, 128), f32),
            pltpu.VMEM((rows, depth), bf16),
            *[pltpu.VMEM((2 * HD, depth), bf16)] * 3,
            dma, dma,
            dma((3,)), dma((3,)),
            dma((2,)), dma((2,)),
            dma((5,)), dma((5,)),
            dma((5, m - 1)), dma((5, m - 1)),
            dma((3,)), dma((3,)),
            dma((5, m - 1)), dma((5, m - 1)),
            dma((5, m)), dma((5, m)),
        ],
        compiler_params=pltpu.CompilerParams(
            collective_id=0, has_side_effects=True, vmem_limit_bytes=63 * 1024 * 1024
        ),
        name="go_back",
    )(lengths, down_g, branch_x, *held)


def shards(
    hidden_in,
    lengths,
    ln1_gain,
    ln1_shift,
    qkv_weight,
    qv_bias,
    out_weight,
    out_bias,
    ln2_gain,
    ln2_shift,
    up_weight,
    up_bias,
    down_weight,
    down_bias,
    out_grad,
):
    n = lax.axis_size("dp")
    ranks = lax.axis_size("tensor")
    me = lax.axis_index("tensor")
    depth = hidden_in.shape[1]
    width = qkv_weight.shape[2]
    hidden = up_bias.shape[0]
    padded = -(-depth // (16 * n)) * 16 * n
    spot = jnp.arange(8)[:, None]
    vecs = jnp.zeros((8, depth), f32)
    for j, vec in enumerate(
        (out_bias, ln2_gain, ln2_shift, down_bias, up_bias.astype(f32), ln1_gain, ln1_shift)
    ):
        vecs = jnp.where(spot == j, vec[None], vecs)
    qkv_rows = jnp.swapaxes(qkv_weight, 1, 2).reshape(3 * width, depth)
    (normed, q1, k1, v1, lse1, o1, q2, k2, v2, lse2, o2, fence, sq, sk, qkv_far, out_far, sel_w,
     *grad_rows) = front(lengths, hidden_in, out_grad, vecs, qkv_rows, qv_bias, out_weight)
    attn_rows, grad_middle, partial, branch_x, up_part, down_part, sums, up_got = feed_forward(
        padded, o1, o2, out_weight, out_far, hidden_in, grad_rows, vecs, up_weight, down_weight
    )
    full_u, full_d, full_b, full_a, small, input_grad, output = go_back(
        n, (q1, k1, v1, lse1), (q2, k2, v2, lse2), fence, sq, sk, attn_rows, o1, o2,
        out_weight, out_far, normed, qkv_rows, qkv_far, sel_w, hidden_in, vecs,
        grad_middle, sums, partial, branch_x, lengths, up_part, up_got, down_part,
    )
    vectors = small[: 6 * depth // 128].reshape(6, depth)
    lines = (6 * depth + ranks * hidden) // 128
    up_all = small[6 * depth // 128 : lines].reshape(ranks, hidden)
    qv_all = small[lines : lines + 4 * ranks].reshape(ranks, 2, 256)
    up_bias_grad = lax.dynamic_index_in_dim(up_all, me, 0, keepdims=False)
    qv_bias_grad = lax.dynamic_index_in_dim(qv_all, me, 0, keepdims=False)[:, :width]
    qkv_grad = jnp.concatenate([full_b[: 2 * width], full_a[:width]], 0).astype(f32)
    qkv_grad = jnp.swapaxes(qkv_grad.reshape(3, width, depth), 1, 2)
    out_weight_grad = full_a[width : 2 * width].astype(f32)
    return (
        output,
        input_grad,
        vectors[0],
        vectors[1],
        qkv_grad,
        qv_bias_grad,
        out_weight_grad,
        vectors[2],
        vectors[3],
        vectors[4],
        full_u[:depth].astype(f32),
        up_bias_grad,
        full_d[:depth].astype(f32),
        vectors[5],
    )


def solution(mesh):
    return jax.shard_map(
        shards,
        mesh=mesh,
        in_specs=(
            P(("dp", "tensor"), None),
            P("dp"),
            P(),
            P(),
            P(None, None, "tensor"),
            P(None, "tensor"),
            P("tensor", None),
            P(),
            P(),
            P(),
            P(None, "tensor"),
            P("tensor"),
            P("tensor", None),
            P(),
            P(("dp", "tensor"), None),
        ),
        out_specs=(
            P(("dp", "tensor"), None),
            P(("dp", "tensor"), None),
            P(),
            P(),
            P(None, None, "tensor"),
            P(None, "tensor"),
            P("tensor", None),
            P(),
            P(),
            P(),
            P(None, "tensor"),
            P("tensor"),
            P("tensor", None),
            P(),
        ),
        check_vma=False,
    )
```

```python
import math

import jax
import jax.numpy as jnp
from jax import lax
from jax.experimental import pallas as pl
from jax.experimental.pallas import tpu as pltpu
from jax.sharding import PartitionSpec as P

HD = 64
BLK = 256
BIG = 1e30
sel_factor = 4.0
score_scale = 1.0 / math.sqrt(HD)
f32 = jnp.float32
bf16 = jnp.bfloat16


def mm(a, b):
    return lax.dot_general(a, b, (((1,), (0,)), ((), ())), preferred_element_type=f32)


def mm_nt(a, b):
    return lax.dot_general(a, b, (((1,), (1,)), ((), ())), preferred_element_type=f32)


def flip(a):
    return a.astype(f32).T.astype(bf16)


def split_mm(tri, x):
    hi = x.astype(bf16)
    lo = (x - hi.astype(f32)).astype(bf16)
    return mm(tri, hi) + mm(tri, lo)


def head_mask(h, width):
    return lax.broadcasted_iota(jnp.int32, (BLK, width), 1) // HD == h


def masked_rows(x, mask, scale):
    return jnp.where(mask, x.astype(f32) * scale, 0.0).astype(bf16)


def fwd_block(i, heads, first, q_ref, k_ref, v_ref, fence, o_ref, lse_ref):
    width = q_ref.shape[1]
    cols = (i + 1) * BLK
    keys = k_ref[:cols, :]
    vals = v_ref[:cols, :]
    fenced = fence[:, :cols]
    lane = lax.broadcasted_iota(jnp.int32, (BLK, 128), 1)
    lse_ref[...] = jnp.zeros_like(lse_ref)
    out_scr = first

    def head(h, _):
        mask = head_mask(h, width)
        s = mm_nt(masked_rows(q_ref[...], mask, score_scale), keys) - fenced
        top = jnp.max(s, -1, keepdims=True)
        e = jnp.exp(s - top)
        total = jnp.sum(e, -1, keepdims=True)
        p = (e * (1.0 / total)).astype(bf16)
        out = mm(p, vals)
        out_scr[...] = jnp.where(mask, out, out_scr[...])
        lse_ref[...] = jnp.where(lane == h, top + jnp.log(total), lse_ref[...])
        return 0

    lax.fori_loop(0, heads, head, 0, unroll=True)
    o_ref[...] = out_scr[...].astype(bf16)


def make_fence(i, seq_len, length, sq_ref, sk_ref, fence, carry):
    cols = (i + 1) * BLK
    s0 = mm_nt(sq_ref[...], sk_ref[:cols, :]) * score_scale
    row = i * BLK + lax.broadcasted_iota(jnp.int32, (BLK, cols), 0)
    col = lax.broadcasted_iota(jnp.int32, (BLK, cols), 1)
    picked = (col >= 1) & (col < row)
    sel = jnp.where(picked, jnp.maximum(s0, 0.0), 0.0) * (sel_factor / seq_len)
    r2 = lax.broadcasted_iota(jnp.int32, (BLK, BLK), 0)
    c2 = lax.broadcasted_iota(jnp.int32, (BLK, BLK), 1)
    tri = jnp.where(c2 < r2, 1.0, 0.0).astype(bf16)
    total = carry[0:1, :cols] + split_mm(tri, sel)
    carry[0:1, :cols] = total[BLK - 1 : BLK, :] + sel[BLK - 1 : BLK, :]
    fence[:, :cols] = jnp.where((col <= row) & (col < length), total, BIG)


def bwd_block(i, heads, q_ref, k_ref, v_ref, do_ref, lse_ref, f_ref, sq_ref, sk_ref,
              dq_ref, dsq_ref, dq_scr, dkt, dvt, dskt, later, fsum, qt, dot_):
    width = q_ref.shape[1]
    seq_len = k_ref.shape[0]
    cols = (i + 1) * BLK
    keys = k_ref[:cols, :]
    vals = v_ref[:cols, :]
    lane = lax.broadcasted_iota(jnp.int32, (BLK, 128), 1)
    qt[...] = (q_ref[...].astype(f32) * score_scale).T.astype(bf16)
    dot_[...] = flip(do_ref[...])
    fsum[:, :cols] = jnp.zeros((BLK, cols), f32)

    def head(h, _):
        mask = head_mask(h, width)
        lse = jnp.sum(jnp.where(lane == h, lse_ref[...], 0.0), -1, keepdims=True)
        s = mm_nt(masked_rows(q_ref[...], mask, score_scale), keys)
        p = jnp.exp(s - f_ref[:, :cols] - lse)
        dp = mm_nt(masked_rows(do_ref[...], mask, 1.0), vals)
        delta = jnp.sum(p * dp, -1, keepdims=True)
        g = (p * (dp - delta)).astype(bf16)
        rows = pl.ds(pl.multiple_of(h * HD, HD), HD)
        dq_scr[...] = jnp.where(mask, mm(g, keys), dq_scr[...])
        dkt[rows, :cols] += mm(qt[rows, :], g)
        dvt[rows, :cols] += mm(dot_[rows, :], p.astype(bf16))
        fsum[:, :cols] += g.astype(f32)
        return 0

    lax.fori_loop(0, heads, head, 0, unroll=True)
    dq_ref[...] = (dq_scr[...] * score_scale).astype(bf16)
    grad = -fsum[:, :cols]
    r2 = lax.broadcasted_iota(jnp.int32, (BLK, BLK), 0)
    c2 = lax.broadcasted_iota(jnp.int32, (BLK, BLK), 1)
    tri = jnp.where(c2 > r2, 1.0, 0.0).astype(bf16)
    dsel = later[0:1, :cols] + split_mm(tri, grad)
    later[0:1, :cols] = dsel[0:1, :] + grad[0:1, :]
    s0 = mm_nt(sq_ref[...], sk_ref[:cols, :])
    row = i * BLK + lax.broadcasted_iota(jnp.int32, (BLK, cols), 0)
    col = lax.broadcasted_iota(jnp.int32, (BLK, cols), 1)
    keep = (col >= 1) & (col < row) & (s0 > 0)
    gsel = jnp.where(keep, dsel * (sel_factor / seq_len), 0.0).astype(bf16)
    dsq_ref[...] = mm(gsel, sk_ref[:cols, :]) * score_scale
    sqt = (sq_ref[...].astype(f32) * score_scale).T.astype(bf16)
    dskt[:, :cols] += mm(sqt, gsel)


epsilon = 1e-05


def mm_tn(a, b):
    return lax.dot_general(a, b, (((0,), (0,)), ((), ())), preferred_element_type=f32)


def send(src, dst, send_sem, recv_sem, **where):
    copy = pltpu.make_async_remote_copy(
        src_ref=src,
        dst_ref=dst,
        send_sem=send_sem,
        recv_sem=recv_sem,
        device_id=where,
        device_id_type=pl.DeviceIdType.MESH,
    )
    copy.start()
    return copy


def meet(devices):
    barrier = pltpu.get_barrier_semaphore()
    for where in devices:
        pl.semaphore_signal(barrier, inc=1, device_id=where, device_id_type=pl.DeviceIdType.MESH)
    pl.semaphore_wait(barrier, len(devices))


def norm_parts(x):
    centre = x - jnp.mean(x, -1, keepdims=True)
    r = lax.rsqrt(jnp.mean(centre * centre, -1, keepdims=True) + epsilon)
    return centre * r, r


def norm_back(e, xhat, r):
    return r * (e - jnp.mean(e, -1, keepdims=True) - xhat * jnp.mean(e * xhat, -1, keepdims=True))


def gelu_pair(u):
    k = math.sqrt(2.0 / math.pi)
    square = u * u
    t = jnp.tanh(k * u * (1.0 + 0.044715 * square))
    act = 0.5 * u * (1.0 + t)
    slope = 0.5 * (1.0 + t) + 0.5 * u * (1.0 - t * t) * (k * (1.0 + 3.0 * 0.044715 * square))
    return act, slope


def feed_kernel(
    o1, o2, wo1, wo2, hidden, g0, g1, g2, g3, vecs, up, down,
    rows_out, gmid, partial, branch_x, up_g, down_g, sums, up_recv,
    inner, gs, act, gpre, mid, attn_send, attn_recv,
    near_send, near_recv, far_send, far_recv, x_send, x_recv,
    bn_send, bn_recv, bf_send, bf_recv, gin, acc_u, acc_d,
    g_sem, a_s, a_r, i_s, i_r, x_s, x_r, f_s, f_r, n_s, n_r, c_s, c_r, r_s, r_r, b_s, b_r, o_s, o_r, u_s, u_r,
):
    me = lax.axis_index("tensor")
    odd = lax.rem(me, 2)
    core = me + 1 - 2 * odd
    far = lax.rem(me + 2, 4)
    rows = hidden.shape[0]
    pieces = rows // BLK
    idx = lax.axis_index("dp")
    par = lax.rem(idx, 2)
    ydev = idx + 1 - 2 * par
    loads = [pltpu.make_async_copy(g, gs.at[i], g_sem.at[i]) for i, g in enumerate((g0, g1, g2, g3))]
    for c in loads:
        c.start()
    meet([{"tensor": core}, {"tensor": far}, {"dp": ydev}])
    out_bias, gain, shift, down_bias, up_bias = (vecs[j : j + 1, :] for j in range(5))

    def attn(start):
        part = pl.ds(pl.multiple_of(start, BLK), BLK)
        return mm(o1[part, :], wo1[...]) + mm(o2[part, :], wo2[...])

    sends = []
    attn_copies = []
    for c in range(pieces):
        here = pl.ds(c * BLK, BLK)
        attn_send[here, :] = attn((1 - odd) * rows + c * BLK).astype(bf16)
        attn_copies.append(send(attn_send.at[here], attn_recv.at[here], a_s.at[c], a_r.at[c], tensor=core))
    inner_copies, far_copies = [], []
    for c in range(pieces):
        here = pl.ds(c * BLK, BLK)
        mine = attn(odd * rows + c * BLK)
        attn_copies[c].wait_recv()
        m = hidden[here, :].astype(f32) + (mine + attn_recv[here, :].astype(f32)) + out_bias
        mid[here, :] = m
        xhat, r = norm_parts(m)
        inner[0, here, :] = (xhat * gain + shift).astype(bf16)
        far_copies.append(send(inner.at[0, here], inner.at[2, here], x_s.at[c], x_r.at[c], tensor=far))
        inner_copies.append(send(inner.at[0, here], inner.at[1, here], i_s.at[c], i_r.at[c], tensor=core))
    sends += attn_copies + inner_copies + far_copies
    for c in loads:
        c.wait()
    sums[...] = jnp.zeros_like(sums)

    def feed(slot, start):
        part = pl.ds(pl.multiple_of(start, BLK), BLK)
        pre = mm(inner[slot, part, :], up[...]) + up_bias
        a, slope = gelu_pair(pre)
        act[slot, part, :] = a.astype(bf16)
        gp = (mm_nt(gs[slot, part, :], down[...]) * slope).astype(bf16)
        gpre[slot, part, :] = gp
        sums[4:5, :] += jnp.sum(gp.astype(f32), 0, keepdims=True)

    def near(i, _):
        @pl.when(i == pieces)
        def _():
            for c in inner_copies:
                c.wait_recv()

        feed(i // pieces, lax.rem(i, pieces) * BLK)
        return 0

    lax.fori_loop(0, 2 * pieces, near, 0)

    def near_other(c, _):
        part = pl.ds(pl.multiple_of(c * BLK, BLK), BLK)
        near_send[part, :] = mm_nt(gpre[1, part, :], up[...]).astype(bf16)
        bn_send[part, :] = mm(act[1, part, :], down[...]).astype(bf16)
        return 0

    lax.fori_loop(0, pieces, near_other, 0)
    near_copy = send(near_send, near_recv, n_s.at[0], n_r.at[0], tensor=core)
    branch_copy = send(bn_send, bn_recv, n_s.at[1], n_r.at[1], tensor=core)

    def near_own(c, _):
        part = pl.ds(pl.multiple_of(c * BLK, BLK), BLK)
        gin[part, :] = mm_nt(gpre[0, part, :], up[...])
        partial[part, :] = mid[part, :] + mm(act[0, part, :], down[...]) + down_bias
        return 0

    lax.fori_loop(0, pieces, near_own, 0)

    def plan(src, dst, c, send_sem, recv_sem, where):
        here = pl.ds(pl.multiple_of(c * BLK, BLK), BLK)
        return pltpu.make_async_remote_copy(
            src_ref=src.at[here], dst_ref=dst.at[here], send_sem=send_sem.at[c],
            recv_sem=recv_sem.at[c], device_id={"tensor": where},
            device_id_type=pl.DeviceIdType.MESH,
        )

    def arrive(c):
        return plan(inner.at[0], inner.at[2], c, x_s, x_r, far)

    def hand_on(c):
        return plan(inner.at[2], inner.at[3], c, f_s, f_r, core)

    def crossed(c):
        return plan(far_send, far_recv, c, c_s, c_r, core)

    def back(c):
        return plan(x_send, x_recv, c, r_s, r_r, far)

    depth = up.shape[0]
    if up_g.shape[0] > depth:
        up_g[depth:, :] = jnp.zeros((up_g.shape[0] - depth, up_g.shape[1]), bf16)
        down_g[depth:, :] = jnp.zeros((up_g.shape[0] - depth, up_g.shape[1]), bf16)

    def weights(first, left, right, out, base=None):
        def tile(j, _):
            part = pl.ds(pl.multiple_of(j * BLK, BLK), BLK)
            total = mm_tn(left[first, :, part], right[first])
            total = total + mm_tn(left[first + 1, :, part], right[first + 1])
            if base is not None:
                total = total + base[part, :]
            out[part, :] = total.astype(out.dtype)
            return 0

        lax.fori_loop(0, depth // BLK, tile, 0)

    def far_step(i, _):
        c = i // 2
        which = lax.rem(i, 2)
        here = pl.ds(pl.multiple_of(c * BLK, BLK), BLK)

        @pl.when(which == 0)
        def _():
            arrive(c).wait_recv()
            hand_on(c).start()

        @pl.when(which == 1)
        def _():
            hand_on(c).wait_recv()

        feed(2 + which, c * BLK)

        @pl.when(which == 1)
        def _():
            far_send[here, :] = mm_nt(gpre[3, here, :], up[...]).astype(bf16)
            crossed(c).start()
            g = mm_nt(gpre[2, here, :], up[...])
            crossed(c).wait_recv()
            x_send[here, :] = (g + far_recv[here, :].astype(f32)).astype(bf16)
            back(c).start()

        @pl.when(i == 1)
        def _():
            weights(0, inner, gpre, acc_u)
            weights(0, act, gs, acc_d)

        return 0

    lax.fori_loop(0, 2 * pieces, far_step, 0)

    def far_out(c, _):
        here = pl.ds(pl.multiple_of(c * BLK, BLK), BLK)
        bf_send[here, :] = mm(act[3, here, :], down[...]).astype(bf16)
        return 0

    weights(2, inner, gpre, up_g, acc_u)
    half = up_g.shape[0] // 2
    give = pl.ds(pl.multiple_of((1 - par) * half, half), half)
    up_copy = send(up_g.at[give], up_recv, u_s, u_r, dp=ydev)
    lax.fori_loop(0, pieces, far_out, 0)
    far_branch = send(bf_send, bf_recv, b_s, b_r, tensor=core)
    weights(2, act, gs, down_g, acc_d)
    far_branch.wait_recv()
    for c in range(pieces):
        here = pl.ds(c * BLK, BLK)
        b = mm(act[2, here, :], down[...])
        branch_x[here, :] = (b + bf_recv[here, :].astype(f32)).astype(bf16)
    near_copy.wait_recv()
    branch_copy.wait_recv()
    partial[...] += bn_recv[...].astype(f32)
    rows_copies = []
    for c in range(pieces):
        here = pl.ds(c * BLK, BLK)
        xhat, r = norm_parts(mid[here, :])
        back(c).wait_recv()
        g = gin[here, :] + near_recv[here, :].astype(f32) + x_recv[here, :].astype(f32)
        g_out = gs[0, here, :].astype(f32)
        gm = g_out + norm_back(g * gain, xhat, r)
        gmid[here, :] = gm
        there = pl.ds(pl.multiple_of(odd * rows + c * BLK, BLK), BLK)
        ga = gm.astype(bf16)
        rows_out[there, :] = ga
        rows_copies.append(
            send(rows_out.at[there], rows_out.at[there], o_s.at[c], o_r.at[c], tensor=core)
        )
        sums[0:1, :] += jnp.sum(g * xhat, 0, keepdims=True)
        sums[1:2, :] += jnp.sum(g, 0, keepdims=True)
        sums[2:3, :] += jnp.sum(ga.astype(f32), 0, keepdims=True)
        sums[3:4, :] += jnp.sum(g_out, 0, keepdims=True)
    for c in rows_copies:
        c.wait_recv()
    up_copy.wait_recv()
    for c in range(pieces):
        sends += [hand_on(c), crossed(c), back(c)]
    for c in sends + rows_copies + [near_copy, branch_copy, far_branch, up_copy]:
        c.wait_send()


def feed_forward(padded, o1, o2, wo1, wo2, hidden, gs, vecs, up, down):
    rows, depth = hidden.shape
    width = up.shape[1]
    pieces = rows // BLK
    vmem = pl.BlockSpec(memory_space=pltpu.VMEM)
    anyw = pl.BlockSpec(memory_space=pl.ANY)
    dma = pltpu.SemaphoreType.DMA
    wide = pltpu.VMEM((rows, depth), bf16)
    each = [dma((pieces,))] * 2
    return pl.pallas_call(
        feed_kernel,
        in_specs=[vmem] * 5 + [anyw] * 4 + [vmem] * 3,
        out_specs=[vmem] * 8,
        out_shape=[
            jax.ShapeDtypeStruct((2 * rows, depth), bf16),
            jax.ShapeDtypeStruct((rows, depth), f32),
            jax.ShapeDtypeStruct((rows, depth), f32),
            jax.ShapeDtypeStruct((rows, depth), bf16),
            jax.ShapeDtypeStruct((padded, width), bf16),
            jax.ShapeDtypeStruct((padded, width), bf16),
            jax.ShapeDtypeStruct((8, depth), f32),
            jax.ShapeDtypeStruct((padded // 2, width), bf16),
        ],
        scratch_shapes=[
            pltpu.VMEM((4, rows, depth), bf16),
            pltpu.VMEM((4, rows, depth), bf16),
            pltpu.VMEM((4, rows, width), bf16),
            pltpu.VMEM((4, rows, width), bf16),
            pltpu.VMEM((rows, depth), f32),
            wide, wide, wide, wide, wide, wide, wide, wide, wide, wide, wide, wide,
            pltpu.VMEM((rows, depth), f32),
            pltpu.VMEM((depth, width), f32),
            pltpu.VMEM((depth, width), f32),
            dma((4,)),
            *each, *each, *each, *each,
            dma((2,)), dma((2,)),
            *each, *each,
            dma, dma,
            *each,
            dma, dma,
        ],
        compiler_params=pltpu.CompilerParams(
            collective_id=1, has_side_effects=True, vmem_limit_bytes=62 * 1024 * 1024
        ),
        name="feed_forward",
    )(o1, o2, wo1, wo2, hidden, *gs, vecs, up, down)

def back_kernel(n, chunk, piece, depth, lengths, down_h, branch_x, *rest):
    held, outs = rest[:LOADS], rest[LOADS : LOADS + 7]
    back_body(n, chunk, piece, depth, lengths, down_h, branch_x, held, outs, *rest[LOADS + 7 :])


LOADS = 28


def back_body(
    n, chunk, piece, depth, lengths, down_h, branch_x, held, outs,
    up_g, up_recv, rows_in, os, wo, qkv, lse, fence, sq, sk, normed, down_g, w, sel_w,
    hidden, gmid, vecs, sums, partial, ld_s,
    go, grads, dsums,
    dq_scr, dkt, dvt, dskt, later, fsum, qt, dot_,
    dsel, ng_send, ng_recv, ng_own, far_s, far_r, faro_s, faro_r, gb, ga,
    yd, yb, ya, ys, su, sd, sb, sa, ss, zu, zd, zb, za, zs,
    ts, small, out_s, bx_recv, sel_mine, sel_core, sel_far,
    core_s, core_r, f_s, f_r, sl_s, sl_r, y_s, y_r, z_s, z_r, t_s, t_r, az_s, az_r, ay_s, ay_r,
):
    fu, fd, fb, fa, small_out, input_grad, output = outs
    places = (
        up_g, up_recv, rows_in, os.at[0], wo.at[0], qkv.at[0, 0], qkv.at[0, 1], qkv.at[0, 2],
        lse.at[0], fence, sq, sk, normed, down_g, wo.at[1], qkv.at[1, 0], qkv.at[1, 1],
        qkv.at[1, 2], lse.at[1], w.at[0], w.at[1], sel_w, os.at[1], hidden, gmid, vecs, sums, partial,
    )
    idx = lax.axis_index("dp")
    par = lax.rem(idx, 2)
    m = n // 2
    own = pl.ds(pl.multiple_of(par * m * chunk, m * chunk), m * chunk)
    loads = [
        pltpu.make_async_copy(h.at[own] if j in (0, 13) else h, v, ld_s.at[j])
        for j, (h, v) in enumerate(zip(held, places))
    ]
    for c in loads:
        c.start()

    def need(*which):
        for j in which:
            loads[j].wait()

    me = lax.axis_index("tensor")
    odd = lax.rem(me, 2)
    z = lax.div(idx, 2)
    rows = hidden.shape[0]
    seq_len = normed.shape[0]
    width = wo.shape[1]
    heads = width // HD
    ranks = 4
    core = me + 1 - 2 * odd
    far = lax.rem(me + 2, ranks)
    ydev = idx + 1 - 2 * par
    peers = [lax.rem(me + d, ranks) for d in range(1, ranks)]
    zdev = [lax.rem(z + d, m) for d in range(1, m)]
    length = jnp.where(me < 2, lengths[0], lengths[1])
    meet(
        [{"tensor": p} for p in peers]
        + [{"dp": ydev}]
        + [{"dp": 2 * p + par} for p in zdev]
    )
    at = par * m + z
    source = (gb, ga, small, up_g, down_g)
    yrecv = (yb, ya, ys, up_recv, yd)
    ysum = (sb, sa, ss, su, sd)
    zrecv = (zb, za, zs, zu, zd)
    full = (fb, fa, out_s, fu, fd)
    size = (gb.shape[0] // n, ga.shape[0] // n, piece, chunk, chunk)

    def plan(src, dst, send_sem, recv_sem, **where):
        return pltpu.make_async_remote_copy(
            src_ref=src, dst_ref=dst, send_sem=send_sem, recv_sem=recv_sem,
            device_id=where, device_id_type=pl.DeviceIdType.MESH,
        )

    def block(start, k):
        return pl.ds(pl.multiple_of(start * size[k], size[k]), size[k])

    def y_copy(k):
        half = m * size[k]
        give = pl.ds(pl.multiple_of((1 - par) * half, half), half)
        src = down_h if k == 4 else source[k]
        return plan(src.at[give], yrecv[k], y_s.at[k], y_r.at[k], dp=ydev)

    def z_copy(k, d):
        return plan(
            ysum[k].at[block(zdev[d], k)], zrecv[k].at[d], z_s.at[k, d], z_r.at[k, d],
            dp=2 * zdev[d] + par,
        )

    def az_copy(k, d):
        mine = full[k].at[block(at, k)]
        return plan(mine, mine, az_s.at[k, d], az_r.at[k, d], dp=2 * zdev[d] + par)

    def ay_copy(k, d):
        came = full[k].at[block(par * m + lax.rem(z - d + m, m), k)]
        return plan(came, came, ay_s.at[k, d], ay_r.at[k, d], dp=ydev)

    def y_finish(k):
        half = m * size[k]
        keep = pl.ds(pl.multiple_of(par * half, half), half)
        if k != 3:
            y_copy(k).wait_recv()
        mine = source[k][...] if k > 2 else source[k][keep, :]
        total = mine.astype(f32) + yrecv[k][...].astype(f32)
        ysum[k][...] = total.astype(ysum[k].dtype)
        for d in range(m - 1):
            z_copy(k, d).start()

    def z_finish(k):
        acc = ysum[k][block(z, k), :].astype(f32)
        for d in range(m - 1):
            z_copy(k, d).wait_recv()
            acc = acc + zrecv[k][d].astype(f32)
        return acc

    def spread(k):
        for d in range(m - 1):
            az_copy(k, d).start()
        ay_copy(k, 0).start()

    def forward(k):
        for d in range(m - 1):
            az_copy(k, d).wait_recv()
            ay_copy(k, d + 1).start()

    far_copy = plan(far_s, far_r, f_s.at[1], f_r.at[1], tensor=far)
    out_copy = plan(faro_s, faro_r, f_s.at[0], f_r.at[0], tensor=far)
    branch_copy = plan(branch_x, bx_recv, f_s.at[2], f_r.at[2], tensor=far)
    core_copy = plan(ng_send, ng_recv, core_s, core_r, tensor=core)
    to_core = plan(sel_mine, sel_core, sl_s.at[0], sl_r.at[0], tensor=core)
    to_first = plan(sel_mine, sel_far, sl_s.at[1], sl_r.at[1], tensor=far)

    y_copy(4).start()
    need(0, 1)
    y_finish(3)
    need(2, 3)
    faro_s[...] = mm_tn(os[0], rows_in[...]).astype(bf16)
    out_copy.start()
    need(*range(4, 13))

    def hook(g, i):
        if i == 1:

            @pl.when(g == 0)
            def _():
                fu[block(at, 3), :] = z_finish(3).astype(bf16)
                spread(3)
                need(13)
                y_finish(4)

        if i == 2:

            @pl.when(g == 1)
            def _():
                forward(3)

    def group(g, _):
        @pl.when(g == 1)
        def _():
            need(*range(14, 19))

        def head_grad(j, _):
            here = pl.ds(pl.multiple_of(j * BLK, BLK), BLK)
            go[here, :] = mm_nt(rows_in[here, :], wo[g]).astype(bf16)
            return 0

        lax.fori_loop(0, seq_len // BLK, head_grad, 0)
        for r in (dkt, dvt, dskt, later):
            r[...] = jnp.zeros_like(r)
        for i in reversed(range(seq_len // BLK)):
            here = pl.ds(i * BLK, BLK)
            bwd_block(
                i, heads, qkv.at[g, 0, here], qkv.at[g, 1], qkv.at[g, 2], go.at[here],
                lse.at[g, here], fence.at[here], sq.at[here], sk,
                grads.at[g, 0, here], dsums.at[g, 0, here],
                dq_scr, dkt, dvt, dskt, later, fsum, qt, dot_,
            )
            hook(g, i)
        grads[g, 1] = dkt[...].T.astype(bf16)
        grads[g, 2] = dvt[...].T.astype(bf16)
        dsums[g, 1] = dskt[...].T

        @pl.when(g == 0)
        def _():
            def far_grad(j, _):
                here = pl.ds(pl.multiple_of(j * width, width), width)
                far_s[here, :] = mm_tn(grads[0, j], normed[...]).astype(bf16)
                return 0

            lax.fori_loop(0, 3, far_grad, 0)
            far_copy.start()
            branch_copy.start()

        return 0

    lax.fori_loop(0, 2, group, 0)
    dsel[:, :HD] = (dsums[0, 0] + dsums[1, 0]).astype(bf16)
    dsel[:, HD:] = (dsums[0, 1] + dsums[1, 1]).astype(bf16)
    sel_mine[...] = mm_tn(dsel[...], normed[...]).astype(bf16)

    @pl.when(odd == 1)
    def _():
        to_core.start()

    need(*range(19, LOADS))
    if gb.shape[0] > 2 * width:
        gb[2 * width :, :] = jnp.zeros((gb.shape[0] - 2 * width, depth), bf16)
        ga[2 * width :, :] = jnp.zeros((ga.shape[0] - 2 * width, depth), bf16)
    own_out = mm_tn(os[1], rows_in[...])
    out_copy.wait_recv()
    ga[width : 2 * width, :] = (own_out + faro_r[...].astype(f32)).astype(bf16)
    own_v = mm_tn(grads[1, 2], normed[...])
    far_copy.wait_recv()
    ga[:width, :] = (own_v + far_r[2 * width :, :].astype(f32)).astype(bf16)
    y_copy(1).start()

    def own_grad(j, _):
        here = pl.ds(pl.multiple_of(j * width, width), width)
        gb[here, :] = (mm_tn(grads[1, j], normed[...]) + far_r[here, :].astype(f32)).astype(bf16)
        return 0

    lax.fori_loop(0, 2, own_grad, 0)

    @pl.when(odd == 0)
    def _():
        to_core.wait_recv()
        sel_mine[...] = (sel_mine[...].astype(f32) + sel_core[...].astype(f32)).astype(bf16)

    @pl.when(me == 2)
    def _():
        to_first.start()

    def normed_grad(t, _):
        mine = t // 2
        step = pl.multiple_of(lax.rem(t, 2) * BLK, BLK)
        side = mine * odd + (1 - mine) * (1 - odd)
        part = pl.ds(pl.multiple_of(side * rows + step, BLK), BLK)
        here = pl.ds(step, BLK)
        total = mm(dsel[part, :], sel_w[...])
        for g in range(2):
            for j in range(3):
                total = total + mm(grads[g, j, part, :], w[g, j * width : (j + 1) * width, :])

        @pl.when(mine == 0)
        def _():
            ng_send[here, :] = total.astype(bf16)

        @pl.when(mine == 1)
        def _():
            ng_own[here, :] = total

        @pl.when(t == 1)
        def _():
            core_copy.start()

        return 0

    lax.fori_loop(0, 4, normed_grad, 0)

    @pl.when(me == 0)
    def _():
        to_first.wait_recv()
        both = sel_mine[...].astype(f32) + sel_far[...].astype(f32)
        gb[:HD, :] = (gb[:HD, :].astype(f32) + both[:HD, :]).astype(bf16)
        gb[width : width + HD, :] = (
            gb[width : width + HD, :].astype(f32) + both[HD:, :]
        ).astype(bf16)

    y_copy(0).start()
    fd[block(at, 4), :] = z_finish(4).astype(bf16)
    spread(4)
    y_finish(1)
    xhat, r = norm_parts(hidden[...].astype(f32))
    core_copy.wait_recv()
    grad = ng_own[...] + ng_recv[...].astype(f32)
    input_grad[...] = (gmid[...] + norm_back(grad * vecs[5:6, :], xhat, r)).astype(bf16)
    small[...] = jnp.zeros_like(small)
    dgain = jnp.sum(grad * xhat, 0, keepdims=True)
    dshift = jnp.sum(grad, 0, keepdims=True)
    lines = depth // 128
    for j in range(lines):
        small[j : j + 1, :] = dgain[:, j * 128 : (j + 1) * 128]
        small[lines + j : lines + j + 1, :] = dshift[:, j * 128 : (j + 1) * 128]
    for slot, which in ((2, 2), (3, 0), (4, 1), (5, 3)):
        for j in range(lines):
            small[slot * lines + j : slot * lines + j + 1, :] = sums[
                which : which + 1, j * 128 : (j + 1) * 128
            ]
    wide_lines = up_g.shape[1] // 128
    for j in range(wide_lines):
        small[pl.ds(6 * lines + me * wide_lines + j, 1), :] = sums[4:5, j * 128 : (j + 1) * 128]
    base = small_lines(depth, up_g.shape[1]) - 4 * ranks
    for owner, g in ((me, 1), (far, 0)):
        for j, which in enumerate((0, 2)):
            total = jnp.sum(grads[g, which].astype(f32), 0, keepdims=True)
            line = base + 4 * owner + 2 * j
            small[pl.ds(line, 1), :] = total[:, :128]
            small[pl.ds(line + 1, 1), : width - 128] = total[:, 128:]
    total = jnp.sum(dsel[...].astype(f32), 0, keepdims=True)
    lane = lax.broadcasted_iota(jnp.int32, total.shape, 1)
    small[base : base + 1, :] += jnp.where(lane < HD, total, 0.0)
    y_copy(2).start()

    y_finish(0)
    y_finish(2)
    forward(4)
    fa[block(at, 1), :] = z_finish(1).astype(bf16)
    spread(1)
    token = odd * rows + lax.broadcasted_iota(jnp.int32, (rows, 1), 0)
    live = jnp.where(token < length, 1.0, 0.0)
    branch_copy.wait_recv()
    output[...] = (live * (partial[...] + bx_recv[...].astype(f32))).astype(bf16)
    fb[block(at, 0), :] = z_finish(0).astype(bf16)
    spread(0)
    ts[me] = z_finish(2)

    def t_copy(d):
        return plan(ts.at[me], ts.at[me], t_s.at[d], t_r.at[d], tensor=peers[d])

    for d in range(ranks - 1):
        t_copy(d).start()
    for d in range(ranks - 1):
        t_copy(d).wait_recv()
    vec = ts[0]
    for d in range(1, ranks):
        vec = vec + ts[d]
    out_s[block(at, 2), :] = vec
    spread(2)
    forward(1)
    forward(0)
    forward(2)
    for k in range(5):
        for d in range(m):
            ay_copy(k, d).wait_recv()

    @pl.when(odd == 1)
    def _():
        to_core.wait_send()

    @pl.when(me == 2)
    def _():
        to_first.wait_send()

    small_out[...] = out_s[...]
    for c in (far_copy, out_copy, branch_copy, core_copy):
        c.wait_send()
    for d in range(ranks - 1):
        t_copy(d).wait_send()
    for k in range(5):
        if k != 3:
            y_copy(k).wait_send()
        for d in range(m - 1):
            z_copy(k, d).wait_send()
            az_copy(k, d).wait_send()
        for d in range(m):
            ay_copy(k, d).wait_send()


def front_kernel(
    lengths, hidden, out_grad, vecs, qkv, qv_bias, wo,
    *rest,
):
    outs, gcore, gfar, gcross = rest[:18], rest[18], rest[19], rest[20]
    kept = rest[21:39]
    front_body(
        lengths, hidden, out_grad, vecs, qkv, qv_bias, wo, outs, kept, gcore, gfar, gcross, *rest[39:]
    )


def front_body(
    lengths, hidden, out_grad, vecs, qkv, qv_bias, wo, outs, kept, gcore, gfar, gcross,
    out_scr, carry, sel_b, bias2,
    st_s, nm_s, nm_r, gc_s, gc_r, sl_s, sl_r, w_s, w_r, p_s, p_r, e_s, e_r, g_s, g_r, h_s, h_r,
):
    me = lax.axis_index("tensor")
    idx = lax.axis_index("dp")
    odd = lax.rem(me, 2)
    core = me + 1 - 2 * odd
    far = lax.rem(me + 2, 4)
    par = lax.rem(idx, 2)
    ydev = idx + 1 - 2 * par
    rows = hidden.shape[0]
    seq_len = 2 * rows
    width = wo.shape[0]
    heads = width // HD
    (normed, q1, k1, v1, lse1, o1, q2, k2, v2, lse2, o2, fence, sq, sk, w2, wo2, selw, g0) = kept
    stores = []

    def store(*which):
        for j in which:
            copy = pltpu.make_async_copy(kept[j], outs[j], st_s.at[j])
            copy.start()
            stores.append(copy)

    length = jnp.where(me < 2, lengths[0], lengths[1])

    def sel_copies(k, where):
        return [
            pltpu.make_async_remote_copy(
                src_ref=a, dst_ref=a, send_sem=sl_s.at[k, j], recv_sem=sl_r.at[j],
                device_id={"tensor": where}, device_id_type=pl.DeviceIdType.MESH,
            )
            for j, a in enumerate((selw, sel_b))
        ]

    @pl.when(me == 0)
    def _():
        selw[:HD, :] = qkv[:HD, :]
        selw[HD:, :] = qkv[width : width + HD, :]
        sel_b[...] = qv_bias[...]

    meet([{"tensor": core}, {"tensor": far}, {"dp": ydev}])

    @pl.when(me == 0)
    def _():
        for c in sel_copies(0, far) + sel_copies(1, core):
            c.start()

    share = width // 2
    halves = [
        (src, dst, pl.ds(pl.multiple_of(base + par * share, share), share))
        for src, dst, base in (
            (qkv, w2, 0), (qkv, w2, width), (qkv, w2, 2 * width), (wo, wo2, 0)
        )
    ]
    extra = send(qv_bias, bias2, e_s, e_r, tensor=far)
    cross = [
        send(src.at[part], dst.at[part], w_s.at[j], w_r.at[j], tensor=far)
        for j, (src, dst, part) in enumerate(halves)
    ]
    passed = []

    def pass_on(j):
        cross[j].wait_recv()
        _, dst, part = halves[j]
        passed.append(send(dst.at[part], dst.at[part], p_s.at[j], p_r.at[j], dp=ydev))

    spot = pl.multiple_of(odd * rows, rows)
    norm_copies = []
    for c in range(rows // BLK):
        here = pl.ds(c * BLK, BLK)
        there = pl.ds(pl.multiple_of(spot + c * BLK, BLK), BLK)
        xhat, _ = norm_parts(hidden[here, :].astype(f32))
        normed[there, :] = (xhat * vecs[5:6, :] + vecs[6:7, :]).astype(bf16)
        norm_copies.append(
            send(normed.at[there], normed.at[there], nm_s.at[c], nm_r.at[c], tensor=core)
        )
    row = odd * rows + lax.broadcasted_iota(jnp.int32, (rows, 1), 0)
    live = jnp.where(row < length, 1.0, 0.0)
    g0[...] = (out_grad[...].astype(f32) * live).astype(bf16)
    store(17)
    gc = send(g0, gcore, gc_s, gc_r, tensor=core)
    g_parts = [pl.ds(c * BLK, BLK) for c in range(rows // BLK)]
    gf = [
        send(g0.at[p], gfar.at[p], g_s.at[c], g_r.at[c], tensor=far) for c, p in enumerate(g_parts)
    ]

    def project(weight, bias, out):
        def tile(j, _):
            here = pl.ds(pl.multiple_of(j * BLK, BLK), BLK)
            y = mm_nt(normed[here, :], weight)
            if bias is not None:
                y = y + bias
            out[here, :] = y.astype(bf16)
            return 0

        lax.fori_loop(0, seq_len // BLK, tile, 0)

    @pl.when(me == 2)
    def _():
        for c in sel_copies(0, far):
            c.wait_recv()
        for c in sel_copies(1, core):
            c.start()

    for c in norm_copies:
        c.wait_recv()
    store(0)
    project(qkv[:width, :], qv_bias[0:1, :], q1)
    project(qkv[width : 2 * width, :], None, k1)
    project(qkv[2 * width :, :], qv_bias[1:2, :], v1)

    @pl.when(odd == 1)
    def _():
        for c in sel_copies(1, core):
            c.wait_recv()

    store(1, 2, 3)
    for j in range(seq_len // BLK):
        here = pl.ds(j * BLK, BLK)
        y = mm_nt(normed[here, :], selw[...])
        sq[here, :] = (y[:, :HD] + sel_b[0:1, :HD]).astype(bf16)
        sk[here, :] = y[:, HD:].astype(bf16)
    store(12, 13, 16)
    carry[...] = jnp.zeros_like(carry)
    pass_on(0)
    for i in range(seq_len // BLK):
        here = pl.ds(i * BLK, BLK)
        make_fence(i, seq_len, length, sq.at[here], sk, fence.at[here], carry)
        fwd_block(
            i, heads, out_scr, q1.at[here], k1, v1, fence.at[here], o1.at[here], lse1.at[here]
        )
        if i < 3:
            pass_on(i + 1)
    store(4, 5, 11)
    extra.wait_recv()
    for j, (out, bias) in enumerate(((q2, bias2[0:1, :]), (k2, None), (v2, bias2[1:2, :]))):
        passed[j].wait_recv()
        project(w2[j * width : (j + 1) * width, :], bias, out)
        store(6 + j)
    store(14)
    gx = []

    def pass_g(c):
        gf[c].wait_recv()
        p = g_parts[c]
        gx.append(send(gfar.at[p], gcross.at[p], h_s.at[c], h_r.at[c], tensor=core))

    for i in range(seq_len // BLK):
        here = pl.ds(i * BLK, BLK)
        fwd_block(
            i, heads, out_scr, q2.at[here], k2, v2, fence.at[here], o2.at[here], lse2.at[here]
        )
    store(9, 10)
    for c in range(rows // BLK):
        pass_g(c)
    gc.wait_recv()
    passed[3].wait_recv()
    store(15)
    for c in gx:
        c.wait_recv()

    @pl.when(me == 0)
    def _():
        for c in sel_copies(0, far):
            c.wait_send()

    @pl.when(odd == 0)
    def _():
        for c in sel_copies(1, core):
            c.wait_send()

    for c in cross + passed + norm_copies + gf + gx + [gc, extra]:
        c.wait_send()
    for c in stores:
        c.wait()


def front(lengths, hidden, out_grad, vecs, qkv, qv_bias, wo):
    rows, depth = hidden.shape
    seq_len, width = 2 * rows, wo.shape[0]
    pieces = rows // BLK
    vmem = pl.BlockSpec(memory_space=pltpu.VMEM)
    dma = pltpu.SemaphoreType.DMA
    heads = jax.ShapeDtypeStruct((seq_len, width), bf16)
    lse = jax.ShapeDtypeStruct((seq_len, 128), f32)
    sel = jax.ShapeDtypeStruct((seq_len, HD), bf16)
    wide = jax.ShapeDtypeStruct((rows, depth), bf16)
    kept = [
        jax.ShapeDtypeStruct((seq_len, depth), bf16),
        heads, heads, heads, lse, heads,
        heads, heads, heads, lse, heads,
        jax.ShapeDtypeStruct((seq_len, seq_len), f32),
        sel, sel,
        jax.ShapeDtypeStruct(qkv.shape, bf16),
        jax.ShapeDtypeStruct(wo.shape, bf16),
        jax.ShapeDtypeStruct((2 * HD, depth), bf16),
        wide,
    ]
    return pl.pallas_call(
        front_kernel,
        in_specs=[pl.BlockSpec(memory_space=pltpu.SMEM)] + [vmem] * 6,
        out_specs=[pl.BlockSpec(memory_space=pl.ANY)] * 21,
        out_shape=kept + [wide, wide, wide],
        scratch_shapes=[pltpu.VMEM(a.shape, a.dtype) for a in kept]
        + [
            pltpu.VMEM((BLK, width), f32),
            pltpu.VMEM((8, seq_len), f32),
            pltpu.VMEM((2, width), f32),
            pltpu.VMEM((2, width), f32),
            dma((18,)),
            dma((pieces,)), dma((pieces,)),
            dma, dma,
            dma((2, 2)), dma((2,)),
            dma((4,)), dma((4,)),
            dma((4,)), dma((4,)),
            dma, dma,
            dma((pieces,)), dma((pieces,)),
            dma((pieces,)), dma((pieces,)),
        ],
        compiler_params=pltpu.CompilerParams(
            collective_id=2, has_side_effects=True, vmem_limit_bytes=60 * 1024 * 1024
        ),
        name="front",
    )(lengths, hidden, out_grad, vecs, qkv, qv_bias, wo)


def small_lines(depth, hidden):
    return (6 * depth + 4 * hidden) // 128 + 16


def go_back(n, set1, set2, fence, sq, sk, rows_in, o1, o2, wo1, wo2, normed, w1, w2, sel_w,
            hidden, vecs, gmid, sums, partial, branch_x, lengths, up_g, up_recv, down_g):
    m = n // 2
    chunk = up_g.shape[0] // n
    rows, depth = hidden.shape
    piece = -(-small_lines(depth, up_g.shape[1]) // (8 * n)) * 8
    seq_len, width = set1[0].shape
    half, shalf = m * chunk, m * piece
    ranks = 4
    wf = up_g.shape[1]
    small_chunk = -(-2 * width // (16 * n)) * 16
    part_half = m * small_chunk
    vmem = pl.BlockSpec(memory_space=pltpu.VMEM)
    dma = pltpu.SemaphoreType.DMA
    q1, k1, v1, lse1 = set1
    q2, k2, v2, lse2 = set2
    held = (up_g, up_recv, rows_in, o2, wo2, q2, k2, v2, lse2, fence, sq, sk, normed, down_g, wo1,
            q1, k1, v1, lse1, w2, w1, sel_w, o1, hidden, gmid, vecs, sums, partial)
    anyw = pl.BlockSpec(memory_space=pl.ANY)
    like = lambda a: pltpu.VMEM(a.shape, a.dtype)
    return pl.pallas_call(
        lambda *refs: back_kernel(n, chunk, piece, depth, *refs),
        in_specs=[pl.BlockSpec(memory_space=pltpu.SMEM)] + [anyw] * (LOADS + 2),
        out_specs=[vmem] * 7,
        out_shape=[
            jax.ShapeDtypeStruct((n * chunk, wf), bf16),
            jax.ShapeDtypeStruct((n * chunk, wf), bf16),
            jax.ShapeDtypeStruct((n * small_chunk, depth), bf16),
            jax.ShapeDtypeStruct((n * small_chunk, depth), bf16),
            jax.ShapeDtypeStruct((n * piece, 128), f32),
            jax.ShapeDtypeStruct((rows, depth), bf16),
            jax.ShapeDtypeStruct((rows, depth), bf16),
        ],
        scratch_shapes=[
            like(up_recv), like(up_recv), like(rows_in),
            pltpu.VMEM((2, seq_len, width), bf16),
            pltpu.VMEM((2, width, depth), bf16),
            pltpu.VMEM((2, 3, seq_len, width), bf16),
            pltpu.VMEM((2, seq_len, 128), f32),
            like(fence), like(sq), like(sk), like(normed), like(up_recv),
            pltpu.VMEM((2, 3 * width, depth), bf16),
            like(sel_w), like(hidden), like(gmid), like(vecs), like(sums), like(partial),
            dma((LOADS,)),
            pltpu.VMEM((seq_len, width), bf16),
            pltpu.VMEM((2, 3, seq_len, width), bf16),
            pltpu.VMEM((2, 2, seq_len, HD), f32),
            pltpu.VMEM((BLK, width), f32),
            pltpu.VMEM((width, seq_len), f32),
            pltpu.VMEM((width, seq_len), f32),
            pltpu.VMEM((HD, seq_len), f32),
            pltpu.VMEM((8, seq_len), f32),
            pltpu.VMEM((BLK, seq_len), f32),
            pltpu.VMEM((width, BLK), bf16),
            pltpu.VMEM((width, BLK), bf16),
            pltpu.VMEM((seq_len, 128), bf16),
            pltpu.VMEM((rows, depth), bf16),
            pltpu.VMEM((rows, depth), bf16),
            pltpu.VMEM((rows, depth), f32),
            pltpu.VMEM((3 * width, depth), bf16),
            pltpu.VMEM((3 * width, depth), bf16),
            pltpu.VMEM((width, depth), bf16),
            pltpu.VMEM((width, depth), bf16),
            pltpu.VMEM((n * small_chunk, depth), bf16),
            pltpu.VMEM((n * small_chunk, depth), bf16),
            *[pltpu.VMEM((h, depth), bf16) for h in (half, part_half, part_half)],
            pltpu.VMEM((shalf, 128), f32),
            *[pltpu.VMEM((h, depth), bf16) for h in (half, half, part_half, part_half)],
            pltpu.VMEM((shalf, 128), f32),
            *[
                pltpu.VMEM((m - 1, c, depth), bf16)
                for c in (chunk, chunk, small_chunk, small_chunk)
            ],
            pltpu.VMEM((m - 1, piece, 128), f32),
            pltpu.VMEM((ranks, piece, 128), f32),
            pltpu.VMEM((n * piece, 128), f32),
            pltpu.VMEM((n * piece, 128), f32),
            pltpu.VMEM((rows, depth), bf16),
            *[pltpu.VMEM((2 * HD, depth), bf16)] * 3,
            dma, dma,
            dma((3,)), dma((3,)),
            dma((2,)), dma((2,)),
            dma((5,)), dma((5,)),
            dma((5, m - 1)), dma((5, m - 1)),
            dma((3,)), dma((3,)),
            dma((5, m - 1)), dma((5, m - 1)),
            dma((5, m)), dma((5, m)),
        ],
        compiler_params=pltpu.CompilerParams(
            collective_id=0, has_side_effects=True, vmem_limit_bytes=63 * 1024 * 1024
        ),
        name="go_back",
    )(lengths, down_g, branch_x, *held)


def shards(
    hidden_in,
    lengths,
    ln1_gain,
    ln1_shift,
    qkv_weight,
    qv_bias,
    out_weight,
    out_bias,
    ln2_gain,
    ln2_shift,
    up_weight,
    up_bias,
    down_weight,
    down_bias,
    out_grad,
):
    n = lax.axis_size("dp")
    ranks = lax.axis_size("tensor")
    me = lax.axis_index("tensor")
    depth = hidden_in.shape[1]
    width = qkv_weight.shape[2]
    hidden = up_bias.shape[0]
    padded = -(-depth // (16 * n)) * 16 * n
    spot = jnp.arange(8)[:, None]
    vecs = jnp.zeros((8, depth), f32)
    for j, vec in enumerate(
        (out_bias, ln2_gain, ln2_shift, down_bias, up_bias.astype(f32), ln1_gain, ln1_shift)
    ):
        vecs = jnp.where(spot == j, vec[None], vecs)
    qkv_rows = jnp.swapaxes(qkv_weight, 1, 2).reshape(3 * width, depth)
    (normed, q1, k1, v1, lse1, o1, q2, k2, v2, lse2, o2, fence, sq, sk, qkv_far, out_far, sel_w,
     *grad_rows) = front(lengths, hidden_in, out_grad, vecs, qkv_rows, qv_bias, out_weight)
    attn_rows, grad_middle, partial, branch_x, up_part, down_part, sums, up_got = feed_forward(
        padded, o1, o2, out_weight, out_far, hidden_in, grad_rows, vecs, up_weight, down_weight
    )
    full_u, full_d, full_b, full_a, small, input_grad, output = go_back(
        n, (q1, k1, v1, lse1), (q2, k2, v2, lse2), fence, sq, sk, attn_rows, o1, o2,
        out_weight, out_far, normed, qkv_rows, qkv_far, sel_w, hidden_in, vecs,
        grad_middle, sums, partial, branch_x, lengths, up_part, up_got, down_part,
    )
    vectors = small[: 6 * depth // 128].reshape(6, depth)
    lines = (6 * depth + ranks * hidden) // 128
    up_all = small[6 * depth // 128 : lines].reshape(ranks, hidden)
    qv_all = small[lines : lines + 4 * ranks].reshape(ranks, 2, 256)
    up_bias_grad = lax.dynamic_index_in_dim(up_all, me, 0, keepdims=False)
    qv_bias_grad = lax.dynamic_index_in_dim(qv_all, me, 0, keepdims=False)[:, :width]
    qkv_grad = jnp.concatenate([full_b[: 2 * width], full_a[:width]], 0).astype(f32)
    qkv_grad = jnp.swapaxes(qkv_grad.reshape(3, width, depth), 1, 2)
    out_weight_grad = full_a[width : 2 * width].astype(f32)
    return (
        output,
        input_grad,
        vectors[0],
        vectors[1],
        qkv_grad,
        qv_bias_grad,
        out_weight_grad,
        vectors[2],
        vectors[3],
        vectors[4],
        full_u[:depth].astype(f32),
        up_bias_grad,
        full_d[:depth].astype(f32),
        vectors[5],
    )


def solution(mesh):
    return jax.shard_map(
        shards,
        mesh=mesh,
        in_specs=(
            P(("dp", "tensor"), None),
            P("dp"),
            P(),
            P(),
            P(None, None, "tensor"),
            P(None, "tensor"),
            P("tensor", None),
            P(),
            P(),
            P(),
            P(None, "tensor"),
            P("tensor"),
            P("tensor", None),
            P(),
            P(("dp", "tensor"), None),
        ),
        out_specs=(
            P(("dp", "tensor"), None),
            P(("dp", "tensor"), None),
            P(),
            P(),
            P(None, None, "tensor"),
            P(None, "tensor"),
            P("tensor", None),
            P(),
            P(),
            P(),
            P(None, "tensor"),
            P("tensor"),
            P("tensor", None),
            P(),
        ),
        check_vma=False,
    )
```

```python
import math

import jax
import jax.numpy as jnp
from jax import lax
from jax.experimental import pallas as pl
from jax.experimental.pallas import tpu as pltpu
from jax.sharding import PartitionSpec as P

HD = 64
BLK = 256
BIG = 1e30
sel_factor = 4.0
score_scale = 1.0 / math.sqrt(HD)
f32 = jnp.float32
bf16 = jnp.bfloat16


def mm(a, b):
    return lax.dot_general(a, b, (((1,), (0,)), ((), ())), preferred_element_type=f32)


def mm_nt(a, b):
    return lax.dot_general(a, b, (((1,), (1,)), ((), ())), preferred_element_type=f32)


def flip(a):
    return a.astype(f32).T.astype(bf16)


def split_mm(tri, x):
    hi = x.astype(bf16)
    lo = (x - hi.astype(f32)).astype(bf16)
    return mm(tri, hi) + mm(tri, lo)


def head_mask(h, width):
    return lax.broadcasted_iota(jnp.int32, (BLK, width), 1) // HD == h


def masked_rows(x, mask, scale):
    return jnp.where(mask, x.astype(f32) * scale, 0.0).astype(bf16)


def fwd_block(i, heads, first, q_ref, k_ref, v_ref, fence, o_ref, lse_ref):
    width = q_ref.shape[1]
    cols = (i + 1) * BLK
    keys = k_ref[:cols, :]
    vals = v_ref[:cols, :]
    fenced = fence[:, :cols]
    lane = lax.broadcasted_iota(jnp.int32, (BLK, 128), 1)
    lse_ref[...] = jnp.zeros_like(lse_ref)
    out_scr = first

    def head(h, _):
        mask = head_mask(h, width)
        s = mm_nt(masked_rows(q_ref[...], mask, score_scale), keys) - fenced
        top = jnp.max(s, -1, keepdims=True)
        e = jnp.exp(s - top)
        total = jnp.sum(e, -1, keepdims=True)
        p = (e * (1.0 / total)).astype(bf16)
        out = mm(p, vals)
        out_scr[...] = jnp.where(mask, out, out_scr[...])
        lse_ref[...] = jnp.where(lane == h, top + jnp.log(total), lse_ref[...])
        return 0

    lax.fori_loop(0, heads, head, 0, unroll=True)
    o_ref[...] = out_scr[...].astype(bf16)


def make_fence(i, seq_len, length, sq_ref, sk_ref, fence, carry):
    cols = (i + 1) * BLK
    s0 = mm_nt(sq_ref[...], sk_ref[:cols, :]) * score_scale
    row = i * BLK + lax.broadcasted_iota(jnp.int32, (BLK, cols), 0)
    col = lax.broadcasted_iota(jnp.int32, (BLK, cols), 1)
    picked = (col >= 1) & (col < row)
    sel = jnp.where(picked, jnp.maximum(s0, 0.0), 0.0) * (sel_factor / seq_len)
    r2 = lax.broadcasted_iota(jnp.int32, (BLK, BLK), 0)
    c2 = lax.broadcasted_iota(jnp.int32, (BLK, BLK), 1)
    tri = jnp.where(c2 < r2, 1.0, 0.0).astype(bf16)
    total = carry[0:1, :cols] + split_mm(tri, sel)
    carry[0:1, :cols] = total[BLK - 1 : BLK, :] + sel[BLK - 1 : BLK, :]
    fence[:, :cols] = jnp.where((col <= row) & (col < length), total, BIG)


def bwd_block(i, heads, q_ref, k_ref, v_ref, do_ref, lse_ref, f_ref, sq_ref, sk_ref,
              dq_ref, dsq_ref, dq_scr, dkt, dvt, dskt, later, fsum, qt, dot_):
    width = q_ref.shape[1]
    seq_len = k_ref.shape[0]
    cols = (i + 1) * BLK
    keys = k_ref[:cols, :]
    vals = v_ref[:cols, :]
    lane = lax.broadcasted_iota(jnp.int32, (BLK, 128), 1)
    qt[...] = (q_ref[...].astype(f32) * score_scale).T.astype(bf16)
    dot_[...] = flip(do_ref[...])
    fsum[:, :cols] = jnp.zeros((BLK, cols), f32)

    def head(h, _):
        mask = head_mask(h, width)
        lse = jnp.sum(jnp.where(lane == h, lse_ref[...], 0.0), -1, keepdims=True)
        s = mm_nt(masked_rows(q_ref[...], mask, score_scale), keys)
        p = jnp.exp(s - f_ref[:, :cols] - lse)
        dp = mm_nt(masked_rows(do_ref[...], mask, 1.0), vals)
        delta = jnp.sum(p * dp, -1, keepdims=True)
        g = (p * (dp - delta)).astype(bf16)
        rows = pl.ds(pl.multiple_of(h * HD, HD), HD)
        dq_scr[...] = jnp.where(mask, mm(g, keys), dq_scr[...])
        dkt[rows, :cols] += mm(qt[rows, :], g)
        dvt[rows, :cols] += mm(dot_[rows, :], p.astype(bf16))
        fsum[:, :cols] += g.astype(f32)
        return 0

    lax.fori_loop(0, heads, head, 0, unroll=True)
    dq_ref[...] = (dq_scr[...] * score_scale).astype(bf16)
    grad = -fsum[:, :cols]
    r2 = lax.broadcasted_iota(jnp.int32, (BLK, BLK), 0)
    c2 = lax.broadcasted_iota(jnp.int32, (BLK, BLK), 1)
    tri = jnp.where(c2 > r2, 1.0, 0.0).astype(bf16)
    dsel = later[0:1, :cols] + split_mm(tri, grad)
    later[0:1, :cols] = dsel[0:1, :] + grad[0:1, :]
    s0 = mm_nt(sq_ref[...], sk_ref[:cols, :])
    row = i * BLK + lax.broadcasted_iota(jnp.int32, (BLK, cols), 0)
    col = lax.broadcasted_iota(jnp.int32, (BLK, cols), 1)
    keep = (col >= 1) & (col < row) & (s0 > 0)
    gsel = jnp.where(keep, dsel * (sel_factor / seq_len), 0.0).astype(bf16)
    dsq_ref[...] = mm(gsel, sk_ref[:cols, :]) * score_scale
    sqt = (sq_ref[...].astype(f32) * score_scale).T.astype(bf16)
    dskt[:, :cols] += mm(sqt, gsel)


epsilon = 1e-05


def mm_tn(a, b):
    return lax.dot_general(a, b, (((0,), (0,)), ((), ())), preferred_element_type=f32)


def send(src, dst, send_sem, recv_sem, **where):
    copy = pltpu.make_async_remote_copy(
        src_ref=src,
        dst_ref=dst,
        send_sem=send_sem,
        recv_sem=recv_sem,
        device_id=where,
        device_id_type=pl.DeviceIdType.MESH,
    )
    copy.start()
    return copy


def meet(devices):
    barrier = pltpu.get_barrier_semaphore()
    for where in devices:
        pl.semaphore_signal(barrier, inc=1, device_id=where, device_id_type=pl.DeviceIdType.MESH)
    pl.semaphore_wait(barrier, len(devices))


def norm_parts(x):
    centre = x - jnp.mean(x, -1, keepdims=True)
    r = lax.rsqrt(jnp.mean(centre * centre, -1, keepdims=True) + epsilon)
    return centre * r, r


def norm_back(e, xhat, r):
    return r * (e - jnp.mean(e, -1, keepdims=True) - xhat * jnp.mean(e * xhat, -1, keepdims=True))


def gelu_pair(u):
    k = math.sqrt(2.0 / math.pi)
    square = u * u
    t = jnp.tanh(k * u * (1.0 + 0.044715 * square))
    act = 0.5 * u * (1.0 + t)
    slope = 0.5 * (1.0 + t) + 0.5 * u * (1.0 - t * t) * (k * (1.0 + 3.0 * 0.044715 * square))
    return act, slope


def feed_kernel(
    o1, o2, wo1, wo2, hidden, g0, g1, g2, g3, vecs, up, down,
    rows_out, gmid, partial, branch_x, up_g, down_g, sums,
    inner, gs, act, gpre, mid, attn_send, attn_recv,
    near_send, near_recv, far_send, far_recv, x_send, x_recv,
    bn_send, bn_recv, bf_send, bf_recv, gin,
    g_sem, a_s, a_r, i_s, i_r, x_s, x_r, f_s, f_r, n_s, n_r, c_s, c_r, r_s, r_r, b_s, b_r, o_s, o_r, u_s, u_r,
):
    me = lax.axis_index("tensor")
    odd = lax.rem(me, 2)
    core = me + 1 - 2 * odd
    far = lax.rem(me + 2, 4)
    rows = hidden.shape[0]
    pieces = rows // BLK
    early, late = pl.ds(0, BLK), pl.ds(BLK, rows - BLK)
    places = (gs.at[0], gs.at[1], gs.at[2, early], gs.at[3, early])
    loads = [
        pltpu.make_async_copy(g, p, g_sem.at[i])
        for i, (g, p) in enumerate(zip((g0, g1, g2, g3), places))
    ]
    for c in loads:
        c.start()
    meet([{"tensor": core}, {"tensor": far}])
    late_copy = send(g0.at[late], gs.at[2, late], u_s.at[0], u_r.at[0], tensor=far)
    out_bias, gain, shift, down_bias, up_bias = (vecs[j : j + 1, :] for j in range(5))

    def attn(start):
        part = pl.ds(pl.multiple_of(start, BLK), BLK)
        return mm(o1[part, :], wo1[...]) + mm(o2[part, :], wo2[...])

    sends = []
    attn_copies = []
    for c in range(pieces):
        here = pl.ds(c * BLK, BLK)
        attn_send[here, :] = attn((1 - odd) * rows + c * BLK).astype(bf16)
        attn_copies.append(send(attn_send.at[here], attn_recv.at[here], a_s.at[c], a_r.at[c], tensor=core))
    inner_copies, far_copies = [], []
    for c in range(pieces):
        here = pl.ds(c * BLK, BLK)
        mine = attn(odd * rows + c * BLK)
        attn_copies[c].wait_recv()
        m = hidden[here, :].astype(f32) + (mine + attn_recv[here, :].astype(f32)) + out_bias
        mid[here, :] = m
        xhat, r = norm_parts(m)
        inner[0, here, :] = (xhat * gain + shift).astype(bf16)
        far_copies.append(send(inner.at[0, here], inner.at[2, here], x_s.at[c], x_r.at[c], tensor=far))
        inner_copies.append(send(inner.at[0, here], inner.at[1, here], i_s.at[c], i_r.at[c], tensor=core))
    sends += attn_copies + inner_copies + far_copies
    for c in loads:
        c.wait()
    sums[...] = jnp.zeros_like(sums)

    def feed(slot, start):
        part = pl.ds(pl.multiple_of(start, BLK), BLK)
        pre = mm(inner[slot, part, :], up[...]) + up_bias
        a, slope = gelu_pair(pre)
        act[slot, part, :] = a.astype(bf16)
        gp = (mm_nt(gs[slot, part, :], down[...]) * slope).astype(bf16)
        gpre[slot, part, :] = gp
        sums[4:5, :] += jnp.sum(gp.astype(f32), 0, keepdims=True)

    def near(i, _):
        @pl.when(i == pieces)
        def _():
            for c in inner_copies:
                c.wait_recv()

        feed(i // pieces, lax.rem(i, pieces) * BLK)
        return 0

    lax.fori_loop(0, 2 * pieces, near, 0)

    def near_other(c, _):
        part = pl.ds(pl.multiple_of(c * BLK, BLK), BLK)
        near_send[part, :] = mm_nt(gpre[1, part, :], up[...]).astype(bf16)
        bn_send[part, :] = mm(act[1, part, :], down[...]).astype(bf16)
        return 0

    lax.fori_loop(0, pieces, near_other, 0)
    near_copy = send(near_send, near_recv, n_s.at[0], n_r.at[0], tensor=core)
    branch_copy = send(bn_send, bn_recv, n_s.at[1], n_r.at[1], tensor=core)

    def near_own(c, _):
        part = pl.ds(pl.multiple_of(c * BLK, BLK), BLK)
        gin[part, :] = mm_nt(gpre[0, part, :], up[...])
        partial[part, :] = mid[part, :] + mm(act[0, part, :], down[...]) + down_bias
        return 0

    lax.fori_loop(0, pieces, near_own, 0)

    def plan(src, dst, c, send_sem, recv_sem, where):
        here = pl.ds(pl.multiple_of(c * BLK, BLK), BLK)
        return pltpu.make_async_remote_copy(
            src_ref=src.at[here], dst_ref=dst.at[here], send_sem=send_sem.at[c],
            recv_sem=recv_sem.at[c], device_id={"tensor": where},
            device_id_type=pl.DeviceIdType.MESH,
        )

    def arrive(c):
        return plan(inner.at[0], inner.at[2], c, x_s, x_r, far)

    def hand_on(c):
        return plan(inner.at[2], inner.at[3], c, f_s, f_r, core)

    def crossed(c):
        return plan(far_send, far_recv, c, c_s, c_r, core)

    def back(c):
        return plan(x_send, x_recv, c, r_s, r_r, far)

    depth = up.shape[0]
    if up_g.shape[0] > depth:
        up_g[depth:, :] = jnp.zeros((up_g.shape[0] - depth, up_g.shape[1]), bf16)
        down_g[depth:, :] = jnp.zeros((up_g.shape[0] - depth, up_g.shape[1]), bf16)

    def weights(left, right, out):
        def tile(j, _):
            part = pl.ds(pl.multiple_of(j * BLK, BLK), BLK)
            total = mm_tn(left[0, :, part], right[0])
            for k in range(1, 4):
                total = total + mm_tn(left[k, :, part], right[k])
            out[part, :] = total.astype(bf16)
            return 0

        lax.fori_loop(0, depth // BLK, tile, 0)

    late_copy.wait_recv()
    late_pass = send(gs.at[2, late], gs.at[3, late], u_s.at[1], u_r.at[1], tensor=core)

    def far_step(i, _):
        c = i // 2
        which = lax.rem(i, 2)
        here = pl.ds(pl.multiple_of(c * BLK, BLK), BLK)

        @pl.when(which == 0)
        def _():
            arrive(c).wait_recv()
            hand_on(c).start()

        @pl.when(which == 1)
        def _():
            hand_on(c).wait_recv()

        @pl.when(i == 3)
        def _():
            late_pass.wait_recv()

        feed(2 + which, c * BLK)

        @pl.when(which == 1)
        def _():
            far_send[here, :] = mm_nt(gpre[3, here, :], up[...]).astype(bf16)
            crossed(c).start()
            g = mm_nt(gpre[2, here, :], up[...])
            crossed(c).wait_recv()
            x_send[here, :] = (g + far_recv[here, :].astype(f32)).astype(bf16)
            back(c).start()

        return 0

    lax.fori_loop(0, 2 * pieces, far_step, 0)

    def far_out(c, _):
        here = pl.ds(pl.multiple_of(c * BLK, BLK), BLK)
        bf_send[here, :] = mm(act[3, here, :], down[...]).astype(bf16)
        return 0

    lax.fori_loop(0, pieces, far_out, 0)
    far_branch = send(bf_send, bf_recv, b_s, b_r, tensor=core)
    weights(inner, gpre, up_g)
    weights(act, gs, down_g)
    far_branch.wait_recv()
    for c in range(pieces):
        here = pl.ds(c * BLK, BLK)
        b = mm(act[2, here, :], down[...])
        branch_x[here, :] = (b + bf_recv[here, :].astype(f32)).astype(bf16)
    near_copy.wait_recv()
    branch_copy.wait_recv()
    partial[...] += bn_recv[...].astype(f32)
    rows_copies = []
    for c in range(pieces):
        here = pl.ds(c * BLK, BLK)
        xhat, r = norm_parts(mid[here, :])
        back(c).wait_recv()
        g = gin[here, :] + near_recv[here, :].astype(f32) + x_recv[here, :].astype(f32)
        g_out = gs[0, here, :].astype(f32)
        gm = g_out + norm_back(g * gain, xhat, r)
        gmid[here, :] = gm
        there = pl.ds(pl.multiple_of(odd * rows + c * BLK, BLK), BLK)
        ga = gm.astype(bf16)
        rows_out[there, :] = ga
        rows_copies.append(
            send(rows_out.at[there], rows_out.at[there], o_s.at[c], o_r.at[c], tensor=core)
        )
        sums[0:1, :] += jnp.sum(g * xhat, 0, keepdims=True)
        sums[1:2, :] += jnp.sum(g, 0, keepdims=True)
        sums[2:3, :] += jnp.sum(ga.astype(f32), 0, keepdims=True)
        sums[3:4, :] += jnp.sum(g_out, 0, keepdims=True)
    for c in rows_copies:
        c.wait_recv()
    for c in range(pieces):
        sends += [hand_on(c), crossed(c), back(c)]
    for c in sends + rows_copies + [near_copy, branch_copy, far_branch, late_copy, late_pass]:
        c.wait_send()


def feed_forward(padded, o1, o2, wo1, wo2, hidden, gs, vecs, up, down):
    rows, depth = hidden.shape
    width = up.shape[1]
    pieces = rows // BLK
    vmem = pl.BlockSpec(memory_space=pltpu.VMEM)
    anyw = pl.BlockSpec(memory_space=pl.ANY)
    dma = pltpu.SemaphoreType.DMA
    wide = pltpu.VMEM((rows, depth), bf16)
    each = [dma((pieces,))] * 2
    return pl.pallas_call(
        feed_kernel,
        in_specs=[vmem] * 5 + [anyw] * 4 + [vmem] * 3,
        out_specs=[vmem] * 7,
        out_shape=[
            jax.ShapeDtypeStruct((2 * rows, depth), bf16),
            jax.ShapeDtypeStruct((rows, depth), f32),
            jax.ShapeDtypeStruct((rows, depth), f32),
            jax.ShapeDtypeStruct((rows, depth), bf16),
            jax.ShapeDtypeStruct((padded, width), bf16),
            jax.ShapeDtypeStruct((padded, width), bf16),
            jax.ShapeDtypeStruct((8, depth), f32),
        ],
        scratch_shapes=[
            pltpu.VMEM((4, rows, depth), bf16),
            pltpu.VMEM((4, rows, depth), bf16),
            pltpu.VMEM((4, rows, width), bf16),
            pltpu.VMEM((4, rows, width), bf16),
            pltpu.VMEM((rows, depth), f32),
            wide, wide, wide, wide, wide, wide, wide, wide, wide, wide, wide, wide,
            pltpu.VMEM((rows, depth), f32),
            dma((4,)),
            *each, *each, *each, *each,
            dma((2,)), dma((2,)),
            *each, *each,
            dma, dma,
            *each,
            dma((2,)), dma((2,)),
        ],
        compiler_params=pltpu.CompilerParams(
            collective_id=1, has_side_effects=True, vmem_limit_bytes=62 * 1024 * 1024
        ),
        name="feed_forward",
    )(o1, o2, wo1, wo2, hidden, *gs, vecs, up, down)

def back_kernel(n, chunk, piece, depth, lengths, up_h, down_h, branch_x, *rest):
    held, outs = rest[:LOADS], rest[LOADS : LOADS + 7]
    back_body(n, chunk, piece, depth, lengths, up_h, down_h, branch_x, held, outs, *rest[LOADS + 7 :])


LOADS = 27


def back_body(
    n, chunk, piece, depth, lengths, up_h, down_h, branch_x, held, outs,
    up_g, up_recv, rows_in, os, wo, qkv, lse, fence, sq, sk, normed, down_g, w, sel_w,
    hidden, gmid, vecs, sums, partial, ld_s,
    go, grads, dsums,
    dq_scr, dkt, dvt, dskt, later, fsum, qt, dot_,
    dsel, ng_send, ng_recv, ng_own, far_s, far_r, faro_s, faro_r, gb, ga,
    yd, yb, ya, ys, su, sd, sb, sa, ss, zu, zd, zb, za, zs,
    ts, small, out_s, bx_recv, sel_mine, sel_core, sel_far,
    core_s, core_r, f_s, f_r, sl_s, sl_r, y_s, y_r, z_s, z_r, t_s, t_r, az_s, az_r, ay_s, ay_r,
):
    fu, fd, fb, fa, small_out, input_grad, output = outs
    places = (
        up_g, rows_in, os.at[0], wo.at[0], qkv.at[0, 0], qkv.at[0, 1], qkv.at[0, 2],
        lse.at[0], fence, sq, sk, normed, down_g, wo.at[1], qkv.at[1, 0], qkv.at[1, 1],
        qkv.at[1, 2], lse.at[1], w.at[0], w.at[1], sel_w, os.at[1], hidden, gmid, vecs, sums, partial,
    )
    idx = lax.axis_index("dp")
    par = lax.rem(idx, 2)
    m = n // 2
    own = pl.ds(pl.multiple_of(par * m * chunk, m * chunk), m * chunk)
    loads = [
        pltpu.make_async_copy(h.at[own] if j in (0, 12) else h, v, ld_s.at[j])
        for j, (h, v) in enumerate(zip(held, places))
    ]
    for c in loads:
        c.start()

    def need(*which):
        for j in which:
            loads[j].wait()

    me = lax.axis_index("tensor")
    odd = lax.rem(me, 2)
    z = lax.div(idx, 2)
    rows = hidden.shape[0]
    seq_len = normed.shape[0]
    width = wo.shape[1]
    heads = width // HD
    ranks = 4
    core = me + 1 - 2 * odd
    far = lax.rem(me + 2, ranks)
    ydev = idx + 1 - 2 * par
    peers = [lax.rem(me + d, ranks) for d in range(1, ranks)]
    mates = []
    for b in range(m.bit_length() - 1):
        bit = lax.rem(lax.div(z, 1 << b), 2)
        mates.append(z + (1 - 2 * bit) * (1 << b))
    length = jnp.where(me < 2, lengths[0], lengths[1])
    meet(
        [{"tensor": p} for p in peers]
        + [{"dp": ydev}]
        + [{"dp": 2 * p + par} for p in mates]
    )
    at = par * m + z
    source = (gb, ga, small, up_g, down_g)
    yrecv = (yb, ya, ys, up_recv, yd)
    ysum = (sb, sa, ss, su, sd)
    zrecv = (zb, za, zs, zu, zd)
    full = (fb, fa, out_s, fu, fd)
    size = (gb.shape[0] // n, ga.shape[0] // n, piece, chunk, chunk)

    def plan(src, dst, send_sem, recv_sem, **where):
        return pltpu.make_async_remote_copy(
            src_ref=src, dst_ref=dst, send_sem=send_sem, recv_sem=recv_sem,
            device_id=where, device_id_type=pl.DeviceIdType.MESH,
        )

    def block(start, k):
        return pl.ds(pl.multiple_of(start * size[k], size[k]), size[k])

    def y_copy(k):
        half = m * size[k]
        give = pl.ds(pl.multiple_of((1 - par) * half, half), half)
        src = {3: up_h, 4: down_h}.get(k, source[k])
        return plan(src.at[give], yrecv[k], y_s.at[k], y_r.at[k], dp=ydev)

    bits = m.bit_length() - 1
    first_slot = [0]
    for b in range(bits):
        first_slot.append(first_slot[-1] + (m >> (b + 1)))

    def held_chunk(who, b, j):
        return lax.rem(who, 2 << b) + j * (2 << b)

    def mate(b):
        return mates[b]

    def z_copy(k, b, j):
        slot = first_slot[b] + j
        return plan(
            ysum[k].at[block(held_chunk(mate(b), b, j), k)], zrecv[k].at[slot],
            z_s.at[k, slot], z_r.at[k, slot], dp=2 * mate(b) + par,
        )

    def az_copy(k, b, j):
        slot = first_slot[b] + j
        mine = full[k].at[block(par * m + held_chunk(z, b, j), k)]
        return plan(mine, mine, az_s.at[k, slot], az_r.at[k, slot], dp=2 * mate(b) + par)

    def ay_copy(k, b, j):
        chunk_id, slot = (z, m - 1) if b is None else (held_chunk(mate(b), b, j), first_slot[b] + j)
        came = full[k].at[block(par * m + chunk_id, k)]
        return plan(came, came, ay_s.at[k, slot], ay_r.at[k, slot], dp=ydev)

    def stage(b):
        return range(m >> (b + 1))

    def z_start(k, b):
        for j in stage(b):
            z_copy(k, b, j).start()

    def y_finish(k):
        half = m * size[k]
        keep = pl.ds(pl.multiple_of(par * half, half), half)
        y_copy(k).wait_recv()
        mine = source[k][...] if k > 2 else source[k][keep, :]
        total = mine.astype(f32) + yrecv[k][...].astype(f32)
        ysum[k][...] = total.astype(ysum[k].dtype)
        z_start(k, 0)

    def z_next(k, b):
        for j in stage(b):
            z_copy(k, b, j).wait_recv()
            here = block(held_chunk(z, b, j), k)
            total = ysum[k][here, :].astype(f32) + zrecv[k][first_slot[b] + j].astype(f32)
            ysum[k][here, :] = total.astype(ysum[k].dtype)
        z_start(k, b + 1)

    def z_finish(k):
        for b in range(1, bits - 1):
            z_next(k, b)
        z_copy(k, bits - 1, 0).wait_recv()
        return ysum[k][block(z, k), :].astype(f32) + zrecv[k][first_slot[bits - 1]].astype(f32)

    def az_start(k, b):
        for j in stage(b):
            az_copy(k, b, j).start()

    def spread(k):
        az_start(k, bits - 1)
        ay_copy(k, None, 0).start()

    def forward(k, b):
        for j in stage(b):
            az_copy(k, b, j).wait_recv()
        if b > 0:
            az_start(k, b - 1)
        for j in stage(b):
            ay_copy(k, b, j).start()

    def forward_early(k):
        for b in reversed(range(1, bits)):
            forward(k, b)

    def far_copy(j):
        part = pl.ds(pl.multiple_of(j * width, width), width)
        return plan(far_s.at[part], far_r.at[part], f_s.at[2 + j], f_r.at[2 + j], tensor=far)

    out_copy = plan(faro_s, faro_r, f_s.at[0], f_r.at[0], tensor=far)
    branch_copy = plan(branch_x, bx_recv, f_s.at[1], f_r.at[1], tensor=far)
    core_copy = plan(ng_send, ng_recv, core_s, core_r, tensor=core)
    to_core = plan(sel_mine, sel_core, sl_s.at[0], sl_r.at[0], tensor=core)
    to_first = plan(sel_mine, sel_far, sl_s.at[1], sl_r.at[1], tensor=far)

    y_copy(3).start()
    y_copy(4).start()
    need(1, 2)
    faro_s[...] = mm_tn(os[0], rows_in[...]).astype(bf16)
    out_copy.start()
    branch_copy.start()
    need(0, *range(3, 13))

    def hook(g, i):
        if i == 1:

            @pl.when(g == 0)
            def _():
                y_finish(3)

            @pl.when(g == 1)
            def _():
                fu[block(at, 3), :] = z_finish(3).astype(bf16)
                spread(3)
                z_next(4, 0)

        if i == seq_len // BLK - 1:

            @pl.when(g == 1)
            def _():
                z_next(3, 0)
                y_finish(4)

    def group(g, _):
        @pl.when(g == 1)
        def _():
            need(*range(13, 18))

        def head_grad(j, _):
            here = pl.ds(pl.multiple_of(j * BLK, BLK), BLK)
            go[here, :] = mm_nt(rows_in[here, :], wo[g]).astype(bf16)
            return 0

        lax.fori_loop(0, seq_len // BLK, head_grad, 0)
        for r in (dkt, dvt, dskt, later):
            r[...] = jnp.zeros_like(r)
        for i in reversed(range(seq_len // BLK)):
            here = pl.ds(i * BLK, BLK)
            bwd_block(
                i, heads, qkv.at[g, 0, here], qkv.at[g, 1], qkv.at[g, 2], go.at[here],
                lse.at[g, here], fence.at[here], sq.at[here], sk,
                grads.at[g, 0, here], dsums.at[g, 0, here],
                dq_scr, dkt, dvt, dskt, later, fsum, qt, dot_,
            )
            hook(g, i)
        grads[g, 1] = dkt[...].T.astype(bf16)
        grads[g, 2] = dvt[...].T.astype(bf16)
        dsums[g, 1] = dskt[...].T

        @pl.when(g == 0)
        def _():
            def far_grad(t, _):
                j = 2 - t
                here = pl.ds(pl.multiple_of(j * width, width), width)
                far_s[here, :] = mm_tn(grads[0, j], normed[...]).astype(bf16)
                far_copy(j).start()
                return 0

            lax.fori_loop(0, 3, far_grad, 0)

        return 0

    lax.fori_loop(0, 2, group, 0)
    need(*range(18, LOADS))
    own_v = mm_tn(grads[1, 2], normed[...])
    own_out = mm_tn(os[1], rows_in[...])
    if gb.shape[0] > 2 * width:
        gb[2 * width :, :] = jnp.zeros((gb.shape[0] - 2 * width, depth), bf16)
        ga[2 * width :, :] = jnp.zeros((ga.shape[0] - 2 * width, depth), bf16)
    out_copy.wait_recv()
    ga[width : 2 * width, :] = (own_out + faro_r[...].astype(f32)).astype(bf16)
    far_copy(2).wait_recv()
    ga[:width, :] = (own_v + far_r[2 * width :, :].astype(f32)).astype(bf16)
    y_copy(1).start()

    dsel[:, :HD] = (dsums[0, 0] + dsums[1, 0]).astype(bf16)
    dsel[:, HD:] = (dsums[0, 1] + dsums[1, 1]).astype(bf16)
    sel_mine[...] = mm_tn(dsel[...], normed[...]).astype(bf16)

    @pl.when(odd == 1)
    def _():
        to_core.start()

    def own_grad(j, _):
        here = pl.ds(pl.multiple_of(j * width, width), width)
        total = mm_tn(grads[1, j], normed[...])
        far_copy(j).wait_recv()
        gb[here, :] = (total + far_r[here, :].astype(f32)).astype(bf16)
        return 0

    @pl.when(odd == 0)
    def _():
        to_core.wait_recv()
        sel_mine[...] = (sel_mine[...].astype(f32) + sel_core[...].astype(f32)).astype(bf16)

    @pl.when(me == 2)
    def _():
        to_first.start()

    def normed_grad(t, _):
        mine = t // 2
        step = pl.multiple_of(lax.rem(t, 2) * BLK, BLK)
        side = mine * odd + (1 - mine) * (1 - odd)
        part = pl.ds(pl.multiple_of(side * rows + step, BLK), BLK)
        here = pl.ds(step, BLK)
        total = mm(dsel[part, :], sel_w[...])
        for g in range(2):
            for j in range(3):
                total = total + mm(grads[g, j, part, :], w[g, j * width : (j + 1) * width, :])

        @pl.when(mine == 0)
        def _():
            ng_send[here, :] = total.astype(bf16)

        @pl.when(mine == 1)
        def _():
            ng_own[here, :] = total

        @pl.when(t == 1)
        def _():
            core_copy.start()

        return 0

    lax.fori_loop(0, 4, normed_grad, 0)
    forward_early(3)
    fd[block(at, 4), :] = z_finish(4).astype(bf16)
    y_finish(1)
    lax.fori_loop(0, 2, own_grad, 0)

    @pl.when(me == 0)
    def _():
        to_first.wait_recv()
        both = sel_mine[...].astype(f32) + sel_far[...].astype(f32)
        gb[:HD, :] = (gb[:HD, :].astype(f32) + both[:HD, :]).astype(bf16)
        gb[width : width + HD, :] = (
            gb[width : width + HD, :].astype(f32) + both[HD:, :]
        ).astype(bf16)

    y_copy(0).start()
    spread(4)
    z_next(1, 0)
    xhat, r = norm_parts(hidden[...].astype(f32))
    core_copy.wait_recv()
    grad = ng_own[...] + ng_recv[...].astype(f32)
    input_grad[...] = (gmid[...] + norm_back(grad * vecs[5:6, :], xhat, r)).astype(bf16)
    small[...] = jnp.zeros_like(small)
    dgain = jnp.sum(grad * xhat, 0, keepdims=True)
    dshift = jnp.sum(grad, 0, keepdims=True)
    lines = depth // 128
    for j in range(lines):
        small[j : j + 1, :] = dgain[:, j * 128 : (j + 1) * 128]
        small[lines + j : lines + j + 1, :] = dshift[:, j * 128 : (j + 1) * 128]
    for slot, which in ((2, 2), (3, 0), (4, 1), (5, 3)):
        for j in range(lines):
            small[slot * lines + j : slot * lines + j + 1, :] = sums[
                which : which + 1, j * 128 : (j + 1) * 128
            ]
    wide_lines = up_g.shape[1] // 128
    for j in range(wide_lines):
        small[pl.ds(6 * lines + me * wide_lines + j, 1), :] = sums[4:5, j * 128 : (j + 1) * 128]
    base = small_lines(depth, up_g.shape[1]) - 4 * ranks
    for owner, g in ((me, 1), (far, 0)):
        for j, which in enumerate((0, 2)):
            total = jnp.sum(grads[g, which].astype(f32), 0, keepdims=True)
            line = base + 4 * owner + 2 * j
            small[pl.ds(line, 1), :] = total[:, :128]
            small[pl.ds(line + 1, 1), : width - 128] = total[:, 128:]
    total = jnp.sum(dsel[...].astype(f32), 0, keepdims=True)
    lane = lax.broadcasted_iota(jnp.int32, total.shape, 1)
    small[base : base + 1, :] += jnp.where(lane < HD, total, 0.0)
    y_copy(2).start()

    forward(3, 0)
    y_finish(0)
    y_finish(2)
    fa[block(at, 1), :] = z_finish(1).astype(bf16)
    spread(1)
    forward_early(4)
    z_next(0, 0)
    z_next(2, 0)
    token = odd * rows + lax.broadcasted_iota(jnp.int32, (rows, 1), 0)
    live = jnp.where(token < length, 1.0, 0.0)
    branch_copy.wait_recv()
    output[...] = (live * (partial[...] + bx_recv[...].astype(f32))).astype(bf16)
    forward_early(1)
    fb[block(at, 0), :] = z_finish(0).astype(bf16)
    spread(0)
    forward(4, 0)
    ts[me] = z_finish(2)

    def t_copy(d):
        return plan(ts.at[me], ts.at[me], t_s.at[d], t_r.at[d], tensor=peers[d])

    for d in range(ranks - 1):
        t_copy(d).start()
    for d in range(ranks - 1):
        t_copy(d).wait_recv()
    vec = ts[0]
    for d in range(1, ranks):
        vec = vec + ts[d]
    out_s[block(at, 2), :] = vec
    spread(2)
    forward(1, 0)
    forward_early(0)
    forward_early(2)
    forward(0, 0)
    forward(2, 0)
    for k in range(5):
        ay_copy(k, None, 0).wait_recv()
        for b in range(bits):
            for j in stage(b):
                ay_copy(k, b, j).wait_recv()

    @pl.when(odd == 1)
    def _():
        to_core.wait_send()

    @pl.when(me == 2)
    def _():
        to_first.wait_send()

    small_out[...] = out_s[...]
    for c in (far_copy(0), far_copy(1), far_copy(2), out_copy, branch_copy, core_copy):
        c.wait_send()
    for d in range(ranks - 1):
        t_copy(d).wait_send()
    for k in range(5):
        y_copy(k).wait_send()
        ay_copy(k, None, 0).wait_send()
        for b in range(bits):
            for j in stage(b):
                z_copy(k, b, j).wait_send()
                az_copy(k, b, j).wait_send()
                ay_copy(k, b, j).wait_send()


def front_kernel(
    lengths, hidden, out_grad, vecs, qkv, qv_bias, wo,
    *rest,
):
    outs, gcore, gfar, gcross = rest[:18], rest[18], rest[19], rest[20]
    kept = rest[21:39]
    front_body(
        lengths, hidden, out_grad, vecs, qkv, qv_bias, wo, outs, kept, gcore, gfar, gcross, *rest[39:]
    )


def front_body(
    lengths, hidden, out_grad, vecs, qkv, qv_bias, wo, outs, kept, gcore, gfar, gcross,
    out_scr, carry, sel_b, bias2,
    st_s, nm_s, nm_r, gc_s, gc_r, sl_s, sl_r, w_s, w_r, p_s, p_r, e_s, e_r, g_s, g_r, h_s, h_r,
):
    me = lax.axis_index("tensor")
    idx = lax.axis_index("dp")
    odd = lax.rem(me, 2)
    core = me + 1 - 2 * odd
    far = lax.rem(me + 2, 4)
    par = lax.rem(idx, 2)
    ydev = idx + 1 - 2 * par
    rows = hidden.shape[0]
    seq_len = 2 * rows
    width = wo.shape[0]
    heads = width // HD
    (normed, q1, k1, v1, lse1, o1, q2, k2, v2, lse2, o2, fence, sq, sk, w2, wo2, selw, g0) = kept
    stores = []

    def store(*which):
        for j in which:
            copy = pltpu.make_async_copy(kept[j], outs[j], st_s.at[j])
            copy.start()
            stores.append(copy)

    length = jnp.where(me < 2, lengths[0], lengths[1])

    def sel_copies(k, where):
        return [
            pltpu.make_async_remote_copy(
                src_ref=a, dst_ref=a, send_sem=sl_s.at[k, j], recv_sem=sl_r.at[j],
                device_id={"tensor": where}, device_id_type=pl.DeviceIdType.MESH,
            )
            for j, a in enumerate((selw, sel_b))
        ]

    @pl.when(me == 0)
    def _():
        selw[:HD, :] = qkv[:HD, :]
        selw[HD:, :] = qkv[width : width + HD, :]
        sel_b[...] = qv_bias[...]

    meet([{"tensor": core}, {"tensor": far}, {"dp": ydev}])

    @pl.when(me == 0)
    def _():
        for c in sel_copies(0, far) + sel_copies(1, core):
            c.start()

    share = width // 2
    halves = [
        (src, dst, pl.ds(pl.multiple_of(base + par * share, share), share))
        for src, dst, base in (
            (qkv, w2, 0), (qkv, w2, width), (qkv, w2, 2 * width), (wo, wo2, 0)
        )
    ]
    extra = send(qv_bias, bias2, e_s, e_r, tensor=far)
    cross = [
        send(src.at[part], dst.at[part], w_s.at[j], w_r.at[j], tensor=far)
        for j, (src, dst, part) in enumerate(halves)
    ]
    passed = []

    def pass_on(j):
        cross[j].wait_recv()
        _, dst, part = halves[j]
        passed.append(send(dst.at[part], dst.at[part], p_s.at[j], p_r.at[j], dp=ydev))

    spot = pl.multiple_of(odd * rows, rows)
    norm_copies = []
    for c in range(rows // BLK):
        here = pl.ds(c * BLK, BLK)
        there = pl.ds(pl.multiple_of(spot + c * BLK, BLK), BLK)
        xhat, _ = norm_parts(hidden[here, :].astype(f32))
        normed[there, :] = (xhat * vecs[5:6, :] + vecs[6:7, :]).astype(bf16)
        norm_copies.append(
            send(normed.at[there], normed.at[there], nm_s.at[c], nm_r.at[c], tensor=core)
        )
    row = odd * rows + lax.broadcasted_iota(jnp.int32, (rows, 1), 0)
    live = jnp.where(row < length, 1.0, 0.0)
    g0[...] = (out_grad[...].astype(f32) * live).astype(bf16)
    store(17)
    gc = send(g0, gcore, gc_s, gc_r, tensor=core)
    g_parts = [pl.ds(0, BLK)]
    gf = [
        send(g0.at[p], gfar.at[p], g_s.at[c], g_r.at[c], tensor=far) for c, p in enumerate(g_parts)
    ]

    def project(weight, bias, out):
        def tile(j, _):
            here = pl.ds(pl.multiple_of(j * BLK, BLK), BLK)
            y = mm_nt(normed[here, :], weight)
            if bias is not None:
                y = y + bias
            out[here, :] = y.astype(bf16)
            return 0

        lax.fori_loop(0, seq_len // BLK, tile, 0)

    @pl.when(me == 2)
    def _():
        for c in sel_copies(0, far):
            c.wait_recv()
        for c in sel_copies(1, core):
            c.start()

    for c in norm_copies:
        c.wait_recv()
    store(0)
    project(qkv[:width, :], qv_bias[0:1, :], q1)
    project(qkv[width : 2 * width, :], None, k1)
    project(qkv[2 * width :, :], qv_bias[1:2, :], v1)

    @pl.when(odd == 1)
    def _():
        for c in sel_copies(1, core):
            c.wait_recv()

    store(1, 2, 3)
    for j in range(seq_len // BLK):
        here = pl.ds(j * BLK, BLK)
        y = mm_nt(normed[here, :], selw[...])
        sq[here, :] = (y[:, :HD] + sel_b[0:1, :HD]).astype(bf16)
        sk[here, :] = y[:, HD:].astype(bf16)
    store(12, 13, 16)
    carry[...] = jnp.zeros_like(carry)
    pass_on(0)
    for i in range(seq_len // BLK):
        here = pl.ds(i * BLK, BLK)
        make_fence(i, seq_len, length, sq.at[here], sk, fence.at[here], carry)
        fwd_block(
            i, heads, out_scr, q1.at[here], k1, v1, fence.at[here], o1.at[here], lse1.at[here]
        )
        if i < 3:
            pass_on(i + 1)
    store(4, 5, 11)
    extra.wait_recv()
    for j, (out, bias) in enumerate(((q2, bias2[0:1, :]), (k2, None), (v2, bias2[1:2, :]))):
        passed[j].wait_recv()
        project(w2[j * width : (j + 1) * width, :], bias, out)
        store(6 + j)
    store(14)
    gx = []

    def pass_g(c):
        gf[c].wait_recv()
        p = g_parts[c]
        gx.append(send(gfar.at[p], gcross.at[p], h_s.at[c], h_r.at[c], tensor=core))

    for i in range(seq_len // BLK):
        here = pl.ds(i * BLK, BLK)
        fwd_block(
            i, heads, out_scr, q2.at[here], k2, v2, fence.at[here], o2.at[here], lse2.at[here]
        )
    store(9, 10)
    pass_g(0)
    gc.wait_recv()
    passed[3].wait_recv()
    store(15)
    for c in gx:
        c.wait_recv()

    @pl.when(me == 0)
    def _():
        for c in sel_copies(0, far):
            c.wait_send()

    @pl.when(odd == 0)
    def _():
        for c in sel_copies(1, core):
            c.wait_send()

    for c in cross + passed + norm_copies + gf + gx + [gc, extra]:
        c.wait_send()
    for c in stores:
        c.wait()


def front(lengths, hidden, out_grad, vecs, qkv, qv_bias, wo):
    rows, depth = hidden.shape
    seq_len, width = 2 * rows, wo.shape[0]
    pieces = rows // BLK
    vmem = pl.BlockSpec(memory_space=pltpu.VMEM)
    dma = pltpu.SemaphoreType.DMA
    heads = jax.ShapeDtypeStruct((seq_len, width), bf16)
    lse = jax.ShapeDtypeStruct((seq_len, 128), f32)
    sel = jax.ShapeDtypeStruct((seq_len, HD), bf16)
    wide = jax.ShapeDtypeStruct((rows, depth), bf16)
    early = jax.ShapeDtypeStruct((BLK, depth), bf16)
    kept = [
        jax.ShapeDtypeStruct((seq_len, depth), bf16),
        heads, heads, heads, lse, heads,
        heads, heads, heads, lse, heads,
        jax.ShapeDtypeStruct((seq_len, seq_len), f32),
        sel, sel,
        jax.ShapeDtypeStruct(qkv.shape, bf16),
        jax.ShapeDtypeStruct(wo.shape, bf16),
        jax.ShapeDtypeStruct((2 * HD, depth), bf16),
        wide,
    ]
    return pl.pallas_call(
        front_kernel,
        in_specs=[pl.BlockSpec(memory_space=pltpu.SMEM)] + [vmem] * 6,
        out_specs=[pl.BlockSpec(memory_space=pl.ANY)] * 21,
        out_shape=kept + [wide, early, early],
        scratch_shapes=[pltpu.VMEM(a.shape, a.dtype) for a in kept]
        + [
            pltpu.VMEM((BLK, width), f32),
            pltpu.VMEM((8, seq_len), f32),
            pltpu.VMEM((2, width), f32),
            pltpu.VMEM((2, width), f32),
            dma((18,)),
            dma((pieces,)), dma((pieces,)),
            dma, dma,
            dma((2, 2)), dma((2,)),
            dma((4,)), dma((4,)),
            dma((4,)), dma((4,)),
            dma, dma,
            dma((pieces,)), dma((pieces,)),
            dma((pieces,)), dma((pieces,)),
        ],
        compiler_params=pltpu.CompilerParams(
            collective_id=2, has_side_effects=True, vmem_limit_bytes=60 * 1024 * 1024
        ),
        name="front",
    )(lengths, hidden, out_grad, vecs, qkv, qv_bias, wo)


def small_lines(depth, hidden):
    return (6 * depth + 4 * hidden) // 128 + 16


def go_back(n, set1, set2, fence, sq, sk, rows_in, o1, o2, wo1, wo2, normed, w1, w2, sel_w,
            hidden, vecs, gmid, sums, partial, branch_x, lengths, up_g, down_g):
    m = n // 2
    chunk = up_g.shape[0] // n
    rows, depth = hidden.shape
    piece = -(-small_lines(depth, up_g.shape[1]) // (8 * n)) * 8
    seq_len, width = set1[0].shape
    half, shalf = m * chunk, m * piece
    ranks = 4
    wf = up_g.shape[1]
    small_chunk = -(-2 * width // (16 * n)) * 16
    part_half = m * small_chunk
    vmem = pl.BlockSpec(memory_space=pltpu.VMEM)
    dma = pltpu.SemaphoreType.DMA
    q1, k1, v1, lse1 = set1
    q2, k2, v2, lse2 = set2
    held = (up_g, rows_in, o2, wo2, q2, k2, v2, lse2, fence, sq, sk, normed, down_g, wo1,
            q1, k1, v1, lse1, w2, w1, sel_w, o1, hidden, gmid, vecs, sums, partial)
    anyw = pl.BlockSpec(memory_space=pl.ANY)
    like = lambda a: pltpu.VMEM(a.shape, a.dtype)
    return pl.pallas_call(
        lambda *refs: back_kernel(n, chunk, piece, depth, *refs),
        in_specs=[pl.BlockSpec(memory_space=pltpu.SMEM)] + [anyw] * (LOADS + 3),
        out_specs=[vmem] * 7,
        out_shape=[
            jax.ShapeDtypeStruct((n * chunk, wf), bf16),
            jax.ShapeDtypeStruct((n * chunk, wf), bf16),
            jax.ShapeDtypeStruct((n * small_chunk, depth), bf16),
            jax.ShapeDtypeStruct((n * small_chunk, depth), bf16),
            jax.ShapeDtypeStruct((n * piece, 128), f32),
            jax.ShapeDtypeStruct((rows, depth), bf16),
            jax.ShapeDtypeStruct((rows, depth), bf16),
        ],
        scratch_shapes=[
            pltpu.VMEM((half, wf), bf16), pltpu.VMEM((half, wf), bf16), like(rows_in),
            pltpu.VMEM((2, seq_len, width), bf16),
            pltpu.VMEM((2, width, depth), bf16),
            pltpu.VMEM((2, 3, seq_len, width), bf16),
            pltpu.VMEM((2, seq_len, 128), f32),
            like(fence), like(sq), like(sk), like(normed), pltpu.VMEM((half, wf), bf16),
            pltpu.VMEM((2, 3 * width, depth), bf16),
            like(sel_w), like(hidden), like(gmid), like(vecs), like(sums), like(partial),
            dma((LOADS,)),
            pltpu.VMEM((seq_len, width), bf16),
            pltpu.VMEM((2, 3, seq_len, width), bf16),
            pltpu.VMEM((2, 2, seq_len, HD), f32),
            pltpu.VMEM((BLK, width), f32),
            pltpu.VMEM((width, seq_len), f32),
            pltpu.VMEM((width, seq_len), f32),
            pltpu.VMEM((HD, seq_len), f32),
            pltpu.VMEM((8, seq_len), f32),
            pltpu.VMEM((BLK, seq_len), f32),
            pltpu.VMEM((width, BLK), bf16),
            pltpu.VMEM((width, BLK), bf16),
            pltpu.VMEM((seq_len, 128), bf16),
            pltpu.VMEM((rows, depth), bf16),
            pltpu.VMEM((rows, depth), bf16),
            pltpu.VMEM((rows, depth), f32),
            pltpu.VMEM((3 * width, depth), bf16),
            pltpu.VMEM((3 * width, depth), bf16),
            pltpu.VMEM((width, depth), bf16),
            pltpu.VMEM((width, depth), bf16),
            pltpu.VMEM((n * small_chunk, depth), bf16),
            pltpu.VMEM((n * small_chunk, depth), bf16),
            *[pltpu.VMEM((h, depth), bf16) for h in (half, part_half, part_half)],
            pltpu.VMEM((shalf, 128), f32),
            *[pltpu.VMEM((h, depth), bf16) for h in (half, half, part_half, part_half)],
            pltpu.VMEM((shalf, 128), f32),
            *[
                pltpu.VMEM((m - 1, c, depth), bf16)
                for c in (chunk, chunk, small_chunk, small_chunk)
            ],
            pltpu.VMEM((m - 1, piece, 128), f32),
            pltpu.VMEM((ranks, piece, 128), f32),
            pltpu.VMEM((n * piece, 128), f32),
            pltpu.VMEM((n * piece, 128), f32),
            pltpu.VMEM((rows, depth), bf16),
            *[pltpu.VMEM((2 * HD, depth), bf16)] * 3,
            dma, dma,
            dma((5,)), dma((5,)),
            dma((2,)), dma((2,)),
            dma((5,)), dma((5,)),
            dma((5, m - 1)), dma((5, m - 1)),
            dma((3,)), dma((3,)),
            dma((5, m - 1)), dma((5, m - 1)),
            dma((5, m)), dma((5, m)),
        ],
        compiler_params=pltpu.CompilerParams(
            collective_id=0, has_side_effects=True, vmem_limit_bytes=66_900_000
        ),
        name="go_back",
    )(lengths, up_g, down_g, branch_x, *held)


def shards(
    hidden_in,
    lengths,
    ln1_gain,
    ln1_shift,
    qkv_weight,
    qv_bias,
    out_weight,
    out_bias,
    ln2_gain,
    ln2_shift,
    up_weight,
    up_bias,
    down_weight,
    down_bias,
    out_grad,
):
    n = lax.axis_size("dp")
    ranks = lax.axis_size("tensor")
    me = lax.axis_index("tensor")
    depth = hidden_in.shape[1]
    width = qkv_weight.shape[2]
    hidden = up_bias.shape[0]
    padded = -(-depth // (16 * n)) * 16 * n
    spot = jnp.arange(8)[:, None]
    vecs = jnp.zeros((8, depth), f32)
    for j, vec in enumerate(
        (out_bias, ln2_gain, ln2_shift, down_bias, up_bias.astype(f32), ln1_gain, ln1_shift)
    ):
        vecs = jnp.where(spot == j, vec[None], vecs)
    qkv_rows = jnp.swapaxes(qkv_weight, 1, 2).reshape(3 * width, depth)
    (normed, q1, k1, v1, lse1, o1, q2, k2, v2, lse2, o2, fence, sq, sk, qkv_far, out_far, sel_w,
     *grad_rows) = front(lengths, hidden_in, out_grad, vecs, qkv_rows, qv_bias, out_weight)
    attn_rows, grad_middle, partial, branch_x, up_part, down_part, sums = feed_forward(
        padded, o1, o2, out_weight, out_far, hidden_in, grad_rows, vecs, up_weight, down_weight
    )
    full_u, full_d, full_b, full_a, small, input_grad, output = go_back(
        n, (q1, k1, v1, lse1), (q2, k2, v2, lse2), fence, sq, sk, attn_rows, o1, o2,
        out_weight, out_far, normed, qkv_rows, qkv_far, sel_w, hidden_in, vecs,
        grad_middle, sums, partial, branch_x, lengths, up_part, down_part,
    )
    vectors = small[: 6 * depth // 128].reshape(6, depth)
    lines = (6 * depth + ranks * hidden) // 128
    up_all = small[6 * depth // 128 : lines].reshape(ranks, hidden)
    qv_all = small[lines : lines + 4 * ranks].reshape(ranks, 2, 256)
    up_bias_grad = lax.dynamic_index_in_dim(up_all, me, 0, keepdims=False)
    qv_bias_grad = lax.dynamic_index_in_dim(qv_all, me, 0, keepdims=False)[:, :width]
    qkv_grad = jnp.concatenate([full_b[: 2 * width], full_a[:width]], 0).astype(f32)
    qkv_grad = jnp.swapaxes(qkv_grad.reshape(3, width, depth), 1, 2)
    out_weight_grad = full_a[width : 2 * width].astype(f32)
    return (
        output,
        input_grad,
        vectors[0],
        vectors[1],
        qkv_grad,
        qv_bias_grad,
        out_weight_grad,
        vectors[2],
        vectors[3],
        vectors[4],
        full_u[:depth].astype(f32),
        up_bias_grad,
        full_d[:depth].astype(f32),
        vectors[5],
    )


def solution(mesh):
    return jax.shard_map(
        shards,
        mesh=mesh,
        in_specs=(
            P(("dp", "tensor"), None),
            P("dp"),
            P(),
            P(),
            P(None, None, "tensor"),
            P(None, "tensor"),
            P("tensor", None),
            P(),
            P(),
            P(),
            P(None, "tensor"),
            P("tensor"),
            P("tensor", None),
            P(),
            P(("dp", "tensor"), None),
        ),
        out_specs=(
            P(("dp", "tensor"), None),
            P(("dp", "tensor"), None),
            P(),
            P(),
            P(None, None, "tensor"),
            P(None, "tensor"),
            P("tensor", None),
            P(),
            P(),
            P(),
            P(None, "tensor"),
            P("tensor"),
            P("tensor", None),
            P(),
        ),
        check_vma=False,
    )
```

```python
import math

import jax
import jax.numpy as jnp
from jax import lax
from jax.experimental import pallas as pl
from jax.experimental.pallas import tpu as pltpu
from jax.sharding import PartitionSpec as P

HD = 64
BLK = 256
BIG = 1e30
sel_factor = 4.0
score_scale = 1.0 / math.sqrt(HD)
f32 = jnp.float32
bf16 = jnp.bfloat16


def mm(a, b):
    return lax.dot_general(a, b, (((1,), (0,)), ((), ())), preferred_element_type=f32)


def mm_nt(a, b):
    return lax.dot_general(a, b, (((1,), (1,)), ((), ())), preferred_element_type=f32)


def flip(a):
    return a.astype(f32).T.astype(bf16)


def split_mm(tri, x):
    hi = x.astype(bf16)
    lo = (x - hi.astype(f32)).astype(bf16)
    return mm(tri, hi) + mm(tri, lo)


def head_mask(h, width):
    return lax.broadcasted_iota(jnp.int32, (BLK, width), 1) // HD == h


def masked_rows(x, mask, scale):
    return jnp.where(mask, x.astype(f32) * scale, 0.0).astype(bf16)


def fwd_block(i, heads, first, q_ref, k_ref, v_ref, fence, o_ref, lse_ref):
    width = q_ref.shape[1]
    cols = (i + 1) * BLK
    keys = k_ref[:cols, :]
    vals = v_ref[:cols, :]
    fenced = fence[:, :cols]
    lane = lax.broadcasted_iota(jnp.int32, (BLK, 128), 1)
    lse_ref[...] = jnp.zeros_like(lse_ref)
    out_scr = first

    def head(h, _):
        mask = head_mask(h, width)
        s = mm_nt(masked_rows(q_ref[...], mask, score_scale), keys) - fenced
        top = jnp.max(s, -1, keepdims=True)
        e = jnp.exp(s - top)
        total = jnp.sum(e, -1, keepdims=True)
        p = (e * (1.0 / total)).astype(bf16)
        out = mm(p, vals)
        out_scr[...] = jnp.where(mask, out, out_scr[...])
        lse_ref[...] = jnp.where(lane == h, top + jnp.log(total), lse_ref[...])
        return 0

    lax.fori_loop(0, heads, head, 0)
    o_ref[...] = out_scr[...].astype(bf16)


def make_fence(i, seq_len, length, sq_ref, sk_ref, fence, carry):
    cols = (i + 1) * BLK
    s0 = mm_nt(sq_ref[...], sk_ref[:cols, :]) * score_scale
    row = i * BLK + lax.broadcasted_iota(jnp.int32, (BLK, cols), 0)
    col = lax.broadcasted_iota(jnp.int32, (BLK, cols), 1)
    picked = (col >= 1) & (col < row)
    sel = jnp.where(picked, jnp.maximum(s0, 0.0), 0.0) * (sel_factor / seq_len)
    r2 = lax.broadcasted_iota(jnp.int32, (BLK, BLK), 0)
    c2 = lax.broadcasted_iota(jnp.int32, (BLK, BLK), 1)
    tri = jnp.where(c2 < r2, 1.0, 0.0).astype(bf16)
    total = carry[0:1, :cols] + split_mm(tri, sel)
    carry[0:1, :cols] = total[BLK - 1 : BLK, :] + sel[BLK - 1 : BLK, :]
    fence[:, :cols] = jnp.where((col <= row) & (col < length), total, BIG)


def bwd_block(i, heads, q_ref, k_ref, v_ref, do_ref, lse_ref, f_ref, sq_ref, sk_ref,
              dq_ref, dsq_ref, dq_scr, dkt, dvt, dskt, later, fsum, qt, dot_):
    width = q_ref.shape[1]
    seq_len = k_ref.shape[0]
    cols = (i + 1) * BLK
    keys = k_ref[:cols, :]
    vals = v_ref[:cols, :]
    lane = lax.broadcasted_iota(jnp.int32, (BLK, 128), 1)
    qt[...] = (q_ref[...].astype(f32) * score_scale).T.astype(bf16)
    dot_[...] = flip(do_ref[...])
    fsum[:, :cols] = jnp.zeros((BLK, cols), f32)

    def head(h, _):
        mask = head_mask(h, width)
        lse = jnp.sum(jnp.where(lane == h, lse_ref[...], 0.0), -1, keepdims=True)
        s = mm_nt(masked_rows(q_ref[...], mask, score_scale), keys)
        p = jnp.exp(s - f_ref[:, :cols] - lse)
        dp = mm_nt(masked_rows(do_ref[...], mask, 1.0), vals)
        delta = jnp.sum(p * dp, -1, keepdims=True)
        g = (p * (dp - delta)).astype(bf16)
        rows = pl.ds(pl.multiple_of(h * HD, HD), HD)
        dq_scr[...] = jnp.where(mask, mm(g, keys), dq_scr[...])
        dkt[rows, :cols] += mm(qt[rows, :], g)
        dvt[rows, :cols] += mm(dot_[rows, :], p.astype(bf16))
        fsum[:, :cols] += g.astype(f32)
        return 0

    lax.fori_loop(0, heads, head, 0, unroll=True)
    dq_ref[...] = (dq_scr[...] * score_scale).astype(bf16)
    grad = -fsum[:, :cols]
    r2 = lax.broadcasted_iota(jnp.int32, (BLK, BLK), 0)
    c2 = lax.broadcasted_iota(jnp.int32, (BLK, BLK), 1)
    tri = jnp.where(c2 > r2, 1.0, 0.0).astype(bf16)
    dsel = later[0:1, :cols] + split_mm(tri, grad)
    later[0:1, :cols] = dsel[0:1, :] + grad[0:1, :]
    s0 = mm_nt(sq_ref[...], sk_ref[:cols, :])
    row = i * BLK + lax.broadcasted_iota(jnp.int32, (BLK, cols), 0)
    col = lax.broadcasted_iota(jnp.int32, (BLK, cols), 1)
    keep = (col >= 1) & (col < row) & (s0 > 0)
    gsel = jnp.where(keep, dsel * (sel_factor / seq_len), 0.0).astype(bf16)
    dsq_ref[...] = mm(gsel, sk_ref[:cols, :]) * score_scale
    sqt = (sq_ref[...].astype(f32) * score_scale).T.astype(bf16)
    dskt[:, :cols] += mm(sqt, gsel)


epsilon = 1e-05


def mm_tn(a, b):
    return lax.dot_general(a, b, (((0,), (0,)), ((), ())), preferred_element_type=f32)


def send(src, dst, send_sem, recv_sem, **where):
    copy = pltpu.make_async_remote_copy(
        src_ref=src,
        dst_ref=dst,
        send_sem=send_sem,
        recv_sem=recv_sem,
        device_id=where,
        device_id_type=pl.DeviceIdType.MESH,
    )
    copy.start()
    return copy


def meet(devices):
    barrier = pltpu.get_barrier_semaphore()
    for where in devices:
        pl.semaphore_signal(barrier, inc=1, device_id=where, device_id_type=pl.DeviceIdType.MESH)
    pl.semaphore_wait(barrier, len(devices))


def norm_parts(x):
    centre = x - jnp.mean(x, -1, keepdims=True)
    r = lax.rsqrt(jnp.mean(centre * centre, -1, keepdims=True) + epsilon)
    return centre * r, r


def norm_back(e, xhat, r):
    return r * (e - jnp.mean(e, -1, keepdims=True) - xhat * jnp.mean(e * xhat, -1, keepdims=True))


def gelu_pair(u):
    k = math.sqrt(2.0 / math.pi)
    square = u * u
    t = jnp.tanh(k * u * (1.0 + 0.044715 * square))
    act = 0.5 * u * (1.0 + t)
    slope = 0.5 * (1.0 + t) + 0.5 * u * (1.0 - t * t) * (k * (1.0 + 3.0 * 0.044715 * square))
    return act, slope


def feed_kernel(
    o1, o2, wo1, wo2, hidden, g0, g1, g2, g3, vecs, up, down,
    rows_out, gmid, partial, branch_x, up_g, down_g, sums,
    inner, gs, act, gpre, mid, attn_send, attn_recv,
    near_send, near_recv, far_send, far_recv, x_send, x_recv,
    bn_send, bn_recv, bf_send, bf_recv, gin,
    g_sem, a_s, a_r, i_s, i_r, x_s, x_r, f_s, f_r, n_s, n_r, c_s, c_r, r_s, r_r, b_s, b_r, o_s, o_r,
):
    me = lax.axis_index("tensor")
    odd = lax.rem(me, 2)
    core = me + 1 - 2 * odd
    far = lax.rem(me + 2, 4)
    rows = hidden.shape[0]
    pieces = rows // BLK
    loads = [pltpu.make_async_copy(g, gs.at[i], g_sem.at[i]) for i, g in enumerate((g0, g1, g2, g3))]
    for c in loads:
        c.start()
    meet([{"tensor": core}, {"tensor": far}])
    out_bias, gain, shift, down_bias, up_bias = (vecs[j : j + 1, :] for j in range(5))

    def attn(start):
        part = pl.ds(pl.multiple_of(start, BLK), BLK)
        return mm(o1[part, :], wo1[...]) + mm(o2[part, :], wo2[...])

    sends = []
    attn_copies = []
    for c in range(pieces):
        here = pl.ds(c * BLK, BLK)
        attn_send[here, :] = attn((1 - odd) * rows + c * BLK).astype(bf16)
        attn_copies.append(send(attn_send.at[here], attn_recv.at[here], a_s.at[c], a_r.at[c], tensor=core))
    inner_copies, far_copies = [], []
    for c in range(pieces):
        here = pl.ds(c * BLK, BLK)
        mine = attn(odd * rows + c * BLK)
        attn_copies[c].wait_recv()
        m = hidden[here, :].astype(f32) + (mine + attn_recv[here, :].astype(f32)) + out_bias
        mid[here, :] = m
        xhat, r = norm_parts(m)
        inner[0, here, :] = (xhat * gain + shift).astype(bf16)
        far_copies.append(send(inner.at[0, here], inner.at[2, here], x_s.at[c], x_r.at[c], tensor=far))
        inner_copies.append(send(inner.at[0, here], inner.at[1, here], i_s.at[c], i_r.at[c], tensor=core))
    sends += attn_copies + inner_copies + far_copies
    for c in loads:
        c.wait()
    sums[...] = jnp.zeros_like(sums)

    def feed(slot, start):
        part = pl.ds(pl.multiple_of(start, BLK), BLK)
        pre = mm(inner[slot, part, :], up[...]) + up_bias
        a, slope = gelu_pair(pre)
        act[slot, part, :] = a.astype(bf16)
        gp = (mm_nt(gs[slot, part, :], down[...]) * slope).astype(bf16)
        gpre[slot, part, :] = gp
        sums[4:5, :] += jnp.sum(gp.astype(f32), 0, keepdims=True)

    def near(i, _):
        @pl.when(i == pieces)
        def _():
            for c in inner_copies:
                c.wait_recv()

        feed(i // pieces, lax.rem(i, pieces) * BLK)
        return 0

    lax.fori_loop(0, 2 * pieces, near, 0)

    def near_other(c, _):
        part = pl.ds(pl.multiple_of(c * BLK, BLK), BLK)
        near_send[part, :] = mm_nt(gpre[1, part, :], up[...]).astype(bf16)
        bn_send[part, :] = mm(act[1, part, :], down[...]).astype(bf16)
        return 0

    lax.fori_loop(0, pieces, near_other, 0)
    near_copy = send(near_send, near_recv, n_s.at[0], n_r.at[0], tensor=core)
    branch_copy = send(bn_send, bn_recv, n_s.at[1], n_r.at[1], tensor=core)

    def near_own(c, _):
        part = pl.ds(pl.multiple_of(c * BLK, BLK), BLK)
        gin[part, :] = mm_nt(gpre[0, part, :], up[...])
        partial[part, :] = mid[part, :] + mm(act[0, part, :], down[...]) + down_bias
        return 0

    lax.fori_loop(0, pieces, near_own, 0)

    def plan(src, dst, c, send_sem, recv_sem, where):
        here = pl.ds(pl.multiple_of(c * BLK, BLK), BLK)
        return pltpu.make_async_remote_copy(
            src_ref=src.at[here], dst_ref=dst.at[here], send_sem=send_sem.at[c],
            recv_sem=recv_sem.at[c], device_id={"tensor": where},
            device_id_type=pl.DeviceIdType.MESH,
        )

    def arrive(c):
        return plan(inner.at[0], inner.at[2], c, x_s, x_r, far)

    def hand_on(c):
        return plan(inner.at[2], inner.at[3], c, f_s, f_r, core)

    def crossed(c):
        return plan(far_send, far_recv, c, c_s, c_r, core)

    def back(c):
        return plan(x_send, x_recv, c, r_s, r_r, far)

    depth = up.shape[0]
    if up_g.shape[0] > depth:
        up_g[depth:, :] = jnp.zeros((up_g.shape[0] - depth, up_g.shape[1]), bf16)
        down_g[depth:, :] = jnp.zeros((up_g.shape[0] - depth, up_g.shape[1]), bf16)

    def weights(left, right, out):
        def tile(j, _):
            part = pl.ds(pl.multiple_of(j * BLK, BLK), BLK)
            total = mm_tn(left[0, :, part], right[0])
            for k in range(1, 4):
                total = total + mm_tn(left[k, :, part], right[k])
            out[part, :] = total.astype(bf16)
            return 0

        lax.fori_loop(0, depth // BLK, tile, 0)

    def far_step(i, _):
        c = i // 2
        which = lax.rem(i, 2)
        here = pl.ds(pl.multiple_of(c * BLK, BLK), BLK)

        @pl.when(which == 0)
        def _():
            arrive(c).wait_recv()
            hand_on(c).start()

        @pl.when(which == 1)
        def _():
            hand_on(c).wait_recv()

        feed(2 + which, c * BLK)

        @pl.when(which == 1)
        def _():
            far_send[here, :] = mm_nt(gpre[3, here, :], up[...]).astype(bf16)
            crossed(c).start()
            g = mm_nt(gpre[2, here, :], up[...])
            crossed(c).wait_recv()
            x_send[here, :] = (g + far_recv[here, :].astype(f32)).astype(bf16)
            back(c).start()

        return 0

    lax.fori_loop(0, 2 * pieces, far_step, 0)

    def far_out(c, _):
        here = pl.ds(pl.multiple_of(c * BLK, BLK), BLK)
        bf_send[here, :] = mm(act[3, here, :], down[...]).astype(bf16)
        return 0

    lax.fori_loop(0, pieces, far_out, 0)
    far_branch = send(bf_send, bf_recv, b_s, b_r, tensor=core)
    weights(inner, gpre, up_g)
    weights(act, gs, down_g)
    far_branch.wait_recv()
    for c in range(pieces):
        here = pl.ds(c * BLK, BLK)
        b = mm(act[2, here, :], down[...])
        branch_x[here, :] = (b + bf_recv[here, :].astype(f32)).astype(bf16)
    near_copy.wait_recv()
    branch_copy.wait_recv()
    partial[...] += bn_recv[...].astype(f32)
    rows_copies = []
    for c in range(pieces):
        here = pl.ds(c * BLK, BLK)
        xhat, r = norm_parts(mid[here, :])
        back(c).wait_recv()
        g = gin[here, :] + near_recv[here, :].astype(f32) + x_recv[here, :].astype(f32)
        g_out = gs[0, here, :].astype(f32)
        gm = g_out + norm_back(g * gain, xhat, r)
        gmid[here, :] = gm
        there = pl.ds(pl.multiple_of(odd * rows + c * BLK, BLK), BLK)
        ga = gm.astype(bf16)
        rows_out[there, :] = ga
        rows_copies.append(
            send(rows_out.at[there], rows_out.at[there], o_s.at[c], o_r.at[c], tensor=core)
        )
        sums[0:1, :] += jnp.sum(g * xhat, 0, keepdims=True)
        sums[1:2, :] += jnp.sum(g, 0, keepdims=True)
        sums[2:3, :] += jnp.sum(ga.astype(f32), 0, keepdims=True)
        sums[3:4, :] += jnp.sum(g_out, 0, keepdims=True)
    for c in rows_copies:
        c.wait_recv()
    for c in range(pieces):
        sends += [hand_on(c), crossed(c), back(c)]
    for c in sends + rows_copies + [near_copy, branch_copy, far_branch]:
        c.wait_send()


def feed_forward(padded, o1, o2, wo1, wo2, hidden, gs, vecs, up, down):
    rows, depth = hidden.shape
    width = up.shape[1]
    pieces = rows // BLK
    vmem = pl.BlockSpec(memory_space=pltpu.VMEM)
    anyw = pl.BlockSpec(memory_space=pl.ANY)
    dma = pltpu.SemaphoreType.DMA
    wide = pltpu.VMEM((rows, depth), bf16)
    each = [dma((pieces,))] * 2
    return pl.pallas_call(
        feed_kernel,
        in_specs=[vmem] * 5 + [anyw] * 4 + [vmem] * 3,
        out_specs=[vmem] * 7,
        out_shape=[
            jax.ShapeDtypeStruct((2 * rows, depth), bf16),
            jax.ShapeDtypeStruct((rows, depth), f32),
            jax.ShapeDtypeStruct((rows, depth), f32),
            jax.ShapeDtypeStruct((rows, depth), bf16),
            jax.ShapeDtypeStruct((padded, width), bf16),
            jax.ShapeDtypeStruct((padded, width), bf16),
            jax.ShapeDtypeStruct((8, depth), f32),
        ],
        scratch_shapes=[
            pltpu.VMEM((4, rows, depth), bf16),
            pltpu.VMEM((4, rows, depth), bf16),
            pltpu.VMEM((4, rows, width), bf16),
            pltpu.VMEM((4, rows, width), bf16),
            pltpu.VMEM((rows, depth), f32),
            wide, wide, wide, wide, wide, wide, wide, wide, wide, wide, wide, wide,
            pltpu.VMEM((rows, depth), f32),
            dma((4,)),
            *each, *each, *each, *each,
            dma((2,)), dma((2,)),
            *each, *each,
            dma, dma,
            *each,
        ],
        compiler_params=pltpu.CompilerParams(
            collective_id=1, has_side_effects=True, vmem_limit_bytes=62 * 1024 * 1024
        ),
        name="feed_forward",
    )(o1, o2, wo1, wo2, hidden, *gs, vecs, up, down)

def back_kernel(n, chunk, piece, depth, lengths, up_h, down_h, branch_x, *rest):
    held, outs = rest[:LOADS], rest[LOADS : LOADS + 7]
    back_body(n, chunk, piece, depth, lengths, up_h, down_h, branch_x, held, outs, *rest[LOADS + 7 :])


LOADS = 27


def back_body(
    n, chunk, piece, depth, lengths, up_h, down_h, branch_x, held, outs,
    up_g, up_recv, rows_in, os, wo, qkv, lse, fence, sq, sk, normed, down_g, w, sel_w,
    hidden, gmid, vecs, sums, partial, ld_s,
    go, grads, dsums,
    dq_scr, dkt, dvt, dskt, later, fsum, qt, dot_,
    dsel, ng_send, ng_recv, ng_own, far_s, far_r, faro_s, faro_r, gb, ga,
    yd, yb, ya, ys, su, sd, sb, sa, ss, zu, zd, zb, za, zs,
    ts, small, out_s, bx_recv, sel_mine, sel_core, sel_far,
    core_s, core_r, f_s, f_r, sl_s, sl_r, y_s, y_r, z_s, z_r, t_s, t_r, az_s, az_r, ay_s, ay_r,
):
    fu, fd, fb, fa, small_out, input_grad, output = outs
    places = (
        up_g, rows_in, os.at[0], wo.at[0], qkv.at[0, 0], qkv.at[0, 1], qkv.at[0, 2],
        lse.at[0], fence, sq, sk, normed, down_g, wo.at[1], qkv.at[1, 0], qkv.at[1, 1],
        qkv.at[1, 2], lse.at[1], w.at[0], w.at[1], sel_w, os.at[1], hidden, gmid, vecs, sums, partial,
    )
    idx = lax.axis_index("dp")
    par = lax.rem(idx, 2)
    m = n // 2
    own = pl.ds(pl.multiple_of(par * m * chunk, m * chunk), m * chunk)
    loads = [
        pltpu.make_async_copy(h.at[own] if j in (0, 12) else h, v, ld_s.at[j])
        for j, (h, v) in enumerate(zip(held, places))
    ]
    for c in loads:
        c.start()

    def need(*which):
        for j in which:
            loads[j].wait()

    me = lax.axis_index("tensor")
    odd = lax.rem(me, 2)
    z = lax.div(idx, 2)
    rows = hidden.shape[0]
    seq_len = normed.shape[0]
    width = wo.shape[1]
    heads = width // HD
    ranks = 4
    core = me + 1 - 2 * odd
    far = lax.rem(me + 2, ranks)
    ydev = idx + 1 - 2 * par
    peers = [lax.rem(me + d, ranks) for d in range(1, ranks)]
    mates = []
    for b in range(m.bit_length() - 1):
        bit = lax.rem(lax.div(z, 1 << b), 2)
        mates.append(z + (1 - 2 * bit) * (1 << b))
    length = jnp.where(me < 2, lengths[0], lengths[1])
    meet(
        [{"tensor": p} for p in peers]
        + [{"dp": ydev}]
        + [{"dp": 2 * p + par} for p in mates]
    )
    at = par * m + z
    source = (gb, ga, small, up_g, down_g)
    yrecv = (yb, ya, ys, up_recv, yd)
    ysum = (sb, sa, ss, su, sd)
    zrecv = (zb, za, zs, zu, zd)
    full = (fb, fa, out_s, fu, fd)
    size = (gb.shape[0] // n, ga.shape[0] // n, piece, chunk, chunk)

    def plan(src, dst, send_sem, recv_sem, **where):
        return pltpu.make_async_remote_copy(
            src_ref=src, dst_ref=dst, send_sem=send_sem, recv_sem=recv_sem,
            device_id=where, device_id_type=pl.DeviceIdType.MESH,
        )

    def block(start, k):
        return pl.ds(pl.multiple_of(start * size[k], size[k]), size[k])

    def y_copy(k):
        half = m * size[k]
        give = pl.ds(pl.multiple_of((1 - par) * half, half), half)
        src = {3: up_h, 4: down_h}.get(k, source[k])
        return plan(src.at[give], yrecv[k], y_s.at[k], y_r.at[k], dp=ydev)

    bits = m.bit_length() - 1
    first_slot = [0]
    for b in range(bits):
        first_slot.append(first_slot[-1] + (m >> (b + 1)))

    def held_chunk(who, b, j):
        return lax.rem(who, 2 << b) + j * (2 << b)

    def mate(b):
        return mates[b]

    def z_copy(k, b, j):
        slot = first_slot[b] + j
        return plan(
            ysum[k].at[block(held_chunk(mate(b), b, j), k)], zrecv[k].at[slot],
            z_s.at[k, slot], z_r.at[k, slot], dp=2 * mate(b) + par,
        )

    def az_copy(k, b, j):
        slot = first_slot[b] + j
        mine = full[k].at[block(par * m + held_chunk(z, b, j), k)]
        return plan(mine, mine, az_s.at[k, slot], az_r.at[k, slot], dp=2 * mate(b) + par)

    def ay_copy(k, b, j):
        chunk_id, slot = (z, m - 1) if b is None else (held_chunk(mate(b), b, j), first_slot[b] + j)
        came = full[k].at[block(par * m + chunk_id, k)]
        return plan(came, came, ay_s.at[k, slot], ay_r.at[k, slot], dp=ydev)

    def stage(b):
        return range(m >> (b + 1))

    def z_start(k, b):
        for j in stage(b):
            z_copy(k, b, j).start()

    def y_finish(k):
        half = m * size[k]
        keep = pl.ds(pl.multiple_of(par * half, half), half)
        y_copy(k).wait_recv()
        mine = source[k][...] if k > 2 else source[k][keep, :]
        total = mine.astype(f32) + yrecv[k][...].astype(f32)
        ysum[k][...] = total.astype(ysum[k].dtype)
        z_start(k, 0)

    def z_next(k, b):
        for j in stage(b):
            z_copy(k, b, j).wait_recv()
            here = block(held_chunk(z, b, j), k)
            total = ysum[k][here, :].astype(f32) + zrecv[k][first_slot[b] + j].astype(f32)
            ysum[k][here, :] = total.astype(ysum[k].dtype)
        z_start(k, b + 1)

    def z_finish(k):
        for b in range(1, bits - 1):
            z_next(k, b)
        z_copy(k, bits - 1, 0).wait_recv()
        return ysum[k][block(z, k), :].astype(f32) + zrecv[k][first_slot[bits - 1]].astype(f32)

    def az_start(k, b):
        for j in stage(b):
            az_copy(k, b, j).start()

    def spread(k):
        az_start(k, bits - 1)
        ay_copy(k, None, 0).start()

    def forward(k, b):
        for j in stage(b):
            az_copy(k, b, j).wait_recv()
        if b > 0:
            az_start(k, b - 1)
        for j in stage(b):
            ay_copy(k, b, j).start()

    def forward_early(k):
        for b in reversed(range(1, bits)):
            forward(k, b)

    def far_copy(j):
        part = pl.ds(pl.multiple_of(j * width, width), width)
        return plan(far_s.at[part], far_r.at[part], f_s.at[2 + j], f_r.at[2 + j], tensor=far)

    out_copy = plan(faro_s, faro_r, f_s.at[0], f_r.at[0], tensor=far)
    branch_copy = plan(branch_x, bx_recv, f_s.at[1], f_r.at[1], tensor=far)
    core_copy = plan(ng_send, ng_recv, core_s, core_r, tensor=core)
    to_core = plan(sel_mine, sel_core, sl_s.at[0], sl_r.at[0], tensor=core)
    to_first = plan(sel_mine, sel_far, sl_s.at[1], sl_r.at[1], tensor=far)

    y_copy(3).start()
    y_copy(4).start()
    need(*range(13))

    def hook(g, i):
        if i == 1:

            @pl.when(g == 0)
            def _():
                y_finish(3)

            @pl.when(g == 1)
            def _():
                fu[block(at, 3), :] = z_finish(3).astype(bf16)
                spread(3)
                z_next(4, 0)

        if i == seq_len // BLK - 1:

            @pl.when(g == 1)
            def _():
                z_next(3, 0)
                y_finish(4)

    def group(g, _):
        @pl.when(g == 1)
        def _():
            need(*range(13, 18), 21)

        total = mm_tn(os[g], rows_in[...])

        @pl.when(g == 0)
        def _():
            faro_s[...] = total.astype(bf16)
            out_copy.start()

        @pl.when(g == 1)
        def _():
            out_copy.wait_recv()
            ga[width : 2 * width, :] = (total + faro_r[...].astype(f32)).astype(bf16)

        def head_grad(j, _):
            here = pl.ds(pl.multiple_of(j * BLK, BLK), BLK)
            go[here, :] = mm_nt(rows_in[here, :], wo[g]).astype(bf16)
            return 0

        lax.fori_loop(0, seq_len // BLK, head_grad, 0)
        for r in (dkt, dvt, dskt, later):
            r[...] = jnp.zeros_like(r)
        for i in reversed(range(seq_len // BLK)):
            here = pl.ds(i * BLK, BLK)
            bwd_block(
                i, heads, qkv.at[g, 0, here], qkv.at[g, 1], qkv.at[g, 2], go.at[here],
                lse.at[g, here], fence.at[here], sq.at[here], sk,
                grads.at[g, 0, here], dsums.at[g, 0, here],
                dq_scr, dkt, dvt, dskt, later, fsum, qt, dot_,
            )
            hook(g, i)
        grads[g, 1] = dkt[...].T.astype(bf16)
        grads[g, 2] = dvt[...].T.astype(bf16)
        dsums[g, 1] = dskt[...].T

        @pl.when(g == 1)
        def _():
            dsel[:, :HD] = (dsums[0, 0] + dsums[1, 0]).astype(bf16)
            dsel[:, HD:] = (dsums[0, 1] + dsums[1, 1]).astype(bf16)
            sel_mine[...] = mm_tn(dsel[...], normed[...]).astype(bf16)

            @pl.when(odd == 1)
            def _():
                to_core.start()

        def weight_grad(t, _):
            j = 2 - t
            here = pl.ds(pl.multiple_of(j * width, width), width)
            total = mm_tn(grads[g, j], normed[...])

            @pl.when(g == 0)
            def _():
                far_s[here, :] = total.astype(bf16)
                far_copy(j).start()

            @pl.when((g == 1) & (t == 0))
            def _():
                far_copy(2).wait_recv()
                ga[:width, :] = (total + far_r[2 * width :, :].astype(f32)).astype(bf16)
                y_copy(1).start()

                @pl.when(odd == 0)
                def _():
                    to_core.wait_recv()
                    sel_mine[...] = (
                        sel_mine[...].astype(f32) + sel_core[...].astype(f32)
                    ).astype(bf16)

                @pl.when(me == 2)
                def _():
                    to_first.start()

                branch_copy.start()

            @pl.when((g == 1) & (t > 0))
            def _():
                far_copy(j).wait_recv()
                gb[here, :] = (total + far_r[here, :].astype(f32)).astype(bf16)

            return 0

        lax.fori_loop(0, 3, weight_grad, 0)
        return 0

    if gb.shape[0] > 2 * width:
        gb[2 * width :, :] = jnp.zeros((gb.shape[0] - 2 * width, depth), bf16)
        ga[2 * width :, :] = jnp.zeros((ga.shape[0] - 2 * width, depth), bf16)
    lax.fori_loop(0, 2, group, 0)

    @pl.when(me == 0)
    def _():
        to_first.wait_recv()
        both = sel_mine[...].astype(f32) + sel_far[...].astype(f32)
        gb[:HD, :] = (gb[:HD, :].astype(f32) + both[:HD, :]).astype(bf16)
        gb[width : width + HD, :] = (
            gb[width : width + HD, :].astype(f32) + both[HD:, :]
        ).astype(bf16)

    y_copy(0).start()
    forward_early(3)
    fd[block(at, 4), :] = z_finish(4).astype(bf16)
    spread(4)
    y_finish(1)
    need(18, 19, 20, *range(22, LOADS))

    def normed_grad(t, _):
        mine = t // 2
        step = pl.multiple_of(lax.rem(t, 2) * BLK, BLK)
        side = mine * odd + (1 - mine) * (1 - odd)
        part = pl.ds(pl.multiple_of(side * rows + step, BLK), BLK)
        here = pl.ds(step, BLK)
        total = mm(dsel[part, :], sel_w[...])
        for g in range(2):
            for j in range(3):
                total = total + mm(grads[g, j, part, :], w[g, j * width : (j + 1) * width, :])

        @pl.when(mine == 0)
        def _():
            ng_send[here, :] = total.astype(bf16)

        @pl.when(mine == 1)
        def _():
            ng_own[here, :] = total

        @pl.when(t == 1)
        def _():
            core_copy.start()

        return 0

    lax.fori_loop(0, 4, normed_grad, 0)
    z_next(1, 0)
    y_finish(0)
    xhat, r = norm_parts(hidden[...].astype(f32))
    core_copy.wait_recv()
    grad = ng_own[...] + ng_recv[...].astype(f32)
    input_grad[...] = (gmid[...] + norm_back(grad * vecs[5:6, :], xhat, r)).astype(bf16)
    small[...] = jnp.zeros_like(small)
    dgain = jnp.sum(grad * xhat, 0, keepdims=True)
    dshift = jnp.sum(grad, 0, keepdims=True)
    lines = depth // 128
    for j in range(lines):
        small[j : j + 1, :] = dgain[:, j * 128 : (j + 1) * 128]
        small[lines + j : lines + j + 1, :] = dshift[:, j * 128 : (j + 1) * 128]
    for slot, which in ((2, 2), (3, 0), (4, 1), (5, 3)):
        for j in range(lines):
            small[slot * lines + j : slot * lines + j + 1, :] = sums[
                which : which + 1, j * 128 : (j + 1) * 128
            ]
    wide_lines = up_g.shape[1] // 128
    for j in range(wide_lines):
        small[pl.ds(6 * lines + me * wide_lines + j, 1), :] = sums[4:5, j * 128 : (j + 1) * 128]
    base = small_lines(depth, up_g.shape[1]) - 4 * ranks
    for owner, g in ((me, 1), (far, 0)):
        for j, which in enumerate((0, 2)):
            total = jnp.sum(grads[g, which].astype(f32), 0, keepdims=True)
            line = base + 4 * owner + 2 * j
            small[pl.ds(line, 1), :] = total[:, :128]
            small[pl.ds(line + 1, 1), : width - 128] = total[:, 128:]
    total = jnp.sum(dsel[...].astype(f32), 0, keepdims=True)
    lane = lax.broadcasted_iota(jnp.int32, total.shape, 1)
    small[base : base + 1, :] += jnp.where(lane < HD, total, 0.0)
    y_copy(2).start()

    fa[block(at, 1), :] = z_finish(1).astype(bf16)
    spread(1)
    z_next(0, 0)
    y_finish(2)
    forward(3, 0)
    forward_early(4)
    z_next(2, 0)
    forward_early(1)
    fb[block(at, 0), :] = z_finish(0).astype(bf16)
    spread(0)
    forward(4, 0)
    ts[me] = z_finish(2)

    def t_copy(d):
        return plan(ts.at[me], ts.at[me], t_s.at[d], t_r.at[d], tensor=peers[d])

    for d in range(ranks - 1):
        t_copy(d).start()
    for d in range(ranks - 1):
        t_copy(d).wait_recv()
    vec = ts[0]
    for d in range(1, ranks):
        vec = vec + ts[d]
    out_s[block(at, 2), :] = vec
    spread(2)
    forward(1, 0)
    forward_early(0)
    forward_early(2)
    token = odd * rows + lax.broadcasted_iota(jnp.int32, (rows, 1), 0)
    live = jnp.where(token < length, 1.0, 0.0)
    branch_copy.wait_recv()
    output[...] = (live * (partial[...] + bx_recv[...].astype(f32))).astype(bf16)
    forward(0, 0)
    forward(2, 0)
    for k in range(5):
        ay_copy(k, None, 0).wait_recv()
        for b in range(bits):
            for j in stage(b):
                ay_copy(k, b, j).wait_recv()

    @pl.when(odd == 1)
    def _():
        to_core.wait_send()

    @pl.when(me == 2)
    def _():
        to_first.wait_send()

    small_out[...] = out_s[...]
    for c in (far_copy(0), far_copy(1), far_copy(2), out_copy, branch_copy, core_copy):
        c.wait_send()
    for d in range(ranks - 1):
        t_copy(d).wait_send()
    for k in range(5):
        y_copy(k).wait_send()
        ay_copy(k, None, 0).wait_send()
        for b in range(bits):
            for j in stage(b):
                z_copy(k, b, j).wait_send()
                az_copy(k, b, j).wait_send()
                ay_copy(k, b, j).wait_send()


def front_kernel(
    lengths, hidden, out_grad, vecs, qkv, qv_bias, wo,
    *rest,
):
    outs, gcore, gfar, gcross = rest[:18], rest[18], rest[19], rest[20]
    kept = rest[21:39]
    front_body(
        lengths, hidden, out_grad, vecs, qkv, qv_bias, wo, outs, kept, gcore, gfar, gcross, *rest[39:]
    )


def front_body(
    lengths, hidden, out_grad, vecs, qkv, qv_bias, wo, outs, kept, gcore, gfar, gcross,
    out_scr, carry, sel_b, bias2,
    st_s, nm_s, nm_r, gc_s, gc_r, sl_s, sl_r, w_s, w_r, p_s, p_r, e_s, e_r, g_s, g_r, h_s, h_r,
):
    me = lax.axis_index("tensor")
    idx = lax.axis_index("dp")
    odd = lax.rem(me, 2)
    core = me + 1 - 2 * odd
    far = lax.rem(me + 2, 4)
    par = lax.rem(idx, 2)
    ydev = idx + 1 - 2 * par
    rows = hidden.shape[0]
    seq_len = 2 * rows
    width = wo.shape[0]
    heads = width // HD
    (normed, q1, k1, v1, lse1, o1, q2, k2, v2, lse2, o2, fence, sq, sk, w2, wo2, selw, g0) = kept
    stores = []

    def store(*which):
        for j in which:
            copy = pltpu.make_async_copy(kept[j], outs[j], st_s.at[j])
            copy.start()
            stores.append(copy)

    length = jnp.where(me < 2, lengths[0], lengths[1])

    def sel_copies(k, where):
        return [
            pltpu.make_async_remote_copy(
                src_ref=a, dst_ref=a, send_sem=sl_s.at[k, j], recv_sem=sl_r.at[j],
                device_id={"tensor": where}, device_id_type=pl.DeviceIdType.MESH,
            )
            for j, a in enumerate((selw, sel_b))
        ]

    @pl.when(me == 0)
    def _():
        selw[:HD, :] = qkv[:HD, :]
        selw[HD:, :] = qkv[width : width + HD, :]
        sel_b[...] = qv_bias[...]

    meet([{"tensor": core}, {"tensor": far}, {"dp": ydev}])

    @pl.when(me == 0)
    def _():
        for c in sel_copies(0, far) + sel_copies(1, core):
            c.start()

    share = width // 2
    halves = [
        (src, dst, pl.ds(pl.multiple_of(base + par * share, share), share))
        for src, dst, base in (
            (qkv, w2, 0), (qkv, w2, width), (qkv, w2, 2 * width), (wo, wo2, 0)
        )
    ]
    extra = send(qv_bias, bias2, e_s, e_r, tensor=far)
    cross = [
        send(src.at[part], dst.at[part], w_s.at[j], w_r.at[j], tensor=far)
        for j, (src, dst, part) in enumerate(halves)
    ]
    passed = []

    def pass_on(j):
        cross[j].wait_recv()
        _, dst, part = halves[j]
        passed.append(send(dst.at[part], dst.at[part], p_s.at[j], p_r.at[j], dp=ydev))

    spot = pl.multiple_of(odd * rows, rows)
    norm_copies = []
    for c in range(rows // BLK):
        here = pl.ds(c * BLK, BLK)
        there = pl.ds(pl.multiple_of(spot + c * BLK, BLK), BLK)
        xhat, _ = norm_parts(hidden[here, :].astype(f32))
        normed[there, :] = (xhat * vecs[5:6, :] + vecs[6:7, :]).astype(bf16)
        norm_copies.append(
            send(normed.at[there], normed.at[there], nm_s.at[c], nm_r.at[c], tensor=core)
        )
    row = odd * rows + lax.broadcasted_iota(jnp.int32, (rows, 1), 0)
    live = jnp.where(row < length, 1.0, 0.0)
    g0[...] = (out_grad[...].astype(f32) * live).astype(bf16)
    store(17)
    gc = send(g0, gcore, gc_s, gc_r, tensor=core)
    g_parts = [pl.ds(c * BLK, BLK) for c in range(rows // BLK)]
    gf = [
        send(g0.at[p], gfar.at[p], g_s.at[c], g_r.at[c], tensor=far) for c, p in enumerate(g_parts)
    ]

    def project(weight, bias, out):
        def tile(j, _):
            here = pl.ds(pl.multiple_of(j * BLK, BLK), BLK)
            y = mm_nt(normed[here, :], weight)
            if bias is not None:
                y = y + bias
            out[here, :] = y.astype(bf16)
            return 0

        lax.fori_loop(0, seq_len // BLK, tile, 0)

    @pl.when(me == 2)
    def _():
        for c in sel_copies(0, far):
            c.wait_recv()
        for c in sel_copies(1, core):
            c.start()

    for c in norm_copies:
        c.wait_recv()
    store(0)
    project(qkv[:width, :], qv_bias[0:1, :], q1)
    project(qkv[width : 2 * width, :], None, k1)
    project(qkv[2 * width :, :], qv_bias[1:2, :], v1)

    @pl.when(odd == 1)
    def _():
        for c in sel_copies(1, core):
            c.wait_recv()

    store(1, 2, 3)
    def select(j, _):
        here = pl.ds(pl.multiple_of(j * BLK, BLK), BLK)
        y = mm_nt(normed[here, :], selw[...])
        sq[here, :] = (y[:, :HD] + sel_b[0:1, :HD]).astype(bf16)
        sk[here, :] = y[:, HD:].astype(bf16)
        return 0

    lax.fori_loop(0, seq_len // BLK, select, 0)
    store(12, 13, 16)
    carry[...] = jnp.zeros_like(carry)
    pass_on(0)
    for i in range(seq_len // BLK):
        here = pl.ds(i * BLK, BLK)
        make_fence(i, seq_len, length, sq.at[here], sk, fence.at[here], carry)
        fwd_block(
            i, heads, out_scr, q1.at[here], k1, v1, fence.at[here], o1.at[here], lse1.at[here]
        )
        if i < 3:
            pass_on(i + 1)
    store(4, 5, 11)
    extra.wait_recv()
    for j, (out, bias) in enumerate(((q2, bias2[0:1, :]), (k2, None), (v2, bias2[1:2, :]))):
        passed[j].wait_recv()
        project(w2[j * width : (j + 1) * width, :], bias, out)
        store(6 + j)
    store(14)
    gx = []

    def pass_g(c):
        gf[c].wait_recv()
        p = g_parts[c]
        gx.append(send(gfar.at[p], gcross.at[p], h_s.at[c], h_r.at[c], tensor=core))

    for i in range(seq_len // BLK):
        here = pl.ds(i * BLK, BLK)
        fwd_block(
            i, heads, out_scr, q2.at[here], k2, v2, fence.at[here], o2.at[here], lse2.at[here]
        )
    store(9, 10)
    for c in range(rows // BLK):
        pass_g(c)
    gc.wait_recv()
    passed[3].wait_recv()
    store(15)
    for c in gx:
        c.wait_recv()

    @pl.when(me == 0)
    def _():
        for c in sel_copies(0, far):
            c.wait_send()

    @pl.when(odd == 0)
    def _():
        for c in sel_copies(1, core):
            c.wait_send()

    for c in cross + passed + norm_copies + gf + gx + [gc, extra]:
        c.wait_send()
    for c in stores:
        c.wait()


def front(lengths, hidden, out_grad, vecs, qkv, qv_bias, wo):
    rows, depth = hidden.shape
    seq_len, width = 2 * rows, wo.shape[0]
    pieces = rows // BLK
    vmem = pl.BlockSpec(memory_space=pltpu.VMEM)
    dma = pltpu.SemaphoreType.DMA
    heads = jax.ShapeDtypeStruct((seq_len, width), bf16)
    lse = jax.ShapeDtypeStruct((seq_len, 128), f32)
    sel = jax.ShapeDtypeStruct((seq_len, HD), bf16)
    wide = jax.ShapeDtypeStruct((rows, depth), bf16)
    kept = [
        jax.ShapeDtypeStruct((seq_len, depth), bf16),
        heads, heads, heads, lse, heads,
        heads, heads, heads, lse, heads,
        jax.ShapeDtypeStruct((seq_len, seq_len), f32),
        sel, sel,
        jax.ShapeDtypeStruct(qkv.shape, bf16),
        jax.ShapeDtypeStruct(wo.shape, bf16),
        jax.ShapeDtypeStruct((2 * HD, depth), bf16),
        wide,
    ]
    return pl.pallas_call(
        front_kernel,
        in_specs=[pl.BlockSpec(memory_space=pltpu.SMEM)] + [vmem] * 6,
        out_specs=[pl.BlockSpec(memory_space=pl.ANY)] * 21,
        out_shape=kept + [wide, wide, wide],
        scratch_shapes=[pltpu.VMEM(a.shape, a.dtype) for a in kept]
        + [
            pltpu.VMEM((BLK, width), f32),
            pltpu.VMEM((8, seq_len), f32),
            pltpu.VMEM((2, width), f32),
            pltpu.VMEM((2, width), f32),
            dma((18,)),
            dma((pieces,)), dma((pieces,)),
            dma, dma,
            dma((2, 2)), dma((2,)),
            dma((4,)), dma((4,)),
            dma((4,)), dma((4,)),
            dma, dma,
            dma((pieces,)), dma((pieces,)),
            dma((pieces,)), dma((pieces,)),
        ],
        compiler_params=pltpu.CompilerParams(
            collective_id=2, has_side_effects=True, vmem_limit_bytes=60 * 1024 * 1024
        ),
        name="front",
    )(lengths, hidden, out_grad, vecs, qkv, qv_bias, wo)


def small_lines(depth, hidden):
    return (6 * depth + 4 * hidden) // 128 + 16


def go_back(n, set1, set2, fence, sq, sk, rows_in, o1, o2, wo1, wo2, normed, w1, w2, sel_w,
            hidden, vecs, gmid, sums, partial, branch_x, lengths, up_g, down_g):
    m = n // 2
    chunk = up_g.shape[0] // n
    rows, depth = hidden.shape
    piece = -(-small_lines(depth, up_g.shape[1]) // (8 * n)) * 8
    seq_len, width = set1[0].shape
    half, shalf = m * chunk, m * piece
    ranks = 4
    wf = up_g.shape[1]
    small_chunk = -(-2 * width // (16 * n)) * 16
    part_half = m * small_chunk
    vmem = pl.BlockSpec(memory_space=pltpu.VMEM)
    dma = pltpu.SemaphoreType.DMA
    q1, k1, v1, lse1 = set1
    q2, k2, v2, lse2 = set2
    held = (up_g, rows_in, o2, wo2, q2, k2, v2, lse2, fence, sq, sk, normed, down_g, wo1,
            q1, k1, v1, lse1, w2, w1, sel_w, o1, hidden, gmid, vecs, sums, partial)
    anyw = pl.BlockSpec(memory_space=pl.ANY)
    like = lambda a: pltpu.VMEM(a.shape, a.dtype)
    return pl.pallas_call(
        lambda *refs: back_kernel(n, chunk, piece, depth, *refs),
        in_specs=[pl.BlockSpec(memory_space=pltpu.SMEM)] + [anyw] * (LOADS + 3),
        out_specs=[vmem] * 7,
        out_shape=[
            jax.ShapeDtypeStruct((n * chunk, wf), bf16),
            jax.ShapeDtypeStruct((n * chunk, wf), bf16),
            jax.ShapeDtypeStruct((n * small_chunk, depth), bf16),
            jax.ShapeDtypeStruct((n * small_chunk, depth), bf16),
            jax.ShapeDtypeStruct((n * piece, 128), f32),
            jax.ShapeDtypeStruct((rows, depth), bf16),
            jax.ShapeDtypeStruct((rows, depth), bf16),
        ],
        scratch_shapes=[
            pltpu.VMEM((half, wf), bf16), pltpu.VMEM((half, wf), bf16), like(rows_in),
            pltpu.VMEM((2, seq_len, width), bf16),
            pltpu.VMEM((2, width, depth), bf16),
            pltpu.VMEM((2, 3, seq_len, width), bf16),
            pltpu.VMEM((2, seq_len, 128), f32),
            like(fence), like(sq), like(sk), like(normed), pltpu.VMEM((half, wf), bf16),
            pltpu.VMEM((2, 3 * width, depth), bf16),
            like(sel_w), like(hidden), like(gmid), like(vecs), like(sums), like(partial),
            dma((LOADS,)),
            pltpu.VMEM((seq_len, width), bf16),
            pltpu.VMEM((2, 3, seq_len, width), bf16),
            pltpu.VMEM((2, 2, seq_len, HD), f32),
            pltpu.VMEM((BLK, width), f32),
            pltpu.VMEM((width, seq_len), f32),
            pltpu.VMEM((width, seq_len), f32),
            pltpu.VMEM((HD, seq_len), f32),
            pltpu.VMEM((8, seq_len), f32),
            pltpu.VMEM((BLK, seq_len), f32),
            pltpu.VMEM((width, BLK), bf16),
            pltpu.VMEM((width, BLK), bf16),
            pltpu.VMEM((seq_len, 128), bf16),
            pltpu.VMEM((rows, depth), bf16),
            pltpu.VMEM((rows, depth), bf16),
            pltpu.VMEM((rows, depth), f32),
            pltpu.VMEM((3 * width, depth), bf16),
            pltpu.VMEM((3 * width, depth), bf16),
            pltpu.VMEM((width, depth), bf16),
            pltpu.VMEM((width, depth), bf16),
            pltpu.VMEM((n * small_chunk, depth), bf16),
            pltpu.VMEM((n * small_chunk, depth), bf16),
            *[pltpu.VMEM((h, depth), bf16) for h in (half, part_half, part_half)],
            pltpu.VMEM((shalf, 128), f32),
            *[pltpu.VMEM((h, depth), bf16) for h in (half, half, part_half, part_half)],
            pltpu.VMEM((shalf, 128), f32),
            *[
                pltpu.VMEM((m - 1, c, depth), bf16)
                for c in (chunk, chunk, small_chunk, small_chunk)
            ],
            pltpu.VMEM((m - 1, piece, 128), f32),
            pltpu.VMEM((ranks, piece, 128), f32),
            pltpu.VMEM((n * piece, 128), f32),
            pltpu.VMEM((n * piece, 128), f32),
            pltpu.VMEM((rows, depth), bf16),
            *[pltpu.VMEM((2 * HD, depth), bf16)] * 3,
            dma, dma,
            dma((5,)), dma((5,)),
            dma((2,)), dma((2,)),
            dma((5,)), dma((5,)),
            dma((5, m - 1)), dma((5, m - 1)),
            dma((3,)), dma((3,)),
            dma((5, m - 1)), dma((5, m - 1)),
            dma((5, m)), dma((5, m)),
        ],
        compiler_params=pltpu.CompilerParams(
            collective_id=0, has_side_effects=True, vmem_limit_bytes=66_900_000
        ),
        name="go_back",
    )(lengths, up_g, down_g, branch_x, *held)


def shards(
    hidden_in,
    lengths,
    ln1_gain,
    ln1_shift,
    qkv_weight,
    qv_bias,
    out_weight,
    out_bias,
    ln2_gain,
    ln2_shift,
    up_weight,
    up_bias,
    down_weight,
    down_bias,
    out_grad,
):
    n = lax.axis_size("dp")
    ranks = lax.axis_size("tensor")
    me = lax.axis_index("tensor")
    depth = hidden_in.shape[1]
    width = qkv_weight.shape[2]
    hidden = up_bias.shape[0]
    padded = -(-depth // (16 * n)) * 16 * n
    spot = jnp.arange(8)[:, None]
    vecs = jnp.zeros((8, depth), f32)
    for j, vec in enumerate(
        (out_bias, ln2_gain, ln2_shift, down_bias, up_bias.astype(f32), ln1_gain, ln1_shift)
    ):
        vecs = jnp.where(spot == j, vec[None], vecs)
    qkv_rows = jnp.swapaxes(qkv_weight, 1, 2).reshape(3 * width, depth)
    (normed, q1, k1, v1, lse1, o1, q2, k2, v2, lse2, o2, fence, sq, sk, qkv_far, out_far, sel_w,
     *grad_rows) = front(lengths, hidden_in, out_grad, vecs, qkv_rows, qv_bias, out_weight)
    attn_rows, grad_middle, partial, branch_x, up_part, down_part, sums = feed_forward(
        padded, o1, o2, out_weight, out_far, hidden_in, grad_rows, vecs, up_weight, down_weight
    )
    full_u, full_d, full_b, full_a, small, input_grad, output = go_back(
        n, (q1, k1, v1, lse1), (q2, k2, v2, lse2), fence, sq, sk, attn_rows, o1, o2,
        out_weight, out_far, normed, qkv_rows, qkv_far, sel_w, hidden_in, vecs,
        grad_middle, sums, partial, branch_x, lengths, up_part, down_part,
    )
    vectors = small[: 6 * depth // 128].reshape(6, depth)
    lines = (6 * depth + ranks * hidden) // 128
    up_all = small[6 * depth // 128 : lines].reshape(ranks, hidden)
    qv_all = small[lines : lines + 4 * ranks].reshape(ranks, 2, 256)
    up_bias_grad = lax.dynamic_index_in_dim(up_all, me, 0, keepdims=False)
    qv_bias_grad = lax.dynamic_index_in_dim(qv_all, me, 0, keepdims=False)[:, :width]
    qkv_grad = jnp.concatenate([full_b[: 2 * width], full_a[:width]], 0).astype(f32)
    qkv_grad = jnp.swapaxes(qkv_grad.reshape(3, width, depth), 1, 2)
    out_weight_grad = full_a[width : 2 * width].astype(f32)
    return (
        output,
        input_grad,
        vectors[0],
        vectors[1],
        qkv_grad,
        qv_bias_grad,
        out_weight_grad,
        vectors[2],
        vectors[3],
        vectors[4],
        full_u[:depth].astype(f32),
        up_bias_grad,
        full_d[:depth].astype(f32),
        vectors[5],
    )


def solution(mesh):
    return jax.shard_map(
        shards,
        mesh=mesh,
        in_specs=(
            P(("dp", "tensor"), None),
            P("dp"),
            P(),
            P(),
            P(None, None, "tensor"),
            P(None, "tensor"),
            P("tensor", None),
            P(),
            P(),
            P(),
            P(None, "tensor"),
            P("tensor"),
            P("tensor", None),
            P(),
            P(("dp", "tensor"), None),
        ),
        out_specs=(
            P(("dp", "tensor"), None),
            P(("dp", "tensor"), None),
            P(),
            P(),
            P(None, None, "tensor"),
            P(None, "tensor"),
            P("tensor", None),
            P(),
            P(),
            P(),
            P(None, "tensor"),
            P("tensor"),
            P("tensor", None),
            P(),
        ),
        check_vma=False,
    )
```

```python
import math

import jax
import jax.numpy as jnp
from jax import lax
from jax.experimental import pallas as pl
from jax.experimental.pallas import tpu as pltpu
from jax.sharding import PartitionSpec as P

HD = 64
BLK = 256
BIG = 1e30
sel_factor = 4.0
score_scale = 1.0 / math.sqrt(HD)
f32 = jnp.float32
bf16 = jnp.bfloat16


def mm(a, b):
    return lax.dot_general(a, b, (((1,), (0,)), ((), ())), preferred_element_type=f32)


def mm_nt(a, b):
    return lax.dot_general(a, b, (((1,), (1,)), ((), ())), preferred_element_type=f32)


def flip(a):
    return a.astype(f32).T.astype(bf16)


def split_mm(tri, x):
    hi = x.astype(bf16)
    lo = (x - hi.astype(f32)).astype(bf16)
    return mm(tri, hi) + mm(tri, lo)


def head_mask(h, width):
    return lax.broadcasted_iota(jnp.int32, (BLK, width), 1) // HD == h


def masked_rows(x, mask, scale):
    return jnp.where(mask, x.astype(f32) * scale, 0.0).astype(bf16)


def fwd_block(i, heads, first, q_ref, k_ref, v_ref, fence, o_ref, lse_ref):
    width = q_ref.shape[1]
    cols = (i + 1) * BLK
    keys = k_ref[:cols, :]
    vals = v_ref[:cols, :]
    fenced = fence[:, :cols]
    lane = lax.broadcasted_iota(jnp.int32, (BLK, 128), 1)
    lse_ref[...] = jnp.zeros_like(lse_ref)
    out_scr = first

    def head(h, _):
        mask = head_mask(h, width)
        s = mm_nt(masked_rows(q_ref[...], mask, score_scale), keys) - fenced
        top = jnp.max(s, -1, keepdims=True)
        e = jnp.exp(s - top)
        total = jnp.sum(e, -1, keepdims=True)
        p = (e * (1.0 / total)).astype(bf16)
        out = mm(p, vals)
        out_scr[...] = jnp.where(mask, out, out_scr[...])
        lse_ref[...] = jnp.where(lane == h, top + jnp.log(total), lse_ref[...])
        return 0

    lax.fori_loop(0, heads, head, 0)
    o_ref[...] = out_scr[...].astype(bf16)


def make_fence(i, seq_len, length, sq_ref, sk_ref, fence, carry):
    cols = (i + 1) * BLK
    s0 = mm_nt(sq_ref[...], sk_ref[:cols, :]) * score_scale
    row = i * BLK + lax.broadcasted_iota(jnp.int32, (BLK, cols), 0)
    col = lax.broadcasted_iota(jnp.int32, (BLK, cols), 1)
    picked = (col >= 1) & (col < row)
    sel = jnp.where(picked, jnp.maximum(s0, 0.0), 0.0) * (sel_factor / seq_len)
    r2 = lax.broadcasted_iota(jnp.int32, (BLK, BLK), 0)
    c2 = lax.broadcasted_iota(jnp.int32, (BLK, BLK), 1)
    tri = jnp.where(c2 < r2, 1.0, 0.0).astype(bf16)
    total = carry[0:1, :cols] + split_mm(tri, sel)
    carry[0:1, :cols] = total[BLK - 1 : BLK, :] + sel[BLK - 1 : BLK, :]
    fence[:, :cols] = jnp.where((col <= row) & (col < length), total, BIG)


def bwd_block(i, heads, q_ref, k_ref, v_ref, do_ref, lse_ref, f_ref, sq_ref, sk_ref,
              dq_ref, dsq_ref, dq_scr, dkt, dvt, dskt, later, fsum, qt, dot_):
    width = q_ref.shape[1]
    seq_len = k_ref.shape[0]
    cols = (i + 1) * BLK
    keys = k_ref[:cols, :]
    vals = v_ref[:cols, :]
    lane = lax.broadcasted_iota(jnp.int32, (BLK, 128), 1)
    qt[...] = (q_ref[...].astype(f32) * score_scale).T.astype(bf16)
    dot_[...] = flip(do_ref[...])
    fsum[:, :cols] = jnp.zeros((BLK, cols), f32)

    def head(h, _):
        mask = head_mask(h, width)
        lse = jnp.sum(jnp.where(lane == h, lse_ref[...], 0.0), -1, keepdims=True)
        s = mm_nt(masked_rows(q_ref[...], mask, score_scale), keys)
        p = jnp.exp(s - f_ref[:, :cols] - lse)
        dp = mm_nt(masked_rows(do_ref[...], mask, 1.0), vals)
        delta = jnp.sum(p * dp, -1, keepdims=True)
        g = (p * (dp - delta)).astype(bf16)
        rows = pl.ds(pl.multiple_of(h * HD, HD), HD)
        dq_scr[...] = jnp.where(mask, mm(g, keys), dq_scr[...])
        dkt[rows, :cols] += mm(qt[rows, :], g)
        dvt[rows, :cols] += mm(dot_[rows, :], p.astype(bf16))
        fsum[:, :cols] += g.astype(f32)
        return 0

    lax.fori_loop(0, heads, head, 0, unroll=True)
    dq_ref[...] = (dq_scr[...] * score_scale).astype(bf16)
    grad = -fsum[:, :cols]
    r2 = lax.broadcasted_iota(jnp.int32, (BLK, BLK), 0)
    c2 = lax.broadcasted_iota(jnp.int32, (BLK, BLK), 1)
    tri = jnp.where(c2 > r2, 1.0, 0.0).astype(bf16)
    dsel = later[0:1, :cols] + split_mm(tri, grad)
    later[0:1, :cols] = dsel[0:1, :] + grad[0:1, :]
    s0 = mm_nt(sq_ref[...], sk_ref[:cols, :])
    row = i * BLK + lax.broadcasted_iota(jnp.int32, (BLK, cols), 0)
    col = lax.broadcasted_iota(jnp.int32, (BLK, cols), 1)
    keep = (col >= 1) & (col < row) & (s0 > 0)
    gsel = jnp.where(keep, dsel * (sel_factor / seq_len), 0.0).astype(bf16)
    dsq_ref[...] = mm(gsel, sk_ref[:cols, :]) * score_scale
    sqt = (sq_ref[...].astype(f32) * score_scale).T.astype(bf16)
    dskt[:, :cols] += mm(sqt, gsel)


epsilon = 1e-05


def mm_tn(a, b):
    return lax.dot_general(a, b, (((0,), (0,)), ((), ())), preferred_element_type=f32)


def send(src, dst, send_sem, recv_sem, **where):
    copy = pltpu.make_async_remote_copy(
        src_ref=src,
        dst_ref=dst,
        send_sem=send_sem,
        recv_sem=recv_sem,
        device_id=where,
        device_id_type=pl.DeviceIdType.MESH,
    )
    copy.start()
    return copy


def meet(devices):
    barrier = pltpu.get_barrier_semaphore()
    for where in devices:
        pl.semaphore_signal(barrier, inc=1, device_id=where, device_id_type=pl.DeviceIdType.MESH)
    pl.semaphore_wait(barrier, len(devices))


def norm_parts(x):
    centre = x - jnp.mean(x, -1, keepdims=True)
    r = lax.rsqrt(jnp.mean(centre * centre, -1, keepdims=True) + epsilon)
    return centre * r, r


def norm_back(e, xhat, r):
    return r * (e - jnp.mean(e, -1, keepdims=True) - xhat * jnp.mean(e * xhat, -1, keepdims=True))


def gelu_pair(u):
    k = math.sqrt(2.0 / math.pi)
    square = u * u
    t = jnp.tanh(k * u * (1.0 + 0.044715 * square))
    act = 0.5 * u * (1.0 + t)
    slope = 0.5 * (1.0 + t) + 0.5 * u * (1.0 - t * t) * (k * (1.0 + 3.0 * 0.044715 * square))
    return act, slope


def feed_kernel(
    o1, o2, wo1, wo2, hidden, g0, g1, g2, g3, vecs, up, down,
    rows_out, gmid, partial, branch_x, up_g, down_g, sums,
    inner, gs, act, gpre, mid, attn_send, attn_recv,
    near_send, near_recv, far_send, far_recv, x_send, x_recv,
    bn_send, bn_recv, bf_send, bf_recv, gin,
    g_sem, a_s, a_r, i_s, i_r, x_s, x_r, f_s, f_r, n_s, n_r, c_s, c_r, r_s, r_r, b_s, b_r, o_s, o_r,
):
    me = lax.axis_index("tensor")
    odd = lax.rem(me, 2)
    core = me + 1 - 2 * odd
    far = lax.rem(me + 2, 4)
    rows = hidden.shape[0]
    pieces = rows // BLK
    loads = [pltpu.make_async_copy(g, gs.at[i], g_sem.at[i]) for i, g in enumerate((g0, g1, g2, g3))]
    for c in loads:
        c.start()
    meet([{"tensor": core}, {"tensor": far}])
    out_bias, gain, shift, down_bias, up_bias = (vecs[j : j + 1, :] for j in range(5))

    def attn(start):
        part = pl.ds(pl.multiple_of(start, BLK), BLK)
        return mm(o1[part, :], wo1[...]) + mm(o2[part, :], wo2[...])

    sends = []
    attn_copies = []
    for c in range(pieces):
        here = pl.ds(c * BLK, BLK)
        attn_send[here, :] = attn((1 - odd) * rows + c * BLK).astype(bf16)
        attn_copies.append(send(attn_send.at[here], attn_recv.at[here], a_s.at[c], a_r.at[c], tensor=core))
    inner_copies, far_copies = [], []
    for c in range(pieces):
        here = pl.ds(c * BLK, BLK)
        mine = attn(odd * rows + c * BLK)
        attn_copies[c].wait_recv()
        m = hidden[here, :].astype(f32) + (mine + attn_recv[here, :].astype(f32)) + out_bias
        mid[here, :] = m
        xhat, r = norm_parts(m)
        inner[0, here, :] = (xhat * gain + shift).astype(bf16)
        far_copies.append(send(inner.at[0, here], inner.at[2, here], x_s.at[c], x_r.at[c], tensor=far))
        inner_copies.append(send(inner.at[0, here], inner.at[1, here], i_s.at[c], i_r.at[c], tensor=core))
    sends += attn_copies + inner_copies + far_copies
    for c in loads:
        c.wait()
    sums[...] = jnp.zeros_like(sums)

    def feed(slot, start):
        part = pl.ds(pl.multiple_of(start, BLK), BLK)
        pre = mm(inner[slot, part, :], up[...]) + up_bias
        a, slope = gelu_pair(pre)
        act[slot, part, :] = a.astype(bf16)
        gp = (mm_nt(gs[slot, part, :], down[...]) * slope).astype(bf16)
        gpre[slot, part, :] = gp
        sums[4:5, :] += jnp.sum(gp.astype(f32), 0, keepdims=True)

    def near(i, _):
        @pl.when(i == pieces)
        def _():
            for c in inner_copies:
                c.wait_recv()

        feed(i // pieces, lax.rem(i, pieces) * BLK)
        return 0

    lax.fori_loop(0, 2 * pieces, near, 0)

    def near_other(c, _):
        part = pl.ds(pl.multiple_of(c * BLK, BLK), BLK)
        near_send[part, :] = mm_nt(gpre[1, part, :], up[...]).astype(bf16)
        bn_send[part, :] = mm(act[1, part, :], down[...]).astype(bf16)
        return 0

    lax.fori_loop(0, pieces, near_other, 0)
    near_copy = send(near_send, near_recv, n_s.at[0], n_r.at[0], tensor=core)
    branch_copy = send(bn_send, bn_recv, n_s.at[1], n_r.at[1], tensor=core)

    def near_own(c, _):
        part = pl.ds(pl.multiple_of(c * BLK, BLK), BLK)
        gin[part, :] = mm_nt(gpre[0, part, :], up[...])
        partial[part, :] = mid[part, :] + mm(act[0, part, :], down[...]) + down_bias
        return 0

    lax.fori_loop(0, pieces, near_own, 0)

    def plan(src, dst, c, send_sem, recv_sem, where):
        here = pl.ds(pl.multiple_of(c * BLK, BLK), BLK)
        return pltpu.make_async_remote_copy(
            src_ref=src.at[here], dst_ref=dst.at[here], send_sem=send_sem.at[c],
            recv_sem=recv_sem.at[c], device_id={"tensor": where},
            device_id_type=pl.DeviceIdType.MESH,
        )

    def arrive(c):
        return plan(inner.at[0], inner.at[2], c, x_s, x_r, far)

    def hand_on(c):
        return plan(inner.at[2], inner.at[3], c, f_s, f_r, core)

    def crossed(c):
        return plan(far_send, far_recv, c, c_s, c_r, core)

    def back(c):
        return plan(x_send, x_recv, c, r_s, r_r, far)

    depth = up.shape[0]
    if up_g.shape[0] > depth:
        up_g[depth:, :] = jnp.zeros((up_g.shape[0] - depth, up_g.shape[1]), bf16)
        down_g[depth:, :] = jnp.zeros((up_g.shape[0] - depth, up_g.shape[1]), bf16)

    def weights(left, right, out):
        def tile(j, _):
            part = pl.ds(pl.multiple_of(j * BLK, BLK), BLK)
            total = mm_tn(left[0, :, part], right[0])
            for k in range(1, 4):
                total = total + mm_tn(left[k, :, part], right[k])
            out[part, :] = total.astype(bf16)
            return 0

        lax.fori_loop(0, depth // BLK, tile, 0)

    def far_step(i, _):
        c = i // 2
        which = lax.rem(i, 2)
        here = pl.ds(pl.multiple_of(c * BLK, BLK), BLK)

        @pl.when(which == 0)
        def _():
            arrive(c).wait_recv()
            hand_on(c).start()

        @pl.when(which == 1)
        def _():
            hand_on(c).wait_recv()

        feed(2 + which, c * BLK)

        @pl.when(which == 1)
        def _():
            far_send[here, :] = mm_nt(gpre[3, here, :], up[...]).astype(bf16)
            crossed(c).start()
            g = mm_nt(gpre[2, here, :], up[...])
            crossed(c).wait_recv()
            x_send[here, :] = (g + far_recv[here, :].astype(f32)).astype(bf16)
            back(c).start()

        return 0

    lax.fori_loop(0, 2 * pieces, far_step, 0)

    def far_out(c, _):
        here = pl.ds(pl.multiple_of(c * BLK, BLK), BLK)
        bf_send[here, :] = mm(act[3, here, :], down[...]).astype(bf16)
        return 0

    lax.fori_loop(0, pieces, far_out, 0)
    far_branch = send(bf_send, bf_recv, b_s, b_r, tensor=core)
    weights(inner, gpre, up_g)
    weights(act, gs, down_g)
    far_branch.wait_recv()
    for c in range(pieces):
        here = pl.ds(c * BLK, BLK)
        b = mm(act[2, here, :], down[...])
        branch_x[here, :] = (b + bf_recv[here, :].astype(f32)).astype(bf16)
    near_copy.wait_recv()
    branch_copy.wait_recv()
    partial[...] += bn_recv[...].astype(f32)
    rows_copies = []
    for c in range(pieces):
        here = pl.ds(c * BLK, BLK)
        xhat, r = norm_parts(mid[here, :])
        back(c).wait_recv()
        g = gin[here, :] + near_recv[here, :].astype(f32) + x_recv[here, :].astype(f32)
        g_out = gs[0, here, :].astype(f32)
        gm = g_out + norm_back(g * gain, xhat, r)
        gmid[here, :] = gm
        there = pl.ds(pl.multiple_of(odd * rows + c * BLK, BLK), BLK)
        ga = gm.astype(bf16)
        rows_out[there, :] = ga
        rows_copies.append(
            send(rows_out.at[there], rows_out.at[there], o_s.at[c], o_r.at[c], tensor=core)
        )
        sums[0:1, :] += jnp.sum(g * xhat, 0, keepdims=True)
        sums[1:2, :] += jnp.sum(g, 0, keepdims=True)
        sums[2:3, :] += jnp.sum(ga.astype(f32), 0, keepdims=True)
        sums[3:4, :] += jnp.sum(g_out, 0, keepdims=True)
    for c in rows_copies:
        c.wait_recv()
    for c in range(pieces):
        sends += [hand_on(c), crossed(c), back(c)]
    for c in sends + rows_copies + [near_copy, branch_copy, far_branch]:
        c.wait_send()


def feed_forward(padded, o1, o2, wo1, wo2, hidden, gs, vecs, up, down):
    rows, depth = hidden.shape
    width = up.shape[1]
    pieces = rows // BLK
    vmem = pl.BlockSpec(memory_space=pltpu.VMEM)
    anyw = pl.BlockSpec(memory_space=pl.ANY)
    dma = pltpu.SemaphoreType.DMA
    wide = pltpu.VMEM((rows, depth), bf16)
    each = [dma((pieces,))] * 2
    return pl.pallas_call(
        feed_kernel,
        in_specs=[vmem] * 5 + [anyw] * 4 + [vmem] * 3,
        out_specs=[vmem] * 7,
        out_shape=[
            jax.ShapeDtypeStruct((2 * rows, depth), bf16),
            jax.ShapeDtypeStruct((rows, depth), f32),
            jax.ShapeDtypeStruct((rows, depth), f32),
            jax.ShapeDtypeStruct((rows, depth), bf16),
            jax.ShapeDtypeStruct((padded, width), bf16),
            jax.ShapeDtypeStruct((padded, width), bf16),
            jax.ShapeDtypeStruct((8, depth), f32),
        ],
        scratch_shapes=[
            pltpu.VMEM((4, rows, depth), bf16),
            pltpu.VMEM((4, rows, depth), bf16),
            pltpu.VMEM((4, rows, width), bf16),
            pltpu.VMEM((4, rows, width), bf16),
            pltpu.VMEM((rows, depth), f32),
            wide, wide, wide, wide, wide, wide, wide, wide, wide, wide, wide, wide,
            pltpu.VMEM((rows, depth), f32),
            dma((4,)),
            *each, *each, *each, *each,
            dma((2,)), dma((2,)),
            *each, *each,
            dma, dma,
            *each,
        ],
        compiler_params=pltpu.CompilerParams(
            collective_id=1, has_side_effects=True, vmem_limit_bytes=62 * 1024 * 1024
        ),
        name="feed_forward",
    )(o1, o2, wo1, wo2, hidden, *gs, vecs, up, down)

def back_kernel(n, chunk, piece, depth, lengths, up_h, down_h, branch_x, *rest):
    held, outs = rest[:LOADS], rest[LOADS : LOADS + 7]
    back_body(n, chunk, piece, depth, lengths, up_h, down_h, branch_x, held, outs, *rest[LOADS + 7 :])


LOADS = 27


def back_body(
    n, chunk, piece, depth, lengths, up_h, down_h, branch_x, held, outs,
    up_g, up_recv, rows_in, os, wo, qkv, lse, fence, sq, sk, normed, down_g, w, sel_w,
    hidden, gmid, vecs, sums, partial, ld_s,
    go, grads, dsums,
    dq_scr, dkt, dvt, dskt, later, fsum, qt, dot_,
    dsel, ng_send, ng_recv, ng_own, far_s, far_r, faro_s, faro_r, gb, ga,
    yd, yb, ya, ys, su, sd, sb, sa, ss, zu, zd, zb, za, zs,
    ts, small, out_s, bx_recv, sel_mine, sel_core, sel_far,
    core_s, core_r, f_s, f_r, sl_s, sl_r, y_s, y_r, z_s, z_r, t_s, t_r, az_s, az_r, ay_s, ay_r,
):
    fu, fd, fb, fa, small_out, input_grad, output = outs
    places = (
        up_g, rows_in, os.at[0], wo.at[0], qkv.at[0, 0], qkv.at[0, 1], qkv.at[0, 2],
        lse.at[0], fence, sq, sk, normed, down_g, wo.at[1], qkv.at[1, 0], qkv.at[1, 1],
        qkv.at[1, 2], lse.at[1], w.at[0], w.at[1], sel_w, os.at[1], hidden, gmid, vecs, sums, partial,
    )
    idx = lax.axis_index("dp")
    par = lax.rem(idx, 2)
    m = n // 2
    own = pl.ds(pl.multiple_of(par * m * chunk, m * chunk), m * chunk)
    loads = [
        pltpu.make_async_copy(h.at[own] if j in (0, 12) else h, v, ld_s.at[j])
        for j, (h, v) in enumerate(zip(held, places))
    ]
    for c in loads:
        c.start()

    def need(*which):
        for j in which:
            loads[j].wait()

    me = lax.axis_index("tensor")
    odd = lax.rem(me, 2)
    z = lax.div(idx, 2)
    rows = hidden.shape[0]
    seq_len = normed.shape[0]
    width = wo.shape[1]
    heads = width // HD
    ranks = 4
    core = me + 1 - 2 * odd
    far = lax.rem(me + 2, ranks)
    ydev = idx + 1 - 2 * par
    peers = [lax.rem(me + d, ranks) for d in range(1, ranks)]
    mates = []
    for b in range(m.bit_length() - 1):
        bit = lax.rem(lax.div(z, 1 << b), 2)
        mates.append(z + (1 - 2 * bit) * (1 << b))
    length = jnp.where(me < 2, lengths[0], lengths[1])
    meet(
        [{"tensor": p} for p in peers]
        + [{"dp": ydev}]
        + [{"dp": 2 * p + par} for p in mates]
    )
    at = par * m + z
    source = (gb, ga, small, up_g, down_g)
    yrecv = (yb, ya, ys, up_recv, yd)
    ysum = (sb, sa, ss, su, sd)
    zrecv = (zb, za, zs, zu, zd)
    full = (fb, fa, out_s, fu, fd)
    size = (gb.shape[0] // n, ga.shape[0] // n, piece, chunk, chunk)

    def plan(src, dst, send_sem, recv_sem, **where):
        return pltpu.make_async_remote_copy(
            src_ref=src, dst_ref=dst, send_sem=send_sem, recv_sem=recv_sem,
            device_id=where, device_id_type=pl.DeviceIdType.MESH,
        )

    def block(start, k):
        return pl.ds(pl.multiple_of(start * size[k], size[k]), size[k])

    def y_copy(k):
        half = m * size[k]
        give = pl.ds(pl.multiple_of((1 - par) * half, half), half)
        src = {3: up_h, 4: down_h}.get(k, source[k])
        return plan(src.at[give], yrecv[k], y_s.at[k], y_r.at[k], dp=ydev)

    bits = m.bit_length() - 1
    first_slot = [0]
    for b in range(bits):
        first_slot.append(first_slot[-1] + (m >> (b + 1)))

    def held_chunk(who, b, j):
        return lax.rem(who, 2 << b) + j * (2 << b)

    def mate(b):
        return mates[b]

    def z_copy(k, b, j):
        slot = first_slot[b] + j
        return plan(
            ysum[k].at[block(held_chunk(mate(b), b, j), k)], zrecv[k].at[slot],
            z_s.at[k, slot], z_r.at[k, slot], dp=2 * mate(b) + par,
        )

    def az_copy(k, b, j):
        slot = first_slot[b] + j
        mine = full[k].at[block(par * m + held_chunk(z, b, j), k)]
        return plan(mine, mine, az_s.at[k, slot], az_r.at[k, slot], dp=2 * mate(b) + par)

    def ay_copy(k, b, j):
        chunk_id, slot = (z, m - 1) if b is None else (held_chunk(mate(b), b, j), first_slot[b] + j)
        came = full[k].at[block(par * m + chunk_id, k)]
        return plan(came, came, ay_s.at[k, slot], ay_r.at[k, slot], dp=ydev)

    def stage(b):
        return range(m >> (b + 1))

    def z_start(k, b):
        for j in stage(b):
            z_copy(k, b, j).start()

    def y_finish(k):
        half = m * size[k]
        keep = pl.ds(pl.multiple_of(par * half, half), half)
        y_copy(k).wait_recv()
        mine = source[k][...] if k > 2 else source[k][keep, :]
        total = mine.astype(f32) + yrecv[k][...].astype(f32)
        ysum[k][...] = total.astype(ysum[k].dtype)
        z_start(k, 0)

    def z_next(k, b):
        for j in stage(b):
            z_copy(k, b, j).wait_recv()
            here = block(held_chunk(z, b, j), k)
            total = ysum[k][here, :].astype(f32) + zrecv[k][first_slot[b] + j].astype(f32)
            ysum[k][here, :] = total.astype(ysum[k].dtype)
        z_start(k, b + 1)

    def z_finish(k):
        for b in range(1, bits - 1):
            z_next(k, b)
        z_copy(k, bits - 1, 0).wait_recv()
        return ysum[k][block(z, k), :].astype(f32) + zrecv[k][first_slot[bits - 1]].astype(f32)

    def az_start(k, b):
        for j in stage(b):
            az_copy(k, b, j).start()

    def spread(k):
        az_start(k, bits - 1)
        ay_copy(k, None, 0).start()

    def forward(k, b):
        for j in stage(b):
            az_copy(k, b, j).wait_recv()
        if b > 0:
            az_start(k, b - 1)
        for j in stage(b):
            ay_copy(k, b, j).start()

    def forward_early(k):
        for b in reversed(range(1, bits)):
            forward(k, b)

    def far_copy(j):
        part = pl.ds(pl.multiple_of(j * width, width), width)
        return plan(far_s.at[part], far_r.at[part], f_s.at[2 + j], f_r.at[2 + j], tensor=far)

    out_copy = plan(faro_s, faro_r, f_s.at[0], f_r.at[0], tensor=far)
    branch_copy = plan(branch_x, bx_recv, f_s.at[1], f_r.at[1], tensor=far)
    core_copy = plan(ng_send, ng_recv, core_s, core_r, tensor=core)
    to_core = plan(sel_mine, sel_core, sl_s.at[0], sl_r.at[0], tensor=core)
    to_first = plan(sel_mine, sel_far, sl_s.at[1], sl_r.at[1], tensor=far)

    y_copy(3).start()
    need(*range(13))

    def hook(g, i):
        if i == 0:

            @pl.when(g == 0)
            def _():
                y_finish(3)
                y_copy(4).start()

        if i == 1:

            @pl.when(g == 1)
            def _():
                fu[block(at, 3), :] = z_finish(3).astype(bf16)
                spread(3)

        if i == seq_len // BLK - 1:

            @pl.when(g == 1)
            def _():
                z_next(3, 0)

        if i == 2:

            @pl.when(g == 1)
            def _():
                y_finish(4)

    def group(g, _):
        @pl.when(g == 1)
        def _():
            need(*range(13, 18), 21)

        total = mm_tn(os[g], rows_in[...])

        @pl.when(g == 0)
        def _():
            faro_s[...] = total.astype(bf16)
            out_copy.start()

        @pl.when(g == 1)
        def _():
            out_copy.wait_recv()
            ga[width : 2 * width, :] = (total + faro_r[...].astype(f32)).astype(bf16)

        def head_grad(j, _):
            here = pl.ds(pl.multiple_of(j * BLK, BLK), BLK)
            go[here, :] = mm_nt(rows_in[here, :], wo[g]).astype(bf16)
            return 0

        lax.fori_loop(0, seq_len // BLK, head_grad, 0)
        for r in (dkt, dvt, dskt, later):
            r[...] = jnp.zeros_like(r)
        for i in reversed(range(seq_len // BLK)):
            here = pl.ds(i * BLK, BLK)
            bwd_block(
                i, heads, qkv.at[g, 0, here], qkv.at[g, 1], qkv.at[g, 2], go.at[here],
                lse.at[g, here], fence.at[here], sq.at[here], sk,
                grads.at[g, 0, here], dsums.at[g, 0, here],
                dq_scr, dkt, dvt, dskt, later, fsum, qt, dot_,
            )
            hook(g, i)
        grads[g, 1] = dkt[...].T.astype(bf16)
        grads[g, 2] = dvt[...].T.astype(bf16)
        dsums[g, 1] = dskt[...].T

        @pl.when(g == 1)
        def _():
            dsel[:, :HD] = (dsums[0, 0] + dsums[1, 0]).astype(bf16)
            dsel[:, HD:] = (dsums[0, 1] + dsums[1, 1]).astype(bf16)
            sel_mine[...] = mm_tn(dsel[...], normed[...]).astype(bf16)

            @pl.when(odd == 1)
            def _():
                to_core.start()

        def weight_grad(t, _):
            j = 2 - t
            here = pl.ds(pl.multiple_of(j * width, width), width)
            total = mm_tn(grads[g, j], normed[...])

            @pl.when(g == 0)
            def _():
                far_s[here, :] = total.astype(bf16)
                far_copy(j).start()

            @pl.when((g == 1) & (t == 0))
            def _():
                far_copy(2).wait_recv()
                ga[:width, :] = (total + far_r[2 * width :, :].astype(f32)).astype(bf16)
                y_copy(1).start()

                @pl.when(odd == 0)
                def _():
                    to_core.wait_recv()
                    sel_mine[...] = (
                        sel_mine[...].astype(f32) + sel_core[...].astype(f32)
                    ).astype(bf16)

                @pl.when(me == 2)
                def _():
                    to_first.start()

                branch_copy.start()

            @pl.when((g == 1) & (t > 0))
            def _():
                far_copy(j).wait_recv()
                gb[here, :] = (total + far_r[here, :].astype(f32)).astype(bf16)

            return 0

        lax.fori_loop(0, 3, weight_grad, 0)
        return 0

    if gb.shape[0] > 2 * width:
        gb[2 * width :, :] = jnp.zeros((gb.shape[0] - 2 * width, depth), bf16)
        ga[2 * width :, :] = jnp.zeros((ga.shape[0] - 2 * width, depth), bf16)
    lax.fori_loop(0, 2, group, 0)

    @pl.when(me == 0)
    def _():
        to_first.wait_recv()
        both = sel_mine[...].astype(f32) + sel_far[...].astype(f32)
        gb[:HD, :] = (gb[:HD, :].astype(f32) + both[:HD, :]).astype(bf16)
        gb[width : width + HD, :] = (
            gb[width : width + HD, :].astype(f32) + both[HD:, :]
        ).astype(bf16)

    y_copy(0).start()
    z_next(4, 0)
    forward_early(3)
    fd[block(at, 4), :] = z_finish(4).astype(bf16)
    spread(4)
    y_finish(1)
    need(18, 19, 20, *range(22, LOADS))

    def normed_grad(t, _):
        mine = t // 2
        step = pl.multiple_of(lax.rem(t, 2) * BLK, BLK)
        side = mine * odd + (1 - mine) * (1 - odd)
        part = pl.ds(pl.multiple_of(side * rows + step, BLK), BLK)
        here = pl.ds(step, BLK)
        total = mm(dsel[part, :], sel_w[...])
        for g in range(2):
            for j in range(3):
                total = total + mm(grads[g, j, part, :], w[g, j * width : (j + 1) * width, :])

        @pl.when(mine == 0)
        def _():
            ng_send[here, :] = total.astype(bf16)

        @pl.when(mine == 1)
        def _():
            ng_own[here, :] = total

        @pl.when(t == 1)
        def _():
            core_copy.start()

        return 0

    lax.fori_loop(0, 4, normed_grad, 0)
    z_next(1, 0)
    y_finish(0)
    xhat, r = norm_parts(hidden[...].astype(f32))
    core_copy.wait_recv()
    grad = ng_own[...] + ng_recv[...].astype(f32)
    input_grad[...] = (gmid[...] + norm_back(grad * vecs[5:6, :], xhat, r)).astype(bf16)
    small[...] = jnp.zeros_like(small)
    dgain = jnp.sum(grad * xhat, 0, keepdims=True)
    dshift = jnp.sum(grad, 0, keepdims=True)
    lines = depth // 128
    for j in range(lines):
        small[j : j + 1, :] = dgain[:, j * 128 : (j + 1) * 128]
        small[lines + j : lines + j + 1, :] = dshift[:, j * 128 : (j + 1) * 128]
    for slot, which in ((2, 2), (3, 0), (4, 1), (5, 3)):
        for j in range(lines):
            small[slot * lines + j : slot * lines + j + 1, :] = sums[
                which : which + 1, j * 128 : (j + 1) * 128
            ]
    wide_lines = up_g.shape[1] // 128
    for j in range(wide_lines):
        small[pl.ds(6 * lines + me * wide_lines + j, 1), :] = sums[4:5, j * 128 : (j + 1) * 128]
    base = small_lines(depth, up_g.shape[1]) - 4 * ranks
    for owner, g in ((me, 1), (far, 0)):
        for j, which in enumerate((0, 2)):
            total = jnp.sum(grads[g, which].astype(f32), 0, keepdims=True)
            line = base + 4 * owner + 2 * j
            small[pl.ds(line, 1), :] = total[:, :128]
            small[pl.ds(line + 1, 1), : width - 128] = total[:, 128:]
    total = jnp.sum(dsel[...].astype(f32), 0, keepdims=True)
    lane = lax.broadcasted_iota(jnp.int32, total.shape, 1)
    small[base : base + 1, :] += jnp.where(lane < HD, total, 0.0)
    y_copy(2).start()

    fa[block(at, 1), :] = z_finish(1).astype(bf16)
    spread(1)
    z_next(0, 0)
    y_finish(2)
    forward(3, 0)
    forward_early(4)
    z_next(2, 0)
    forward_early(1)
    fb[block(at, 0), :] = z_finish(0).astype(bf16)
    spread(0)
    forward(4, 0)
    ts[me] = z_finish(2)

    def t_copy(d):
        return plan(ts.at[me], ts.at[me], t_s.at[d], t_r.at[d], tensor=peers[d])

    for d in range(ranks - 1):
        t_copy(d).start()
    for d in range(ranks - 1):
        t_copy(d).wait_recv()
    vec = ts[0]
    for d in range(1, ranks):
        vec = vec + ts[d]
    out_s[block(at, 2), :] = vec
    spread(2)
    forward(1, 0)
    forward_early(0)
    forward_early(2)
    token = odd * rows + lax.broadcasted_iota(jnp.int32, (rows, 1), 0)
    live = jnp.where(token < length, 1.0, 0.0)
    branch_copy.wait_recv()
    output[...] = (live * (partial[...] + bx_recv[...].astype(f32))).astype(bf16)
    forward(0, 0)
    forward(2, 0)
    for k in range(5):
        ay_copy(k, None, 0).wait_recv()
        for b in range(bits):
            for j in stage(b):
                ay_copy(k, b, j).wait_recv()

    @pl.when(odd == 1)
    def _():
        to_core.wait_send()

    @pl.when(me == 2)
    def _():
        to_first.wait_send()

    small_out[...] = out_s[...]
    for c in (far_copy(0), far_copy(1), far_copy(2), out_copy, branch_copy, core_copy):
        c.wait_send()
    for d in range(ranks - 1):
        t_copy(d).wait_send()
    for k in range(5):
        y_copy(k).wait_send()
        ay_copy(k, None, 0).wait_send()
        for b in range(bits):
            for j in stage(b):
                z_copy(k, b, j).wait_send()
                az_copy(k, b, j).wait_send()
                ay_copy(k, b, j).wait_send()


def front_kernel(
    lengths, hidden, out_grad, vecs, qkv, qv_bias, wo,
    *rest,
):
    outs, gcore, gfar, gcross = rest[:18], rest[18], rest[19], rest[20]
    kept = rest[21:39]
    front_body(
        lengths, hidden, out_grad, vecs, qkv, qv_bias, wo, outs, kept, gcore, gfar, gcross, *rest[39:]
    )


def front_body(
    lengths, hidden, out_grad, vecs, qkv, qv_bias, wo, outs, kept, gcore, gfar, gcross,
    out_scr, carry, sel_b, bias2,
    st_s, nm_s, nm_r, gc_s, gc_r, sl_s, sl_r, w_s, w_r, p_s, p_r, e_s, e_r, g_s, g_r, h_s, h_r,
):
    me = lax.axis_index("tensor")
    idx = lax.axis_index("dp")
    odd = lax.rem(me, 2)
    core = me + 1 - 2 * odd
    far = lax.rem(me + 2, 4)
    par = lax.rem(idx, 2)
    ydev = idx + 1 - 2 * par
    rows = hidden.shape[0]
    seq_len = 2 * rows
    width = wo.shape[0]
    heads = width // HD
    (normed, q1, k1, v1, lse1, o1, q2, k2, v2, lse2, o2, fence, sq, sk, w2, wo2, selw, g0) = kept
    stores = []

    def store(*which):
        for j in which:
            copy = pltpu.make_async_copy(kept[j], outs[j], st_s.at[j])
            copy.start()
            stores.append(copy)

    length = jnp.where(me < 2, lengths[0], lengths[1])

    def sel_copies(k, where):
        return [
            pltpu.make_async_remote_copy(
                src_ref=a, dst_ref=a, send_sem=sl_s.at[k, j], recv_sem=sl_r.at[j],
                device_id={"tensor": where}, device_id_type=pl.DeviceIdType.MESH,
            )
            for j, a in enumerate((selw, sel_b))
        ]

    @pl.when(me == 0)
    def _():
        selw[:HD, :] = qkv[:HD, :]
        selw[HD:, :] = qkv[width : width + HD, :]
        sel_b[...] = qv_bias[...]

    meet([{"tensor": core}, {"tensor": far}, {"dp": ydev}])

    @pl.when(me == 0)
    def _():
        for c in sel_copies(0, far) + sel_copies(1, core):
            c.start()

    share = width // 2
    halves = [
        (src, dst, pl.ds(pl.multiple_of(base + par * share, share), share))
        for src, dst, base in (
            (qkv, w2, 0), (qkv, w2, width), (qkv, w2, 2 * width), (wo, wo2, 0)
        )
    ]
    extra = send(qv_bias, bias2, e_s, e_r, tensor=far)
    cross = [
        send(src.at[part], dst.at[part], w_s.at[j], w_r.at[j], tensor=far)
        for j, (src, dst, part) in enumerate(halves)
    ]
    passed = []

    def pass_on(j):
        cross[j].wait_recv()
        _, dst, part = halves[j]
        passed.append(send(dst.at[part], dst.at[part], p_s.at[j], p_r.at[j], dp=ydev))

    spot = pl.multiple_of(odd * rows, rows)
    norm_copies = []
    for c in range(rows // BLK):
        here = pl.ds(c * BLK, BLK)
        there = pl.ds(pl.multiple_of(spot + c * BLK, BLK), BLK)
        xhat, _ = norm_parts(hidden[here, :].astype(f32))
        normed[there, :] = (xhat * vecs[5:6, :] + vecs[6:7, :]).astype(bf16)
        norm_copies.append(
            send(normed.at[there], normed.at[there], nm_s.at[c], nm_r.at[c], tensor=core)
        )
    row = odd * rows + lax.broadcasted_iota(jnp.int32, (rows, 1), 0)
    live = jnp.where(row < length, 1.0, 0.0)
    g0[...] = (out_grad[...].astype(f32) * live).astype(bf16)
    store(17)
    gc = send(g0, gcore, gc_s, gc_r, tensor=core)
    g_parts = [pl.ds(c * BLK, BLK) for c in range(rows // BLK)]
    gf = [
        send(g0.at[p], gfar.at[p], g_s.at[c], g_r.at[c], tensor=far) for c, p in enumerate(g_parts)
    ]

    def project(weight, bias, out):
        def tile(j, _):
            here = pl.ds(pl.multiple_of(j * BLK, BLK), BLK)
            y = mm_nt(normed[here, :], weight)
            if bias is not None:
                y = y + bias
            out[here, :] = y.astype(bf16)
            return 0

        lax.fori_loop(0, seq_len // BLK, tile, 0)

    @pl.when(me == 2)
    def _():
        for c in sel_copies(0, far):
            c.wait_recv()
        for c in sel_copies(1, core):
            c.start()

    for c in norm_copies:
        c.wait_recv()
    store(0)
    project(qkv[:width, :], qv_bias[0:1, :], q1)
    project(qkv[width : 2 * width, :], None, k1)
    project(qkv[2 * width :, :], qv_bias[1:2, :], v1)

    @pl.when(odd == 1)
    def _():
        for c in sel_copies(1, core):
            c.wait_recv()

    store(1, 2, 3)
    def select(j, _):
        here = pl.ds(pl.multiple_of(j * BLK, BLK), BLK)
        y = mm_nt(normed[here, :], selw[...])
        sq[here, :] = (y[:, :HD] + sel_b[0:1, :HD]).astype(bf16)
        sk[here, :] = y[:, HD:].astype(bf16)
        return 0

    lax.fori_loop(0, seq_len // BLK, select, 0)
    store(12, 13, 16)
    carry[...] = jnp.zeros_like(carry)
    pass_on(0)
    for i in range(seq_len // BLK):
        here = pl.ds(i * BLK, BLK)
        make_fence(i, seq_len, length, sq.at[here], sk, fence.at[here], carry)
        fwd_block(
            i, heads, out_scr, q1.at[here], k1, v1, fence.at[here], o1.at[here], lse1.at[here]
        )
        if i < 3:
            pass_on(i + 1)
    store(4, 5, 11)
    extra.wait_recv()
    for j, (out, bias) in enumerate(((q2, bias2[0:1, :]), (k2, None), (v2, bias2[1:2, :]))):
        passed[j].wait_recv()
        project(w2[j * width : (j + 1) * width, :], bias, out)
        store(6 + j)
    store(14)
    gx = []

    def pass_g(c):
        gf[c].wait_recv()
        p = g_parts[c]
        gx.append(send(gfar.at[p], gcross.at[p], h_s.at[c], h_r.at[c], tensor=core))

    for i in range(seq_len // BLK):
        here = pl.ds(i * BLK, BLK)
        fwd_block(
            i, heads, out_scr, q2.at[here], k2, v2, fence.at[here], o2.at[here], lse2.at[here]
        )
    store(9, 10)
    for c in range(rows // BLK):
        pass_g(c)
    gc.wait_recv()
    passed[3].wait_recv()
    store(15)
    for c in gx:
        c.wait_recv()

    @pl.when(me == 0)
    def _():
        for c in sel_copies(0, far):
            c.wait_send()

    @pl.when(odd == 0)
    def _():
        for c in sel_copies(1, core):
            c.wait_send()

    for c in cross + passed + norm_copies + gf + gx + [gc, extra]:
        c.wait_send()
    for c in stores:
        c.wait()


def front(lengths, hidden, out_grad, vecs, qkv, qv_bias, wo):
    rows, depth = hidden.shape
    seq_len, width = 2 * rows, wo.shape[0]
    pieces = rows // BLK
    vmem = pl.BlockSpec(memory_space=pltpu.VMEM)
    dma = pltpu.SemaphoreType.DMA
    heads = jax.ShapeDtypeStruct((seq_len, width), bf16)
    lse = jax.ShapeDtypeStruct((seq_len, 128), f32)
    sel = jax.ShapeDtypeStruct((seq_len, HD), bf16)
    wide = jax.ShapeDtypeStruct((rows, depth), bf16)
    kept = [
        jax.ShapeDtypeStruct((seq_len, depth), bf16),
        heads, heads, heads, lse, heads,
        heads, heads, heads, lse, heads,
        jax.ShapeDtypeStruct((seq_len, seq_len), f32),
        sel, sel,
        jax.ShapeDtypeStruct(qkv.shape, bf16),
        jax.ShapeDtypeStruct(wo.shape, bf16),
        jax.ShapeDtypeStruct((2 * HD, depth), bf16),
        wide,
    ]
    return pl.pallas_call(
        front_kernel,
        in_specs=[pl.BlockSpec(memory_space=pltpu.SMEM)] + [vmem] * 6,
        out_specs=[pl.BlockSpec(memory_space=pl.ANY)] * 21,
        out_shape=kept + [wide, wide, wide],
        scratch_shapes=[pltpu.VMEM(a.shape, a.dtype) for a in kept]
        + [
            pltpu.VMEM((BLK, width), f32),
            pltpu.VMEM((8, seq_len), f32),
            pltpu.VMEM((2, width), f32),
            pltpu.VMEM((2, width), f32),
            dma((18,)),
            dma((pieces,)), dma((pieces,)),
            dma, dma,
            dma((2, 2)), dma((2,)),
            dma((4,)), dma((4,)),
            dma((4,)), dma((4,)),
            dma, dma,
            dma((pieces,)), dma((pieces,)),
            dma((pieces,)), dma((pieces,)),
        ],
        compiler_params=pltpu.CompilerParams(
            collective_id=2, has_side_effects=True, vmem_limit_bytes=60 * 1024 * 1024
        ),
        name="front",
    )(lengths, hidden, out_grad, vecs, qkv, qv_bias, wo)


def small_lines(depth, hidden):
    return (6 * depth + 4 * hidden) // 128 + 16


def go_back(n, set1, set2, fence, sq, sk, rows_in, o1, o2, wo1, wo2, normed, w1, w2, sel_w,
            hidden, vecs, gmid, sums, partial, branch_x, lengths, up_g, down_g):
    m = n // 2
    chunk = up_g.shape[0] // n
    rows, depth = hidden.shape
    piece = -(-small_lines(depth, up_g.shape[1]) // (8 * n)) * 8
    seq_len, width = set1[0].shape
    half, shalf = m * chunk, m * piece
    ranks = 4
    wf = up_g.shape[1]
    small_chunk = -(-2 * width // (16 * n)) * 16
    part_half = m * small_chunk
    vmem = pl.BlockSpec(memory_space=pltpu.VMEM)
    dma = pltpu.SemaphoreType.DMA
    q1, k1, v1, lse1 = set1
    q2, k2, v2, lse2 = set2
    held = (up_g, rows_in, o2, wo2, q2, k2, v2, lse2, fence, sq, sk, normed, down_g, wo1,
            q1, k1, v1, lse1, w2, w1, sel_w, o1, hidden, gmid, vecs, sums, partial)
    anyw = pl.BlockSpec(memory_space=pl.ANY)
    like = lambda a: pltpu.VMEM(a.shape, a.dtype)
    return pl.pallas_call(
        lambda *refs: back_kernel(n, chunk, piece, depth, *refs),
        in_specs=[pl.BlockSpec(memory_space=pltpu.SMEM)] + [anyw] * (LOADS + 3),
        out_specs=[vmem] * 7,
        out_shape=[
            jax.ShapeDtypeStruct((n * chunk, wf), bf16),
            jax.ShapeDtypeStruct((n * chunk, wf), bf16),
            jax.ShapeDtypeStruct((n * small_chunk, depth), bf16),
            jax.ShapeDtypeStruct((n * small_chunk, depth), bf16),
            jax.ShapeDtypeStruct((n * piece, 128), f32),
            jax.ShapeDtypeStruct((rows, depth), bf16),
            jax.ShapeDtypeStruct((rows, depth), bf16),
        ],
        scratch_shapes=[
            pltpu.VMEM((half, wf), bf16), pltpu.VMEM((half, wf), bf16), like(rows_in),
            pltpu.VMEM((2, seq_len, width), bf16),
            pltpu.VMEM((2, width, depth), bf16),
            pltpu.VMEM((2, 3, seq_len, width), bf16),
            pltpu.VMEM((2, seq_len, 128), f32),
            like(fence), like(sq), like(sk), like(normed), pltpu.VMEM((half, wf), bf16),
            pltpu.VMEM((2, 3 * width, depth), bf16),
            like(sel_w), like(hidden), like(gmid), like(vecs), like(sums), like(partial),
            dma((LOADS,)),
            pltpu.VMEM((seq_len, width), bf16),
            pltpu.VMEM((2, 3, seq_len, width), bf16),
            pltpu.VMEM((2, 2, seq_len, HD), f32),
            pltpu.VMEM((BLK, width), f32),
            pltpu.VMEM((width, seq_len), f32),
            pltpu.VMEM((width, seq_len), f32),
            pltpu.VMEM((HD, seq_len), f32),
            pltpu.VMEM((8, seq_len), f32),
            pltpu.VMEM((BLK, seq_len), f32),
            pltpu.VMEM((width, BLK), bf16),
            pltpu.VMEM((width, BLK), bf16),
            pltpu.VMEM((seq_len, 128), bf16),
            pltpu.VMEM((rows, depth), bf16),
            pltpu.VMEM((rows, depth), bf16),
            pltpu.VMEM((rows, depth), f32),
            pltpu.VMEM((3 * width, depth), bf16),
            pltpu.VMEM((3 * width, depth), bf16),
            pltpu.VMEM((width, depth), bf16),
            pltpu.VMEM((width, depth), bf16),
            pltpu.VMEM((n * small_chunk, depth), bf16),
            pltpu.VMEM((n * small_chunk, depth), bf16),
            *[pltpu.VMEM((h, depth), bf16) for h in (half, part_half, part_half)],
            pltpu.VMEM((shalf, 128), f32),
            *[pltpu.VMEM((h, depth), bf16) for h in (half, half, part_half, part_half)],
            pltpu.VMEM((shalf, 128), f32),
            *[
                pltpu.VMEM((m - 1, c, depth), bf16)
                for c in (chunk, chunk, small_chunk, small_chunk)
            ],
            pltpu.VMEM((m - 1, piece, 128), f32),
            pltpu.VMEM((ranks, piece, 128), f32),
            pltpu.VMEM((n * piece, 128), f32),
            pltpu.VMEM((n * piece, 128), f32),
            pltpu.VMEM((rows, depth), bf16),
            *[pltpu.VMEM((2 * HD, depth), bf16)] * 3,
            dma, dma,
            dma((5,)), dma((5,)),
            dma((2,)), dma((2,)),
            dma((5,)), dma((5,)),
            dma((5, m - 1)), dma((5, m - 1)),
            dma((3,)), dma((3,)),
            dma((5, m - 1)), dma((5, m - 1)),
            dma((5, m)), dma((5, m)),
        ],
        compiler_params=pltpu.CompilerParams(
            collective_id=0, has_side_effects=True, vmem_limit_bytes=66_900_000
        ),
        name="go_back",
    )(lengths, up_g, down_g, branch_x, *held)


def shards(
    hidden_in,
    lengths,
    ln1_gain,
    ln1_shift,
    qkv_weight,
    qv_bias,
    out_weight,
    out_bias,
    ln2_gain,
    ln2_shift,
    up_weight,
    up_bias,
    down_weight,
    down_bias,
    out_grad,
):
    n = lax.axis_size("dp")
    ranks = lax.axis_size("tensor")
    me = lax.axis_index("tensor")
    depth = hidden_in.shape[1]
    width = qkv_weight.shape[2]
    hidden = up_bias.shape[0]
    padded = -(-depth // (16 * n)) * 16 * n
    spot = jnp.arange(8)[:, None]
    vecs = jnp.zeros((8, depth), f32)
    for j, vec in enumerate(
        (out_bias, ln2_gain, ln2_shift, down_bias, up_bias.astype(f32), ln1_gain, ln1_shift)
    ):
        vecs = jnp.where(spot == j, vec[None], vecs)
    qkv_rows = jnp.swapaxes(qkv_weight, 1, 2).reshape(3 * width, depth)
    (normed, q1, k1, v1, lse1, o1, q2, k2, v2, lse2, o2, fence, sq, sk, qkv_far, out_far, sel_w,
     *grad_rows) = front(lengths, hidden_in, out_grad, vecs, qkv_rows, qv_bias, out_weight)
    attn_rows, grad_middle, partial, branch_x, up_part, down_part, sums = feed_forward(
        padded, o1, o2, out_weight, out_far, hidden_in, grad_rows, vecs, up_weight, down_weight
    )
    full_u, full_d, full_b, full_a, small, input_grad, output = go_back(
        n, (q1, k1, v1, lse1), (q2, k2, v2, lse2), fence, sq, sk, attn_rows, o1, o2,
        out_weight, out_far, normed, qkv_rows, qkv_far, sel_w, hidden_in, vecs,
        grad_middle, sums, partial, branch_x, lengths, up_part, down_part,
    )
    vectors = small[: 6 * depth // 128].reshape(6, depth)
    lines = (6 * depth + ranks * hidden) // 128
    up_all = small[6 * depth // 128 : lines].reshape(ranks, hidden)
    qv_all = small[lines : lines + 4 * ranks].reshape(ranks, 2, 256)
    up_bias_grad = lax.dynamic_index_in_dim(up_all, me, 0, keepdims=False)
    qv_bias_grad = lax.dynamic_index_in_dim(qv_all, me, 0, keepdims=False)[:, :width]
    qkv_grad = jnp.concatenate([full_b[: 2 * width], full_a[:width]], 0).astype(f32)
    qkv_grad = jnp.swapaxes(qkv_grad.reshape(3, width, depth), 1, 2)
    out_weight_grad = full_a[width : 2 * width].astype(f32)
    return (
        output,
        input_grad,
        vectors[0],
        vectors[1],
        qkv_grad,
        qv_bias_grad,
        out_weight_grad,
        vectors[2],
        vectors[3],
        vectors[4],
        full_u[:depth].astype(f32),
        up_bias_grad,
        full_d[:depth].astype(f32),
        vectors[5],
    )


def solution(mesh):
    return jax.shard_map(
        shards,
        mesh=mesh,
        in_specs=(
            P(("dp", "tensor"), None),
            P("dp"),
            P(),
            P(),
            P(None, None, "tensor"),
            P(None, "tensor"),
            P("tensor", None),
            P(),
            P(),
            P(),
            P(None, "tensor"),
            P("tensor"),
            P("tensor", None),
            P(),
            P(("dp", "tensor"), None),
        ),
        out_specs=(
            P(("dp", "tensor"), None),
            P(("dp", "tensor"), None),
            P(),
            P(),
            P(None, None, "tensor"),
            P(None, "tensor"),
            P("tensor", None),
            P(),
            P(),
            P(),
            P(None, "tensor"),
            P("tensor"),
            P("tensor", None),
            P(),
        ),
        check_vma=False,
    )
```
